32 devices in a mesh: dp: 4 (over y, x), row: 2 (over core), col: 4 (over z).
Axes of the slice: x: 2, y: 2, z: 4, core: 2. Of those that a mesh axis runs over, the one named last changes fastest.
Arguments:
- block_input: bfloat16 [8192, 1536], P(('dp', 'row', 'col')), may hold values from -6 to 6
- segment_ids: int32 [8192], P(('dp', 'row', 'col')), may hold values from 0 to 6, as said below
- norm_gain: float32 [1536], replicated, may hold values from 0.1 to 1.9
- proj_zx: bfloat16 [1536, 2, 3072], P(('dp', 'row'), None, 'col'), may hold values from -0.15625 to 0.15625
- proj_bc: bfloat16 [1536, 256], P(('dp', 'row')), may hold values from -0.15625 to 0.15625
- proj_dt: bfloat16 [1536, 48], P(('dp', 'row'), 'col'), may hold values from -0.15625 to 0.15625
- conv_inner: float32 [4, 3072], P(None, 'col'), may hold values from -3 to 3
- conv_inner_bias: float32 [3072], P('col'), may hold values from -3 to 3
- conv_shared: float32 [4, 256], replicated, may hold values from -3 to 3
- conv_shared_bias: float32 [256], replicated, may hold values from -3 to 3
- step_bias: float32 [48], P('col'), may hold values from -6.9 to -2.3
- rate_log: float32 [48], P('col'), may hold values from 0 to 2.77
- skip_gain: float32 [48], P('col'), may hold values from 0.5 to 2
- gated_gain: float32 [3072], P('col'), may hold values from 0.1 to 1.9
- proj_out: bfloat16 [3072, 1536], P('col', ('dp', 'row')), may hold values from -0.109375 to 0.109375
- cotangent: bfloat16 [8192, 1536], P(('dp', 'row', 'col')), may hold values from -6 to 6
Outputs:
- block_output: bfloat16 [8192, 1536], P(('dp', 'row', 'col'))
- grad_input: bfloat16 [8192, 1536], P(('dp', 'row', 'col'))
- grad_norm_gain: float32 [1536], replicated
- grad_proj_zx: float32 [1536, 2, 3072], P(('dp', 'row'), None, 'col')
- grad_proj_bc: float32 [1536, 256], P(('dp', 'row'))
- grad_proj_dt: float32 [1536, 48], P(('dp', 'row'), 'col')
- grad_conv_inner: float32 [4, 3072], P(None, 'col')
- grad_conv_inner_bias: float32 [3072], P('col')
- grad_conv_shared: float32 [4, 256], replicated
- grad_conv_shared_bias: float32 [256], replicated
- grad_step_bias: float32 [48], P('col')
- grad_rate_log: float32 [48], P('col')
- grad_skip_gain: float32 [48], P('col')
- grad_gated_gain: float32 [3072], P('col')
- grad_proj_out: float32 [3072, 1536], P('col', ('dp', 'row'))
The draws below stay inside these ranges and needn't reach their ends.
Inputs may be any that keep to these rules, and one draw needn't show every extreme that they name: `segment_ids`: within each aligned sequence of 2048 tokens the ids start at 0 on its first token, never fall, and rise by one at exactly six document starts: three in the first quarter of the sequence (never its first token) and three in its last quarter; so every sequence holds seven documents and its middle half lies in one of them.
All inputs are finite; a program needn't handle non-finite values.
Results may differ from the reference program's by a relative error of at most 0.011.
Values may be sent and summed in bfloat16 or wider, within the bound.
A program may use at most 256 MiB of HBM per device.

```python
from functools import partial
import jax
import jax.numpy as jnp
from jax import lax

D = 1536
H = 48
N = 128
K = 4
SPAN = 256
SEQ = 2048
DI = 3072
TOKENS = 8192
N_COL = 4


def draw_segment_ids(key, part):
    seq_count = TOKENS // SEQ
    quarter = SEQ // 4
    keys = jax.random.split(key, seq_count)

    def one_sequence(seq_key):
        first_key, second_key = jax.random.split(seq_key)
        early = jax.random.permutation(first_key, quarter - 1)[:3] + 1
        late = jax.random.permutation(second_key, quarter)[:3] + 3 * quarter
        starts = jnp.concatenate([early, late]).astype(jnp.int32)
        position = jnp.arange(SEQ, dtype=jnp.int32)
        flags = jnp.sum((position[:, None] == starts[None, :]).astype(jnp.int32), axis=1)
        return jnp.cumsum(flags).astype(jnp.int32)
    return jax.vmap(one_sequence)(keys).reshape(-1).astype(jnp.int32)


def block_levels(rng, extent, cuts, low, high):
    loudness, own = 1.0, jax.random.fold_in(rng, 6)
    for axis_at, shards_of in cuts:
        heights = jnp.exp(jax.random.uniform(jax.random.fold_in(own, axis_at), (shards_of,), jnp.float32, low / len(cuts), high / len(cuts)))
        loudness = loudness * jnp.repeat(heights, extent[axis_at] // shards_of).reshape([-1 if axis == axis_at else 1 for axis in range(len(extent))])
    return loudness


def scatter_about(rng, dims, deviation, reach, cuts=(), held_as=jnp.bfloat16):
    level = block_levels(rng, dims, cuts, -0.22, 0.18) if cuts else 1.0
    values = jax.random.normal(rng, dims, jnp.float32) * deviation * level
    return jnp.minimum(jnp.maximum(values, -reach), reach).astype(held_as)


def setup_inputs(seed: int = 0) -> dict:
    key_of = jax.random.split(jax.random.key(seed), 17)
    block_input = scatter_about(key_of[0], (TOKENS, D), 1.0, 6.0, ((0, 32),))
    segment_ids = draw_segment_ids(jax.random.fold_in(key_of[16], 71), 0)
    norm_gain = jnp.clip(1.0 + 0.18 * jax.random.normal(key_of[2], (D,), jnp.float32), 0.1, 1.9)
    proj_zx = scatter_about(key_of[3], (D, 2, DI), D ** -0.5, 0.15625, ((0, 8), (2, 4)))
    proj_bc = scatter_about(key_of[4], (D, 2 * N), D ** -0.5, 0.15625, ((0, 8),))
    proj_dt = scatter_about(key_of[5], (D, H), D ** -0.5, 0.15625, ((0, 8), (1, 4)))
    conv_inner = scatter_about(key_of[6], (K, DI), K ** -0.5, 3.0, ((1, 4),), jnp.float32)
    conv_inner_bias = scatter_about(key_of[7], (DI,), 0.5, 3.0, ((0, 4),), jnp.float32)
    conv_shared = scatter_about(key_of[8], (K, 2 * N), K ** -0.5, 3.0, (), jnp.float32)
    conv_shared_bias = scatter_about(key_of[9], (2 * N,), 0.5, 3.0, (), jnp.float32)
    step_bias = jnp.clip(-6.9 + 4.6000001430511475 * jax.random.uniform(key_of[10], (H,), jnp.float32) ** block_levels(key_of[10], (H,), ((0, 4),), -0.2, 0.2), -6.9, -2.3)
    rate_log = jnp.clip(2.77 * jax.random.uniform(key_of[11], (H,), jnp.float32) ** block_levels(key_of[11], (H,), ((0, 4),), -0.2, 0.2), 0.0, 2.77)
    skip_gain = jnp.clip(0.5 + 1.5 * jax.random.uniform(key_of[12], (H,), jnp.float32) ** block_levels(key_of[12], (H,), ((0, 4),), -0.2, 0.2), 0.5, 2.0)
    gated_gain = jnp.clip(1.0 + 0.18 * jax.random.normal(key_of[13], (DI,), jnp.float32), 0.1, 1.9)
    proj_out = scatter_about(key_of[14], (DI, D), DI ** -0.5, 0.109375, ((0, 4), (1, 8)))
    cotangent = scatter_about(key_of[15], (TOKENS, D), 1.0, 6.0, ((0, 32),))
    return {"block_input": block_input, "segment_ids": segment_ids, "norm_gain": norm_gain, "proj_zx": proj_zx, "proj_bc": proj_bc, "proj_dt": proj_dt, "conv_inner": conv_inner, "conv_inner_bias": conv_inner_bias, "conv_shared": conv_shared, "conv_shared_bias": conv_shared_bias, "step_bias": step_bias, "rate_log": rate_log, "skip_gain": skip_gain, "gated_gain": gated_gain, "proj_out": proj_out, "cotangent": cotangent}


EPS = 1e-05
HIGH = lax.Precision.HIGHEST

def delayed(values, delay_steps, filler):
    padding = jnp.full((delay_steps,) + values.shape[1:], filler, values.dtype)
    return jnp.concatenate([padding, values[:-delay_steps]], axis=0)

def causal_conv(values, kernel, offset, segment):
    kernel_size = kernel.shape[0]
    running = kernel[kernel_size - 1][None, :] * values + offset[None, :]
    for delay_steps in range(1, kernel_size):
        linked = (delayed(segment, delay_steps, -1) == segment).astype(jnp.float32)
        running = running + kernel[kernel_size - 1 - delay_steps][None, :] * delayed(values, delay_steps, 0.0) * linked[:, None]
    return running

def span_scan(heads_in, step_size, log_decay, b_matrix, c_matrix, segment, block_len):
    seq_len, head_count, head_dim = heads_in.shape
    state_dim = b_matrix.shape[1]
    blocks_count = seq_len // block_len

    def reshaped(tensor):
        return tensor.reshape((blocks_count, block_len) + tensor.shape[1:])

    def advance(carry, block):
        carried, previous = carry
        x_block, step_block, log_block, b_block, c_block, seg_block = block
        cumulative = jnp.cumsum(log_block, axis=0)
        position = jnp.arange(block_len)
        linked = (position[:, None] >= position[None, :]) & (seg_block[:, None] == seg_block[None, :])
        linked_float = linked.astype(jnp.float32)
        spread = cumulative.T[:, :, None] - cumulative.T[:, None, :]
        decays = jnp.exp(jnp.where(linked[None], spread, 0.0)) * linked_float[None]
        scores = jnp.dot(c_block, b_block.T, precision=HIGH)
        mixing = decays * scores[None] * step_block.T[:, None, :]
        output = jnp.einsum('hts,shp->thp', mixing, x_block, precision=HIGH)
        entering = jnp.exp(cumulative) * (seg_block == previous).astype(jnp.float32)[:, None]
        output = output + jnp.einsum('tn,hpn->thp', c_block, carried, precision=HIGH) * entering[:, :, None]
        closing = seg_block[-1]
        leaving = jnp.exp(cumulative[-1][None, :] - cumulative) * (seg_block == closing).astype(jnp.float32)[:, None] * step_block
        retained = jnp.exp(cumulative[-1]) * (closing == previous).astype(jnp.float32)
        carried = carried * retained[:, None, None] + jnp.einsum('sh,shp,sn->hpn', leaving, x_block, b_block, precision=HIGH)
        return ((carried, closing), output)
    initial = (jnp.zeros((head_count, head_dim, state_dim), jnp.float32), jnp.array(-1, jnp.int32))
    blocks = tuple((reshaped(member) for member in (heads_in, step_size, log_decay, b_matrix, c_matrix, segment)))
    _, outputs = lax.scan(jax.checkpoint(advance), initial, blocks)
    return outputs.reshape(seq_len, head_count, head_dim)

def mixer(gate_part, inner_part, shared_part, step_part, conv_inner, conv_inner_bias, conv_shared, conv_shared_bias, step_bias, rate_log, skip_gain, segment):
    seq_len = inner_part.shape[0]
    head_count = step_part.shape[1]
    head_dim = inner_part.shape[1] // head_count
    state_dim = shared_part.shape[1] // 2
    inner = jax.nn.silu(causal_conv(inner_part, conv_inner, conv_inner_bias, segment))
    shared = jax.nn.silu(causal_conv(shared_part, conv_shared, conv_shared_bias, segment))
    step_size = jax.nn.softplus(step_part + step_bias[None, :])
    log_decay = -jnp.exp(rate_log)[None, :] * step_size
    heads_in = inner.reshape(seq_len, head_count, head_dim)
    mixed = span_scan(heads_in, step_size, log_decay, shared[:, :state_dim], shared[:, state_dim:], segment, SPAN)
    mixed = mixed + skip_gain[None, :, None] * heads_in
    return mixed.reshape(seq_len, head_count * head_dim) * jax.nn.silu(gate_part)

def sequence_pass(params, tokens, segment, cotan):
    norm_gain, proj_zx, proj_bc, proj_dt, conv_inner, conv_inner_bias, conv_shared, conv_shared_bias, step_bias, rate_log, skip_gain, gated_gain, proj_out = params
    model_dim = tokens.shape[1]
    inner_dim = proj_out.shape[0]
    group_inner = inner_dim // N_COL
    group_heads = proj_dt.shape[1] // N_COL
    flat_zx = proj_zx.reshape(model_dim, 2 * inner_dim)
    wide = tokens.astype(jnp.float32)
    scale = lax.rsqrt(lax.optimization_barrier(jnp.mean(wide * wide, axis=1, keepdims=True)) + EPS)
    normed = (wide * scale * norm_gain[None, :]).astype(jnp.bfloat16)
    both = jnp.dot(normed, flat_zx, preferred_element_type=jnp.float32).astype(jnp.bfloat16)
    both = lax.optimization_barrier(both)
    shared_in = jnp.dot(normed, proj_bc, preferred_element_type=jnp.float32).astype(jnp.bfloat16)
    shared_in = lax.optimization_barrier(shared_in)
    step_raw = jnp.dot(normed, proj_dt, preferred_element_type=jnp.float32)
    both_wide = both.astype(jnp.float32)
    shared_wide = shared_in.astype(jnp.float32)
    gated_groups = []
    pullbacks = []
    for group in range(N_COL):
        low_col = group * group_inner
        high_col = low_col + group_inner
        low_head = group * group_heads
        high_head = low_head + group_heads
        arguments = (both_wide[:, low_col:high_col], both_wide[:, inner_dim + low_col:inner_dim + high_col], shared_wide, step_raw[:, low_head:high_head], conv_inner[:, low_col:high_col], conv_inner_bias[low_col:high_col], conv_shared, conv_shared_bias, step_bias[low_head:high_head], rate_log[low_head:high_head], skip_gain[low_head:high_head])
        gated_group, pullback = jax.vjp(partial(mixer, segment=segment), *arguments)
        gated_groups.append(gated_group)
        pullbacks.append(pullback)
    gated = jnp.concatenate(gated_groups, axis=1)
    rescale = lax.rsqrt(lax.optimization_barrier(jnp.sum(gated * gated, axis=1, keepdims=True)) / inner_dim + EPS)
    gated_normed = (gated * rescale * gated_gain[None, :]).astype(jnp.bfloat16)
    projected = jnp.dot(gated_normed, proj_out, preferred_element_type=jnp.float32)
    result = (wide + projected).astype(jnp.bfloat16)
    grad_out_w = jnp.dot(gated_normed.T, cotan, preferred_element_type=jnp.float32)
    back = jnp.dot(cotan, proj_out.T, preferred_element_type=jnp.float32)
    grad_gain_out = lax.optimization_barrier(jnp.sum(back * gated * rescale, axis=0))
    weighted = back * gated_gain[None, :]
    inner_sum = lax.optimization_barrier(jnp.sum(weighted * gated, axis=1, keepdims=True))
    grad_gated = rescale * weighted - gated * (rescale ** 3 * inner_sum / inner_dim)
    gate_grads = []
    inner_grads = []
    step_grads = []
    conv_inner_grads = []
    conv_bias_grads = []
    step_bias_grads = []
    rate_grads = []
    skip_grads = []
    conv_shared_total = jnp.zeros(conv_shared.shape, jnp.float32)
    conv_shared_bias_total = jnp.zeros(conv_shared_bias.shape, jnp.float32)
    grad_bc = jnp.zeros(proj_bc.shape, jnp.float32)
    pushback = jnp.zeros(tokens.shape, jnp.float32)
    for group in range(N_COL):
        low_col = group * group_inner
        pulled = pullbacks[group](grad_gated[:, low_col:low_col + group_inner])
        gate_grads.append(pulled[0])
        inner_grads.append(pulled[1])
        shared_back = pulled[2].astype(jnp.bfloat16)
        step_grads.append(pulled[3])
        conv_inner_grads.append(pulled[4])
        conv_bias_grads.append(pulled[5])
        conv_shared_total = conv_shared_total + pulled[6]
        conv_shared_bias_total = conv_shared_bias_total + pulled[7]
        step_bias_grads.append(pulled[8])
        rate_grads.append(pulled[9])
        skip_grads.append(pulled[10])
        grad_bc = grad_bc + jnp.dot(normed.T, shared_back, preferred_element_type=jnp.float32)
        pushback = pushback + jnp.dot(shared_back, proj_bc.T, preferred_element_type=jnp.float32)
    grad_both = jnp.concatenate(gate_grads + inner_grads, axis=1).astype(jnp.bfloat16)
    step_back = jnp.concatenate(step_grads, axis=1).astype(jnp.bfloat16)
    grad_zx = jnp.dot(normed.T, grad_both, preferred_element_type=jnp.float32).reshape(model_dim, 2, inner_dim)
    grad_dt = jnp.dot(normed.T, step_back, preferred_element_type=jnp.float32)
    pushback = pushback + jnp.dot(grad_both, flat_zx.T, preferred_element_type=jnp.float32)
    pushback = pushback + jnp.dot(step_back, proj_dt.T, preferred_element_type=jnp.float32)
    grad_gain_in = lax.optimization_barrier(jnp.sum(pushback * wide * scale, axis=0))
    pushed = pushback * norm_gain[None, :]
    grad_wide = scale * pushed - wide * scale ** 3 * lax.optimization_barrier(jnp.mean(pushed * wide, axis=1, keepdims=True))
    grad_tokens = (cotan.astype(jnp.float32) + grad_wide).astype(jnp.bfloat16)
    grads = (grad_gain_in, grad_zx, grad_bc, grad_dt, jnp.concatenate(conv_inner_grads, axis=1), jnp.concatenate(conv_bias_grads, axis=0), conv_shared_total, conv_shared_bias_total, jnp.concatenate(step_bias_grads, axis=0), jnp.concatenate(rate_grads, axis=0), jnp.concatenate(skip_grads, axis=0), grad_gain_out, grad_out_w)
    return (result, grad_tokens, grads)

def reference(block_input, segment_ids, norm_gain, proj_zx, proj_bc, proj_dt, conv_inner, conv_inner_bias, conv_shared, conv_shared_bias, step_bias, rate_log, skip_gain, gated_gain, proj_out, cotangent):
    params = (norm_gain, proj_zx, proj_bc, proj_dt, conv_inner, conv_inner_bias, conv_shared, conv_shared_bias, step_bias, rate_log, skip_gain, gated_gain, proj_out)
    seq_count = TOKENS // SEQ
    tokens_all = block_input.reshape(seq_count, SEQ, D)
    segments_all = segment_ids.reshape(seq_count, SEQ)
    cotan_all = cotangent.reshape(seq_count, SEQ, D)

    def visit(totals, item):
        tokens, segment, cotan = item
        result, grad_tokens, grads = sequence_pass(params, tokens, segment, cotan)
        return (tuple((total + grad for total, grad in zip(totals, grads))), (result, grad_tokens))
    initial = tuple((jnp.zeros(member.shape, jnp.float32) for member in params))
    totals, (results, grad_rows) = lax.scan(visit, initial, (tokens_all, segments_all, cotan_all))
    grad_norm_gain, grad_proj_zx, grad_proj_bc, grad_proj_dt, grad_conv_inner, grad_conv_inner_bias, grad_conv_shared, grad_conv_shared_bias, grad_step_bias, grad_rate_log, grad_skip_gain, grad_gated_gain, grad_proj_out = totals
    return (results.reshape(TOKENS, D), grad_rows.reshape(TOKENS, D), grad_norm_gain, grad_proj_zx, grad_proj_bc, grad_proj_dt, grad_conv_inner, grad_conv_inner_bias, grad_conv_shared, grad_conv_shared_bias, grad_step_bias, grad_rate_log, grad_skip_gain, grad_gated_gain, grad_proj_out)
```

```python
import functools
import jax, jax.numpy as jnp
from jax import lax
from jax.experimental import pallas as pl
from jax.experimental.pallas import tpu as pltpu
from jax.sharding import PartitionSpec as P

F32, BF16 = jnp.float32, jnp.bfloat16
HIGH = lax.Precision.HIGHEST
SPAN = 256
HALO = 16
EPS = 1e-5


def nn(a, b):
    return lax.dot_general(a, b, (((1,), (0,)), ((), ())), preferred_element_type=F32)


def nt(a, b):
    return lax.dot_general(a, b, (((1,), (1,)), ((), ())), preferred_element_type=F32)


def tn(a, b):
    return lax.dot_general(a, b, (((0,), (0,)), ((), ())), preferred_element_type=F32)


def iota(shape, axis):
    return lax.broadcasted_iota(jnp.int32, shape, axis)


def split_dot(a, b01):
    hi = a.astype(BF16)
    lo = (a - hi.astype(F32)).astype(BF16)
    return nn(hi, b01) + nn(lo, b01)


def sigmoid(v):
    return 1.0 / (1.0 + jnp.exp(-v))


def softplus(v):
    return jnp.maximum(v, 0.0) + jnp.log1p(jnp.exp(-jnp.abs(v)))


def chunk_links(segc, halo):
    ext = jnp.concatenate([halo[HALO - 8 :], segc], axis=0)
    length = segc.shape[0]
    return [(ext[8 - j : 8 - j + length] == segc).astype(F32) for j in range(1, 4)]


def conv_tile(cur, halo, links, taps, sl):
    v = jnp.concatenate([halo[HALO - 8 :, sl].astype(F32), cur[:, sl].astype(F32)], axis=0)
    length = cur.shape[0]
    shifted = [v[8 - j : 8 - j + length] * links[j - 1] for j in range(1, 4)]
    pre = taps[4:5, sl] + taps[3:4, sl] * v[8:]
    for j in range(1, 4):
        pre = pre + taps[3 - j : 4 - j, sl] * shifted[j - 1]
    return pre, [v[8:]] + shifted


def pick(lo, cols, h):
    return jnp.where(lo, cols[:, h : h + 1], cols[:, h + 1 : h + 2])


def forward_kernel(
    inner, inner_halo, shared, shared_halo, step_raw, segc, segc_halo, segr, taps, taps_s, heads,
    y_out, x_out, bc_out, dt_out, c_out, ct_out, dec_out, enter_out, final_out, state, total,
):
    k = pl.program_id(0)
    length, width = inner.shape
    pairs = width // 128
    state_dim = state.shape[0]

    @pl.when(k == 0)
    def _():
        state[...] = jnp.zeros_like(state)
        total[...] = jnp.zeros_like(total)

    seg = segc[...]
    seg_halo = segc_halo[...]
    links = chunk_links(seg, seg_halo)
    closing = (seg == seg[length - 1 :]).astype(F32)
    entering = (seg == seg_halo[HALO - 1 :]).astype(F32)
    kept = (seg[length - 1 :] == seg_halo[HALO - 1 :]).astype(F32)
    dt = softplus(step_raw[...] + heads[0:1])
    log_decay = -jnp.exp(heads[1:2]) * dt
    rows, cols = iota((length, length), 0), iota((length, length), 1)
    lower = (rows >= cols).astype(F32)
    c = jnp.dot(lower, log_decay, precision=HIGH, preferred_element_type=F32)
    ct = c.T
    dt_out[...] = dt
    c_out[...] = c
    ct_out[...] = ct[: ct_out.shape[0]]
    whole = c + total[0:1]
    dec_out[...] = jnp.exp(whole) * (seg == heads[7:8, 0:1].astype(jnp.int32)).astype(F32)
    total[0:1] = whole[length - 1 :]
    for half in range(2):
        sl = slice(half * state_dim, (half + 1) * state_dim)
        pre, _ = conv_tile(shared, shared_halo, links, taps_s, sl)
        bc_out[:, sl] = (pre * sigmoid(pre)).astype(BF16)
    b = bc_out[:, :state_dim]
    cc = bc_out[:, state_dim:]
    scores = jnp.where((rows >= cols) & (seg == segr[...]), nt(cc, b), 0.0)
    lo = iota((length, 128), 1) < 64
    enter_out[...] = state[...].astype(BF16)
    for p in range(pairs):
        sl = slice(p * 128, (p + 1) * 128)
        pre, _ = conv_tile(inner, inner_halo, links, taps, sl)
        xp = pre * sigmoid(pre)
        xb = xp.astype(BF16)
        x_out[:, sl] = xb
        xdt = xb.astype(F32) * pick(lo, dt, 2 * p)
        cb = pick(lo, c, 2 * p)
        acc = nn(cc, state[:, sl].astype(BF16)) * (jnp.exp(cb) * entering)
        for a in range(2):
            h = 2 * p + a
            weights = jnp.exp(jnp.minimum(c[:, h : h + 1] - ct[h : h + 1], 0.0)) * scores
            mine = lo if a == 0 else ~lo
            acc = acc + nn(weights.astype(BF16), jnp.where(mine, xdt, 0.0).astype(BF16))
        y_out[:, sl] = acc
        last = cb[length - 1 :]
        leaving = jnp.exp(last - cb) * closing * xdt
        state[:, sl] = state[:, sl] * (jnp.exp(last) * kept) + tn(b, leaving.astype(BF16))

    @pl.when(k == pl.num_programs(0) - 1)
    def _():
        final_out[...] = state[...]


def halo_index(chunk, chunks):
    return jnp.where(chunk == 0, chunks * (SPAN // HALO), chunk * (SPAN // HALO) - 1)


def run_forward(both_ext, shared_ext, step_raw, segc_ext, segr, taps, taps_s, heads):
    width = taps.shape[1]
    scols = taps_s.shape[1]
    length = segr.shape[1]
    chunks = length // SPAN
    nrow = -(-heads.shape[1] // 8) * 0 + 16
    row = lambda k: (k, 0)
    halo = lambda col: (lambda k: (halo_index(k, chunks), col))
    fixed = lambda k: (0, 0)
    S = jax.ShapeDtypeStruct
    return pl.pallas_call(
        forward_kernel,
        grid=(chunks,),
        in_specs=[
            pl.BlockSpec((SPAN, width), lambda k: (k, 1)),
            pl.BlockSpec((HALO, width), halo(1)),
            pl.BlockSpec((SPAN, scols), row),
            pl.BlockSpec((HALO, scols), halo(0)),
            pl.BlockSpec((SPAN, 128), row),
            pl.BlockSpec((SPAN, 1), row),
            pl.BlockSpec((HALO, 1), halo(0)),
            pl.BlockSpec((1, SPAN), lambda k: (0, k)),
            pl.BlockSpec(taps.shape, fixed),
            pl.BlockSpec(taps_s.shape, fixed),
            pl.BlockSpec(heads.shape, fixed),
        ],
        out_specs=[
            pl.BlockSpec((SPAN, width), row),
            pl.BlockSpec((SPAN, width), row),
            pl.BlockSpec((SPAN, scols), row),
            pl.BlockSpec((SPAN, 128), row),
            pl.BlockSpec((SPAN, 128), row),
            pl.BlockSpec((nrow, SPAN), lambda k: (0, k)),
            pl.BlockSpec((SPAN, 128), row),
            pl.BlockSpec((None, scols // 2, width), lambda k: (k, 0, 0)),
            pl.BlockSpec((scols // 2, width), fixed),
        ],
        out_shape=[
            S((length, width), F32),
            S((length, width), BF16),
            S((length, scols), BF16),
            S((length, 128), F32),
            S((length, 128), F32),
            S((nrow, length), F32),
            S((length, 128), F32),
            S((chunks, scols // 2, width), BF16),
            S((scols // 2, width), F32),
        ],
        scratch_shapes=[pltpu.VMEM((scols // 2, width), F32), pltpu.VMEM((8, 128), F32)],
        name="scan_forward",
    )(both_ext, both_ext, shared_ext, shared_ext, step_raw, segc_ext, segc_ext, segr, taps, taps_s, heads)


def row_sums(value):
    hi = value.astype(BF16)
    lo = (value - hi.astype(F32)).astype(BF16)
    ones = jnp.ones((8, value.shape[1]), BF16)
    return nt(ones, hi) + nt(ones, lo)


def gate_kernel(y, x, bc, dec, start, gate, back, taps, ssd_out, sums_out):
    length, width = x.shape
    state_dim = start.shape[0]
    cc = bc[:, state_dim:]
    lo = iota((length, 128), 1) < 64
    squares = jnp.zeros((length, 128), F32)
    inner = jnp.zeros((length, 128), F32)
    for p in range(width // 128):
        sl = slice(p * 128, (p + 1) * 128)
        corr = nn(cc, start[:, sl].astype(BF16)) * pick(lo, dec, 2 * p)
        ssd = y[:, sl] + corr + taps[6:7, sl] * x[:, sl].astype(F32)
        ssd_out[:, sl] = ssd
        g = gate[:, sl].astype(F32)
        gated = ssd * (g * sigmoid(g))
        squares = squares + gated * gated
        inner = inner + back[:, sl].astype(F32) * taps[5:6, sl] * gated
    sums_out[0:8] = row_sums(squares)
    sums_out[8:16] = row_sums(inner)


def run_gate(y, x, bc, dec, start, both_ext, back, taps):
    length, width = x.shape
    row = lambda k: (k, 0)
    fixed = lambda k: (0, 0)
    S = jax.ShapeDtypeStruct
    return pl.pallas_call(
        gate_kernel,
        grid=(length // SPAN,),
        in_specs=[
            pl.BlockSpec((SPAN, width), row),
            pl.BlockSpec((SPAN, width), row),
            pl.BlockSpec((SPAN, bc.shape[1]), row),
            pl.BlockSpec((SPAN, 128), row),
            pl.BlockSpec(start.shape, fixed),
            pl.BlockSpec((SPAN, width), row),
            pl.BlockSpec((SPAN, width), row),
            pl.BlockSpec(taps.shape, fixed),
        ],
        out_specs=[pl.BlockSpec((SPAN, width), row), pl.BlockSpec((16, SPAN), lambda k: (0, k))],
        out_shape=[S((length, width), F32), S((16, length), F32)],
        name="gate_sums",
    )(y, x, bc, dec, start, both_ext, back, taps)


def columns(row):
    return jnp.broadcast_to(row, (128, row.shape[1])).T


def back_kernel(
    full_width, ssd, x, bc, dec, gate, back, sums, taps,
    normed_out, dy_out, ggate_out, row_out, colsum_out, dstart_out,
):
    length, width = x.shape
    state_dim = dstart_out.shape[0]

    @pl.when(pl.program_id(0) == 0)
    def _():
        colsum_out[...] = jnp.zeros_like(colsum_out)
        dstart_out[...] = jnp.zeros_like(dstart_out)

    cc = bc[:, state_dim:]
    lo = iota((length, 128), 1) < 64
    rescale = columns(lax.rsqrt(sums[0:1] / full_width + EPS))
    pull = columns(sums[1:2]) * (rescale * rescale * rescale / full_width)
    rowterm = jnp.zeros((length, 128), F32)
    for p in range(width // 128):
        sl = slice(p * 128, (p + 1) * 128)
        s_ssd = ssd[:, sl]
        xp = x[:, sl].astype(F32)
        g = gate[:, sl].astype(F32)
        s = sigmoid(g)
        gated = s_ssd * (g * s)
        bk = back[:, sl].astype(F32)
        gain = taps[5:6, sl]
        normed_out[:, sl] = (gated * rescale * gain).astype(BF16)
        gg = rescale * (bk * gain) - gated * pull
        dy = gg * (g * s)
        dyb = dy.astype(BF16)
        dy_out[:, sl] = dyb
        ggate_out[:, sl] = (gg * s_ssd * s * (1.0 + g * (1.0 - s))).astype(BF16)
        colsum_out[0:1, sl] += jnp.sum(bk * gated * rescale, axis=0, keepdims=True)
        colsum_out[1:2, sl] += jnp.sum(dy * xp, axis=0, keepdims=True)
        dstart_out[:, sl] += tn(cc, (dy * pick(lo, dec, 2 * p)).astype(BF16))
        rowterm = rowterm + split_dot(dyb.astype(F32) * (s_ssd - taps[6:7, sl] * xp), head_map(p))
    row_out[...] = rowterm


def head_map(p):
    lane, head = iota((128, 128), 0), iota((128, 128), 1)
    return (head == 2 * p + lane // 64).astype(BF16)


def run_back(full_width, ssd, x, bc, dec, both_ext, back, sums, taps):
    length, width = x.shape
    row = lambda k: (k, 0)
    fixed = lambda k: (0, 0)
    S = jax.ShapeDtypeStruct
    return pl.pallas_call(
        functools.partial(back_kernel, full_width),
        grid=(length // SPAN,),
        in_specs=[
            pl.BlockSpec((SPAN, width), row),
            pl.BlockSpec((SPAN, width), row),
            pl.BlockSpec((SPAN, bc.shape[1]), row),
            pl.BlockSpec((SPAN, 128), row),
            pl.BlockSpec((SPAN, width), row),
            pl.BlockSpec((SPAN, width), row),
            pl.BlockSpec((sums.shape[0], SPAN), lambda k: (0, k)),
            pl.BlockSpec(taps.shape, fixed),
        ],
        out_specs=[
            pl.BlockSpec((SPAN, width), row),
            pl.BlockSpec((SPAN, width), row),
            pl.BlockSpec((SPAN, width), row),
            pl.BlockSpec((SPAN, 128), row),
            pl.BlockSpec((8, width), fixed),
            pl.BlockSpec((bc.shape[1] // 2, width), fixed),
        ],
        out_shape=[
            S((length, width), BF16),
            S((length, width), BF16),
            S((length, width), BF16),
            S((length, 128), F32),
            S((8, width), F32),
            S((bc.shape[1] // 2, width), F32),
        ],
        name="gated_back",
    )(ssd, x, bc, dec, both_ext, back, sums, taps)


def conv_back(dout, pre, shifts, links, taps, sl, carry, carry_links, par_out):
    length = dout.shape[0]
    s = sigmoid(pre)
    dconv = dout * (s * (1.0 + pre * (1.0 - s)))
    nxt = carry[:, sl]
    grad = taps[3:4, sl] * dconv
    above = jnp.zeros((8, dout.shape[1]), F32)
    par_out[3:4, sl] += jnp.sum(dconv * shifts[0], axis=0, keepdims=True)
    par_out[4:5, sl] += jnp.sum(dconv, axis=0, keepdims=True)
    for j in range(1, 4):
        z = dconv * links[j - 1]
        w = taps[3 - j : 4 - j, sl]
        low = jnp.concatenate([z, nxt * carry_links[:, j - 1 : j]], axis=0)
        grad = grad + w * low[j : j + length]
        high = jnp.concatenate([above * 0.0, z[0:8]], axis=0)
        above = above + w * high[j : j + 8]
        par_out[3 - j : 4 - j, sl] += jnp.sum(dconv * shifts[j], axis=0, keepdims=True)
    carry[:, sl] = dconv[0:8]
    return grad, above


def backward_kernel(
    inner, inner_halo, shared, shared_halo, step_raw, segc, segc_halo, segr, taps, taps_s, heads,
    dy, x, bc, dt_in, c_in, ct_in, dec_halo, enter, start, row_in, dend,
    ginner_out, gshared_out, gstep_out, par_out, par_s_out, par_h_out, edge_out, edge_s_out, last_out, last_s_out,
    dstate, carry, carry_s, carry_links, grads_bc,
):
    i = pl.program_id(0)
    k = pl.num_programs(0) - 1 - i
    length, width = x.shape
    state_dim = dstate.shape[0]

    @pl.when(i == 0)
    def _():
        dstate[...] = dend[...]
        carry[...] = jnp.zeros_like(carry)
        carry_s[...] = jnp.zeros_like(carry_s)
        carry_links[...] = jnp.zeros_like(carry_links)
        par_out[...] = jnp.zeros_like(par_out)
        par_s_out[...] = jnp.zeros_like(par_s_out)
        par_h_out[...] = jnp.zeros_like(par_h_out)

    seg = segc[...]
    seg_halo = segc_halo[...]
    links = chunk_links(seg, seg_halo)
    closing = (seg == seg[length - 1 :]).astype(F32)
    entering = (seg == seg_halo[HALO - 1 :]).astype(F32)
    kept = (seg[length - 1 :] == seg_halo[HALO - 1 :]).astype(F32)
    next_links = carry_links[...]
    dt = dt_in[...]
    c = c_in[...]
    ct = ct_in[...]
    first = (k == 0).astype(F32)
    reach = dec_halo[7:8] * (1.0 - first) + first
    b = bc[:, :state_dim]
    cc = bc[:, state_dim:]
    rows, cols = iota((length, length), 0), iota((length, length), 1)
    allowed = (rows <= cols) & (seg == segr[...])
    scores = jnp.where(allowed, nt(b, cc), 0.0)
    lo = iota((length, 128), 1) < 64
    lo1 = lo[0:1]
    dscores = jnp.zeros((length, length), F32)
    db = jnp.zeros((length, state_dim), F32)
    dc_mat = jnp.zeros((length, state_dim), F32)
    direct = jnp.zeros((length, 128), F32)
    matched = jnp.zeros((length, 128), F32)
    closing_term = jnp.zeros((1, 128), F32)
    for p in range(width // 128):
        sl = slice(p * 128, (p + 1) * 128)
        pre, shifts = conv_tile(inner, inner_halo, links, taps, sl)
        dyb = dy[:, sl]
        dyf = dyb.astype(F32)
        xp = x[:, sl].astype(F32)
        dtb = pick(lo, dt, 2 * p)
        xdt = xp * dtb
        cb = pick(lo, c, 2 * p)
        hm = head_map(p)
        last = cb[length - 1 :]
        entry = enter[:, sl].astype(F32) + start[:, sl] * pick(lo1, reach, 2 * p)
        entryb = entry.astype(BF16)
        ds = dstate[:, sl]
        dsb = ds.astype(BF16)
        leaving = jnp.exp(last - cb) * closing
        bds = nn(b, dsb)
        dxdt = jnp.zeros((length, 128), F32)
        for a in range(2):
            h = 2 * p + a
            mine = lo if a == 0 else ~lo
            decay = jnp.exp(jnp.minimum(ct[h : h + 1] - c[:, h : h + 1], 0.0))
            dscores = dscores + decay * nt(jnp.where(mine, xdt, 0.0).astype(BF16), dyb)
            dxdt = dxdt + nn((decay * scores).astype(BF16), jnp.where(mine, dyf, 0.0).astype(BF16))
        spread = leaving * xdt
        moved = spread * bds
        matched = matched + split_dot(xdt.astype(BF16).astype(F32) * dxdt + moved, hm)
        dxdt = dxdt + leaving * bds
        held = jnp.exp(last) * kept
        col = jnp.sum(moved, axis=0, keepdims=True) + held * jnp.sum(entry * ds, axis=0, keepdims=True)
        closing_term = closing_term + split_dot(jnp.broadcast_to(col, (8, 128)), hm)[0:1]
        direct = direct + split_dot(xp * dxdt, hm)
        edy = (jnp.exp(cb) * entering * dyf).astype(BF16)
        db = db + nt(spread.astype(BF16), dsb)
        dc_mat = dc_mat + nt(edy, entryb)
        dstate[:, sl] = ds * held + tn(cc, edy)
        dx = dtb * dxdt + taps[6:7, sl] * dyf
        grad, above = conv_back(dx, pre, shifts, links, taps, sl, carry, next_links, par_out)
        ginner_out[:, sl] = grad.astype(BF16)
        edge_out[:, sl] = above

        @pl.when(i == 0)
        def _():
            last_out[:, sl] = grad[length - 8 :]

    dsc = jnp.where(allowed, dscores, 0.0).astype(BF16)
    grads_bc[:, :state_dim] = db + nn(dsc, cc)
    grads_bc[:, state_dim:] = dc_mat + tn(dsc, b)
    for half in range(2):
        sl = slice(half * state_dim, (half + 1) * state_dim)
        pre, shifts = conv_tile(shared, shared_halo, links, taps_s, sl)
        grad, above = conv_back(grads_bc[:, sl], pre, shifts, links, taps_s, sl, carry_s, next_links, par_s_out)
        gshared_out[:, sl] = grad.astype(BF16)
        edge_s_out[:, sl] = above

        @pl.when(i == 0)
        def _():
            last_s_out[:, sl] = grad[length - 8 :]

    for j in range(3):
        carry_links[:, j : j + 1] = links[j][0:8]
    dcum = row_in[...] - matched
    upper = (rows <= cols).astype(F32)
    dlog = jnp.dot(upper, dcum, precision=HIGH, preferred_element_type=F32) + closing_term
    rate = -jnp.exp(heads[1:2])
    dstep = (direct + dlog * rate) * sigmoid(step_raw[...] + heads[0:1])
    gstep_out[...] = dstep.astype(BF16)
    par_h_out[0:1] += jnp.sum(dstep, axis=0, keepdims=True)
    par_h_out[1:2] += jnp.sum(dlog * (rate * dt), axis=0, keepdims=True)


def run_backward(
    both_ext, shared_ext, step_raw, segc_ext, segr, taps, taps_s, heads,
    dy, x, bc, dt, c, ct, dec, enter, start, rowterm, dend,
):
    length, width = x.shape
    scols = bc.shape[1]
    chunks = length // SPAN
    at = lambda i: chunks - 1 - i
    row = lambda i: (at(i), 0)
    halo = lambda col: (lambda i: (halo_index(at(i), chunks), col))
    fixed = lambda i: (0, 0)
    S = jax.ShapeDtypeStruct
    return pl.pallas_call(
        backward_kernel,
        grid=(chunks,),
        in_specs=[
            pl.BlockSpec((SPAN, width), lambda i: (at(i), 1)),
            pl.BlockSpec((HALO, width), halo(1)),
            pl.BlockSpec((SPAN, scols), row),
            pl.BlockSpec((HALO, scols), halo(0)),
            pl.BlockSpec((SPAN, 128), row),
            pl.BlockSpec((SPAN, 1), row),
            pl.BlockSpec((HALO, 1), halo(0)),
            pl.BlockSpec((1, SPAN), lambda i: (0, at(i))),
            pl.BlockSpec(taps.shape, fixed),
            pl.BlockSpec(taps_s.shape, fixed),
            pl.BlockSpec(heads.shape, fixed),
            pl.BlockSpec((SPAN, width), row),
            pl.BlockSpec((SPAN, width), row),
            pl.BlockSpec((SPAN, scols), row),
            pl.BlockSpec((SPAN, 128), row),
            pl.BlockSpec((SPAN, 128), row),
            pl.BlockSpec((ct.shape[0], SPAN), lambda i: (0, at(i))),
            pl.BlockSpec((8, 128), lambda i: (jnp.maximum(at(i) * (SPAN // 8) - 1, 0), 0)),
            pl.BlockSpec((None, scols // 2, width), lambda i: (at(i), 0, 0)),
            pl.BlockSpec(start.shape, fixed),
            pl.BlockSpec((SPAN, 128), row),
            pl.BlockSpec(dend.shape, fixed),
        ],
        out_specs=[
            pl.BlockSpec((SPAN, width), row),
            pl.BlockSpec((SPAN, scols), row),
            pl.BlockSpec((SPAN, 128), row),
            pl.BlockSpec((8, width), fixed),
            pl.BlockSpec((8, scols), fixed),
            pl.BlockSpec((8, 128), fixed),
            pl.BlockSpec((8, width), fixed),
            pl.BlockSpec((8, scols), fixed),
            pl.BlockSpec((8, width), fixed),
            pl.BlockSpec((8, scols), fixed),
        ],
        out_shape=[
            S((length, width), BF16),
            S((length, scols), BF16),
            S((length, 128), BF16),
            S((8, width), F32),
            S((8, scols), F32),
            S((8, 128), F32),
            S((8, width), F32),
            S((8, scols), F32),
            S((8, width), F32),
            S((8, scols), F32),
        ],
        scratch_shapes=[
            pltpu.VMEM((scols // 2, width), F32),
            pltpu.VMEM((8, width), F32),
            pltpu.VMEM((8, scols), F32),
            pltpu.VMEM((8, 128), F32),
            pltpu.VMEM((SPAN, scols), F32),
        ],
        name="scan_backward",
    )(both_ext, both_ext, shared_ext, shared_ext, step_raw, segc_ext, segc_ext, segr, taps, taps_s, heads,
      dy, x, bc, dt, c, ct, dec, enter, start, rowterm, dend)


def pass_on(value, axis, by):
    count = lax.axis_size(axis)
    pairs = [(i, i + by) for i in range(count) if 0 <= i + by < count]
    return lax.ppermute(value, axis, pairs)


def pack_rows(rows, width):
    used = sum(r.shape[0] for r in rows)
    return jnp.concatenate(rows + [jnp.zeros((8 - used, width), F32)], axis=0)


def per_device(
    block_input, segment_ids, norm_gain, proj_zx, proj_bc, proj_dt, conv_inner, conv_inner_bias,
    conv_shared, conv_shared_bias, step_bias, rate_log, skip_gain, gated_gain, proj_out, cotangent,
):
    model_dim = block_input.shape[1]
    width = proj_zx.shape[2]
    scols = proj_bc.shape[1]
    nheads = proj_dt.shape[1]
    full_width = float(width * lax.axis_size("col"))
    shards = ("dp", "row")
    x_all = lax.all_gather(block_input, "col", axis=0, tiled=True)
    cot_all = lax.all_gather(cotangent, "col", axis=0, tiled=True)
    seg_all = lax.all_gather(segment_ids, "col", axis=0, tiled=True)
    w_in = lax.all_gather(proj_zx.reshape(-1, 2 * width), shards, axis=0, tiled=True)
    small_own = jnp.concatenate(
        [proj_bc, proj_dt, jnp.zeros((proj_dt.shape[0], 128 - nheads), BF16)], axis=1
    )
    w_small = lax.all_gather(small_own, shards, axis=0, tiled=True)
    out_t = lax.all_gather(proj_out.T, shards, axis=0, tiled=True)

    length = x_all.shape[0]
    tail_x, tail_seg = pass_on((x_all[-HALO:], seg_all[-HALO:] + 1), "row", 1)
    x_ext = jnp.concatenate([x_all, tail_x], axis=0)
    seg_ext = jnp.concatenate([seg_all, tail_seg - 1], axis=0)
    wide = x_ext.astype(F32)
    scale = lax.rsqrt(jnp.mean(wide * wide, axis=1, keepdims=True) + EPS)
    normed_ext = (wide * scale * norm_gain[None, :]).astype(BF16)
    normed = normed_ext[:length]
    both_ext = nn(normed_ext, w_in).astype(BF16)
    small_ext = nn(normed_ext, w_small)
    shared_ext = small_ext[:, :scols].astype(BF16)
    step_ext = small_ext[:, scols:]

    head_dim = width // nheads
    taps = pack_rows(
        [conv_inner, conv_inner_bias[None], gated_gain[None], jnp.repeat(skip_gain, head_dim)[None]], width
    )
    taps_s = pack_rows([conv_shared, conv_shared_bias[None]], scols)
    fill = (0, 128 - nheads)
    heads = pack_rows([jnp.pad(step_bias, fill)[None], jnp.pad(rate_log, fill)[None], jnp.zeros((5, 128), F32)], 128)
    heads = jnp.concatenate([heads[:7], jnp.full((1, 128), seg_ext[-1], F32)], axis=0)
    common = (both_ext, shared_ext, step_ext, seg_ext[:, None], seg_all[None, :], taps, taps_s, heads)
    y, x, bc, dt, c, ct, dec, enter, final = run_forward(*common)
    start = pass_on(final, "row", 1)
    back = nn(cot_all, out_t).astype(BF16)
    ssd, sums = run_gate(y, x, bc, dec, start, both_ext, back, taps)
    sums = lax.psum(jnp.concatenate([sums[0:1], sums[8:9]], axis=0), "col")
    sums = jnp.concatenate([sums, jnp.zeros((6, length), F32)], axis=0)
    gated_normed, dy, ggate, rowterm, colsum, dstart = run_back(
        full_width, ssd, x, bc, dec, both_ext, back, sums, taps
    )
    dend = pass_on(dstart, "row", -1)
    projected = lax.psum_scatter(
        nt(gated_normed, out_t).astype(BF16), "col", scatter_dimension=0, tiled=True
    )
    block_output = (block_input.astype(F32) + projected.astype(F32)).astype(BF16)
    grad_out = lax.psum_scatter(
        tn(cot_all, gated_normed).astype(BF16), shards, scatter_dimension=0, tiled=True
    )
    ginner, gshared, gstep, par, par_s, par_h, edge, edge_s, last, last_s = run_backward(
        *common, dy, x, bc, dt, c, ct, dec, enter, start, rowterm, dend
    )
    edge, edge_s = pass_on((edge, edge_s), "row", -1)
    ginner = lax.dynamic_update_slice(ginner, (last + edge).astype(BF16), (length - 8, 0))
    gshared = lax.dynamic_update_slice(gshared, (last_s + edge_s).astype(BF16), (length - 8, 0))
    gsmall = jnp.concatenate([gshared, gstep], axis=1)
    part_normed = nt(ggate, w_in[:, :width]) + nt(ginner, w_in[:, width:]) + nt(gsmall, w_small)
    grad_normed = lax.psum_scatter(
        part_normed.astype(BF16), "col", scatter_dimension=0, tiled=True
    ).astype(F32)
    gain_part = jnp.sum(part_normed * (wide * scale)[:length], axis=0)
    gboth = jnp.concatenate([ggate, ginner], axis=1)
    gzx = lax.psum_scatter(tn(normed, gboth).astype(BF16), shards, scatter_dimension=0, tiled=True)
    gsm = lax.psum_scatter(tn(normed, gsmall), shards, scatter_dimension=0, tiled=True)
    rows_a = jnp.concatenate([par[:5], colsum[:2], jnp.zeros((1, width), F32)], axis=0)
    vec_a = jnp.concatenate([rows_a.reshape(-1), par_h[:2].reshape(-1)])
    vec_b = jnp.concatenate([par_s[:5].reshape(-1), gain_part])
    vec_a = lax.psum(vec_a, shards)
    vec_b = lax.psum(vec_b, shards)
    vec_b, grad_bc = lax.psum((vec_b, gsm[:, :scols]), "col")
    rows_a = vec_a[: 8 * width].reshape(8, width)
    par_h = vec_a[8 * width :].reshape(2, 128)[:, :nheads]
    rows_b = vec_b[: 5 * scols].reshape(5, scols)
    own = block_input.astype(F32)
    own_scale = lax.rsqrt(jnp.mean(own * own, axis=1, keepdims=True) + EPS)
    pushed = grad_normed * norm_gain[None, :]
    grad_wide = own_scale * pushed - own * own_scale**3 * jnp.mean(pushed * own, axis=1, keepdims=True)
    grad_input = (cotangent.astype(F32) + grad_wide).astype(BF16)
    return (
        block_output,
        grad_input,
        vec_b[5 * scols :],
        gzx.astype(F32).reshape(-1, 2, width),
        grad_bc,
        gsm[:, scols : scols + nheads],
        rows_a[:4],
        rows_a[4],
        rows_b[:4],
        rows_b[4],
        par_h[0],
        par_h[1],
        jnp.sum(rows_a[6].reshape(nheads, head_dim), axis=1),
        rows_a[5],
        grad_out.astype(F32).T,
    )


def solution(mesh):
    shards = ("dp", "row")
    tokens = P(("dp", "row", "col"), None)
    zx = P(shards, None, "col")
    in_specs = (
        tokens, P(("dp", "row", "col")), P(), zx, P(shards, None), P(shards, "col"), P(None, "col"), P("col"),
        P(), P(), P("col"), P("col"), P("col"), P("col"), P("col", shards), tokens,
    )
    out_specs = (
        tokens, tokens, P(), zx, P(shards, None), P(shards, "col"), P(None, "col"), P("col"),
        P(), P(), P("col"), P("col"), P("col"), P("col"), P("col", shards),
    )
    return jax.shard_map(per_device, mesh=mesh, in_specs=in_specs, out_specs=out_specs, check_vma=False)
```

```python
import functools
import jax, jax.numpy as jnp
from jax import lax
from jax.experimental import pallas as pl
from jax.experimental.pallas import tpu as pltpu
from jax.sharding import PartitionSpec as P

F32, BF16 = jnp.float32, jnp.bfloat16
HIGH = lax.Precision.HIGHEST
SPAN = 256
HALO = 16
EPS = 1e-5


def nn(a, b):
    return lax.dot_general(a, b, (((1,), (0,)), ((), ())), preferred_element_type=F32)


def nt(a, b):
    return lax.dot_general(a, b, (((1,), (1,)), ((), ())), preferred_element_type=F32)


def tn(a, b):
    return lax.dot_general(a, b, (((0,), (0,)), ((), ())), preferred_element_type=F32)


def iota(shape, axis):
    return lax.broadcasted_iota(jnp.int32, shape, axis)


def split_dot(a, b01):
    hi = a.astype(BF16)
    lo = (a - hi.astype(F32)).astype(BF16)
    return nn(hi, b01) + nn(lo, b01)


def sigmoid(v):
    return 1.0 / (1.0 + jnp.exp(-v))


def softplus(v):
    return jnp.maximum(v, 0.0) + jnp.log1p(jnp.exp(-jnp.abs(v)))


def columns(row):
    return jnp.broadcast_to(row, (128, row.shape[1])).T


def segments(seg_row, prev_row, tail_row):
    row = seg_row[0:1].astype(F32)
    seg = columns(row)[:, 0:1]
    length = row.shape[1]
    prev = columns(prev_row[0:1].astype(F32))[length - 8 :, 0:1]
    tail = tail_row[0:1, length - 1 :].astype(F32)
    return row, seg, prev, tail


def chunk_links(segc, halo):
    ext = jnp.concatenate([halo, segc], axis=0)
    length = segc.shape[0]
    return [(ext[8 - j : 8 - j + length] == segc).astype(F32) for j in range(1, 4)]


def conv_tile(cur, halo, links, taps, sl):
    v = jnp.concatenate([halo[HALO - 8 :, sl].astype(F32), cur[:, sl].astype(F32)], axis=0)
    length = cur.shape[0]
    shifted = [v[8 - j : 8 - j + length] * links[j - 1] for j in range(1, 4)]
    pre = taps[4:5, sl] + taps[3:4, sl] * v[8:]
    for j in range(1, 4):
        pre = pre + taps[3 - j : 4 - j, sl] * shifted[j - 1]
    return pre, [v[8:]] + shifted


def pick(lo, cols, h):
    return jnp.where(lo, cols[:, h : h + 1], cols[:, h + 1 : h + 2])


def forward_kernel(
    inner, inner_halo, shared, shared_halo, step_raw, seg_row, seg_prev, seg_tail, taps, taps_s, heads,
    y_out, x_out, bc_out, dt_out, c_out, ct_out, dec_out, enter_out, final_out, state, total,
):
    k = pl.program_id(0)
    length, width = inner.shape
    pairs = width // 128
    state_dim = state.shape[0]

    @pl.when(k == 0)
    def _():
        state[...] = jnp.zeros_like(state)
        total[...] = jnp.zeros_like(total)

    segr, seg, seg_halo, tail_seg = segments(seg_row, seg_prev, seg_tail)
    links = chunk_links(seg, seg_halo)
    closing = (seg == seg[length - 1 :]).astype(F32)
    entering = (seg == seg_halo[7:]).astype(F32)
    kept = (seg[length - 1 :] == seg_halo[7:]).astype(F32)
    dt = softplus(step_raw[...] + heads[0:1])
    log_decay = -jnp.exp(heads[1:2]) * dt
    rows, cols = iota((length, length), 0), iota((length, length), 1)
    lower = (rows >= cols).astype(F32)
    c = jnp.dot(lower, log_decay, precision=HIGH, preferred_element_type=F32)
    ct = c.T
    dt_out[...] = dt
    c_out[...] = c
    ct_out[...] = ct[: ct_out.shape[0]]
    whole = c + total[0:1]
    dec_out[...] = jnp.exp(whole) * (seg == tail_seg).astype(F32)
    total[0:1] = whole[length - 1 :]
    for half in range(2):
        sl = slice(half * state_dim, (half + 1) * state_dim)
        pre, _ = conv_tile(shared, shared_halo, links, taps_s, sl)
        bc_out[:, sl] = (pre * sigmoid(pre)).astype(BF16)
    b = bc_out[:, :state_dim]
    cc = bc_out[:, state_dim:]
    scores = jnp.where((rows >= cols) & (seg == segr), nt(cc, b), 0.0)
    lo = iota((length, 128), 1) < 64
    enter_out[...] = state[...].astype(BF16)
    for p in range(pairs):
        sl = slice(p * 128, (p + 1) * 128)
        pre, _ = conv_tile(inner, inner_halo, links, taps, sl)
        xp = pre * sigmoid(pre)
        xb = xp.astype(BF16)
        x_out[:, sl] = xb
        xdt = xb.astype(F32) * pick(lo, dt, 2 * p)
        cb = pick(lo, c, 2 * p)
        acc = nn(cc, state[:, sl].astype(BF16)) * (jnp.exp(cb) * entering)
        for a in range(2):
            h = 2 * p + a
            weights = jnp.exp(jnp.minimum(c[:, h : h + 1] - ct[h : h + 1], 0.0)) * scores
            mine = lo if a == 0 else ~lo
            acc = acc + nn(weights.astype(BF16), jnp.where(mine, xdt, 0.0).astype(BF16))
        y_out[:, sl] = acc
        last = cb[length - 1 :]
        leaving = jnp.exp(last - cb) * closing * xdt
        state[:, sl] = state[:, sl] * (jnp.exp(last) * kept) + tn(b, leaving.astype(BF16))

    @pl.when(k == pl.num_programs(0) - 1)
    def _():
        final_out[...] = state[...]


def halo_index(chunk, chunks):
    return jnp.where(chunk == 0, chunks * (SPAN // HALO), chunk * (SPAN // HALO) - 1)


def seg_specs(at, chunks):
    return [
        pl.BlockSpec((8, SPAN), lambda k: (at(k), 0)),
        pl.BlockSpec((8, SPAN), lambda k: (jnp.where(at(k) == 0, chunks, at(k) - 1), 0)),
        pl.BlockSpec((8, SPAN), lambda k: (chunks, 0)),
    ]


def run_forward(both_ext, shared_ext, step_raw, seg, taps, taps_s, heads):
    width = taps.shape[1]
    scols = taps_s.shape[1]
    chunks = seg.shape[0] // 8 - 1
    length = chunks * SPAN
    nrow = 16
    row = lambda k: (k, 0)
    halo = lambda col: (lambda k: (halo_index(k, chunks), col))
    fixed = lambda k: (0, 0)
    S = jax.ShapeDtypeStruct
    return pl.pallas_call(
        forward_kernel,
        grid=(chunks,),
        in_specs=[
            pl.BlockSpec((SPAN, width), lambda k: (k, 1)),
            pl.BlockSpec((HALO, width), halo(1)),
            pl.BlockSpec((SPAN, scols), row),
            pl.BlockSpec((HALO, scols), halo(0)),
            pl.BlockSpec((SPAN, 128), row),
            *seg_specs(lambda k: k, chunks),
            pl.BlockSpec(taps.shape, fixed),
            pl.BlockSpec(taps_s.shape, fixed),
            pl.BlockSpec(heads.shape, fixed),
        ],
        out_specs=[
            pl.BlockSpec((SPAN, width), row),
            pl.BlockSpec((SPAN, width), row),
            pl.BlockSpec((SPAN, scols), row),
            pl.BlockSpec((SPAN, 128), row),
            pl.BlockSpec((SPAN, 128), row),
            pl.BlockSpec((nrow, SPAN), lambda k: (0, k)),
            pl.BlockSpec((SPAN, 128), row),
            pl.BlockSpec((None, scols // 2, width), lambda k: (k, 0, 0)),
            pl.BlockSpec((scols // 2, width), fixed),
        ],
        out_shape=[
            S((length, width), F32),
            S((length, width), BF16),
            S((length, scols), BF16),
            S((length, 128), F32),
            S((length, 128), F32),
            S((nrow, length), F32),
            S((length, 128), F32),
            S((chunks, scols // 2, width), BF16),
            S((scols // 2, width), F32),
        ],
        scratch_shapes=[pltpu.VMEM((scols // 2, width), F32), pltpu.VMEM((8, 128), F32)],
        name="scan_forward",
    )(both_ext, both_ext, shared_ext, shared_ext, step_raw, seg, seg, seg, taps, taps_s, heads)


def row_sums(value):
    hi = value.astype(BF16)
    lo = (value - hi.astype(F32)).astype(BF16)
    ones = jnp.ones((8, value.shape[1]), BF16)
    return nt(ones, hi) + nt(ones, lo)


def first_rows(value):
    return jnp.where(iota(value.shape, 0) == 0, value, 0.0)


def gate_kernel(y, x, bc, dec, start, gate, taps, ssd_out, gated_out, sums_out):
    length, width = x.shape
    state_dim = start.shape[0]
    cc = bc[:, state_dim:]
    lo = iota((length, 128), 1) < 64
    squares = jnp.zeros((length, 128), F32)
    for p in range(width // 128):
        sl = slice(p * 128, (p + 1) * 128)
        corr = nn(cc, start[:, sl].astype(BF16)) * pick(lo, dec, 2 * p)
        ssd = y[:, sl] + corr + taps[6:7, sl] * x[:, sl].astype(F32)
        ssd_out[:, sl] = ssd
        g = gate[:, sl].astype(F32)
        gated = ssd * (g * sigmoid(g))
        gated_out[:, sl] = gated.astype(BF16)
        squares = squares + gated * gated
    sums_out[...] = row_sums(squares)


def run_gate(y, x, bc, dec, start, both_ext, taps):
    length, width = x.shape
    row = lambda k: (k, 0)
    fixed = lambda k: (0, 0)
    S = jax.ShapeDtypeStruct
    return pl.pallas_call(
        gate_kernel,
        grid=(length // SPAN,),
        in_specs=[
            pl.BlockSpec((SPAN, width), row),
            pl.BlockSpec((SPAN, width), row),
            pl.BlockSpec((SPAN, bc.shape[1]), row),
            pl.BlockSpec((SPAN, 128), row),
            pl.BlockSpec(start.shape, fixed),
            pl.BlockSpec((SPAN, width), row),
            pl.BlockSpec(taps.shape, fixed),
        ],
        out_specs=[
            pl.BlockSpec((SPAN, width), row),
            pl.BlockSpec((SPAN, width), row),
            pl.BlockSpec((8, SPAN), lambda k: (0, k)),
        ],
        out_shape=[S((length, width), F32), S((length, width), BF16), S((8, length), F32)],
        name="gate_sums",
    )(y, x, bc, dec, start, both_ext, taps)


def project_kernel(full_width, gated, sums, taps, out_t, normed_out, proj_out):
    rescale = columns(lax.rsqrt(sums[0:1] / full_width + EPS))
    for p in range(gated.shape[1] // 128):
        sl = slice(p * 128, (p + 1) * 128)
        normed_out[:, sl] = (gated[:, sl].astype(F32) * rescale * taps[5:6, sl]).astype(BF16)
    proj_out[...] = nt(normed_out[...], out_t[...]).astype(BF16)


def run_project(full_width, gated, sums, taps, out_t):
    length, width = gated.shape
    row = lambda k: (k, 0)
    fixed = lambda k: (0, 0)
    S = jax.ShapeDtypeStruct
    return pl.pallas_call(
        functools.partial(project_kernel, full_width),
        grid=(length // SPAN,),
        in_specs=[
            pl.BlockSpec((SPAN, width), row),
            pl.BlockSpec((8, SPAN), lambda k: (0, k)),
            pl.BlockSpec(taps.shape, fixed),
            pl.BlockSpec(out_t.shape, fixed),
        ],
        out_specs=[pl.BlockSpec((SPAN, width), row), pl.BlockSpec((SPAN, out_t.shape[0]), row)],
        out_shape=[S((length, width), BF16), S((length, out_t.shape[0]), BF16)],
        name="project",
    )(gated, sums, taps, out_t)


def pull_kernel(cot, out_t, gated, taps, back_out, sums_out):
    back = nn(cot[...], out_t[...])
    back_out[...] = back.astype(BF16)
    inner = jnp.zeros((cot.shape[0], 128), F32)
    for p in range(back.shape[1] // 128):
        sl = slice(p * 128, (p + 1) * 128)
        inner = inner + back[:, sl] * taps[5:6, sl] * gated[:, sl].astype(F32)
    sums_out[...] = row_sums(inner)


def run_pull(cot, out_t, gated, taps):
    length, width = gated.shape
    row = lambda k: (k, 0)
    fixed = lambda k: (0, 0)
    S = jax.ShapeDtypeStruct
    return pl.pallas_call(
        pull_kernel,
        grid=(length // SPAN,),
        in_specs=[
            pl.BlockSpec((SPAN, cot.shape[1]), row),
            pl.BlockSpec(out_t.shape, fixed),
            pl.BlockSpec((SPAN, width), row),
            pl.BlockSpec(taps.shape, fixed),
        ],
        out_specs=[pl.BlockSpec((SPAN, width), row), pl.BlockSpec((8, SPAN), lambda k: (0, k))],
        out_shape=[S((length, width), BF16), S((8, length), F32)],
        name="pull_back",
    )(cot, out_t, gated, taps)


def back_kernel(
    full_width, ssd, x, bc, dec, gate, back, squares, inner, taps,
    dy_out, ggate_out, row_out, colsum_out, dstart_out,
):
    length, width = x.shape
    state_dim = dstart_out.shape[0]

    @pl.when(pl.program_id(0) == 0)
    def _():
        colsum_out[...] = jnp.zeros_like(colsum_out)
        dstart_out[...] = jnp.zeros_like(dstart_out)

    cc = bc[:, state_dim:]
    lo = iota((length, 128), 1) < 64
    rescale = columns(lax.rsqrt(squares[0:1] / full_width + EPS))
    pull = columns(inner[0:1]) * (rescale * rescale * rescale / full_width)
    rowterm = jnp.zeros((length, 128), F32)
    for p in range(width // 128):
        sl = slice(p * 128, (p + 1) * 128)
        s_ssd = ssd[:, sl]
        xp = x[:, sl].astype(F32)
        g = gate[:, sl].astype(F32)
        s = sigmoid(g)
        gated = s_ssd * (g * s)
        bk = back[:, sl].astype(F32)
        gain = taps[5:6, sl]
        gg = rescale * (bk * gain) - gated * pull
        dy = gg * (g * s)
        dyb = dy.astype(BF16)
        dy_out[:, sl] = dyb
        ggate_out[:, sl] = (gg * s_ssd * s * (1.0 + g * (1.0 - s))).astype(BF16)
        colsum_out[5:6, sl] += jnp.sum(bk * gated * rescale, axis=0, keepdims=True)
        colsum_out[6:7, sl] += jnp.sum(dy * xp, axis=0, keepdims=True)
        dstart_out[:, sl] += tn(cc, (dy * pick(lo, dec, 2 * p)).astype(BF16))
        rowterm = rowterm + split_dot(dyb.astype(F32) * (s_ssd - taps[6:7, sl] * xp), head_map(p))
    row_out[...] = rowterm


def head_map(p):
    lane, head = iota((128, 128), 0), iota((128, 128), 1)
    return (head == 2 * p + lane // 64).astype(BF16)


def run_back(full_width, ssd, x, bc, dec, both_ext, back, squares, inner, taps):
    length, width = x.shape
    row = lambda k: (k, 0)
    fixed = lambda k: (0, 0)
    S = jax.ShapeDtypeStruct
    return pl.pallas_call(
        functools.partial(back_kernel, full_width),
        grid=(length // SPAN,),
        in_specs=[
            pl.BlockSpec((SPAN, width), row),
            pl.BlockSpec((SPAN, width), row),
            pl.BlockSpec((SPAN, bc.shape[1]), row),
            pl.BlockSpec((SPAN, 128), row),
            pl.BlockSpec((SPAN, width), row),
            pl.BlockSpec((SPAN, width), row),
            pl.BlockSpec((8, SPAN), lambda k: (0, k)),
            pl.BlockSpec((8, SPAN), lambda k: (0, k)),
            pl.BlockSpec(taps.shape, fixed),
        ],
        out_specs=[
            pl.BlockSpec((SPAN, width), row),
            pl.BlockSpec((SPAN, width), row),
            pl.BlockSpec((SPAN, 128), row),
            pl.BlockSpec((8, width), fixed),
            pl.BlockSpec((bc.shape[1] // 2, width), fixed),
        ],
        out_shape=[
            S((length, width), BF16),
            S((length, width), BF16),
            S((length, 128), F32),
            S((8, width), F32),
            S((bc.shape[1] // 2, width), F32),
        ],
        name="gated_back",
    )(ssd, x, bc, dec, both_ext, back, squares, inner, taps)


def conv_back(dout, pre, shifts, links, taps, sl, carry, carry_links, par_out):
    length = dout.shape[0]
    s = sigmoid(pre)
    dconv = dout * (s * (1.0 + pre * (1.0 - s)))
    nxt = carry[:, sl]
    grad = taps[3:4, sl] * dconv
    above = jnp.zeros((8, dout.shape[1]), F32)
    par_out[3:4, sl] += jnp.sum(dconv * shifts[0], axis=0, keepdims=True)
    par_out[4:5, sl] += jnp.sum(dconv, axis=0, keepdims=True)
    for j in range(1, 4):
        z = dconv * links[j - 1]
        w = taps[3 - j : 4 - j, sl]
        low = jnp.concatenate([z, nxt * carry_links[:, j - 1 : j]], axis=0)
        grad = grad + w * low[j : j + length]
        high = jnp.concatenate([above * 0.0, z[0:8]], axis=0)
        above = above + w * high[j : j + 8]
        par_out[3 - j : 4 - j, sl] += jnp.sum(dconv * shifts[j], axis=0, keepdims=True)
    carry[:, sl] = dconv[0:8]
    return grad, above


def backward_kernel(
    inner, inner_halo, shared, shared_halo, step_raw, seg_row, seg_prev, seg_tail, taps, taps_s, heads,
    dy, x, bc, dt_in, c_in, ct_in, dec_halo, enter, start, row_in, dend, colsum,
    ginner_out, gshared_out, gstep_out, par_out, par_s_out, par_h_out, edge_out, edge_s_out, last_out, last_s_out,
    dstate, carry, carry_s, carry_links, grads_bc,
):
    i = pl.program_id(0)
    k = pl.num_programs(0) - 1 - i
    length, width = x.shape
    state_dim = dstate.shape[0]

    @pl.when(i == 0)
    def _():
        dstate[...] = dend[...]
        carry[...] = jnp.zeros_like(carry)
        carry_s[...] = jnp.zeros_like(carry_s)
        carry_links[...] = jnp.zeros_like(carry_links)
        par_out[...] = colsum[...]
        par_s_out[...] = jnp.zeros_like(par_s_out)
        par_h_out[...] = jnp.zeros_like(par_h_out)

    segr, seg, seg_halo, tail_seg = segments(seg_row, seg_prev, seg_tail)
    links = chunk_links(seg, seg_halo)
    closing = (seg == seg[length - 1 :]).astype(F32)
    entering = (seg == seg_halo[7:]).astype(F32)
    kept = (seg[length - 1 :] == seg_halo[7:]).astype(F32)
    next_links = carry_links[...]
    dt = dt_in[...]
    c = c_in[...]
    ct = ct_in[...]
    first = (k == 0).astype(F32)
    reach = dec_halo[7:8] * (1.0 - first) + first
    b = bc[:, :state_dim]
    cc = bc[:, state_dim:]
    rows, cols = iota((length, length), 0), iota((length, length), 1)
    allowed = (rows <= cols) & (seg == segr)
    scores = jnp.where(allowed, nt(b, cc), 0.0)
    lo = iota((length, 128), 1) < 64
    lo1 = lo[0:1]
    dscores = jnp.zeros((length, length), F32)
    db = jnp.zeros((length, state_dim), F32)
    dc_mat = jnp.zeros((length, state_dim), F32)
    direct = jnp.zeros((length, 128), F32)
    matched = jnp.zeros((length, 128), F32)
    closing_term = jnp.zeros((1, 128), F32)
    for p in range(width // 128):
        sl = slice(p * 128, (p + 1) * 128)
        pre, shifts = conv_tile(inner, inner_halo, links, taps, sl)
        dyb = dy[:, sl]
        dyf = dyb.astype(F32)
        xp = x[:, sl].astype(F32)
        dtb = pick(lo, dt, 2 * p)
        xdt = xp * dtb
        cb = pick(lo, c, 2 * p)
        hm = head_map(p)
        last = cb[length - 1 :]
        entry = enter[:, sl].astype(F32) + start[:, sl] * pick(lo1, reach, 2 * p)
        entryb = entry.astype(BF16)
        ds = dstate[:, sl]
        dsb = ds.astype(BF16)
        leaving = jnp.exp(last - cb) * closing
        bds = nn(b, dsb)
        dxdt = jnp.zeros((length, 128), F32)
        for a in range(2):
            h = 2 * p + a
            mine = lo if a == 0 else ~lo
            decay = jnp.exp(jnp.minimum(ct[h : h + 1] - c[:, h : h + 1], 0.0))
            dscores = dscores + decay * nt(jnp.where(mine, xdt, 0.0).astype(BF16), dyb)
            dxdt = dxdt + nn((decay * scores).astype(BF16), jnp.where(mine, dyf, 0.0).astype(BF16))
        spread = leaving * xdt
        moved = spread * bds
        matched = matched + split_dot(xdt.astype(BF16).astype(F32) * dxdt + moved, hm)
        dxdt = dxdt + leaving * bds
        held = jnp.exp(last) * kept
        col = jnp.sum(moved, axis=0, keepdims=True) + held * jnp.sum(entry * ds, axis=0, keepdims=True)
        closing_term = closing_term + split_dot(jnp.broadcast_to(col, (8, 128)), hm)[0:1]
        direct = direct + split_dot(xp * dxdt, hm)
        edy = (jnp.exp(cb) * entering * dyf).astype(BF16)
        db = db + nt(spread.astype(BF16), dsb)
        dc_mat = dc_mat + nt(edy, entryb)
        dstate[:, sl] = ds * held + tn(cc, edy)
        dx = dtb * dxdt + taps[6:7, sl] * dyf
        grad, above = conv_back(dx, pre, shifts, links, taps, sl, carry, next_links, par_out)
        ginner_out[:, sl] = grad.astype(BF16)
        edge_out[:, sl] = above

        @pl.when(i == 0)
        def _():
            last_out[:, sl] = grad[length - 8 :]

    dsc = jnp.where(allowed, dscores, 0.0).astype(BF16)
    grads_bc[:, :state_dim] = db + nn(dsc, cc)
    grads_bc[:, state_dim:] = dc_mat + tn(dsc, b)
    for half in range(2):
        sl = slice(half * state_dim, (half + 1) * state_dim)
        pre, shifts = conv_tile(shared, shared_halo, links, taps_s, sl)
        grad, above = conv_back(grads_bc[:, sl], pre, shifts, links, taps_s, sl, carry_s, next_links, par_s_out)
        gshared_out[:, sl] = grad.astype(BF16)
        edge_s_out[:, sl] = above

        @pl.when(i == 0)
        def _():
            last_s_out[:, sl] = grad[length - 8 :]

    for j in range(3):
        carry_links[:, j : j + 1] = links[j][0:8]
    dcum = row_in[...] - matched
    upper = (rows <= cols).astype(F32)
    dlog = jnp.dot(upper, dcum, precision=HIGH, preferred_element_type=F32) + closing_term
    rate = -jnp.exp(heads[1:2])
    dstep = (direct + dlog * rate) * sigmoid(step_raw[...] + heads[0:1])
    gstep_out[...] = dstep.astype(BF16)
    par_h_out[0:1] += jnp.sum(dstep, axis=0, keepdims=True)
    par_h_out[1:2] += jnp.sum(dlog * (rate * dt), axis=0, keepdims=True)


def run_backward(
    both_ext, shared_ext, step_raw, seg, taps, taps_s, heads,
    dy, x, bc, dt, c, ct, dec, enter, start, rowterm, dend, colsum,
):
    length, width = x.shape
    scols = bc.shape[1]
    chunks = length // SPAN
    at = lambda i: chunks - 1 - i
    row = lambda i: (at(i), 0)
    halo = lambda col: (lambda i: (halo_index(at(i), chunks), col))
    fixed = lambda i: (0, 0)
    S = jax.ShapeDtypeStruct
    return pl.pallas_call(
        backward_kernel,
        grid=(chunks,),
        in_specs=[
            pl.BlockSpec((SPAN, width), lambda i: (at(i), 1)),
            pl.BlockSpec((HALO, width), halo(1)),
            pl.BlockSpec((SPAN, scols), row),
            pl.BlockSpec((HALO, scols), halo(0)),
            pl.BlockSpec((SPAN, 128), row),
            *seg_specs(at, chunks),
            pl.BlockSpec(taps.shape, fixed),
            pl.BlockSpec(taps_s.shape, fixed),
            pl.BlockSpec(heads.shape, fixed),
            pl.BlockSpec((SPAN, width), row),
            pl.BlockSpec((SPAN, width), row),
            pl.BlockSpec((SPAN, scols), row),
            pl.BlockSpec((SPAN, 128), row),
            pl.BlockSpec((SPAN, 128), row),
            pl.BlockSpec((ct.shape[0], SPAN), lambda i: (0, at(i))),
            pl.BlockSpec((8, 128), lambda i: (jnp.maximum(at(i) * (SPAN // 8) - 1, 0), 0)),
            pl.BlockSpec((None, scols // 2, width), lambda i: (at(i), 0, 0)),
            pl.BlockSpec(start.shape, fixed),
            pl.BlockSpec((SPAN, 128), row),
            pl.BlockSpec(dend.shape, fixed),
            pl.BlockSpec(colsum.shape, fixed),
        ],
        out_specs=[
            pl.BlockSpec((SPAN, width), row),
            pl.BlockSpec((SPAN, scols), row),
            pl.BlockSpec((SPAN, 128), row),
            pl.BlockSpec((8, width), fixed),
            pl.BlockSpec((8, scols), fixed),
            pl.BlockSpec((8, 128), fixed),
            pl.BlockSpec((8, width), fixed),
            pl.BlockSpec((8, scols), fixed),
            pl.BlockSpec((8, width), fixed),
            pl.BlockSpec((8, scols), fixed),
        ],
        out_shape=[
            S((length, width), BF16),
            S((length, scols), BF16),
            S((length, 128), BF16),
            S((8, width), F32),
            S((8, scols), F32),
            S((8, 128), F32),
            S((8, width), F32),
            S((8, scols), F32),
            S((8, width), F32),
            S((8, scols), F32),
        ],
        scratch_shapes=[
            pltpu.VMEM((scols // 2, width), F32),
            pltpu.VMEM((8, width), F32),
            pltpu.VMEM((8, scols), F32),
            pltpu.VMEM((8, 128), F32),
            pltpu.VMEM((SPAN, scols), F32),
        ],
        name="scan_backward",
    )(both_ext, both_ext, shared_ext, shared_ext, step_raw, seg, seg, seg, taps, taps_s, heads,
      dy, x, bc, dt, c, ct, dec, enter, start, rowterm, dend, colsum)


def spread_kernel(ggate, ginner, gsmall, w_in, w_small, normed, part_out, gain_out):
    width = ggate.shape[1]
    part = nt(ggate[...], w_in[:, :width]) + nt(ginner[...], w_in[:, width:]) + nt(gsmall[...], w_small[...])
    part_out[...] = part.astype(BF16)
    gain_out[...] = first_rows(jnp.broadcast_to(
        jnp.sum(part * normed[...].astype(F32), axis=0, keepdims=True), gain_out.shape))


def run_spread(ggate, ginner, gsmall, w_in, w_small, normed_ext):
    length = ggate.shape[0]
    model = w_in.shape[0]
    tile = 256
    fixed = lambda n: (0, 0)
    down = lambda n: (n, 0)
    across = lambda n: (0, n)
    S = jax.ShapeDtypeStruct
    return pl.pallas_call(
        spread_kernel,
        grid=(model // tile,),
        in_specs=[
            pl.BlockSpec(ggate.shape, fixed),
            pl.BlockSpec(ginner.shape, fixed),
            pl.BlockSpec(gsmall.shape, fixed),
            pl.BlockSpec((tile, w_in.shape[1]), down),
            pl.BlockSpec((tile, w_small.shape[1]), down),
            pl.BlockSpec((length, tile), across),
        ],
        out_specs=[pl.BlockSpec((length, tile), across), pl.BlockSpec((8, tile), across)],
        out_shape=[S((length, model), BF16), S((8, model), F32)],
        name="spread_back",
    )(ggate, ginner, gsmall, w_in, w_small, normed_ext)


MESH = pl.DeviceIdType.MESH
ANY = pl.BlockSpec(memory_space=pl.ANY)


def remote(src, dst, send, recv, **to):
    return pltpu.make_async_remote_copy(
        src_ref=src, dst_ref=dst, send_sem=send, recv_sem=recv, device_id=to, device_id_type=MESH
    )


def greet(barrier, when, **to):
    @pl.when(when)
    def _():
        pl.semaphore_signal(barrier, inc=1, device_id=to, device_id_type=MESH)


def gather_kernel(
    ncol, ndp,
    own, seg_own, w0, w1, w2, zero_tail, no_seg,
    all_out, seg_out, w0_out, w1_out, w2_out,
    z_send, z_recv, w_send, c_send, w_recv, t_send, t_recv, here,
):
    dp, row, z = lax.axis_index("dp"), lax.axis_index("row"), lax.axis_index("col")
    other = 1 - row
    last = ncol - 1
    tokens, tail = own.shape[0], zero_tail.shape[0]
    weights = ((w0, w0_out), (w1, w1_out), (w2, w2_out))
    rows = w0.shape[0]
    sends_tail = (row == 0) & (z == last)

    barrier = pltpu.get_barrier_semaphore()
    greet(barrier, z > 0, col=z - 1)
    greet(barrier, z < last, col=z + 1)
    greet(barrier, row >= 0, row=other)
    for m in range(1, ndp):
        greet(barrier, row >= 0, dp=dp ^ m)
    greet(barrier, row == 1, row=0, col=last)
    for c in range(ncol):
        greet(barrier, sends_tail, row=1, col=c)
    count = (z > 0).astype(jnp.int32) + (z < last).astype(jnp.int32) + ndp
    count = count + row + jnp.where(sends_tail, ncol, 0)
    pl.semaphore_wait(barrier, count)

    def token_refs(s, mine):
        if mine:
            srcs = (own, seg_own)
        else:
            srcs = (all_out.at[pl.ds(s * tokens, tokens)], seg_out.at[pl.ds(s * 8, 8)])
        return tuple(zip(srcs, (all_out.at[pl.ds(s * tokens, tokens)], seg_out.at[pl.ds(s * 8, 8)])))

    def token_copies(s, mine, way):
        target = z + 1 if way == 0 else z - 1
        return [
            remote(src, dst, z_send.at[way, s, i], z_recv.at[s, i], col=target)
            for i, (src, dst) in enumerate(token_refs(s, mine))
        ]

    def weight_copies(j, mine, send, **to):
        copies = []
        for i, (src, dst) in enumerate(weights):
            place = dst.at[pl.ds(j * rows, rows)]
            copies.append(remote(src if mine else place, place, send.at[i], w_recv.at[j, i], **to))
        return copies

    def tail_copies(c):
        return [
            remote(own.at[pl.ds(tokens - tail, tail)], all_out.at[pl.ds(ncol * tokens, tail)],
                   t_send.at[c, 0], t_recv.at[0], row=1, col=c),
            remote(seg_own, seg_out.at[pl.ds(ncol * 8, 8)], t_send.at[c, 1], t_recv.at[1], row=1, col=c),
        ]

    def start(copies):
        for copy in copies:
            copy.start()

    def guarded(when, action):
        @pl.when(when)
        def _():
            action()

    me = dp * 2 + row
    guarded(z < last, lambda: start(token_copies(z, True, 0)))
    guarded(z > 0, lambda: start(token_copies(z, True, 1)))
    for m in range(1, ndp):
        start(weight_copies(me, True, w_send.at[m], dp=dp ^ m))
    start(weight_copies(me, True, c_send.at[0], row=other))
    for c in range(ncol):
        guarded(sends_tail, lambda c=c: start(tail_copies(c)))
    local = [
        pltpu.make_async_copy(own, all_out.at[pl.ds(z * tokens, tokens)], here.at[0]),
        pltpu.make_async_copy(seg_own, seg_out.at[pl.ds(z * 8, 8)], here.at[1]),
    ]
    for i, (src, dst) in enumerate(weights):
        local.append(pltpu.make_async_copy(src, dst.at[pl.ds(me * rows, rows)], here.at[2 + i]))
    start(local)
    fill = [
        pltpu.make_async_copy(zero_tail, all_out.at[pl.ds(ncol * tokens, tail)], here.at[5]),
        pltpu.make_async_copy(no_seg, seg_out.at[pl.ds(ncol * 8, 8)], here.at[6]),
    ]
    guarded(row == 0, lambda: start(fill))

    def pass_tokens(s):
        def from_below():
            for copy in token_copies(z - s, False, 0):
                copy.wait_recv()
            guarded(z < last, lambda: start(token_copies(z - s, False, 0)))

        def from_above():
            for copy in token_copies(z + s, False, 1):
                copy.wait_recv()
            guarded(z > 0, lambda: start(token_copies(z + s, False, 1)))

        guarded(z - s >= 0, from_below)
        guarded(z + s <= last, from_above)

    def pass_weights(m):
        j = (dp ^ m) * 2 + row
        for copy in weight_copies(j, False, w_send.at[m], dp=dp ^ m):
            copy.wait_recv()
        start(weight_copies(j, False, c_send.at[m], row=other))

    done = 0
    for s in range(1, ncol):
        pass_tokens(s)
        upto = (ndp - 1) * s // (ncol - 2) if s < ncol - 1 else ndp - 1
        for m in range(done + 1, upto + 1):
            pass_weights(m)
        done = max(done, upto)
    for m in range(ndp):
        j = (dp ^ m) * 2 + other
        for copy in weight_copies(j, False, c_send.at[m], row=other):
            copy.wait_recv()
    guarded(row == 1, lambda: [copy.wait_recv() for copy in tail_copies(0)])
    for m in range(ndp):
        if m:
            for copy in weight_copies(me, True, w_send.at[m], dp=dp ^ m):
                copy.wait_send()
        for copy in weight_copies((dp ^ m) * 2 + row, m == 0, c_send.at[m], row=other):
            copy.wait_send()
    for s in range(ncol):
        for way in range(2):
            open_way = z < last if way == 0 else z > 0
            mine = (z - s >= 0) if way == 0 else (z + s <= last)
            src = z - s if way == 0 else z + s

            def drain(way=way, src=src, s=s):
                for copy in token_copies(src, s == 0, way):
                    copy.wait_send()

            guarded(open_way & mine, drain)
    for c in range(ncol):
        guarded(sends_tail, lambda c=c: [copy.wait_send() for copy in tail_copies(c)])
    for copy in local:
        copy.wait()
    guarded(row == 0, lambda: [copy.wait() for copy in fill])


def gather_inputs(own, seg_own, w0, w1, w2):
    ncol, ndp = lax.axis_size("col"), lax.axis_size("dp")
    tokens, width = own.shape
    S = jax.ShapeDtypeStruct
    shards = 2 * ndp
    zero_tail = jnp.zeros((HALO, width), own.dtype)
    no_seg = jnp.full((8, tokens), -1, jnp.int32)
    dma = pltpu.SemaphoreType.DMA
    sent = 2 * own.size * own.dtype.itemsize
    return pl.pallas_call(
        functools.partial(gather_kernel, ncol, ndp),
        in_specs=[ANY] * 7,
        out_specs=[ANY] * 5,
        out_shape=[
            S((ncol * tokens + HALO, width), own.dtype),
            S(((ncol + 1) * 8, tokens), jnp.int32),
        ] + [S((shards * w.shape[0], w.shape[1]), w.dtype) for w in (w0, w1, w2)],
        scratch_shapes=[
            dma((2, ncol, 2)), dma((ncol, 2)), dma((ndp, 3)), dma((ndp, 3)), dma((shards, 3)),
            dma((ncol, 2)), dma((2,)), dma((7,)),
        ],
        compiler_params=pltpu.CompilerParams(collective_id=1, has_side_effects=True),
        cost_estimate=pl.CostEstimate(flops=0, bytes_accessed=200_000_000, transcendentals=0),
        name="gather_inputs",
    )(own, seg_own, w0, w1, w2, zero_tail, no_seg)


def sum_col_kernel(ncol, value, out, slots, send, recv):
    z = lax.axis_index("col")
    barrier = pltpu.get_barrier_semaphore()
    for s in range(1, ncol):
        pl.semaphore_signal(barrier, inc=1, device_id={"col": lax.rem(z + s, ncol)}, device_id_type=MESH)
    pl.semaphore_wait(barrier, ncol - 1)
    copies = [
        remote(value, slots.at[z], send.at[s], recv.at[z], col=lax.rem(z + s, ncol)) for s in range(1, ncol)
    ]
    for copy in copies:
        copy.start()
    total = value[...]
    for s in range(1, ncol):
        source = lax.rem(z + s, ncol)
        remote(value, slots.at[source], send.at[s], recv.at[source], col=source).wait_recv()
        total = total + slots[source]
    out[...] = total
    for copy in copies:
        copy.wait_send()


def sum_col(value, collective_id):
    ncol = lax.axis_size("col")
    dma = pltpu.SemaphoreType.DMA
    vmem = pl.BlockSpec(memory_space=pltpu.VMEM)
    return pl.pallas_call(
        functools.partial(sum_col_kernel, ncol),
        in_specs=[vmem],
        out_specs=vmem,
        out_shape=jax.ShapeDtypeStruct(value.shape, F32),
        scratch_shapes=[pltpu.VMEM((ncol,) + value.shape, F32), dma((ncol,)), dma((ncol,))],
        compiler_params=pltpu.CompilerParams(collective_id=collective_id, has_side_effects=True),
        name="sum_col",
    )(value)


def reduce_kernel(ncol, ndp, *refs):
    g, vecs = refs[0:3], refs[3:7]
    r, vec_outs = refs[7:10], refs[10:14]
    own, near, sent, far = refs[14:17], refs[17:20], refs[20:23], refs[23:26]
    vec_slots, col_slots, bc_slots = refs[26:30], refs[30:32], refs[32]
    c_send, c_recv, p_send, p_recv, here, v_send, v_recv, u_send, u_recv, b_send, b_recv = refs[33:]
    dp, row, z = lax.axis_index("dp"), lax.axis_index("row"), lax.axis_index("col")
    other = 1 - row
    me = dp * 2 + row
    rows = [out.shape[0] for out in r]
    barrier = pltpu.get_barrier_semaphore()
    for q in range(1, 2 * ndp):
        greet(barrier, row >= 0, dp=dp ^ (q >> 1), row=row ^ (q & 1))
    for s in range(1, ncol):
        greet(barrier, row >= 0, col=lax.rem(z + s, ncol))
    pl.semaphore_wait(barrier, 2 * ndp + ncol - 2)

    vec_copies = []
    for q in range(1, 2 * ndp):
        for i in range(4):
            vec_copies.append(
                remote(vecs[i], vec_slots[i].at[me], v_send.at[q, i], v_recv.at[me, i],
                       dp=dp ^ (q >> 1), row=row ^ (q & 1))
            )
    for copy in vec_copies:
        copy.start()

    order = (1, 2, 0)

    def core_copy(i, d):
        return remote(g[i].at[pl.ds((d * 2 + other) * rows[i], rows[i])], near[i].at[d],
                      c_send.at[i, d], c_recv.at[i, d], row=other)

    def own_copy(i, d):
        return pltpu.make_async_copy(g[i].at[pl.ds((d * 2 + row) * rows[i], rows[i])], own[i].at[d], here.at[i, d])

    def peer_copy(i, m):
        return remote(sent[i].at[m], far[i].at[m], p_send.at[i, m], p_recv.at[i, m], dp=dp ^ m)

    turns = list(range(1, ndp)) + [0]
    for i in order:
        for m in turns:
            core_copy(i, dp ^ m).start()
            own_copy(i, dp ^ m).start()
    waiting = []
    for i in order:
        for m in turns:
            d = dp ^ m
            core_copy(i, d).wait_recv()
            own_copy(i, d).wait()
            if m == 0:
                continue

            def add(step, carry, i=i, d=d, m=m):
                at = pl.ds(pl.multiple_of(step * 16, 16), 16)
                total = own[i][d, at].astype(F32) + near[i][d, at].astype(F32)
                sent[i][m, at] = total.astype(BF16)
                return carry

            lax.fori_loop(0, rows[i] // 16, add, 0)
            if waiting:
                waiting.pop().start()
            waiting.append(peer_copy(i, m))

    def gather_vec():
        for q in range(1, 2 * ndp):
            j = me ^ q
            for i in range(4):
                remote(vecs[i], vec_slots[i].at[j], v_send.at[q, i], v_recv.at[j, i],
                       dp=dp ^ (q >> 1), row=row ^ (q & 1)).wait_recv()
        for i in range(4):
            vec_slots[i][me] = vecs[i][...]
            total = vec_slots[i][0]
            for j in range(1, 2 * ndp):
                total = total + vec_slots[i][j]
            if i < 2:
                vec_outs[i][...] = total
            else:
                col_slots[i - 2][z] = total

    gather_vec()
    waiting.pop().start()

    def finish(i):
        for m in range(1, ndp):
            peer_copy(i, m).wait_recv()

        def add(step, carry):
            at = pl.ds(pl.multiple_of(step * 16, 16), 16)
            total = own[i][dp, at].astype(F32) + near[i][dp, at].astype(F32)
            for m in range(1, ndp):
                total = total + far[i][m, at].astype(F32)
            r[i][at] = total
            if i == 1:
                bc_slots[z, at] = total[:, : bc_slots.shape[2]].astype(BF16)
            return carry

        lax.fori_loop(0, rows[i] // 16, add, 0)

    def col_copies(s, source):
        to = lax.rem(z + s, ncol)
        copies = [remote(col_slots[i].at[source], col_slots[i].at[source], u_send.at[s, i], u_recv.at[source, i], col=to)
                  for i in range(2)]
        return copies + [remote(bc_slots.at[source], bc_slots.at[source], b_send.at[s], b_recv.at[source], col=to)]

    finish(1)
    finish(2)
    for s in range(1, ncol):
        for copy in col_copies(s, z):
            copy.start()
    finish(0)
    for s in range(1, ncol):
        for copy in col_copies(s, lax.rem(z + s, ncol)):
            copy.wait_recv()
    for i in range(2):
        total = col_slots[i][0]
        for j in range(1, ncol):
            total = total + col_slots[i][j]
        vec_outs[2 + i][...] = total
    total = bc_slots[0].astype(F32)
    for j in range(1, ncol):
        total = total + bc_slots[j].astype(F32)
    r[1][:, : bc_slots.shape[2]] = total

    for copy in vec_copies:
        copy.wait_send()
    for i in order:
        for m in turns:
            core_copy(i, dp ^ m).wait_send()
            if m:
                peer_copy(i, m).wait_send()
    for s in range(1, ncol):
        for copy in col_copies(s, z):
            copy.wait_send()


def reduce_grads(grads, vecs, scols):
    ncol, ndp = lax.axis_size("col"), lax.axis_size("dp")
    dma = pltpu.SemaphoreType.DMA
    vmem = pl.BlockSpec(memory_space=pltpu.VMEM)
    S = jax.ShapeDtypeStruct
    blocks = [(g.shape[0] // (2 * ndp), g.shape[1]) for g in grads]
    stack = [pltpu.VMEM((ndp,) + b, BF16) for b in blocks]
    return pl.pallas_call(
        functools.partial(reduce_kernel, ncol, ndp),
        in_specs=[ANY] * 3 + [vmem] * 4,
        out_specs=[vmem] * 7,
        out_shape=[S(b, F32) for b in blocks] + [S(v.shape, F32) for v in vecs],
        scratch_shapes=stack * 4
        + [pltpu.VMEM((2 * ndp,) + v.shape, F32) for v in vecs]
        + [pltpu.VMEM((ncol,) + v.shape, F32) for v in vecs[2:]]
        + [pltpu.VMEM((ncol, blocks[1][0], scols), BF16)]
        + [dma((3, ndp))] * 5
        + [dma((2 * ndp, 4))] * 2
        + [dma((ncol, 2))] * 2
        + [dma((ncol,))] * 2,
        compiler_params=pltpu.CompilerParams(collective_id=2, has_side_effects=True),
        cost_estimate=pl.CostEstimate(flops=0, bytes_accessed=200_000_000, transcendentals=0),
        name="reduce_grads",
    )(*grads, *vecs)


def pass_on(value, axis, by):
    count = lax.axis_size(axis)
    pairs = [(i, i + by) for i in range(count) if 0 <= i + by < count]
    return lax.ppermute(value, axis, pairs)


def pack_rows(rows, width):
    used = sum(r.shape[0] for r in rows)
    return jnp.concatenate(rows + [jnp.zeros((8 - used, width), F32)], axis=0)


def normalized(tokens, gain):
    wide = tokens.astype(F32)
    scale = lax.rsqrt(jnp.mean(wide * wide, axis=1, keepdims=True) + EPS)
    return wide, scale, (wide * scale * gain[None, :]).astype(BF16)


def per_device(
    block_input, segment_ids, norm_gain, proj_zx, proj_bc, proj_dt, conv_inner, conv_inner_bias,
    conv_shared, conv_shared_bias, step_bias, rate_log, skip_gain, gated_gain, proj_out, cotangent,
):
    width = proj_zx.shape[2]
    scols = proj_bc.shape[1]
    nheads = proj_dt.shape[1]
    head_dim = width // nheads
    full_width = float(width * lax.axis_size("col"))
    small_own = jnp.concatenate(
        [proj_bc, proj_dt, jnp.zeros((proj_dt.shape[0], 128 - nheads), BF16)], axis=1
    )
    wide, scale, normed_own = normalized(block_input, norm_gain)
    seg_own = jnp.broadcast_to(segment_ids[None], (8, segment_ids.shape[0]))
    taps = pack_rows(
        [conv_inner, conv_inner_bias[None], gated_gain[None], jnp.repeat(skip_gain, head_dim)[None]], width
    )
    taps_s = pack_rows([conv_shared, conv_shared_bias[None]], scols)
    fill = (0, 128 - nheads)
    heads = pack_rows([jnp.pad(step_bias, fill)[None], jnp.pad(rate_log, fill)[None]], 128)

    normed_ext, seg, w_in, w_small, out_t = gather_inputs(
        normed_own, seg_own, proj_zx.reshape(-1, 2 * width), small_own, proj_out.T
    )
    length = normed_ext.shape[0] - HALO
    cot, normed_ext = lax.optimization_barrier((cotangent, normed_ext))
    cot_all = lax.all_gather(cot, "col", axis=0, tiled=True)

    both_ext = nn(normed_ext, w_in).astype(BF16)
    small_ext = nn(normed_ext, w_small)
    shared_ext = small_ext[:, :scols].astype(BF16)
    step_ext = small_ext[:, scols:]
    common = (both_ext, shared_ext, step_ext, seg, taps, taps_s, heads)
    y, x, bc, dt, c, ct, dec, enter, final = run_forward(*common)
    start = pass_on(final, "row", 1)
    ssd, gated, squares = run_gate(y, x, bc, dec, start, both_ext, taps)
    squares = sum_col(squares, 3)
    gated_normed, projected = run_project(full_width, gated, squares, taps, out_t)
    projected = lax.psum_scatter(projected, "col", scatter_dimension=0, tiled=True)
    block_output = (wide + projected.astype(F32)).astype(BF16)
    back, inner = run_pull(cot_all, out_t, gated, taps)
    inner = sum_col(inner, 4)
    dy, ggate, rowterm, colsum, dstart = run_back(
        full_width, ssd, x, bc, dec, both_ext, back, squares, inner, taps
    )
    dend = pass_on(dstart, "row", -1)
    gout = tn(cot_all, gated_normed).astype(BF16)
    ginner, gshared, gstep, par, par_s, par_h, edge, edge_s, last, last_s = run_backward(
        *common, dy, x, bc, dt, c, ct, dec, enter, start, rowterm, dend, colsum
    )
    edge, edge_s = pass_on((edge, edge_s), "row", -1)
    ginner = lax.dynamic_update_slice(ginner, (last + edge).astype(BF16), (length - 8, 0))
    gshared = lax.dynamic_update_slice(gshared, (last_s + edge_s).astype(BF16), (length - 8, 0))
    gsmall = jnp.concatenate([gshared, gstep], axis=1)
    part, gain_part = run_spread(ggate, ginner, gsmall, w_in, w_small, normed_ext)
    grad_normed = lax.psum_scatter(part, "col", scatter_dimension=0, tiled=True).astype(F32)
    normed = normed_ext[:length]
    gzx = jnp.concatenate([tn(normed, ggate).astype(BF16), tn(normed, ginner).astype(BF16)], axis=1)
    gsm = tn(normed, gsmall).astype(BF16)
    gzx, gsm, gout, par, par_h, par_s, gain_sum = reduce_grads((gzx, gsm, gout), (par, par_h, par_s, gain_part), scols)
    pushed = grad_normed * norm_gain[None, :]
    grad_wide = scale * pushed - wide * scale**3 * jnp.mean(pushed * wide, axis=1, keepdims=True)
    grad_input = (cotangent.astype(F32) + grad_wide).astype(BF16)
    return (
        block_output,
        grad_input,
        gain_sum[0] / norm_gain,
        gzx.reshape(-1, 2, width),
        gsm[:, :scols],
        gsm[:, scols : scols + nheads],
        par[:4],
        par[4],
        par_s[:4],
        par_s[4],
        par_h[0, :nheads],
        par_h[1, :nheads],
        jnp.sum(par[6].reshape(nheads, head_dim), axis=1),
        par[5],
        gout.T,
    )


def solution(mesh):
    shards = ("dp", "row")
    tokens = P(("dp", "row", "col"), None)
    zx = P(shards, None, "col")
    in_specs = (
        tokens, P(("dp", "row", "col")), P(), zx, P(shards, None), P(shards, "col"), P(None, "col"), P("col"),
        P(), P(), P("col"), P("col"), P("col"), P("col"), P("col", shards), tokens,
    )
    out_specs = (
        tokens, tokens, P(), zx, P(shards, None), P(shards, "col"), P(None, "col"), P("col"),
        P(), P(), P("col"), P("col"), P("col"), P("col"), P("col", shards),
    )
    return jax.shard_map(per_device, mesh=mesh, in_specs=in_specs, out_specs=out_specs, check_vma=False)
```

```python
import functools
import jax, jax.numpy as jnp
from jax import lax
from jax.experimental import pallas as pl
from jax.experimental.pallas import tpu as pltpu
from jax.sharding import PartitionSpec as P

F32, BF16 = jnp.float32, jnp.bfloat16
HIGH = lax.Precision.HIGHEST
SPAN = 256
HALO = 16
EPS = 1e-5


def nn(a, b):
    return lax.dot_general(a, b, (((1,), (0,)), ((), ())), preferred_element_type=F32)


def nt(a, b):
    return lax.dot_general(a, b, (((1,), (1,)), ((), ())), preferred_element_type=F32)


def tn(a, b):
    return lax.dot_general(a, b, (((0,), (0,)), ((), ())), preferred_element_type=F32)


def iota(shape, axis):
    return lax.broadcasted_iota(jnp.int32, shape, axis)


def split_dot(a, b01):
    hi = a.astype(BF16)
    lo = (a - hi.astype(F32)).astype(BF16)
    return nn(hi, b01) + nn(lo, b01)


def sigmoid(v):
    return 1.0 / (1.0 + jnp.exp(-v))


def softplus(v):
    return jnp.maximum(v, 0.0) + jnp.log1p(jnp.exp(-jnp.abs(v)))


def columns(row):
    return jnp.broadcast_to(row, (128, row.shape[1])).T


def segments(seg_row, prev_row, tail_row):
    row = seg_row[0:1].astype(F32)
    seg = columns(row)[:, 0:1]
    length = row.shape[1]
    prev = columns(prev_row[0:1].astype(F32))[length - 8 :, 0:1]
    tail = tail_row[0:1, length - 1 :].astype(F32)
    return row, seg, prev, tail


def chunk_links(segc, halo):
    ext = jnp.concatenate([halo, segc], axis=0)
    length = segc.shape[0]
    return [(ext[8 - j : 8 - j + length] == segc).astype(F32) for j in range(1, 4)]


def conv_tile(cur, halo, links, taps, sl):
    v = jnp.concatenate([halo[HALO - 8 :, sl].astype(F32), cur[:, sl].astype(F32)], axis=0)
    length = cur.shape[0]
    shifted = [v[8 - j : 8 - j + length] * links[j - 1] for j in range(1, 4)]
    pre = taps[4:5, sl] + taps[3:4, sl] * v[8:]
    for j in range(1, 4):
        pre = pre + taps[3 - j : 4 - j, sl] * shifted[j - 1]
    return pre, [v[8:]] + shifted


def pick(lo, cols, h):
    return jnp.where(lo, cols[:, h : h + 1], cols[:, h + 1 : h + 2])


def forward_kernel(
    inner, inner_halo, shared, shared_halo, step_raw, seg_row, seg_prev, seg_tail, taps, taps_s, heads,
    y_out, x_out, bc_out, dt_out, c_out, ct_out, dec_out, enter_out, final_out, state, total,
):
    k = pl.program_id(0)
    length, width = inner.shape
    pairs = width // 128
    state_dim = state.shape[0]

    @pl.when(k == 0)
    def _():
        state[...] = jnp.zeros_like(state)
        total[...] = jnp.zeros_like(total)

    segr, seg, seg_halo, tail_seg = segments(seg_row, seg_prev, seg_tail)
    links = chunk_links(seg, seg_halo)
    closing = (seg == seg[length - 1 :]).astype(F32)
    entering = (seg == seg_halo[7:]).astype(F32)
    kept = (seg[length - 1 :] == seg_halo[7:]).astype(F32)
    dt = softplus(step_raw[...] + heads[0:1])
    log_decay = -jnp.exp(heads[1:2]) * dt
    rows, cols = iota((length, length), 0), iota((length, length), 1)
    lower = (rows >= cols).astype(F32)
    c = jnp.dot(lower, log_decay, precision=HIGH, preferred_element_type=F32)
    ct = c.T
    dt_out[...] = dt
    c_out[...] = c
    ct_out[...] = ct[: ct_out.shape[0]]
    whole = c + total[0:1]
    dec_out[...] = jnp.exp(whole) * (seg == tail_seg).astype(F32)
    total[0:1] = whole[length - 1 :]
    for half in range(2):
        sl = slice(half * state_dim, (half + 1) * state_dim)
        pre, _ = conv_tile(shared, shared_halo, links, taps_s, sl)
        bc_out[:, sl] = (pre * sigmoid(pre)).astype(BF16)
    b = bc_out[:, :state_dim]
    cc = bc_out[:, state_dim:]
    scores = jnp.where((rows >= cols) & (seg == segr), nt(cc, b), 0.0)
    lo = iota((length, 128), 1) < 64
    enter_out[...] = state[...].astype(BF16)
    for p in range(pairs):
        sl = slice(p * 128, (p + 1) * 128)
        pre, _ = conv_tile(inner, inner_halo, links, taps, sl)
        xp = pre * sigmoid(pre)
        xb = xp.astype(BF16)
        x_out[:, sl] = xb
        xdt = xb.astype(F32) * pick(lo, dt, 2 * p)
        cb = pick(lo, c, 2 * p)
        acc = nn(cc, state[:, sl].astype(BF16)) * (jnp.exp(cb) * entering)
        for a in range(2):
            h = 2 * p + a
            weights = jnp.exp(jnp.minimum(c[:, h : h + 1] - ct[h : h + 1], 0.0)) * scores
            mine = lo if a == 0 else ~lo
            acc = acc + nn(weights.astype(BF16), jnp.where(mine, xdt, 0.0).astype(BF16))
        y_out[:, sl] = acc
        last = cb[length - 1 :]
        leaving = jnp.exp(last - cb) * closing * xdt
        state[:, sl] = state[:, sl] * (jnp.exp(last) * kept) + tn(b, leaving.astype(BF16))

    @pl.when(k == pl.num_programs(0) - 1)
    def _():
        final_out[...] = state[...]


def halo_index(chunk, chunks):
    return jnp.where(chunk == 0, chunks * (SPAN // HALO), chunk * (SPAN // HALO) - 1)


def seg_specs(at, chunks):
    return [
        pl.BlockSpec((8, SPAN), lambda k: (at(k), 0)),
        pl.BlockSpec((8, SPAN), lambda k: (jnp.where(at(k) == 0, chunks, at(k) - 1), 0)),
        pl.BlockSpec((8, SPAN), lambda k: (chunks, 0)),
    ]


def run_forward(both_ext, shared_ext, step_raw, seg, taps, taps_s, heads):
    width = taps.shape[1]
    scols = taps_s.shape[1]
    chunks = seg.shape[0] // 8 - 1
    length = chunks * SPAN
    nrow = 16
    row = lambda k: (k, 0)
    halo = lambda col: (lambda k: (halo_index(k, chunks), col))
    fixed = lambda k: (0, 0)
    S = jax.ShapeDtypeStruct
    return pl.pallas_call(
        forward_kernel,
        grid=(chunks,),
        in_specs=[
            pl.BlockSpec((SPAN, width), lambda k: (k, 1)),
            pl.BlockSpec((HALO, width), halo(1)),
            pl.BlockSpec((SPAN, scols), row),
            pl.BlockSpec((HALO, scols), halo(0)),
            pl.BlockSpec((SPAN, 128), row),
            *seg_specs(lambda k: k, chunks),
            pl.BlockSpec(taps.shape, fixed),
            pl.BlockSpec(taps_s.shape, fixed),
            pl.BlockSpec(heads.shape, fixed),
        ],
        out_specs=[
            pl.BlockSpec((SPAN, width), row),
            pl.BlockSpec((SPAN, width), row),
            pl.BlockSpec((SPAN, scols), row),
            pl.BlockSpec((SPAN, 128), row),
            pl.BlockSpec((SPAN, 128), row),
            pl.BlockSpec((nrow, SPAN), lambda k: (0, k)),
            pl.BlockSpec((SPAN, 128), row),
            pl.BlockSpec((None, scols // 2, width), lambda k: (k, 0, 0)),
            pl.BlockSpec((scols // 2, width), fixed),
        ],
        out_shape=[
            S((length, width), F32),
            S((length, width), BF16),
            S((length, scols), BF16),
            S((length, 128), F32),
            S((length, 128), F32),
            S((nrow, length), F32),
            S((length, 128), F32),
            S((chunks, scols // 2, width), BF16),
            S((scols // 2, width), F32),
        ],
        scratch_shapes=[pltpu.VMEM((scols // 2, width), F32), pltpu.VMEM((8, 128), F32)],
        name="scan_forward",
    )(both_ext, both_ext, shared_ext, shared_ext, step_raw, seg, seg, seg, taps, taps_s, heads)


def row_sums(value):
    hi = value.astype(BF16)
    lo = (value - hi.astype(F32)).astype(BF16)
    ones = jnp.ones((8, value.shape[1]), BF16)
    return nt(ones, hi) + nt(ones, lo)


def first_rows(value):
    return jnp.where(iota(value.shape, 0) == 0, value, 0.0)


def gate_kernel(y, x, bc, dec, start, gate, taps, ssd_out, gated_out, sums_out):
    length, width = x.shape
    state_dim = start.shape[0]
    cc = bc[:, state_dim:]
    lo = iota((length, 128), 1) < 64
    squares = jnp.zeros((length, 128), F32)
    for p in range(width // 128):
        sl = slice(p * 128, (p + 1) * 128)
        corr = nn(cc, start[:, sl].astype(BF16)) * pick(lo, dec, 2 * p)
        ssd = y[:, sl] + corr + taps[6:7, sl] * x[:, sl].astype(F32)
        ssd_out[:, sl] = ssd
        g = gate[:, sl].astype(F32)
        gated = ssd * (g * sigmoid(g))
        gated_out[:, sl] = gated.astype(BF16)
        squares = squares + gated * gated
    sums_out[...] = row_sums(squares)


def run_gate(y, x, bc, dec, start, both_ext, taps):
    length, width = x.shape
    row = lambda k: (k, 0)
    fixed = lambda k: (0, 0)
    S = jax.ShapeDtypeStruct
    return pl.pallas_call(
        gate_kernel,
        grid=(length // SPAN,),
        in_specs=[
            pl.BlockSpec((SPAN, width), row),
            pl.BlockSpec((SPAN, width), row),
            pl.BlockSpec((SPAN, bc.shape[1]), row),
            pl.BlockSpec((SPAN, 128), row),
            pl.BlockSpec(start.shape, fixed),
            pl.BlockSpec((SPAN, width), row),
            pl.BlockSpec(taps.shape, fixed),
        ],
        out_specs=[
            pl.BlockSpec((SPAN, width), row),
            pl.BlockSpec((SPAN, width), row),
            pl.BlockSpec((8, SPAN), lambda k: (0, k)),
        ],
        out_shape=[S((length, width), F32), S((length, width), BF16), S((8, length), F32)],
        name="gate_sums",
    )(y, x, bc, dec, start, both_ext, taps)


def project_kernel(full_width, gated, sums, taps, out_t, normed_out, proj_out):
    rescale = columns(lax.rsqrt(sums[0:1] / full_width + EPS))
    for p in range(gated.shape[1] // 128):
        sl = slice(p * 128, (p + 1) * 128)
        normed_out[:, sl] = (gated[:, sl].astype(F32) * rescale * taps[5:6, sl]).astype(BF16)
    proj_out[...] = nt(normed_out[...], out_t[...]).astype(BF16)


def run_project(full_width, gated, sums, taps, out_t):
    length, width = gated.shape
    row = lambda k: (k, 0)
    fixed = lambda k: (0, 0)
    S = jax.ShapeDtypeStruct
    return pl.pallas_call(
        functools.partial(project_kernel, full_width),
        grid=(length // SPAN,),
        in_specs=[
            pl.BlockSpec((SPAN, width), row),
            pl.BlockSpec((8, SPAN), lambda k: (0, k)),
            pl.BlockSpec(taps.shape, fixed),
            pl.BlockSpec(out_t.shape, fixed),
        ],
        out_specs=[pl.BlockSpec((SPAN, width), row), pl.BlockSpec((SPAN, out_t.shape[0]), row)],
        out_shape=[S((length, width), BF16), S((length, out_t.shape[0]), BF16)],
        name="project",
    )(gated, sums, taps, out_t)


def pull_kernel(cot, out_t, gated, taps, back_out, sums_out):
    back = nn(cot[...], out_t[...])
    back_out[...] = back.astype(BF16)
    inner = jnp.zeros((cot.shape[0], 128), F32)
    for p in range(back.shape[1] // 128):
        sl = slice(p * 128, (p + 1) * 128)
        inner = inner + back[:, sl] * taps[5:6, sl] * gated[:, sl].astype(F32)
    sums_out[...] = row_sums(inner)


def run_pull(cot, out_t, gated, taps):
    length, width = gated.shape
    row = lambda k: (k, 0)
    fixed = lambda k: (0, 0)
    S = jax.ShapeDtypeStruct
    return pl.pallas_call(
        pull_kernel,
        grid=(length // SPAN,),
        in_specs=[
            pl.BlockSpec((SPAN, cot.shape[1]), row),
            pl.BlockSpec(out_t.shape, fixed),
            pl.BlockSpec((SPAN, width), row),
            pl.BlockSpec(taps.shape, fixed),
        ],
        out_specs=[pl.BlockSpec((SPAN, width), row), pl.BlockSpec((8, SPAN), lambda k: (0, k))],
        out_shape=[S((length, width), BF16), S((8, length), F32)],
        name="pull_back",
    )(cot, out_t, gated, taps)


def back_kernel(
    full_width, ssd, x, bc, dec, gate, back, squares, inner, taps,
    dy_out, ggate_out, row_out, colsum_out, dstart_out,
):
    length, width = x.shape
    state_dim = dstart_out.shape[0]

    @pl.when(pl.program_id(0) == 0)
    def _():
        colsum_out[...] = jnp.zeros_like(colsum_out)
        dstart_out[...] = jnp.zeros_like(dstart_out)

    cc = bc[:, state_dim:]
    lo = iota((length, 128), 1) < 64
    rescale = columns(lax.rsqrt(squares[0:1] / full_width + EPS))
    pull = columns(inner[0:1]) * (rescale * rescale * rescale / full_width)
    rowterm = jnp.zeros((length, 128), F32)
    for p in range(width // 128):
        sl = slice(p * 128, (p + 1) * 128)
        s_ssd = ssd[:, sl]
        xp = x[:, sl].astype(F32)
        g = gate[:, sl].astype(F32)
        s = sigmoid(g)
        gated = s_ssd * (g * s)
        bk = back[:, sl].astype(F32)
        gain = taps[5:6, sl]
        gg = rescale * (bk * gain) - gated * pull
        dy = gg * (g * s)
        dyb = dy.astype(BF16)
        dy_out[:, sl] = dyb
        ggate_out[:, sl] = (gg * s_ssd * s * (1.0 + g * (1.0 - s))).astype(BF16)
        colsum_out[5:6, sl] += jnp.sum(bk * gated * rescale, axis=0, keepdims=True)
        colsum_out[6:7, sl] += jnp.sum(dy * xp, axis=0, keepdims=True)
        dstart_out[:, sl] += tn(cc, (dy * pick(lo, dec, 2 * p)).astype(BF16))
        rowterm = rowterm + split_dot(dyb.astype(F32) * (s_ssd - taps[6:7, sl] * xp), head_map(p))
    row_out[...] = rowterm


def head_map(p):
    lane, head = iota((128, 128), 0), iota((128, 128), 1)
    return (head == 2 * p + lane // 64).astype(BF16)


def run_back(full_width, ssd, x, bc, dec, both_ext, back, squares, inner, taps):
    length, width = x.shape
    row = lambda k: (k, 0)
    fixed = lambda k: (0, 0)
    S = jax.ShapeDtypeStruct
    return pl.pallas_call(
        functools.partial(back_kernel, full_width),
        grid=(length // SPAN,),
        in_specs=[
            pl.BlockSpec((SPAN, width), row),
            pl.BlockSpec((SPAN, width), row),
            pl.BlockSpec((SPAN, bc.shape[1]), row),
            pl.BlockSpec((SPAN, 128), row),
            pl.BlockSpec((SPAN, width), row),
            pl.BlockSpec((SPAN, width), row),
            pl.BlockSpec((8, SPAN), lambda k: (0, k)),
            pl.BlockSpec((8, SPAN), lambda k: (0, k)),
            pl.BlockSpec(taps.shape, fixed),
        ],
        out_specs=[
            pl.BlockSpec((SPAN, width), row),
            pl.BlockSpec((SPAN, width), row),
            pl.BlockSpec((SPAN, 128), row),
            pl.BlockSpec((8, width), fixed),
            pl.BlockSpec((bc.shape[1] // 2, width), fixed),
        ],
        out_shape=[
            S((length, width), BF16),
            S((length, width), BF16),
            S((length, 128), F32),
            S((8, width), F32),
            S((bc.shape[1] // 2, width), F32),
        ],
        name="gated_back",
    )(ssd, x, bc, dec, both_ext, back, squares, inner, taps)


def conv_back(dout, pre, shifts, links, taps, sl, carry, carry_links, par_out):
    length = dout.shape[0]
    s = sigmoid(pre)
    dconv = dout * (s * (1.0 + pre * (1.0 - s)))
    nxt = carry[:, sl]
    grad = taps[3:4, sl] * dconv
    above = jnp.zeros((8, dout.shape[1]), F32)
    par_out[3:4, sl] += jnp.sum(dconv * shifts[0], axis=0, keepdims=True)
    par_out[4:5, sl] += jnp.sum(dconv, axis=0, keepdims=True)
    for j in range(1, 4):
        z = dconv * links[j - 1]
        w = taps[3 - j : 4 - j, sl]
        low = jnp.concatenate([z, nxt * carry_links[:, j - 1 : j]], axis=0)
        grad = grad + w * low[j : j + length]
        high = jnp.concatenate([above * 0.0, z[0:8]], axis=0)
        above = above + w * high[j : j + 8]
        par_out[3 - j : 4 - j, sl] += jnp.sum(dconv * shifts[j], axis=0, keepdims=True)
    carry[:, sl] = dconv[0:8]
    return grad, above


def backward_kernel(
    inner, inner_halo, shared, shared_halo, step_raw, seg_row, seg_prev, seg_tail, taps, taps_s, heads,
    dy, x, bc, dt_in, c_in, ct_in, dec_halo, enter, start, row_in, dend, colsum,
    ginner_out, gsmall_out, par_out, par_s_out, par_h_out, edge_out, last_out,
    dstate, carry, carry_s, carry_links, grads_bc,
):
    i = pl.program_id(0)
    k = pl.num_programs(0) - 1 - i
    length, width = x.shape
    state_dim = dstate.shape[0]

    @pl.when(i == 0)
    def _():
        dstate[...] = dend[...]
        carry[...] = jnp.zeros_like(carry)
        carry_s[...] = jnp.zeros_like(carry_s)
        carry_links[...] = jnp.zeros_like(carry_links)
        par_out[...] = colsum[...]
        par_s_out[...] = jnp.zeros_like(par_s_out)
        par_h_out[...] = jnp.zeros_like(par_h_out)

    segr, seg, seg_halo, tail_seg = segments(seg_row, seg_prev, seg_tail)
    links = chunk_links(seg, seg_halo)
    closing = (seg == seg[length - 1 :]).astype(F32)
    entering = (seg == seg_halo[7:]).astype(F32)
    kept = (seg[length - 1 :] == seg_halo[7:]).astype(F32)
    next_links = carry_links[...]
    dt = dt_in[...]
    c = c_in[...]
    ct = ct_in[...]
    first = (k == 0).astype(F32)
    reach = dec_halo[7:8] * (1.0 - first) + first
    b = bc[:, :state_dim]
    cc = bc[:, state_dim:]
    rows, cols = iota((length, length), 0), iota((length, length), 1)
    allowed = (rows <= cols) & (seg == segr)
    scores = jnp.where(allowed, nt(b, cc), 0.0)
    lo = iota((length, 128), 1) < 64
    lo1 = lo[0:1]
    dscores = jnp.zeros((length, length), F32)
    db = jnp.zeros((length, state_dim), F32)
    dc_mat = jnp.zeros((length, state_dim), F32)
    direct = jnp.zeros((length, 128), F32)
    matched = jnp.zeros((length, 128), F32)
    closing_term = jnp.zeros((1, 128), F32)
    for p in range(width // 128):
        sl = slice(p * 128, (p + 1) * 128)
        pre, shifts = conv_tile(inner, inner_halo, links, taps, sl)
        dyb = dy[:, sl]
        dyf = dyb.astype(F32)
        xp = x[:, sl].astype(F32)
        dtb = pick(lo, dt, 2 * p)
        xdt = xp * dtb
        cb = pick(lo, c, 2 * p)
        hm = head_map(p)
        last = cb[length - 1 :]
        entry = enter[:, sl].astype(F32) + start[:, sl] * pick(lo1, reach, 2 * p)
        entryb = entry.astype(BF16)
        ds = dstate[:, sl]
        dsb = ds.astype(BF16)
        leaving = jnp.exp(last - cb) * closing
        bds = nn(b, dsb)
        dxdt = jnp.zeros((length, 128), F32)
        for a in range(2):
            h = 2 * p + a
            mine = lo if a == 0 else ~lo
            decay = jnp.exp(jnp.minimum(ct[h : h + 1] - c[:, h : h + 1], 0.0))
            dscores = dscores + decay * nt(jnp.where(mine, xdt, 0.0).astype(BF16), dyb)
            dxdt = dxdt + nn((decay * scores).astype(BF16), jnp.where(mine, dyf, 0.0).astype(BF16))
        spread = leaving * xdt
        moved = spread * bds
        matched = matched + split_dot(xdt.astype(BF16).astype(F32) * dxdt + moved, hm)
        dxdt = dxdt + leaving * bds
        held = jnp.exp(last) * kept
        col = jnp.sum(moved, axis=0, keepdims=True) + held * jnp.sum(entry * ds, axis=0, keepdims=True)
        closing_term = closing_term + split_dot(jnp.broadcast_to(col, (8, 128)), hm)[0:1]
        direct = direct + split_dot(xp * dxdt, hm)
        edy = (jnp.exp(cb) * entering * dyf).astype(BF16)
        db = db + nt(spread.astype(BF16), dsb)
        dc_mat = dc_mat + nt(edy, entryb)
        dstate[:, sl] = ds * held + tn(cc, edy)
        dx = dtb * dxdt + taps[6:7, sl] * dyf
        grad, above = conv_back(dx, pre, shifts, links, taps, sl, carry, next_links, par_out)
        ginner_out[:, sl] = grad.astype(BF16)
        edge_out[:, sl] = above

        @pl.when(i == 0)
        def _():
            last_out[:, sl] = grad[length - 8 :]

    dsc = jnp.where(allowed, dscores, 0.0).astype(BF16)
    grads_bc[:, :state_dim] = db + nn(dsc, cc)
    grads_bc[:, state_dim:] = dc_mat + tn(dsc, b)
    for half in range(2):
        sl = slice(half * state_dim, (half + 1) * state_dim)
        pre, shifts = conv_tile(shared, shared_halo, links, taps_s, sl)
        grad, above = conv_back(grads_bc[:, sl], pre, shifts, links, taps_s, sl, carry_s, next_links, par_s_out)
        gsmall_out[:, sl] = grad.astype(BF16)
        at = slice(width + half * state_dim, width + (half + 1) * state_dim)
        edge_out[:, at] = above

        @pl.when(i == 0)
        def _():
            last_out[:, at] = grad[length - 8 :]

    for j in range(3):
        carry_links[:, j : j + 1] = links[j][0:8]
    dcum = row_in[...] - matched
    upper = (rows <= cols).astype(F32)
    dlog = jnp.dot(upper, dcum, precision=HIGH, preferred_element_type=F32) + closing_term
    rate = -jnp.exp(heads[1:2])
    dstep = (direct + dlog * rate) * sigmoid(step_raw[...] + heads[0:1])
    gsmall_out[:, 2 * state_dim :] = dstep.astype(BF16)
    par_h_out[0:1] += jnp.sum(dstep, axis=0, keepdims=True)
    par_h_out[1:2] += jnp.sum(dlog * (rate * dt), axis=0, keepdims=True)


def run_backward(
    both_ext, shared_ext, step_raw, seg, taps, taps_s, heads,
    dy, x, bc, dt, c, ct, dec, enter, start, rowterm, dend, colsum,
):
    length, width = x.shape
    scols = bc.shape[1]
    chunks = length // SPAN
    at = lambda i: chunks - 1 - i
    row = lambda i: (at(i), 0)
    halo = lambda col: (lambda i: (halo_index(at(i), chunks), col))
    fixed = lambda i: (0, 0)
    S = jax.ShapeDtypeStruct
    return pl.pallas_call(
        backward_kernel,
        grid=(chunks,),
        in_specs=[
            pl.BlockSpec((SPAN, width), lambda i: (at(i), 1)),
            pl.BlockSpec((HALO, width), halo(1)),
            pl.BlockSpec((SPAN, scols), row),
            pl.BlockSpec((HALO, scols), halo(0)),
            pl.BlockSpec((SPAN, 128), row),
            *seg_specs(at, chunks),
            pl.BlockSpec(taps.shape, fixed),
            pl.BlockSpec(taps_s.shape, fixed),
            pl.BlockSpec(heads.shape, fixed),
            pl.BlockSpec((SPAN, width), row),
            pl.BlockSpec((SPAN, width), row),
            pl.BlockSpec((SPAN, scols), row),
            pl.BlockSpec((SPAN, 128), row),
            pl.BlockSpec((SPAN, 128), row),
            pl.BlockSpec((ct.shape[0], SPAN), lambda i: (0, at(i))),
            pl.BlockSpec((8, 128), lambda i: (jnp.maximum(at(i) * (SPAN // 8) - 1, 0), 0)),
            pl.BlockSpec((None, scols // 2, width), lambda i: (at(i), 0, 0)),
            pl.BlockSpec(start.shape, fixed),
            pl.BlockSpec((SPAN, 128), row),
            pl.BlockSpec(dend.shape, fixed),
            pl.BlockSpec(colsum.shape, fixed),
        ],
        out_specs=[
            pl.BlockSpec((SPAN, width), row),
            pl.BlockSpec((SPAN, scols + 128), row),
            pl.BlockSpec((8, width), fixed),
            pl.BlockSpec((8, scols), fixed),
            pl.BlockSpec((8, 128), fixed),
            pl.BlockSpec((8, width + scols), fixed),
            pl.BlockSpec((8, width + scols), fixed),
        ],
        out_shape=[
            S((length, width), BF16),
            S((length, scols + 128), BF16),
            S((8, width), F32),
            S((8, scols), F32),
            S((8, 128), F32),
            S((8, width + scols), F32),
            S((8, width + scols), F32),
        ],
        scratch_shapes=[
            pltpu.VMEM((scols // 2, width), F32),
            pltpu.VMEM((8, width), F32),
            pltpu.VMEM((8, scols), F32),
            pltpu.VMEM((8, 128), F32),
            pltpu.VMEM((SPAN, scols), F32),
        ],
        name="scan_backward",
    )(both_ext, both_ext, shared_ext, shared_ext, step_raw, seg, seg, seg, taps, taps_s, heads,
      dy, x, bc, dt, c, ct, dec, enter, start, rowterm, dend, colsum)


def spread_kernel(ggate, ginner, gsmall, w_in, w_small, normed, part_out, gain_out):
    width = ggate.shape[1]
    part = nt(ggate[...], w_in[:, :width]) + nt(ginner[...], w_in[:, width:]) + nt(gsmall[...], w_small[...])
    part_out[...] = part.astype(BF16)
    gain_out[...] = first_rows(jnp.broadcast_to(
        jnp.sum(part * normed[...].astype(F32), axis=0, keepdims=True), gain_out.shape))


def run_spread(ggate, ginner, gsmall, w_in, w_small, normed_ext):
    length = ggate.shape[0]
    model = w_in.shape[0]
    tile = 256
    fixed = lambda n: (0, 0)
    down = lambda n: (n, 0)
    across = lambda n: (0, n)
    S = jax.ShapeDtypeStruct
    return pl.pallas_call(
        spread_kernel,
        grid=(model // tile,),
        in_specs=[
            pl.BlockSpec(ggate.shape, fixed),
            pl.BlockSpec(ginner.shape, fixed),
            pl.BlockSpec(gsmall.shape, fixed),
            pl.BlockSpec((tile, w_in.shape[1]), down),
            pl.BlockSpec((tile, w_small.shape[1]), down),
            pl.BlockSpec((length, tile), across),
        ],
        out_specs=[pl.BlockSpec((length, tile), across), pl.BlockSpec((8, tile), across)],
        out_shape=[S((length, model), BF16), S((8, model), F32)],
        name="spread_back",
    )(ggate, ginner, gsmall, w_in, w_small, normed_ext)


MESH = pl.DeviceIdType.MESH
ANY = pl.BlockSpec(memory_space=pl.ANY)


def remote(src, dst, send, recv, **to):
    return pltpu.make_async_remote_copy(
        src_ref=src, dst_ref=dst, send_sem=send, recv_sem=recv, device_id=to, device_id_type=MESH
    )


def greet(barrier, when, **to):
    @pl.when(when)
    def _():
        pl.semaphore_signal(barrier, inc=1, device_id=to, device_id_type=MESH)


PIECES = 2


def gather_kernel(
    ncol, ndp,
    tokens_in, gain, seg_in, w0, w1, w2,
    all_out, seg_out, w0_out, w1_out, w2_out,
    z_send, z_recv, w_send, c_send, w_recv, t_send, t_recv, here, own, seg_own, zero_tail, no_seg,
):
    dp, row, z = lax.axis_index("dp"), lax.axis_index("row"), lax.axis_index("col")
    other = 1 - row
    last = ncol - 1
    tokens, tail, part = own.shape[0], zero_tail.shape[0], own.shape[0] // PIECES
    weights = ((w0, w0_out), (w1, w1_out), (w2, w2_out))
    rows = w0.shape[0]
    sends_tail = (row == 0) & (z == last)

    barrier = pltpu.get_barrier_semaphore()
    greet(barrier, z > 0, col=z - 1)
    greet(barrier, z < last, col=z + 1)
    greet(barrier, row >= 0, row=other)
    for m in range(1, ndp):
        greet(barrier, row >= 0, dp=dp ^ m)
    greet(barrier, row == 1, row=0, col=last)
    for c in range(ncol):
        greet(barrier, sends_tail, row=1, col=c)
    count = (z > 0).astype(jnp.int32) + (z < last).astype(jnp.int32) + ndp
    count = count + row + jnp.where(sends_tail, ncol, 0)
    seg_own[...] = jnp.broadcast_to(seg_in[...], seg_own.shape)
    no_seg[...] = jnp.full(no_seg.shape, -1, jnp.int32)
    zero_tail[...] = jnp.zeros_like(zero_tail)

    def normalize(step, carry):
        at = pl.ds(pl.multiple_of(step * 32, 32), 32)
        wide = tokens_in[at].astype(F32)
        scale = lax.rsqrt(jnp.sum(wide * wide, axis=1, keepdims=True) / wide.shape[1] + EPS)
        own[at] = (wide * scale * gain[...]).astype(BF16)
        return carry

    lax.fori_loop(0, tokens // 32, normalize, 0)
    pl.semaphore_wait(barrier, count)

    def token_copies(s, mine, way, which=None):
        target = z + 1 if way == 0 else z - 1
        copies = []
        for i in range(PIECES + 1) if which is None else which:
            if i < PIECES:
                dst = all_out.at[pl.ds(s * tokens + i * part, part)]
                src = own.at[pl.ds(i * part, part)] if mine else dst
            else:
                dst = seg_out.at[pl.ds(s * 8, 8)]
                src = seg_own if mine else dst
            copies.append(remote(src, dst, z_send.at[way, s, i], z_recv.at[s, i], col=target))
        return copies

    def weight_copies(j, mine, send, **to):
        copies = []
        for i, (src, dst) in enumerate(weights):
            place = dst.at[pl.ds(j * rows, rows)]
            copies.append(remote(src if mine else place, place, send.at[i], w_recv.at[j, i], **to))
        return copies

    def tail_copies(c):
        return [
            remote(own.at[pl.ds(tokens - tail, tail)], all_out.at[pl.ds(ncol * tokens, tail)],
                   t_send.at[c, 0], t_recv.at[0], row=1, col=c),
            remote(seg_own, seg_out.at[pl.ds(ncol * 8, 8)], t_send.at[c, 1], t_recv.at[1], row=1, col=c),
        ]

    def start(copies):
        for copy in copies:
            copy.start()

    def guarded(when, action):
        @pl.when(when)
        def _():
            action()

    me = dp * 2 + row
    guarded(z < last, lambda: start(token_copies(z, True, 0)))
    guarded(z > 0, lambda: start(token_copies(z, True, 1)))
    for m in range(1, ndp):
        start(weight_copies(me, True, w_send.at[m], dp=dp ^ m))
    start(weight_copies(me, True, c_send.at[0], row=other))
    for c in range(ncol):
        guarded(sends_tail, lambda c=c: start(tail_copies(c)))
    local = [
        pltpu.make_async_copy(own, all_out.at[pl.ds(z * tokens, tokens)], here.at[0]),
        pltpu.make_async_copy(seg_own, seg_out.at[pl.ds(z * 8, 8)], here.at[1]),
    ]
    for i, (src, dst) in enumerate(weights):
        local.append(pltpu.make_async_copy(src, dst.at[pl.ds(me * rows, rows)], here.at[2 + i]))
    start(local)
    fill = [
        pltpu.make_async_copy(zero_tail, all_out.at[pl.ds(ncol * tokens, tail)], here.at[5]),
        pltpu.make_async_copy(no_seg, seg_out.at[pl.ds(ncol * 8, 8)], here.at[6]),
    ]
    guarded(row == 0, lambda: start(fill))

    def pass_tokens(s):
        for which in [(i,) for i in range(PIECES - 1)] + [(PIECES - 1, PIECES)]:

            def from_below(which=which):
                for copy in token_copies(z - s, False, 0, which):
                    copy.wait_recv()
                guarded(z < last, lambda: start(token_copies(z - s, False, 0, which)))

            def from_above(which=which):
                for copy in token_copies(z + s, False, 1, which):
                    copy.wait_recv()
                guarded(z > 0, lambda: start(token_copies(z + s, False, 1, which)))

            guarded(z - s >= 0, from_below)
            guarded(z + s <= last, from_above)

    def pass_weights(m):
        j = (dp ^ m) * 2 + row
        for copy in weight_copies(j, False, w_send.at[m], dp=dp ^ m):
            copy.wait_recv()
        start(weight_copies(j, False, c_send.at[m], row=other))

    done = 0
    for s in range(1, ncol):
        pass_tokens(s)
        upto = (ndp - 1) * s // (ncol - 2) if s < ncol - 1 else ndp - 1
        for m in range(done + 1, upto + 1):
            pass_weights(m)
        done = max(done, upto)
    for m in range(ndp):
        j = (dp ^ m) * 2 + other
        for copy in weight_copies(j, False, c_send.at[m], row=other):
            copy.wait_recv()
    guarded(row == 1, lambda: [copy.wait_recv() for copy in tail_copies(0)])
    for m in range(ndp):
        if m:
            for copy in weight_copies(me, True, w_send.at[m], dp=dp ^ m):
                copy.wait_send()
        for copy in weight_copies((dp ^ m) * 2 + row, m == 0, c_send.at[m], row=other):
            copy.wait_send()
    for s in range(ncol):
        for way in range(2):
            open_way = z < last if way == 0 else z > 0
            mine = (z - s >= 0) if way == 0 else (z + s <= last)
            src = z - s if way == 0 else z + s

            def drain(way=way, src=src, s=s):
                for copy in token_copies(src, s == 0, way):
                    copy.wait_send()

            guarded(open_way & mine, drain)
    for c in range(ncol):
        guarded(sends_tail, lambda c=c: [copy.wait_send() for copy in tail_copies(c)])
    for copy in local:
        copy.wait()
    guarded(row == 0, lambda: [copy.wait() for copy in fill])


def gather_inputs(tokens_in, gain, seg, w0, w1, w2):
    ncol, ndp = lax.axis_size("col"), lax.axis_size("dp")
    tokens, width = tokens_in.shape
    S = jax.ShapeDtypeStruct
    shards = 2 * ndp
    dma = pltpu.SemaphoreType.DMA
    vmem = pl.BlockSpec(memory_space=pltpu.VMEM)
    return pl.pallas_call(
        functools.partial(gather_kernel, ncol, ndp),
        in_specs=[vmem] * 3 + [ANY] * 3,
        out_specs=[ANY] * 5,
        out_shape=[
            S((ncol * tokens + HALO, width), BF16),
            S(((ncol + 1) * 8, tokens), jnp.int32),
        ] + [S((shards * w.shape[0], w.shape[1]), w.dtype) for w in (w0, w1, w2)],
        scratch_shapes=[
            dma((2, ncol, PIECES + 1)), dma((ncol, PIECES + 1)), dma((ndp, 3)), dma((ndp, 3)), dma((shards, 3)),
            dma((ncol, 2)), dma((2,)), dma((7,)),
            pltpu.VMEM((tokens, width), BF16), pltpu.VMEM((8, tokens), jnp.int32),
            pltpu.VMEM((HALO, width), BF16), pltpu.VMEM((8, tokens), jnp.int32),
        ],
        compiler_params=pltpu.CompilerParams(collective_id=1, has_side_effects=True),
        cost_estimate=pl.CostEstimate(flops=0, bytes_accessed=200_000_000, transcendentals=0),
        name="gather_inputs",
    )(tokens_in, gain[None], seg[None], w0, w1, w2)


def sum_col_kernel(ncol, value, out, slots, send, recv):
    z = lax.axis_index("col")
    barrier = pltpu.get_barrier_semaphore()
    for s in range(1, ncol):
        pl.semaphore_signal(barrier, inc=1, device_id={"col": lax.rem(z + s, ncol)}, device_id_type=MESH)
    pl.semaphore_wait(barrier, ncol - 1)
    copies = [
        remote(value, slots.at[z], send.at[s], recv.at[z], col=lax.rem(z + s, ncol)) for s in range(1, ncol)
    ]
    for copy in copies:
        copy.start()
    total = value[...]
    for s in range(1, ncol):
        source = lax.rem(z + s, ncol)
        remote(value, slots.at[source], send.at[s], recv.at[source], col=source).wait_recv()
        total = total + slots[source]
    out[...] = total
    for copy in copies:
        copy.wait_send()


def sum_col(value, collective_id):
    ncol = lax.axis_size("col")
    dma = pltpu.SemaphoreType.DMA
    vmem = pl.BlockSpec(memory_space=pltpu.VMEM)
    return pl.pallas_call(
        functools.partial(sum_col_kernel, ncol),
        in_specs=[vmem],
        out_specs=vmem,
        out_shape=jax.ShapeDtypeStruct(value.shape, F32),
        scratch_shapes=[pltpu.VMEM((ncol,) + value.shape, F32), dma((ncol,)), dma((ncol,))],
        compiler_params=pltpu.CompilerParams(collective_id=collective_id, has_side_effects=True),
        name="sum_col",
    )(value)


def reduce_kernel(ncol, ndp, *refs):
    count = 4
    refs = list(refs)

    def take(number):
        taken = refs[:number]
        del refs[:number]
        return taken

    g, vecs = take(count), take(4)
    r, vec_outs = take(count), take(4)
    own, near, sent, far = take(count), take(count), take(count), take(count)
    vec_slots, col_slots = take(4), take(2)
    bc_slots, c_send, c_recv, p_send, p_recv, here, v_send, v_recv, u_send, u_recv, b_send, b_recv = refs
    dp, row, z = lax.axis_index("dp"), lax.axis_index("row"), lax.axis_index("col")
    other = 1 - row
    me = dp * 2 + row
    rows = [out.shape[0] for out in r]
    barrier = pltpu.get_barrier_semaphore()
    for q in range(1, 2 * ndp):
        greet(barrier, row >= 0, dp=dp ^ (q >> 1), row=row ^ (q & 1))
    for s in range(1, ncol):
        greet(barrier, row >= 0, col=lax.rem(z + s, ncol))
    pl.semaphore_wait(barrier, 2 * ndp + ncol - 2)

    order = (0, 1, 2, 3)
    turns = [3, 1, 2, 0] if ndp == 4 else list(range(1, ndp)) + [0]

    def core_copy(i, d):
        return remote(g[i].at[pl.ds((d * 2 + other) * rows[i], rows[i])], near[i].at[d],
                      c_send.at[i, d], c_recv.at[i, d], row=other)

    def own_copy(i, d):
        return pltpu.make_async_copy(g[i].at[pl.ds((d * 2 + row) * rows[i], rows[i])], own[i].at[d], here.at[i, d])

    def vec_copy(q, i, j):
        return remote(vecs[i], vec_slots[i].at[j], v_send.at[q, i], v_recv.at[j, i],
                      dp=dp ^ (q >> 1), row=row ^ (q & 1))

    for i in order:
        for m in turns:
            core_copy(i, dp ^ m).start()
            own_copy(i, dp ^ m).start()
    for q in range(1, 2 * ndp):
        for i in range(4):
            vec_copy(q, i, me).start()

    waiting = []

    def later(copy):
        if waiting:
            waiting.pop().start()
        if copy is not None:
            waiting.append(copy)

    def accumulate(i, first, number, terms, store):
        def step(k, carry):
            at = first + pl.multiple_of(k * 16, 16)
            total = terms[0](at)
            for term in terms[1:]:
                total = total + term(at)
            store(at, total)
            return carry

        lax.fori_loop(0, number // 16, step, 0)

    def read(ref, index, shift=0):
        return lambda at: ref[index, pl.ds(at - shift, 16)].astype(F32)

    def write(ref, index, shift):
        def store(at, total):
            ref[index, pl.ds(at - shift, 16)] = total.astype(BF16)

        return store

    def arrived(i, d):
        core_copy(i, d).wait_recv()
        own_copy(i, d).wait()

    if ndp == 4:
        halves = ((0, 1, 2), (1, 2, 1))

        def leg(i, slot, m):
            return remote(sent[i].at[slot], far[i].at[slot], p_send.at[i, slot], p_recv.at[i, slot], dp=dp ^ m)

        for i in order:
            half = rows[i] // 2
            arrived(i, dp ^ 3)
            for h, m1, m2 in halves:
                accumulate(i, h * half, half, [read(own[i], dp ^ 3), read(near[i], dp ^ 3)],
                           write(sent[i], 3 * h + 1, h * half))
                later(leg(i, 3 * h + 1, m1))
            for h, m1, m2 in halves:
                arrived(i, dp ^ m1)
                accumulate(i, h * half, half, [read(own[i], dp ^ m1), read(near[i], dp ^ m1)],
                           write(sent[i], 3 * h, h * half))
                later(leg(i, 3 * h, m1))
        later(None)

        def relay(i):
            half = rows[i] // 2
            for h, m1, m2 in halves:
                leg(i, 3 * h + 1, m1).wait_recv()
                accumulate(i, h * half, half,
                           [read(own[i], dp ^ m2), read(near[i], dp ^ m2), read(far[i], 3 * h + 1, h * half)],
                           write(sent[i], 3 * h + 2, h * half))
                later(leg(i, 3 * h + 2, m2))

        def finish(i, store):
            half = rows[i] // 2
            for h, m1, m2 in halves:
                leg(i, 3 * h, m1).wait_recv()
                leg(i, 3 * h + 2, m2).wait_recv()
                accumulate(i, h * half, half,
                           [read(own[i], dp), read(near[i], dp), read(far[i], 3 * h, h * half),
                            read(far[i], 3 * h + 2, h * half)], store)

        sends = [leg(i, 3 * h + k, m2 if k == 2 else m1) for i in order for h, m1, m2 in halves for k in range(3)]
    else:

        def peer(i, m):
            return remote(sent[i].at[m], far[i].at[m], p_send.at[i, m], p_recv.at[i, m], dp=dp ^ m)

        for i in order:
            for m in turns[:-1]:
                arrived(i, dp ^ m)
                accumulate(i, 0, rows[i], [read(own[i], dp ^ m), read(near[i], dp ^ m)], write(sent[i], m, 0))
                later(peer(i, m))
        later(None)

        def relay(i):
            pass

        def finish(i, store):
            for m in range(1, ndp):
                peer(i, m).wait_recv()
            accumulate(i, 0, rows[i],
                       [read(own[i], dp), read(near[i], dp)] + [read(far[i], m) for m in range(1, ndp)], store)

        sends = [peer(i, m) for i in order for m in range(1, ndp)]

    for i in order:
        arrived(i, dp)
    for q in range(1, 2 * ndp):
        for i in range(4):
            vec_copy(q, i, me ^ q).wait_recv()
    for i in range(4):
        vec_slots[i][me] = vecs[i][...]
        total = vec_slots[i][0]
        for j in range(1, 2 * ndp):
            total = total + vec_slots[i][j]
        if i < 2:
            vec_outs[i][...] = total
        else:
            col_slots[i - 2][z] = total

    def plain(i):
        def store(at, total):
            r[i][pl.ds(at, 16)] = total

        return store

    def shared_rows(at, total):
        r[0][pl.ds(at, 16)] = total
        bc_slots[z, pl.ds(at, 16)] = total[:, : bc_slots.shape[2]].astype(BF16)

    def col_copies(s, source):
        to = lax.rem(z + s, ncol)
        copies = [remote(col_slots[i].at[source], col_slots[i].at[source], u_send.at[s, i], u_recv.at[source, i], col=to)
                  for i in range(2)]
        return copies + [remote(bc_slots.at[source], bc_slots.at[source], b_send.at[s], b_recv.at[source], col=to)]

    relay(0)
    relay(1)
    relay(2)
    finish(0, shared_rows)
    relay(3)
    later(None)
    for s in range(1, ncol):
        for copy in col_copies(s, z):
            copy.start()
    finish(1, plain(1))
    finish(2, plain(2))
    finish(3, plain(3))
    for s in range(1, ncol):
        for copy in col_copies(s, lax.rem(z + s, ncol)):
            copy.wait_recv()
    for i in range(2):
        total = col_slots[i][0]
        for j in range(1, ncol):
            total = total + col_slots[i][j]
        vec_outs[2 + i][...] = total
    total = bc_slots[0].astype(F32)
    for j in range(1, ncol):
        total = total + bc_slots[j].astype(F32)
    r[0][:, : bc_slots.shape[2]] = total

    for q in range(1, 2 * ndp):
        for i in range(4):
            vec_copy(q, i, me).wait_send()
    for i in order:
        for m in turns:
            core_copy(i, dp ^ m).wait_send()
    for copy in sends:
        copy.wait_send()
    for s in range(1, ncol):
        for copy in col_copies(s, z):
            copy.wait_send()


def reduce_grads(grads, vecs, scols):
    ncol, ndp = lax.axis_size("col"), lax.axis_size("dp")
    dma = pltpu.SemaphoreType.DMA
    vmem = pl.BlockSpec(memory_space=pltpu.VMEM)
    S = jax.ShapeDtypeStruct
    count = len(grads)
    blocks = [(g.shape[0] // (2 * ndp), g.shape[1]) for g in grads]
    stack = [pltpu.VMEM((ndp,) + b, BF16) for b in blocks]
    slots = 6 if ndp == 4 else ndp
    legs = [pltpu.VMEM((6, b[0] // 2, b[1]) if ndp == 4 else (ndp,) + b, BF16) for b in blocks]
    return pl.pallas_call(
        functools.partial(reduce_kernel, ncol, ndp),
        in_specs=[ANY] * count + [vmem] * 4,
        out_specs=[vmem] * (count + 4),
        out_shape=[S(b, F32) for b in blocks] + [S(v.shape, F32) for v in vecs],
        scratch_shapes=stack * 2 + legs * 2
        + [pltpu.VMEM((2 * ndp,) + v.shape, F32) for v in vecs]
        + [pltpu.VMEM((ncol,) + v.shape, F32) for v in vecs[2:]]
        + [pltpu.VMEM((ncol, blocks[0][0], scols), BF16)]
        + [dma((count, ndp))] * 2
        + [dma((count, slots))] * 2
        + [dma((count, ndp))]
        + [dma((2 * ndp, 4))] * 2
        + [dma((ncol, 2))] * 2
        + [dma((ncol,))] * 2,
        compiler_params=pltpu.CompilerParams(collective_id=2, has_side_effects=True),
        cost_estimate=pl.CostEstimate(flops=0, bytes_accessed=200_000_000, transcendentals=0),
        name="reduce_grads",
    )(*grads, *vecs)


def finish_kernel(
    nheads, small, gate, inner, out, par, par_h, par_s, gain_sum, gain, tokens, cot, gnormed,
    zx_out, bc_out, dt_out, out_out, ci_out, cib_out, cs_out, csb_out, sb_out, rl_out, sg_out, gg_out, ng_out, gin_out,
):
    width = par.shape[1]
    scols = par_s.shape[1]
    zx_out[:, 0, :] = gate[...]
    zx_out[:, 1, :] = inner[...]
    bc_out[...] = small[:, :scols]
    dt_out[...] = small[:, scols:].T[:nheads]
    out_out[...] = out[...]
    ci_out[...] = par[0:4]
    cib_out[...] = par[4:5]
    gg_out[...] = par[5:6]
    cs_out[...] = par_s[0:4]
    csb_out[...] = par_s[4:5]
    sb_out[...] = par_h[0:1, :nheads]
    rl_out[...] = par_h[1:2, :nheads]
    skip = jnp.zeros((8, 128), F32)
    for p in range(width // 128):
        skip = skip + split_dot(jnp.broadcast_to(par[6:7, p * 128 : (p + 1) * 128], (8, 128)), head_map(p))
    sg_out[...] = skip[0:1, :nheads]
    ng_out[...] = gain_sum[0:1] / gain[...]

    def rows(step, carry):
        at = pl.ds(pl.multiple_of(step * 32, 32), 32)
        wide = tokens[at].astype(F32)
        scale = lax.rsqrt(jnp.sum(wide * wide, axis=1, keepdims=True) / wide.shape[1] + EPS)
        pushed = gnormed[at].astype(F32) * gain[...]
        mean = jnp.sum(pushed * wide, axis=1, keepdims=True) / wide.shape[1]
        grad = scale * pushed - wide * (scale * scale * scale * mean)
        gin_out[at] = (cot[at].astype(F32) + grad).astype(BF16)
        return carry

    lax.fori_loop(0, tokens.shape[0] // 32, rows, 0)


def run_finish(nheads, small, gate, inner, out, par, par_h, par_s, gain_sum, gain, tokens, cot, gnormed):
    rows, width = gate.shape
    scols = par_s.shape[1]
    model = gain.shape[0]
    S = jax.ShapeDtypeStruct
    shapes = [
        (rows, 2, width), (rows, scols), (nheads, rows), (rows, width), (4, width), (1, width), (4, scols), (1, scols),
        (1, nheads), (1, nheads), (1, nheads), (1, width), (1, model),
    ]
    return pl.pallas_call(
        functools.partial(finish_kernel, nheads),
        out_shape=[S(shape, F32) for shape in shapes] + [S(tokens.shape, BF16)],
        name="finish",
    )(small, gate, inner, out, par, par_h, par_s, gain_sum, gain[None], tokens, cot, gnormed)


def pass_on(value, axis, by):
    count = lax.axis_size(axis)
    pairs = [(i, i + by) for i in range(count) if 0 <= i + by < count]
    return lax.ppermute(value, axis, pairs)


def pack_rows(rows, width):
    used = sum(r.shape[0] for r in rows)
    return jnp.concatenate(rows + [jnp.zeros((8 - used, width), F32)], axis=0)


def per_device(
    block_input, segment_ids, norm_gain, proj_zx, proj_bc, proj_dt, conv_inner, conv_inner_bias,
    conv_shared, conv_shared_bias, step_bias, rate_log, skip_gain, gated_gain, proj_out, cotangent,
):
    width = proj_zx.shape[2]
    scols = proj_bc.shape[1]
    nheads = proj_dt.shape[1]
    head_dim = width // nheads
    full_width = float(width * lax.axis_size("col"))
    fill = (0, 128 - nheads)
    small_own = jnp.concatenate([proj_bc, jnp.pad(proj_dt, ((0, 0), fill))], axis=1)
    normed_ext, seg, w_in, w_small, out_t = gather_inputs(
        block_input, norm_gain, segment_ids, proj_zx.reshape(-1, 2 * width), small_own, proj_out.T
    )
    length = normed_ext.shape[0] - HALO
    (cot, normed_ext, conv_inner, conv_inner_bias, conv_shared, conv_shared_bias, step_bias, rate_log, skip_gain,
     gated_gain) = lax.optimization_barrier((
        cotangent, normed_ext, conv_inner, conv_inner_bias, conv_shared, conv_shared_bias, step_bias, rate_log,
        skip_gain, gated_gain))
    cot_all = lax.all_gather(cot, "col", axis=0, tiled=True)
    taps = pack_rows(
        [conv_inner, conv_inner_bias[None], gated_gain[None], jnp.repeat(skip_gain, head_dim)[None]], width
    )
    taps_s = pack_rows([conv_shared, conv_shared_bias[None]], scols)
    heads = pack_rows([jnp.pad(step_bias, fill)[None], jnp.pad(rate_log, fill)[None]], 128)

    both_ext = nn(normed_ext, w_in).astype(BF16)
    small_ext = nn(normed_ext, w_small)
    shared_ext = small_ext[:, :scols].astype(BF16)
    step_ext = small_ext[:, scols:]
    common = (both_ext, shared_ext, step_ext, seg, taps, taps_s, heads)
    y, x, bc, dt, c, ct, dec, enter, final = run_forward(*common)
    start = pass_on(final, "row", 1)
    ssd, gated, squares = run_gate(y, x, bc, dec, start, both_ext, taps)
    squares = sum_col(squares, 3)
    gated_normed, projected = run_project(full_width, gated, squares, taps, out_t)
    cot_all, projected = lax.optimization_barrier((cot_all, projected))
    projected = lax.psum_scatter(projected, "col", scatter_dimension=0, tiled=True)
    block_output = (block_input.astype(F32) + projected.astype(F32)).astype(BF16)
    back, inner = run_pull(cot_all, out_t, gated, taps)
    inner = sum_col(inner, 4)
    dy, ggate, rowterm, colsum, dstart = run_back(
        full_width, ssd, x, bc, dec, both_ext, back, squares, inner, taps
    )
    dend = pass_on(dstart, "row", -1)
    ginner, gsmall, par, par_s, par_h, edge, last = run_backward(
        *common, dy, x, bc, dt, c, ct, dec, enter, start, rowterm, dend, colsum
    )
    edge = pass_on(edge, "row", -1)
    fixed = (last + edge).astype(BF16)
    ginner = lax.dynamic_update_slice(ginner, fixed[:, :width], (length - 8, 0))
    gsmall = lax.dynamic_update_slice(gsmall, fixed[:, width:], (length - 8, 0))
    part, gain_part = run_spread(ggate, ginner, gsmall, w_in, w_small, normed_ext)
    grad_normed = lax.psum_scatter(part, "col", scatter_dimension=0, tiled=True)
    normed = normed_ext[:length]
    grads = (
        tn(normed, gsmall).astype(BF16),
        tn(normed, ggate).astype(BF16),
        tn(cot_all, gated_normed).astype(BF16),
        tn(normed, ginner).astype(BF16),
    )
    gsm, gz, gout, gx, par, par_h, par_s, gain_sum = reduce_grads(grads, (par, par_h, par_s, gain_part), scols)
    zx, gbc, gdt, gout, ci, cib, cs, csb, sb, rl, sg, gg, ng, grad_input = run_finish(
        nheads, gsm, gz, gx, gout, par, par_h, par_s, gain_sum, norm_gain, block_input, cotangent, grad_normed
    )
    return (
        block_output, grad_input, ng[0], zx, gbc, gdt.T, ci, cib[0], cs, csb[0], sb[0], rl[0], sg[0], gg[0], gout.T,
    )


def solution(mesh):
    shards = ("dp", "row")
    tokens = P(("dp", "row", "col"), None)
    zx = P(shards, None, "col")
    in_specs = (
        tokens, P(("dp", "row", "col")), P(), zx, P(shards, None), P(shards, "col"), P(None, "col"), P("col"),
        P(), P(), P("col"), P("col"), P("col"), P("col"), P("col", shards), tokens,
    )
    out_specs = (
        tokens, tokens, P(), zx, P(shards, None), P(shards, "col"), P(None, "col"), P("col"),
        P(), P(), P("col"), P("col"), P("col"), P("col"), P("col", shards),
    )
    return jax.shard_map(per_device, mesh=mesh, in_specs=in_specs, out_specs=out_specs, check_vma=False)
```

```python
import functools
import jax, jax.numpy as jnp
from jax import lax
from jax.experimental import pallas as pl
from jax.experimental.pallas import tpu as pltpu
from jax.sharding import PartitionSpec as P

F32, BF16 = jnp.float32, jnp.bfloat16
HIGH = lax.Precision.HIGHEST
SPAN = 256
HALO = 16
EPS = 1e-5


def nn(a, b):
    return lax.dot_general(a, b, (((1,), (0,)), ((), ())), preferred_element_type=F32)


def nt(a, b):
    return lax.dot_general(a, b, (((1,), (1,)), ((), ())), preferred_element_type=F32)


def tn(a, b):
    return lax.dot_general(a, b, (((0,), (0,)), ((), ())), preferred_element_type=F32)


def iota(shape, axis):
    return lax.broadcasted_iota(jnp.int32, shape, axis)


def split_dot(a, b01):
    hi = a.astype(BF16)
    lo = (a - hi.astype(F32)).astype(BF16)
    return nn(hi, b01) + nn(lo, b01)


def sigmoid(v):
    return 1.0 / (1.0 + jnp.exp(-v))


def softplus(v):
    return jnp.maximum(v, 0.0) + jnp.log1p(jnp.exp(-jnp.abs(v)))


def columns(row):
    return jnp.broadcast_to(row, (128, row.shape[1])).T


def segments(seg_row, prev_row, tail_row):
    row = seg_row[0:1].astype(F32)
    seg = columns(row)[:, 0:1]
    length = row.shape[1]
    prev = columns(prev_row[0:1].astype(F32))[length - 8 :, 0:1]
    tail = tail_row[0:1, length - 1 :].astype(F32)
    return row, seg, prev, tail


def chunk_links(segc, halo):
    ext = jnp.concatenate([halo, segc], axis=0)
    length = segc.shape[0]
    return [(ext[8 - j : 8 - j + length] == segc).astype(F32) for j in range(1, 4)]


def conv_tile(cur, halo, links, taps, sl):
    v = jnp.concatenate([halo[HALO - 8 :, sl].astype(F32), cur[:, sl].astype(F32)], axis=0)
    length = cur.shape[0]
    shifted = [v[8 - j : 8 - j + length] * links[j - 1] for j in range(1, 4)]
    pre = taps[4:5, sl] + taps[3:4, sl] * v[8:]
    for j in range(1, 4):
        pre = pre + taps[3 - j : 4 - j, sl] * shifted[j - 1]
    return pre, [v[8:]] + shifted


def pick(lo, cols, h):
    return jnp.where(lo, cols[:, h : h + 1], cols[:, h + 1 : h + 2])


def forward_kernel(
    inner, inner_halo, shared, shared_halo, step_raw, seg_row, seg_prev, seg_tail, taps, taps_s, heads,
    y_out, x_out, bc_out, dt_out, c_out, ct_out, dec_out, enter_out, final_out, state, total,
):
    k = pl.program_id(0)
    length, width = inner.shape
    pairs = width // 128
    state_dim = state.shape[0]

    @pl.when(k == 0)
    def _():
        state[...] = jnp.zeros_like(state)
        total[...] = jnp.zeros_like(total)

    segr, seg, seg_halo, tail_seg = segments(seg_row, seg_prev, seg_tail)
    links = chunk_links(seg, seg_halo)
    closing = (seg == seg[length - 1 :]).astype(F32)
    entering = (seg == seg_halo[7:]).astype(F32)
    kept = (seg[length - 1 :] == seg_halo[7:]).astype(F32)
    dt = softplus(step_raw[...] + heads[0:1])
    log_decay = -jnp.exp(heads[1:2]) * dt
    rows, cols = iota((length, length), 0), iota((length, length), 1)
    lower = (rows >= cols).astype(F32)
    c = jnp.dot(lower, log_decay, precision=HIGH, preferred_element_type=F32)
    ct = c.T
    dt_out[...] = dt
    c_out[...] = c
    ct_out[...] = ct[: ct_out.shape[0]]
    whole = c + total[0:1]
    dec_out[...] = jnp.exp(whole) * (seg == tail_seg).astype(F32)
    total[0:1] = whole[length - 1 :]
    for half in range(2):
        sl = slice(half * state_dim, (half + 1) * state_dim)
        pre, _ = conv_tile(shared, shared_halo, links, taps_s, sl)
        bc_out[:, sl] = (pre * sigmoid(pre)).astype(BF16)
    b = bc_out[:, :state_dim]
    cc = bc_out[:, state_dim:]
    scores = jnp.where((rows >= cols) & (seg == segr), nt(cc, b), 0.0)
    lo = iota((length, 128), 1) < 64
    enter_out[...] = state[...].astype(BF16)
    for p in range(pairs):
        sl = slice(p * 128, (p + 1) * 128)
        pre, _ = conv_tile(inner, inner_halo, links, taps, sl)
        xp = pre * sigmoid(pre)
        xb = xp.astype(BF16)
        x_out[:, sl] = xb
        xdt = xb.astype(F32) * pick(lo, dt, 2 * p)
        cb = pick(lo, c, 2 * p)
        acc = nn(cc, state[:, sl].astype(BF16)) * (jnp.exp(cb) * entering)
        for a in range(2):
            h = 2 * p + a
            weights = jnp.exp(jnp.minimum(c[:, h : h + 1] - ct[h : h + 1], 0.0)) * scores
            mine = lo if a == 0 else ~lo
            acc = acc + nn(weights.astype(BF16), jnp.where(mine, xdt, 0.0).astype(BF16))
        y_out[:, sl] = acc
        last = cb[length - 1 :]
        leaving = jnp.exp(last - cb) * closing * xdt
        state[:, sl] = state[:, sl] * (jnp.exp(last) * kept) + tn(b, leaving.astype(BF16))

    @pl.when(k == pl.num_programs(0) - 1)
    def _():
        final_out[...] = state[...]


def halo_index(chunk, chunks):
    return jnp.where(chunk == 0, chunks * (SPAN // HALO), chunk * (SPAN // HALO) - 1)


def seg_specs(at, chunks):
    return [
        pl.BlockSpec((8, SPAN), lambda k: (at(k), 0)),
        pl.BlockSpec((8, SPAN), lambda k: (jnp.where(at(k) == 0, chunks, at(k) - 1), 0)),
        pl.BlockSpec((8, SPAN), lambda k: (chunks, 0)),
    ]


def run_forward(both_ext, shared_ext, step_raw, seg, taps, taps_s, heads):
    width = taps.shape[1]
    scols = taps_s.shape[1]
    chunks = seg.shape[0] // 8 - 1
    length = chunks * SPAN
    nrow = 16
    row = lambda k: (k, 0)
    halo = lambda col: (lambda k: (halo_index(k, chunks), col))
    fixed = lambda k: (0, 0)
    S = jax.ShapeDtypeStruct
    return pl.pallas_call(
        forward_kernel,
        grid=(chunks,),
        in_specs=[
            pl.BlockSpec((SPAN, width), lambda k: (k, 1)),
            pl.BlockSpec((HALO, width), halo(1)),
            pl.BlockSpec((SPAN, scols), row),
            pl.BlockSpec((HALO, scols), halo(0)),
            pl.BlockSpec((SPAN, 128), row),
            *seg_specs(lambda k: k, chunks),
            pl.BlockSpec(taps.shape, fixed),
            pl.BlockSpec(taps_s.shape, fixed),
            pl.BlockSpec(heads.shape, fixed),
        ],
        out_specs=[
            pl.BlockSpec((SPAN, width), row),
            pl.BlockSpec((SPAN, width), row),
            pl.BlockSpec((SPAN, scols), row),
            pl.BlockSpec((SPAN, 128), row),
            pl.BlockSpec((SPAN, 128), row),
            pl.BlockSpec((nrow, SPAN), lambda k: (0, k)),
            pl.BlockSpec((SPAN, 128), row),
            pl.BlockSpec((None, scols // 2, width), lambda k: (k, 0, 0)),
            pl.BlockSpec((scols // 2, width), fixed),
        ],
        out_shape=[
            S((length, width), F32),
            S((length, width), BF16),
            S((length, scols), BF16),
            S((length, 128), F32),
            S((length, 128), F32),
            S((nrow, length), F32),
            S((length, 128), F32),
            S((chunks, scols // 2, width), BF16),
            S((scols // 2, width), F32),
        ],
        scratch_shapes=[pltpu.VMEM((scols // 2, width), F32), pltpu.VMEM((8, 128), F32)],
        name="scan_forward",
    )(both_ext, both_ext, shared_ext, shared_ext, step_raw, seg, seg, seg, taps, taps_s, heads)


def row_sums(value):
    hi = value.astype(BF16)
    lo = (value - hi.astype(F32)).astype(BF16)
    ones = jnp.ones((8, value.shape[1]), BF16)
    return nt(ones, hi) + nt(ones, lo)


def first_rows(value):
    return jnp.where(iota(value.shape, 0) == 0, value, 0.0)


def gate_kernel(y, x, bc, dec, start, gate, taps, ssd_out, gated_out, sums_out):
    length, width = x.shape
    state_dim = start.shape[0]
    cc = bc[:, state_dim:]
    lo = iota((length, 128), 1) < 64
    squares = jnp.zeros((length, 128), F32)
    for p in range(width // 128):
        sl = slice(p * 128, (p + 1) * 128)
        corr = nn(cc, start[:, sl].astype(BF16)) * pick(lo, dec, 2 * p)
        ssd = y[:, sl] + corr + taps[6:7, sl] * x[:, sl].astype(F32)
        ssd_out[:, sl] = ssd
        g = gate[:, sl].astype(F32)
        gated = ssd * (g * sigmoid(g))
        gated_out[:, sl] = gated.astype(BF16)
        squares = squares + gated * gated
    sums_out[...] = row_sums(squares)


def run_gate(y, x, bc, dec, start, both_ext, taps):
    length, width = x.shape
    row = lambda k: (k, 0)
    fixed = lambda k: (0, 0)
    S = jax.ShapeDtypeStruct
    return pl.pallas_call(
        gate_kernel,
        grid=(length // SPAN,),
        in_specs=[
            pl.BlockSpec((SPAN, width), row),
            pl.BlockSpec((SPAN, width), row),
            pl.BlockSpec((SPAN, bc.shape[1]), row),
            pl.BlockSpec((SPAN, 128), row),
            pl.BlockSpec(start.shape, fixed),
            pl.BlockSpec((SPAN, width), row),
            pl.BlockSpec(taps.shape, fixed),
        ],
        out_specs=[
            pl.BlockSpec((SPAN, width), row),
            pl.BlockSpec((SPAN, width), row),
            pl.BlockSpec((8, SPAN), lambda k: (0, k)),
        ],
        out_shape=[S((length, width), F32), S((length, width), BF16), S((8, length), F32)],
        name="gate_sums",
    )(y, x, bc, dec, start, both_ext, taps)


def project_kernel(full_width, gated, sums, taps, out_t, normed_out, proj_out):
    rescale = columns(lax.rsqrt(sums[0:1] / full_width + EPS))
    for p in range(gated.shape[1] // 128):
        sl = slice(p * 128, (p + 1) * 128)
        normed_out[:, sl] = (gated[:, sl].astype(F32) * rescale * taps[5:6, sl]).astype(BF16)
    proj_out[...] = nt(normed_out[...], out_t[...]).astype(BF16)


def run_project(full_width, gated, sums, taps, out_t):
    length, width = gated.shape
    row = lambda k: (k, 0)
    fixed = lambda k: (0, 0)
    S = jax.ShapeDtypeStruct
    return pl.pallas_call(
        functools.partial(project_kernel, full_width),
        grid=(length // SPAN,),
        in_specs=[
            pl.BlockSpec((SPAN, width), row),
            pl.BlockSpec((8, SPAN), lambda k: (0, k)),
            pl.BlockSpec(taps.shape, fixed),
            pl.BlockSpec(out_t.shape, fixed),
        ],
        out_specs=[pl.BlockSpec((SPAN, width), row), pl.BlockSpec((SPAN, out_t.shape[0]), row)],
        out_shape=[S((length, width), BF16), S((length, out_t.shape[0]), BF16)],
        name="project",
    )(gated, sums, taps, out_t)


def pull_kernel(cot, out_t, gated, taps, back_out, sums_out):
    back = nn(cot[...], out_t[...])
    back_out[...] = back.astype(BF16)
    inner = jnp.zeros((cot.shape[0], 128), F32)
    for p in range(back.shape[1] // 128):
        sl = slice(p * 128, (p + 1) * 128)
        inner = inner + back[:, sl] * taps[5:6, sl] * gated[:, sl].astype(F32)
    sums_out[...] = row_sums(inner)


def run_pull(cot, out_t, gated, taps):
    length, width = gated.shape
    row = lambda k: (k, 0)
    fixed = lambda k: (0, 0)
    S = jax.ShapeDtypeStruct
    return pl.pallas_call(
        pull_kernel,
        grid=(length // SPAN,),
        in_specs=[
            pl.BlockSpec((SPAN, cot.shape[1]), row),
            pl.BlockSpec(out_t.shape, fixed),
            pl.BlockSpec((SPAN, width), row),
            pl.BlockSpec(taps.shape, fixed),
        ],
        out_specs=[pl.BlockSpec((SPAN, width), row), pl.BlockSpec((8, SPAN), lambda k: (0, k))],
        out_shape=[S((length, width), BF16), S((8, length), F32)],
        name="pull_back",
    )(cot, out_t, gated, taps)


def back_kernel(
    full_width, ssd, x, bc, dec, gate, back, squares, inner, taps,
    dy_out, ggate_out, row_out, colsum_out, dstart_out,
):
    length, width = x.shape
    state_dim = dstart_out.shape[0]

    @pl.when(pl.program_id(0) == 0)
    def _():
        colsum_out[...] = jnp.zeros_like(colsum_out)
        dstart_out[...] = jnp.zeros_like(dstart_out)

    cc = bc[:, state_dim:]
    lo = iota((length, 128), 1) < 64
    rescale = columns(lax.rsqrt(squares[0:1] / full_width + EPS))
    pull = columns(inner[0:1]) * (rescale * rescale * rescale / full_width)
    rowterm = jnp.zeros((length, 128), F32)
    for p in range(width // 128):
        sl = slice(p * 128, (p + 1) * 128)
        s_ssd = ssd[:, sl]
        xp = x[:, sl].astype(F32)
        g = gate[:, sl].astype(F32)
        s = sigmoid(g)
        gated = s_ssd * (g * s)
        bk = back[:, sl].astype(F32)
        gain = taps[5:6, sl]
        gg = rescale * (bk * gain) - gated * pull
        dy = gg * (g * s)
        dyb = dy.astype(BF16)
        dy_out[:, sl] = dyb
        ggate_out[:, sl] = (gg * s_ssd * s * (1.0 + g * (1.0 - s))).astype(BF16)
        colsum_out[5:6, sl] += jnp.sum(bk * gated * rescale, axis=0, keepdims=True)
        colsum_out[6:7, sl] += jnp.sum(dy * xp, axis=0, keepdims=True)
        dstart_out[:, sl] += tn(cc, (dy * pick(lo, dec, 2 * p)).astype(BF16))
        rowterm = rowterm + split_dot(dyb.astype(F32) * (s_ssd - taps[6:7, sl] * xp), head_map(p))
    row_out[...] = rowterm


def head_map(p):
    lane, head = iota((128, 128), 0), iota((128, 128), 1)
    return (head == 2 * p + lane // 64).astype(BF16)


def run_back(full_width, ssd, x, bc, dec, both_ext, back, squares, inner, taps):
    length, width = x.shape
    row = lambda k: (k, 0)
    fixed = lambda k: (0, 0)
    S = jax.ShapeDtypeStruct
    return pl.pallas_call(
        functools.partial(back_kernel, full_width),
        grid=(length // SPAN,),
        in_specs=[
            pl.BlockSpec((SPAN, width), row),
            pl.BlockSpec((SPAN, width), row),
            pl.BlockSpec((SPAN, bc.shape[1]), row),
            pl.BlockSpec((SPAN, 128), row),
            pl.BlockSpec((SPAN, width), row),
            pl.BlockSpec((SPAN, width), row),
            pl.BlockSpec((8, SPAN), lambda k: (0, k)),
            pl.BlockSpec((8, SPAN), lambda k: (0, k)),
            pl.BlockSpec(taps.shape, fixed),
        ],
        out_specs=[
            pl.BlockSpec((SPAN, width), row),
            pl.BlockSpec((SPAN, width), row),
            pl.BlockSpec((SPAN, 128), row),
            pl.BlockSpec((8, width), fixed),
            pl.BlockSpec((bc.shape[1] // 2, width), fixed),
        ],
        out_shape=[
            S((length, width), BF16),
            S((length, width), BF16),
            S((length, 128), F32),
            S((8, width), F32),
            S((bc.shape[1] // 2, width), F32),
        ],
        name="gated_back",
    )(ssd, x, bc, dec, both_ext, back, squares, inner, taps)


def conv_back(dout, pre, shifts, links, taps, sl, carry, carry_links, par_out):
    length = dout.shape[0]
    s = sigmoid(pre)
    dconv = dout * (s * (1.0 + pre * (1.0 - s)))
    nxt = carry[:, sl]
    grad = taps[3:4, sl] * dconv
    above = jnp.zeros((8, dout.shape[1]), F32)
    par_out[3:4, sl] += jnp.sum(dconv * shifts[0], axis=0, keepdims=True)
    par_out[4:5, sl] += jnp.sum(dconv, axis=0, keepdims=True)
    for j in range(1, 4):
        z = dconv * links[j - 1]
        w = taps[3 - j : 4 - j, sl]
        low = jnp.concatenate([z, nxt * carry_links[:, j - 1 : j]], axis=0)
        grad = grad + w * low[j : j + length]
        high = jnp.concatenate([above * 0.0, z[0:8]], axis=0)
        above = above + w * high[j : j + 8]
        par_out[3 - j : 4 - j, sl] += jnp.sum(dconv * shifts[j], axis=0, keepdims=True)
    carry[:, sl] = dconv[0:8]
    return grad, above


def backward_kernel(
    inner, inner_halo, shared, shared_halo, step_raw, seg_row, seg_prev, seg_tail, taps, taps_s, heads,
    dy, x, bc, dt_in, c_in, ct_in, dec_halo, enter, start, row_in, dend, colsum,
    ginner_out, gsmall_out, par_out, par_s_out, par_h_out, edge_out, last_out,
    dstate, carry, carry_s, carry_links, grads_bc,
):
    i = pl.program_id(0)
    k = pl.num_programs(0) - 1 - i
    length, width = x.shape
    state_dim = dstate.shape[0]

    @pl.when(i == 0)
    def _():
        dstate[...] = dend[...]
        carry[...] = jnp.zeros_like(carry)
        carry_s[...] = jnp.zeros_like(carry_s)
        carry_links[...] = jnp.zeros_like(carry_links)
        par_out[...] = colsum[...]
        par_s_out[...] = jnp.zeros_like(par_s_out)
        par_h_out[...] = jnp.zeros_like(par_h_out)

    segr, seg, seg_halo, tail_seg = segments(seg_row, seg_prev, seg_tail)
    links = chunk_links(seg, seg_halo)
    closing = (seg == seg[length - 1 :]).astype(F32)
    entering = (seg == seg_halo[7:]).astype(F32)
    kept = (seg[length - 1 :] == seg_halo[7:]).astype(F32)
    next_links = carry_links[...]
    dt = dt_in[...]
    c = c_in[...]
    ct = ct_in[...]
    first = (k == 0).astype(F32)
    reach = dec_halo[7:8] * (1.0 - first) + first
    b = bc[:, :state_dim]
    cc = bc[:, state_dim:]
    rows, cols = iota((length, length), 0), iota((length, length), 1)
    allowed = (rows <= cols) & (seg == segr)
    scores = jnp.where(allowed, nt(b, cc), 0.0)
    lo = iota((length, 128), 1) < 64
    lo1 = lo[0:1]
    dscores = jnp.zeros((length, length), F32)
    db = jnp.zeros((length, state_dim), F32)
    dc_mat = jnp.zeros((length, state_dim), F32)
    direct = jnp.zeros((length, 128), F32)
    matched = jnp.zeros((length, 128), F32)
    closing_term = jnp.zeros((1, 128), F32)
    for p in range(width // 128):
        sl = slice(p * 128, (p + 1) * 128)
        pre, shifts = conv_tile(inner, inner_halo, links, taps, sl)
        dyb = dy[:, sl]
        dyf = dyb.astype(F32)
        xp = x[:, sl].astype(F32)
        dtb = pick(lo, dt, 2 * p)
        xdt = xp * dtb
        cb = pick(lo, c, 2 * p)
        hm = head_map(p)
        last = cb[length - 1 :]
        entry = enter[:, sl].astype(F32) + start[:, sl] * pick(lo1, reach, 2 * p)
        entryb = entry.astype(BF16)
        ds = dstate[:, sl]
        dsb = ds.astype(BF16)
        leaving = jnp.exp(last - cb) * closing
        bds = nn(b, dsb)
        dxdt = jnp.zeros((length, 128), F32)
        for a in range(2):
            h = 2 * p + a
            mine = lo if a == 0 else ~lo
            decay = jnp.exp(jnp.minimum(ct[h : h + 1] - c[:, h : h + 1], 0.0))
            dscores = dscores + decay * nt(jnp.where(mine, xdt, 0.0).astype(BF16), dyb)
            dxdt = dxdt + nn((decay * scores).astype(BF16), jnp.where(mine, dyf, 0.0).astype(BF16))
        spread = leaving * xdt
        moved = spread * bds
        matched = matched + split_dot(xdt.astype(BF16).astype(F32) * dxdt + moved, hm)
        dxdt = dxdt + leaving * bds
        held = jnp.exp(last) * kept
        col = jnp.sum(moved, axis=0, keepdims=True) + held * jnp.sum(entry * ds, axis=0, keepdims=True)
        closing_term = closing_term + split_dot(jnp.broadcast_to(col, (8, 128)), hm)[0:1]
        direct = direct + split_dot(xp * dxdt, hm)
        edy = (jnp.exp(cb) * entering * dyf).astype(BF16)
        db = db + nt(spread.astype(BF16), dsb)
        dc_mat = dc_mat + nt(edy, entryb)
        dstate[:, sl] = ds * held + tn(cc, edy)
        dx = dtb * dxdt + taps[6:7, sl] * dyf
        grad, above = conv_back(dx, pre, shifts, links, taps, sl, carry, next_links, par_out)
        ginner_out[:, sl] = grad.astype(BF16)
        edge_out[:, sl] = above

        @pl.when(i == 0)
        def _():
            last_out[:, sl] = grad[length - 8 :]

    dsc = jnp.where(allowed, dscores, 0.0).astype(BF16)
    grads_bc[:, :state_dim] = db + nn(dsc, cc)
    grads_bc[:, state_dim:] = dc_mat + tn(dsc, b)
    for half in range(2):
        sl = slice(half * state_dim, (half + 1) * state_dim)
        pre, shifts = conv_tile(shared, shared_halo, links, taps_s, sl)
        grad, above = conv_back(grads_bc[:, sl], pre, shifts, links, taps_s, sl, carry_s, next_links, par_s_out)
        gsmall_out[:, sl] = grad.astype(BF16)
        at = slice(width + half * state_dim, width + (half + 1) * state_dim)
        edge_out[:, at] = above

        @pl.when(i == 0)
        def _():
            last_out[:, at] = grad[length - 8 :]

    for j in range(3):
        carry_links[:, j : j + 1] = links[j][0:8]
    dcum = row_in[...] - matched
    upper = (rows <= cols).astype(F32)
    dlog = jnp.dot(upper, dcum, precision=HIGH, preferred_element_type=F32) + closing_term
    rate = -jnp.exp(heads[1:2])
    dstep = (direct + dlog * rate) * sigmoid(step_raw[...] + heads[0:1])
    gsmall_out[:, 2 * state_dim :] = dstep.astype(BF16)
    par_h_out[0:1] += jnp.sum(dstep, axis=0, keepdims=True)
    par_h_out[1:2] += jnp.sum(dlog * (rate * dt), axis=0, keepdims=True)


def run_backward(
    both_ext, shared_ext, step_raw, seg, taps, taps_s, heads,
    dy, x, bc, dt, c, ct, dec, enter, start, rowterm, dend, colsum,
):
    length, width = x.shape
    scols = bc.shape[1]
    chunks = length // SPAN
    at = lambda i: chunks - 1 - i
    row = lambda i: (at(i), 0)
    halo = lambda col: (lambda i: (halo_index(at(i), chunks), col))
    fixed = lambda i: (0, 0)
    S = jax.ShapeDtypeStruct
    return pl.pallas_call(
        backward_kernel,
        grid=(chunks,),
        in_specs=[
            pl.BlockSpec((SPAN, width), lambda i: (at(i), 1)),
            pl.BlockSpec((HALO, width), halo(1)),
            pl.BlockSpec((SPAN, scols), row),
            pl.BlockSpec((HALO, scols), halo(0)),
            pl.BlockSpec((SPAN, 128), row),
            *seg_specs(at, chunks),
            pl.BlockSpec(taps.shape, fixed),
            pl.BlockSpec(taps_s.shape, fixed),
            pl.BlockSpec(heads.shape, fixed),
            pl.BlockSpec((SPAN, width), row),
            pl.BlockSpec((SPAN, width), row),
            pl.BlockSpec((SPAN, scols), row),
            pl.BlockSpec((SPAN, 128), row),
            pl.BlockSpec((SPAN, 128), row),
            pl.BlockSpec((ct.shape[0], SPAN), lambda i: (0, at(i))),
            pl.BlockSpec((8, 128), lambda i: (jnp.maximum(at(i) * (SPAN // 8) - 1, 0), 0)),
            pl.BlockSpec((None, scols // 2, width), lambda i: (at(i), 0, 0)),
            pl.BlockSpec(start.shape, fixed),
            pl.BlockSpec((SPAN, 128), row),
            pl.BlockSpec(dend.shape, fixed),
            pl.BlockSpec(colsum.shape, fixed),
        ],
        out_specs=[
            pl.BlockSpec((SPAN, width), row),
            pl.BlockSpec((SPAN, scols + 128), row),
            pl.BlockSpec((8, width), fixed),
            pl.BlockSpec((8, scols), fixed),
            pl.BlockSpec((8, 128), fixed),
            pl.BlockSpec((8, width + scols), fixed),
            pl.BlockSpec((8, width + scols), fixed),
        ],
        out_shape=[
            S((length, width), BF16),
            S((length, scols + 128), BF16),
            S((8, width), F32),
            S((8, scols), F32),
            S((8, 128), F32),
            S((8, width + scols), F32),
            S((8, width + scols), F32),
        ],
        scratch_shapes=[
            pltpu.VMEM((scols // 2, width), F32),
            pltpu.VMEM((8, width), F32),
            pltpu.VMEM((8, scols), F32),
            pltpu.VMEM((8, 128), F32),
            pltpu.VMEM((SPAN, scols), F32),
        ],
        name="scan_backward",
    )(both_ext, both_ext, shared_ext, shared_ext, step_raw, seg, seg, seg, taps, taps_s, heads,
      dy, x, bc, dt, c, ct, dec, enter, start, rowterm, dend, colsum)


def spread_kernel(ggate, ginner, gsmall, w_in, w_small, normed, part_out, gain_out):
    width = ggate.shape[1]
    part = nt(ggate[...], w_in[:, :width]) + nt(ginner[...], w_in[:, width:]) + nt(gsmall[...], w_small[...])
    part_out[...] = part.astype(BF16)
    gain_out[...] = first_rows(jnp.broadcast_to(
        jnp.sum(part * normed[...].astype(F32), axis=0, keepdims=True), gain_out.shape))


def run_spread(ggate, ginner, gsmall, w_in, w_small, normed_ext):
    length = ggate.shape[0]
    model = w_in.shape[0]
    tile = 256
    fixed = lambda n: (0, 0)
    down = lambda n: (n, 0)
    across = lambda n: (0, n)
    S = jax.ShapeDtypeStruct
    return pl.pallas_call(
        spread_kernel,
        grid=(model // tile,),
        in_specs=[
            pl.BlockSpec(ggate.shape, fixed),
            pl.BlockSpec(ginner.shape, fixed),
            pl.BlockSpec(gsmall.shape, fixed),
            pl.BlockSpec((tile, w_in.shape[1]), down),
            pl.BlockSpec((tile, w_small.shape[1]), down),
            pl.BlockSpec((length, tile), across),
        ],
        out_specs=[pl.BlockSpec((length, tile), across), pl.BlockSpec((8, tile), across)],
        out_shape=[S((length, model), BF16), S((8, model), F32)],
        name="spread_back",
    )(ggate, ginner, gsmall, w_in, w_small, normed_ext)


MESH = pl.DeviceIdType.MESH
ANY = pl.BlockSpec(memory_space=pl.ANY)


def remote(src, dst, send, recv, **to):
    return pltpu.make_async_remote_copy(
        src_ref=src, dst_ref=dst, send_sem=send, recv_sem=recv, device_id=to, device_id_type=MESH
    )


def greet(barrier, when, **to):
    @pl.when(when)
    def _():
        pl.semaphore_signal(barrier, inc=1, device_id=to, device_id_type=MESH)


PIECES = 2


def gather_kernel(
    ncol, ndp,
    tokens_in, gain, seg_in, w0, w1, w2,
    all_out, seg_out, w0_out, w1_out, w2_out,
    z_send, z_recv, w_send, c_send, w_recv, t_send, t_recv, here, own, seg_own, zero_tail, no_seg,
):
    dp, row, z = lax.axis_index("dp"), lax.axis_index("row"), lax.axis_index("col")
    other = 1 - row
    last = ncol - 1
    tokens, tail, part = own.shape[0], zero_tail.shape[0], own.shape[0] // PIECES
    weights = ((w0, w0_out), (w1, w1_out), (w2, w2_out))
    rows = w0.shape[0]
    sends_tail = (row == 0) & (z == last)

    barrier = pltpu.get_barrier_semaphore()
    greet(barrier, z > 0, col=z - 1)
    greet(barrier, z < last, col=z + 1)
    greet(barrier, row >= 0, row=other)
    for m in range(1, ndp):
        greet(barrier, row >= 0, dp=dp ^ m)
    greet(barrier, row == 1, row=0, col=last)
    for c in range(ncol):
        greet(barrier, sends_tail, row=1, col=c)
    count = (z > 0).astype(jnp.int32) + (z < last).astype(jnp.int32) + ndp
    count = count + row + jnp.where(sends_tail, ncol, 0)
    seg_own[...] = jnp.broadcast_to(seg_in[...], seg_own.shape)
    no_seg[...] = jnp.full(no_seg.shape, -1, jnp.int32)
    zero_tail[...] = jnp.zeros_like(zero_tail)

    def normalize(step, carry):
        at = pl.ds(pl.multiple_of(step * 32, 32), 32)
        wide = tokens_in[at].astype(F32)
        scale = lax.rsqrt(jnp.sum(wide * wide, axis=1, keepdims=True) / wide.shape[1] + EPS)
        own[at] = (wide * scale * gain[...]).astype(BF16)
        return carry

    lax.fori_loop(0, tokens // 32, normalize, 0)
    pl.semaphore_wait(barrier, count)

    def token_copies(s, mine, way, which=None):
        target = z + 1 if way == 0 else z - 1
        copies = []
        for i in range(PIECES + 1) if which is None else which:
            if i < PIECES:
                dst = all_out.at[pl.ds(s * tokens + i * part, part)]
                src = own.at[pl.ds(i * part, part)] if mine else dst
            else:
                dst = seg_out.at[pl.ds(s * 8, 8)]
                src = seg_own if mine else dst
            copies.append(remote(src, dst, z_send.at[way, s, i], z_recv.at[s, i], col=target))
        return copies

    def weight_copies(j, mine, send, **to):
        copies = []
        for i, (src, dst) in enumerate(weights):
            place = dst.at[pl.ds(j * rows, rows)]
            copies.append(remote(src if mine else place, place, send.at[i], w_recv.at[j, i], **to))
        return copies

    def tail_copies(c):
        return [
            remote(own.at[pl.ds(tokens - tail, tail)], all_out.at[pl.ds(ncol * tokens, tail)],
                   t_send.at[c, 0], t_recv.at[0], row=1, col=c),
            remote(seg_own, seg_out.at[pl.ds(ncol * 8, 8)], t_send.at[c, 1], t_recv.at[1], row=1, col=c),
        ]

    def start(copies):
        for copy in copies:
            copy.start()

    def guarded(when, action):
        @pl.when(when)
        def _():
            action()

    me = dp * 2 + row
    guarded(z < last, lambda: start(token_copies(z, True, 0)))
    guarded(z > 0, lambda: start(token_copies(z, True, 1)))
    for m in range(1, ndp):
        start(weight_copies(me, True, w_send.at[m], dp=dp ^ m))
    start(weight_copies(me, True, c_send.at[0], row=other))
    for c in range(ncol):
        guarded(sends_tail, lambda c=c: start(tail_copies(c)))
    local = [
        pltpu.make_async_copy(own, all_out.at[pl.ds(z * tokens, tokens)], here.at[0]),
        pltpu.make_async_copy(seg_own, seg_out.at[pl.ds(z * 8, 8)], here.at[1]),
    ]
    for i, (src, dst) in enumerate(weights):
        local.append(pltpu.make_async_copy(src, dst.at[pl.ds(me * rows, rows)], here.at[2 + i]))
    start(local)
    fill = [
        pltpu.make_async_copy(zero_tail, all_out.at[pl.ds(ncol * tokens, tail)], here.at[5]),
        pltpu.make_async_copy(no_seg, seg_out.at[pl.ds(ncol * 8, 8)], here.at[6]),
    ]
    guarded(row == 0, lambda: start(fill))

    def pass_tokens(s):
        for which in [(i,) for i in range(PIECES - 1)] + [(PIECES - 1, PIECES)]:

            def from_below(which=which):
                for copy in token_copies(z - s, False, 0, which):
                    copy.wait_recv()
                guarded(z < last, lambda: start(token_copies(z - s, False, 0, which)))

            def from_above(which=which):
                for copy in token_copies(z + s, False, 1, which):
                    copy.wait_recv()
                guarded(z > 0, lambda: start(token_copies(z + s, False, 1, which)))

            guarded(z - s >= 0, from_below)
            guarded(z + s <= last, from_above)

    def pass_weights(m):
        j = (dp ^ m) * 2 + row
        for copy in weight_copies(j, False, w_send.at[m], dp=dp ^ m):
            copy.wait_recv()
        start(weight_copies(j, False, c_send.at[m], row=other))

    done = 0
    for s in range(1, ncol):
        pass_tokens(s)
        upto = (ndp - 1) * s // (ncol - 2) if s < ncol - 1 else ndp - 1
        for m in range(done + 1, upto + 1):
            pass_weights(m)
        done = max(done, upto)
    for m in range(ndp):
        j = (dp ^ m) * 2 + other
        for copy in weight_copies(j, False, c_send.at[m], row=other):
            copy.wait_recv()
    guarded(row == 1, lambda: [copy.wait_recv() for copy in tail_copies(0)])
    for m in range(ndp):
        if m:
            for copy in weight_copies(me, True, w_send.at[m], dp=dp ^ m):
                copy.wait_send()
        for copy in weight_copies((dp ^ m) * 2 + row, m == 0, c_send.at[m], row=other):
            copy.wait_send()
    for s in range(ncol):
        for way in range(2):
            open_way = z < last if way == 0 else z > 0
            mine = (z - s >= 0) if way == 0 else (z + s <= last)
            src = z - s if way == 0 else z + s

            def drain(way=way, src=src, s=s):
                for copy in token_copies(src, s == 0, way):
                    copy.wait_send()

            guarded(open_way & mine, drain)
    for c in range(ncol):
        guarded(sends_tail, lambda c=c: [copy.wait_send() for copy in tail_copies(c)])
    for copy in local:
        copy.wait()
    guarded(row == 0, lambda: [copy.wait() for copy in fill])


def gather_inputs(tokens_in, gain, seg, w0, w1, w2):
    ncol, ndp = lax.axis_size("col"), lax.axis_size("dp")
    tokens, width = tokens_in.shape
    S = jax.ShapeDtypeStruct
    shards = 2 * ndp
    dma = pltpu.SemaphoreType.DMA
    vmem = pl.BlockSpec(memory_space=pltpu.VMEM)
    return pl.pallas_call(
        functools.partial(gather_kernel, ncol, ndp),
        in_specs=[vmem] * 3 + [ANY] * 3,
        out_specs=[ANY] * 5,
        out_shape=[
            S((ncol * tokens + HALO, width), BF16),
            S(((ncol + 1) * 8, tokens), jnp.int32),
        ] + [S((shards * w.shape[0], w.shape[1]), w.dtype) for w in (w0, w1, w2)],
        scratch_shapes=[
            dma((2, ncol, PIECES + 1)), dma((ncol, PIECES + 1)), dma((ndp, 3)), dma((ndp, 3)), dma((shards, 3)),
            dma((ncol, 2)), dma((2,)), dma((7,)),
            pltpu.VMEM((tokens, width), BF16), pltpu.VMEM((8, tokens), jnp.int32),
            pltpu.VMEM((HALO, width), BF16), pltpu.VMEM((8, tokens), jnp.int32),
        ],
        compiler_params=pltpu.CompilerParams(collective_id=1, has_side_effects=True),
        cost_estimate=pl.CostEstimate(flops=0, bytes_accessed=200_000_000, transcendentals=0),
        name="gather_inputs",
    )(tokens_in, gain[None], seg[None], w0, w1, w2)


def sum_col_kernel(ncol, value, out, slots, send, recv):
    z = lax.axis_index("col")
    barrier = pltpu.get_barrier_semaphore()
    for s in range(1, ncol):
        pl.semaphore_signal(barrier, inc=1, device_id={"col": lax.rem(z + s, ncol)}, device_id_type=MESH)
    pl.semaphore_wait(barrier, ncol - 1)
    copies = [
        remote(value, slots.at[z], send.at[s], recv.at[z], col=lax.rem(z + s, ncol)) for s in range(1, ncol)
    ]
    for copy in copies:
        copy.start()
    total = value[...]
    for s in range(1, ncol):
        source = lax.rem(z + s, ncol)
        remote(value, slots.at[source], send.at[s], recv.at[source], col=source).wait_recv()
        total = total + slots[source]
    out[...] = total
    for copy in copies:
        copy.wait_send()


def sum_col(value, collective_id):
    ncol = lax.axis_size("col")
    dma = pltpu.SemaphoreType.DMA
    vmem = pl.BlockSpec(memory_space=pltpu.VMEM)
    return pl.pallas_call(
        functools.partial(sum_col_kernel, ncol),
        in_specs=[vmem],
        out_specs=vmem,
        out_shape=jax.ShapeDtypeStruct(value.shape, F32),
        scratch_shapes=[pltpu.VMEM((ncol,) + value.shape, F32), dma((ncol,)), dma((ncol,))],
        compiler_params=pltpu.CompilerParams(collective_id=collective_id, has_side_effects=True),
        name="sum_col",
    )(value)


class LineReduce:
    def __init__(self, ncol, z, source, local, inbox, send, recv):
        self.ncol, self.z, self.last = ncol, z, ncol - 1
        self.source, self.local, self.inbox = source, local, inbox
        self.send, self.recv = send, recv
        self.tokens = local.shape[0] // ncol
        self.part = self.tokens // PIECES

    def rows(self, way, t, p):
        d = self.last - t if way == 0 else t
        return pl.multiple_of(d * self.tokens + p * self.part, self.part)

    def copy(self, way, t, p, first):
        src = self.source.at[pl.ds(self.rows(way, t, p), self.part)] if first else self.inbox.at[way, t, p]
        to = self.z + 1 if way == 0 else self.z - 1
        return remote(src, self.inbox.at[way, t, p], self.send.at[way, t, p], self.recv.at[way, t, p], col=to)

    def edge(self, way):
        return self.z == (0 if way == 0 else self.last)

    def depth(self, way):
        return self.z if way == 0 else self.last - self.z

    def start(self):
        for way in range(2):

            @pl.when(self.edge(way))
            def _(way=way):
                for t in range(self.last):
                    for p in range(PIECES):
                        self.copy(way, t, p, True).start()

    ticks = property(lambda self: self.last * PIECES)

    def tick(self, tau):
        for stage in range(2):
            for way in range(2):
                depth = self.depth(way)
                index = tau - depth
                t, p = index // PIECES, lax.rem(index, PIECES)

                @pl.when((depth > 0) & (index >= 0) & (index < (self.ncol - depth) * PIECES))
                def _(way=way, depth=depth, t=t, p=p, stage=stage):
                    onward = t < self.last - depth
                    if stage == 0:
                        self.copy(way, t, p, False).wait_recv()

                        @pl.when(onward)
                        def _():
                            base = self.rows(way, t, p)

                            def add(k, carry):
                                at = pl.multiple_of(k * 16, 16)
                                mine = self.local[pl.ds(pl.multiple_of(base + at, 16), 16)].astype(F32)
                                here = pl.ds(at, 16)
                                self.inbox[way, t, p, here] = (self.inbox[way, t, p, here].astype(F32) + mine).astype(BF16)
                                return carry

                            lax.fori_loop(0, self.part // 16, add, 0)
                    else:

                        @pl.when(onward)
                        def _():
                            self.copy(way, t, p, False).start()

    def total(self, store):
        z, last = self.z, self.last
        for p in range(PIECES):

            def add(k, carry, p=p):
                at = pl.multiple_of(k * 16, 16)
                here = pl.ds(at, 16)
                row = p * self.part + at
                value = self.local[pl.ds(pl.multiple_of(z * self.tokens + row, 16), 16)].astype(F32)
                low = self.inbox[0, jnp.minimum(last - z, last - 1), p, here].astype(F32)
                high = self.inbox[1, jnp.minimum(z, last - 1), p, here].astype(F32)
                value = value + jnp.where(z > 0, low, 0.0) + jnp.where(z < last, high, 0.0)
                store(row, value)
                return carry

            lax.fori_loop(0, self.part // 16, add, 0)

    def drain(self):
        for way in range(2):
            depth = self.depth(way)
            for t in range(self.last):

                @pl.when((depth < self.last) & (t < self.last - depth))
                def _(way=way, t=t):
                    for p in range(PIECES):
                        self.copy(way, t, p, False).wait_send()


def line_scratch(ncol, tokens, width):
    shape = (2, ncol - 1, PIECES)
    dma = pltpu.SemaphoreType.DMA
    return [pltpu.VMEM(shape + (tokens // PIECES, width), BF16), dma(shape), dma(shape)]


def reduce_kernel(ncol, ndp, scols, *refs):
    count = 4
    refs = list(refs)

    def take(number):
        taken = refs[:number]
        del refs[:number]
        return taken

    sources = take(7)
    vecs = take(4)
    r, vec_outs, gsum_out = take(count), take(4), refs.pop(0)
    held = take(7)
    (line_box, line_send, line_recv) = take(3)
    g, near, sent, far = take(count), take(count), take(count), take(count)
    vec_slots, col_slots = take(4), take(2)
    bc_slots, load, c_send, c_recv, p_send, p_recv, v_send, v_recv, u_send, u_recv, b_send, b_recv = refs
    dp, row, z = lax.axis_index("dp"), lax.axis_index("row"), lax.axis_index("col")
    other = 1 - row
    me = dp * 2 + row
    rows = [out.shape[0] for out in r]
    barrier = pltpu.get_barrier_semaphore()
    for q in range(1, 2 * ndp):
        greet(barrier, row >= 0, dp=dp ^ (q >> 1), row=row ^ (q & 1))
    for s in range(1, ncol):
        greet(barrier, row >= 0, col=lax.rem(z + s, ncol))
    loads = []
    for i, (src, dst) in enumerate(zip(sources, held)):
        src = src.at[pl.ds(0, dst.shape[0])]
        loads.append(pltpu.make_async_copy(src, dst, load.at[i]))
        loads[-1].start()
    normed, gsmall, ggate, cot, gnorm, ginner, part = held
    pl.semaphore_wait(barrier, 2 * ndp + ncol - 2)
    line = LineReduce(ncol, z, sources[6], part, line_box, line_send, line_recv)
    line.start()

    order = (0, 1, 2, 3)
    turns = [3, 1, 2, 0] if ndp == 4 else list(range(1, ndp)) + [0]

    def core_copy(i, d):
        return remote(g[i].at[pl.ds((d * 2 + other) * rows[i], rows[i])], near[i].at[d],
                      c_send.at[i, d], c_recv.at[i, d], row=other)

    def vec_copy(q, i, j):
        return remote(vecs[i], vec_slots[i].at[j], v_send.at[q, i], v_recv.at[j, i],
                      dp=dp ^ (q >> 1), row=row ^ (q & 1))

    for q in range(1, 2 * ndp):
        for i in range(4):
            vec_copy(q, i, me).start()

    waiting = []

    def later(copy):
        if waiting:
            waiting.pop().start()
        if copy is not None:
            waiting.append(copy)

    def accumulate(i, first, number, terms, store):
        def step(k, carry):
            at = first + pl.multiple_of(k * 16, 16)
            total = terms[0](at)
            for term in terms[1:]:
                total = total + term(at)
            store(at, total)
            return carry

        lax.fori_loop(0, number // 16, step, 0)

    def read(ref, index, shift=0):
        return lambda at: ref[index, pl.ds(at - shift, 16)].astype(F32)

    def mine(i, d):
        return lambda at: g[i][pl.ds(pl.multiple_of((d * 2 + row) * rows[i] + at, 16), 16)].astype(F32)

    def write(ref, index, shift):
        def store(at, total):
            ref[index, pl.ds(at - shift, 16)] = total.astype(BF16)

        return store

    def arrived(i, d):
        core_copy(i, d).wait_recv()

    model = normed.shape[1]
    block = model // 4
    ends = [[] for _ in range(4)]
    products = ((normed, gsmall), (normed, ggate), (cot, gnorm), (normed, ginner))
    ready = {0: (0, 1), 1: (2,), 2: (3, 4), 3: (5,)}
    ticks = list(range(1, line.ticks + 1))
    loaded = [False]
    for i in order:
        for at in ready[i]:
            loads[at].wait()
        left, right = products[i]
        for m in ([3, 1, 2, 0] if ndp == 4 else range(4)):
            b = dp ^ m if ndp == 4 else m
            first = pl.multiple_of(b * block, 128)
            g[i][pl.ds(pl.multiple_of(b * block, 16), block)] = tn(left[:, pl.ds(first, block)], right[...]).astype(BF16)
            if ndp == 4:
                later(core_copy(i, b))
        if i == 1:
            loads[6].wait()
            line.tick(ticks.pop(0))
        if i == 3 and ticks:
            line.tick(ticks.pop(0))
    later(None)
    if ndp != 4:
        for i in order:
            for m in turns:
                core_copy(i, dp ^ m).start()

    def tick():
        if ticks:
            line.tick(ticks.pop(0))

    if ndp == 4:
        halves = ((0, 1, 2), (1, 2, 1))

        def leg(i, slot, m):
            return remote(sent[i].at[slot], far[i].at[slot], p_send.at[i, slot], p_recv.at[i, slot], dp=dp ^ m)

        for i in order:
            half = rows[i] // 2
            arrived(i, dp ^ 3)
            for h, m1, m2 in halves:
                accumulate(i, h * half, half, [mine(i, dp ^ 3), read(near[i], dp ^ 3)],
                           write(sent[i], 3 * h + 1, h * half))
                later(leg(i, 3 * h + 1, m1))
            for h, m1, m2 in halves:
                arrived(i, dp ^ m1)
                accumulate(i, h * half, half, [mine(i, dp ^ m1), read(near[i], dp ^ m1)],
                           write(sent[i], 3 * h, h * half))
                later(leg(i, 3 * h, m1))
        later(None)

        def relay(i):
            half = rows[i] // 2
            for h, m1, m2 in halves:
                leg(i, 3 * h + 1, m1).wait_recv()
                accumulate(i, h * half, half,
                           [mine(i, dp ^ m2), read(near[i], dp ^ m2), read(far[i], 3 * h + 1, h * half)],
                           write(sent[i], 3 * h + 2, h * half))
                later(leg(i, 3 * h + 2, m2))

        def finish(i, store):
            half = rows[i] // 2
            for h, m1, m2 in halves:
                leg(i, 3 * h, m1).wait_recv()
                leg(i, 3 * h + 2, m2).wait_recv()
                accumulate(i, h * half, half,
                           [mine(i, dp), read(near[i], dp), read(far[i], 3 * h, h * half),
                            read(far[i], 3 * h + 2, h * half)], store)

        sends = [leg(i, 3 * h + k, m2 if k == 2 else m1) for i in order for h, m1, m2 in halves for k in range(3)]
    else:

        def peer(i, m):
            return remote(sent[i].at[m], far[i].at[m], p_send.at[i, m], p_recv.at[i, m], dp=dp ^ m)

        for i in order:
            for m in turns[:-1]:
                arrived(i, dp ^ m)
                accumulate(i, 0, rows[i], [mine(i, dp ^ m), read(near[i], dp ^ m)], write(sent[i], m, 0))
                later(peer(i, m))
        later(None)

        def relay(i):
            pass

        def finish(i, store):
            for m in range(1, ndp):
                peer(i, m).wait_recv()
            accumulate(i, 0, rows[i],
                       [mine(i, dp), read(near[i], dp)] + [read(far[i], m) for m in range(1, ndp)], store)

        sends = [peer(i, m) for i in order for m in range(1, ndp)]

    for i in order:
        arrived(i, dp)
    tick()
    for q in range(1, 2 * ndp):
        for i in range(4):
            vec_copy(q, i, me ^ q).wait_recv()
    for i in range(4):
        vec_slots[i][me] = vecs[i][...]
        total = vec_slots[i][0]
        for j in range(1, 2 * ndp):
            total = total + vec_slots[i][j]
        if i < 2:
            vec_outs[i][...] = total
        else:
            col_slots[i - 2][z] = total

    def plain(i):
        def store(at, total):
            r[i][pl.ds(at, 16)] = total

        return store

    def shared_rows(at, total):
        r[0][pl.ds(at, 16)] = total
        bc_slots[z, pl.ds(at, 16)] = total[:, : bc_slots.shape[2]].astype(BF16)

    def col_copies(s, source):
        to = lax.rem(z + s, ncol)
        copies = [remote(col_slots[i].at[source], col_slots[i].at[source], u_send.at[s, i], u_recv.at[source, i], col=to)
                  for i in range(2)]
        return copies + [remote(bc_slots.at[source], bc_slots.at[source], b_send.at[s], b_recv.at[source], col=to)]

    relay(0)
    relay(1)
    tick()
    relay(2)
    relay(3)
    later(None)
    finish(0, shared_rows)
    for s in range(1, ncol):
        for copy in col_copies(s, z):
            copy.start()
    while len(ticks) > 1:
        tick()
    finish(1, plain(1))
    finish(2, plain(2))
    finish(3, plain(3))
    while ticks:
        tick()

    def keep(at, value):
        gsum_out[pl.ds(pl.multiple_of(at, 16), 16)] = value.astype(BF16)

    line.total(keep)
    for s in range(1, ncol):
        for copy in col_copies(s, lax.rem(z + s, ncol)):
            copy.wait_recv()
    for i in range(2):
        total = col_slots[i][0]
        for j in range(1, ncol):
            total = total + col_slots[i][j]
        vec_outs[2 + i][...] = total
    total = bc_slots[0].astype(F32)
    for j in range(1, ncol):
        total = total + bc_slots[j].astype(F32)
    r[0][:, : bc_slots.shape[2]] = total

    for q in range(1, 2 * ndp):
        for i in range(4):
            vec_copy(q, i, me).wait_send()
    for i in order:
        for m in turns:
            core_copy(i, dp ^ m).wait_send()
    for copy in sends:
        copy.wait_send()
    for s in range(1, ncol):
        for copy in col_copies(s, z):
            copy.wait_send()
    line.drain()


def reduce_grads(sources, vecs, scols):
    ncol, ndp = lax.axis_size("col"), lax.axis_size("dp")
    dma = pltpu.SemaphoreType.DMA
    vmem = pl.BlockSpec(memory_space=pltpu.VMEM)
    S = jax.ShapeDtypeStruct
    length = sources[1].shape[0]
    model = sources[0].shape[1]
    widths = [sources[1].shape[1], sources[2].shape[1], sources[4].shape[1], sources[5].shape[1]]
    count = len(widths)
    blocks = [(model // (2 * ndp), w) for w in widths]
    near = [pltpu.VMEM((ndp,) + b, BF16) for b in blocks]
    slots = 6 if ndp == 4 else ndp
    legs = [pltpu.VMEM((6, b[0] // 2, b[1]) if ndp == 4 else (ndp,) + b, BF16) for b in blocks]
    tokens = length // ncol
    return pl.pallas_call(
        functools.partial(reduce_kernel, ncol, ndp, scols),
        in_specs=[ANY] * 7 + [vmem] * 4,
        out_specs=[vmem] * (count + 5),
        out_shape=[S(b, F32) for b in blocks] + [S(v.shape, F32) for v in vecs] + [S((tokens, model), BF16)],
        scratch_shapes=[pltpu.VMEM((length, s.shape[1]), BF16) for s in sources]
        + line_scratch(ncol, tokens, model)
        + [pltpu.VMEM((model, w), BF16) for w in widths]
        + near + legs * 2
        + [pltpu.VMEM((2 * ndp,) + v.shape, F32) for v in vecs]
        + [pltpu.VMEM((ncol,) + v.shape, F32) for v in vecs[2:]]
        + [pltpu.VMEM((ncol, blocks[0][0], scols), BF16)]
        + [dma((7,))]
        + [dma((count, ndp))] * 2
        + [dma((count, slots))] * 2
        + [dma((2 * ndp, 4))] * 2
        + [dma((ncol, 2))] * 2
        + [dma((ncol,))] * 2,
        compiler_params=pltpu.CompilerParams(
            collective_id=2, has_side_effects=True, vmem_limit_bytes=60 * 1024 * 1024
        ),
        cost_estimate=pl.CostEstimate(flops=0, bytes_accessed=200_000_000, transcendentals=0),
        name="reduce_grads",
    )(*sources, *vecs)


def finish_kernel(
    nheads, small, gate, inner, out, par, par_h, par_s, gain_sum, gain, tokens, cot, gnormed,
    zx_out, bc_out, dt_out, out_out, ci_out, cib_out, cs_out, csb_out, sb_out, rl_out, sg_out, gg_out, ng_out, gin_out,
):
    width = par.shape[1]
    scols = par_s.shape[1]
    zx_out[:, 0, :] = gate[...]
    zx_out[:, 1, :] = inner[...]
    bc_out[...] = small[:, :scols]
    dt_out[...] = small[:, scols:].T[:nheads]
    out_out[...] = out[...]
    ci_out[...] = par[0:4]
    cib_out[...] = par[4:5]
    gg_out[...] = par[5:6]
    cs_out[...] = par_s[0:4]
    csb_out[...] = par_s[4:5]
    sb_out[...] = par_h[0:1, :nheads]
    rl_out[...] = par_h[1:2, :nheads]
    skip = jnp.zeros((8, 128), F32)
    for p in range(width // 128):
        skip = skip + split_dot(jnp.broadcast_to(par[6:7, p * 128 : (p + 1) * 128], (8, 128)), head_map(p))
    sg_out[...] = skip[0:1, :nheads]
    ng_out[...] = gain_sum[0:1] / gain[...]

    def rows(step, carry):
        at = pl.ds(pl.multiple_of(step * 32, 32), 32)
        wide = tokens[at].astype(F32)
        scale = lax.rsqrt(jnp.sum(wide * wide, axis=1, keepdims=True) / wide.shape[1] + EPS)
        pushed = gnormed[at].astype(F32) * gain[...]
        mean = jnp.sum(pushed * wide, axis=1, keepdims=True) / wide.shape[1]
        grad = scale * pushed - wide * (scale * scale * scale * mean)
        gin_out[at] = (cot[at].astype(F32) + grad).astype(BF16)
        return carry

    lax.fori_loop(0, tokens.shape[0] // 32, rows, 0)


def run_finish(nheads, small, gate, inner, out, par, par_h, par_s, gain_sum, gain, tokens, cot, gnormed):
    rows, width = gate.shape
    scols = par_s.shape[1]
    model = gain.shape[0]
    S = jax.ShapeDtypeStruct
    shapes = [
        (rows, 2, width), (rows, scols), (nheads, rows), (rows, width), (4, width), (1, width), (4, scols), (1, scols),
        (1, nheads), (1, nheads), (1, nheads), (1, width), (1, model),
    ]
    return pl.pallas_call(
        functools.partial(finish_kernel, nheads),
        out_shape=[S(shape, F32) for shape in shapes] + [S(tokens.shape, BF16)],
        name="finish",
    )(small, gate, inner, out, par, par_h, par_s, gain_sum, gain[None], tokens, cot, gnormed)


def pass_on(value, axis, by):
    count = lax.axis_size(axis)
    pairs = [(i, i + by) for i in range(count) if 0 <= i + by < count]
    return lax.ppermute(value, axis, pairs)


def pack_rows(rows, width):
    used = sum(r.shape[0] for r in rows)
    return jnp.concatenate(rows + [jnp.zeros((8 - used, width), F32)], axis=0)


def per_device(
    block_input, segment_ids, norm_gain, proj_zx, proj_bc, proj_dt, conv_inner, conv_inner_bias,
    conv_shared, conv_shared_bias, step_bias, rate_log, skip_gain, gated_gain, proj_out, cotangent,
):
    width = proj_zx.shape[2]
    scols = proj_bc.shape[1]
    nheads = proj_dt.shape[1]
    head_dim = width // nheads
    full_width = float(width * lax.axis_size("col"))
    fill = (0, 128 - nheads)
    small_own = jnp.concatenate([proj_bc, jnp.pad(proj_dt, ((0, 0), fill))], axis=1)
    normed_ext, seg, w_in, w_small, out_t = gather_inputs(
        block_input, norm_gain, segment_ids, proj_zx.reshape(-1, 2 * width), small_own, proj_out.T
    )
    length = normed_ext.shape[0] - HALO
    (cot, normed_ext, conv_inner, conv_inner_bias, conv_shared, conv_shared_bias, step_bias, rate_log, skip_gain,
     gated_gain) = lax.optimization_barrier((
        cotangent, normed_ext, conv_inner, conv_inner_bias, conv_shared, conv_shared_bias, step_bias, rate_log,
        skip_gain, gated_gain))
    cot_all = lax.all_gather(cot, "col", axis=0, tiled=True)
    taps = pack_rows(
        [conv_inner, conv_inner_bias[None], gated_gain[None], jnp.repeat(skip_gain, head_dim)[None]], width
    )
    taps_s = pack_rows([conv_shared, conv_shared_bias[None]], scols)
    heads = pack_rows([jnp.pad(step_bias, fill)[None], jnp.pad(rate_log, fill)[None]], 128)

    both_ext = nn(normed_ext, w_in).astype(BF16)
    small_ext = nn(normed_ext, w_small)
    shared_ext = small_ext[:, :scols].astype(BF16)
    step_ext = small_ext[:, scols:]
    common = (both_ext, shared_ext, step_ext, seg, taps, taps_s, heads)
    y, x, bc, dt, c, ct, dec, enter, final = run_forward(*common)
    start = pass_on(final, "row", 1)
    ssd, gated, squares = run_gate(y, x, bc, dec, start, both_ext, taps)
    squares = sum_col(squares, 3)
    gated_normed, projected = run_project(full_width, gated, squares, taps, out_t)
    cot_all, projected = lax.optimization_barrier((cot_all, projected))
    projected = lax.psum_scatter(projected, "col", scatter_dimension=0, tiled=True)
    block_output = (block_input.astype(F32) + projected.astype(F32)).astype(BF16)
    back, inner = run_pull(cot_all, out_t, gated, taps)
    inner = sum_col(inner, 4)
    dy, ggate, rowterm, colsum, dstart = run_back(
        full_width, ssd, x, bc, dec, both_ext, back, squares, inner, taps
    )
    dend = pass_on(dstart, "row", -1)
    ginner, gsmall, par, par_s, par_h, edge, last = run_backward(
        *common, dy, x, bc, dt, c, ct, dec, enter, start, rowterm, dend, colsum
    )
    edge = pass_on(edge, "row", -1)
    fixed = (last + edge).astype(BF16)
    ginner = lax.dynamic_update_slice(ginner, fixed[:, :width], (length - 8, 0))
    gsmall = lax.dynamic_update_slice(gsmall, fixed[:, width:], (length - 8, 0))
    part, gain_part = run_spread(ggate, ginner, gsmall, w_in, w_small, normed_ext)
    gsm, gz, gout, gx, par, par_h, par_s, gain_sum, grad_normed = reduce_grads(
        (normed_ext, gsmall, ggate, cot_all, gated_normed, ginner, part), (par, par_h, par_s, gain_part), scols
    )
    zx, gbc, gdt, gout, ci, cib, cs, csb, sb, rl, sg, gg, ng, grad_input = run_finish(
        nheads, gsm, gz, gx, gout, par, par_h, par_s, gain_sum, norm_gain, block_input, cotangent, grad_normed
    )
    return (
        block_output, grad_input, ng[0], zx, gbc, gdt.T, ci, cib[0], cs, csb[0], sb[0], rl[0], sg[0], gg[0], gout.T,
    )


def solution(mesh):
    shards = ("dp", "row")
    tokens = P(("dp", "row", "col"), None)
    zx = P(shards, None, "col")
    in_specs = (
        tokens, P(("dp", "row", "col")), P(), zx, P(shards, None), P(shards, "col"), P(None, "col"), P("col"),
        P(), P(), P("col"), P("col"), P("col"), P("col"), P("col", shards), tokens,
    )
    out_specs = (
        tokens, tokens, P(), zx, P(shards, None), P(shards, "col"), P(None, "col"), P("col"),
        P(), P(), P("col"), P("col"), P("col"), P("col"), P("col", shards),
    )
    return jax.shard_map(per_device, mesh=mesh, in_specs=in_specs, out_specs=out_specs, check_vma=False)
```

```python
import functools
import jax, jax.numpy as jnp
from jax import lax
from jax.experimental import pallas as pl
from jax.experimental.pallas import tpu as pltpu
from jax.sharding import PartitionSpec as P

F32, BF16 = jnp.float32, jnp.bfloat16
HIGH = lax.Precision.HIGHEST
SPAN = 256
HALO = 16
EPS = 1e-5


def nn(a, b):
    return lax.dot_general(a, b, (((1,), (0,)), ((), ())), preferred_element_type=F32)


def nt(a, b):
    return lax.dot_general(a, b, (((1,), (1,)), ((), ())), preferred_element_type=F32)


def tn(a, b):
    return lax.dot_general(a, b, (((0,), (0,)), ((), ())), preferred_element_type=F32)


def iota(shape, axis):
    return lax.broadcasted_iota(jnp.int32, shape, axis)


def split_dot(a, b01):
    hi = a.astype(BF16)
    lo = (a - hi.astype(F32)).astype(BF16)
    return nn(hi, b01) + nn(lo, b01)


def sigmoid(v):
    return 1.0 / (1.0 + jnp.exp(-v))


def softplus(v):
    return jnp.maximum(v, 0.0) + jnp.log1p(jnp.exp(-jnp.abs(v)))


def columns(row):
    return jnp.broadcast_to(row, (128, row.shape[1])).T


def segments(seg_row, prev_row, tail_row):
    row = seg_row[0:1].astype(F32)
    seg = columns(row)[:, 0:1]
    length = row.shape[1]
    prev = columns(prev_row[0:1].astype(F32))[length - 8 :, 0:1]
    tail = tail_row[0:1, length - 1 :].astype(F32)
    return row, seg, prev, tail


def chunk_links(segc, halo):
    ext = jnp.concatenate([halo, segc], axis=0)
    length = segc.shape[0]
    return [(ext[8 - j : 8 - j + length] == segc).astype(F32) for j in range(1, 4)]


def conv_tile(cur, halo, links, taps, sl):
    v = jnp.concatenate([halo[HALO - 8 :, sl].astype(F32), cur[:, sl].astype(F32)], axis=0)
    length = cur.shape[0]
    shifted = [v[8 - j : 8 - j + length] * links[j - 1] for j in range(1, 4)]
    pre = taps[4:5, sl] + taps[3:4, sl] * v[8:]
    for j in range(1, 4):
        pre = pre + taps[3 - j : 4 - j, sl] * shifted[j - 1]
    return pre, [v[8:]] + shifted


def pick(lo, cols, h):
    return jnp.where(lo, cols[:, h : h + 1], cols[:, h + 1 : h + 2])


def forward_body(
    inner, inner_halo, shared, shared_halo, step_raw, seg_row, seg_prev, seg_tail, taps, taps_s, heads,
    y_out, x_out, bc_out, dt_out, c_out, ct_out, dec_out, enter_out, state, total,
):
    length, width = inner.shape
    pairs = width // 128
    state_dim = state.shape[0]

    segr, seg, seg_halo, tail_seg = segments(seg_row, seg_prev, seg_tail)
    links = chunk_links(seg, seg_halo)
    closing = (seg == seg[length - 1 :]).astype(F32)
    entering = (seg == seg_halo[7:]).astype(F32)
    kept = (seg[length - 1 :] == seg_halo[7:]).astype(F32)
    dt = softplus(step_raw[...] + heads[0:1])
    log_decay = -jnp.exp(heads[1:2]) * dt
    rows, cols = iota((length, length), 0), iota((length, length), 1)
    lower = (rows >= cols).astype(F32)
    c = jnp.dot(lower, log_decay, precision=HIGH, preferred_element_type=F32)
    ct = c.T
    dt_out[...] = dt
    c_out[...] = c
    ct_out[...] = ct[: ct_out.shape[0]]
    whole = c + total[0:1]
    dec_out[...] = jnp.exp(whole) * (seg == tail_seg).astype(F32)
    total[0:1] = whole[length - 1 :]
    for half in range(2):
        sl = slice(half * state_dim, (half + 1) * state_dim)
        pre, _ = conv_tile(shared, shared_halo, links, taps_s, sl)
        bc_out[:, sl] = (pre * sigmoid(pre)).astype(BF16)
    b = bc_out[:, :state_dim]
    cc = bc_out[:, state_dim:]
    scores = jnp.where((rows >= cols) & (seg == segr), nt(cc, b), 0.0)
    lo = iota((length, 128), 1) < 64
    enter_out[...] = state[...].astype(BF16)
    for p in range(pairs):
        sl = slice(p * 128, (p + 1) * 128)
        pre, _ = conv_tile(inner, inner_halo, links, taps, sl)
        xp = pre * sigmoid(pre)
        xb = xp.astype(BF16)
        x_out[:, sl] = xb
        xdt = xb.astype(F32) * pick(lo, dt, 2 * p)
        cb = pick(lo, c, 2 * p)
        acc = nn(cc, state[:, sl].astype(BF16)) * (jnp.exp(cb) * entering)
        for a in range(2):
            h = 2 * p + a
            weights = jnp.exp(jnp.minimum(c[:, h : h + 1] - ct[h : h + 1], 0.0)) * scores
            mine = lo if a == 0 else ~lo
            acc = acc + nn(weights.astype(BF16), jnp.where(mine, xdt, 0.0).astype(BF16))
        y_out[:, sl] = acc
        last = cb[length - 1 :]
        leaving = jnp.exp(last - cb) * closing * xdt
        state[:, sl] = state[:, sl] * (jnp.exp(last) * kept) + tn(b, leaving.astype(BF16))


def row_sums(value):
    hi = value.astype(BF16)
    lo = (value - hi.astype(F32)).astype(BF16)
    ones = jnp.ones((8, value.shape[1]), BF16)
    return nt(ones, hi) + nt(ones, lo)


def first_rows(value):
    return jnp.where(iota(value.shape, 0) == 0, value, 0.0)


def head_map(p):
    lane, head = iota((128, 128), 0), iota((128, 128), 1)
    return (head == 2 * p + lane // 64).astype(BF16)


def gate_body(y, x, bc, dec, start, gate, taps, ssd_out, gated_out, sums_out):
    length, width = x.shape
    state_dim = start.shape[0]
    cc = bc[:, state_dim:]
    lo = iota((length, 128), 1) < 64
    squares = jnp.zeros((length, 128), F32)
    for p in range(width // 128):
        sl = slice(p * 128, (p + 1) * 128)
        corr = nn(cc, start[:, sl].astype(BF16)) * pick(lo, dec, 2 * p)
        ssd = y[:, sl] + corr + taps[6:7, sl] * x[:, sl].astype(F32)
        ssd_out[:, sl] = ssd
        g = gate[:, sl].astype(F32)
        gated = ssd * (g * sigmoid(g))
        gated_out[:, sl] = gated.astype(BF16)
        squares = squares + gated * gated
    sums_out[...] = row_sums(squares)


def project_body(full_width, gated, sums, taps, out_t, normed_out, proj_out):
    rescale = columns(lax.rsqrt(sums[0:1] / full_width + EPS))
    for p in range(gated.shape[1] // 128):
        sl = slice(p * 128, (p + 1) * 128)
        normed_out[:, sl] = (gated[:, sl].astype(F32) * rescale * taps[5:6, sl]).astype(BF16)
    proj_out[...] = nt(normed_out[...], out_t[...]).astype(BF16)


def pull_body(cot, out_t, gated, taps, back_out, sums_out):
    back = nn(cot[...], out_t[...])
    back_out[...] = back.astype(BF16)
    inner = jnp.zeros((cot.shape[0], 128), F32)
    for p in range(back.shape[1] // 128):
        sl = slice(p * 128, (p + 1) * 128)
        inner = inner + back[:, sl] * taps[5:6, sl] * gated[:, sl].astype(F32)
    sums_out[...] = row_sums(inner)


def back_body(
    full_width, ssd, x, bc, dec, gate, back, squares, inner, taps,
    dy_out, ggate_out, row_out, colsum_out, dstart_out,
):
    length, width = x.shape
    state_dim = dstart_out.shape[0]

    cc = bc[:, state_dim:]
    lo = iota((length, 128), 1) < 64
    rescale = columns(lax.rsqrt(squares[0:1] / full_width + EPS))
    pull = columns(inner[0:1]) * (rescale * rescale * rescale / full_width)
    rowterm = jnp.zeros((length, 128), F32)
    for p in range(width // 128):
        sl = slice(p * 128, (p + 1) * 128)
        s_ssd = ssd[:, sl]
        xp = x[:, sl].astype(F32)
        g = gate[:, sl].astype(F32)
        s = sigmoid(g)
        gated = s_ssd * (g * s)
        bk = back[:, sl].astype(F32)
        gain = taps[5:6, sl]
        gg = rescale * (bk * gain) - gated * pull
        dy = gg * (g * s)
        dyb = dy.astype(BF16)
        dy_out[:, sl] = dyb
        ggate_out[:, sl] = (gg * s_ssd * s * (1.0 + g * (1.0 - s))).astype(BF16)
        colsum_out[5:6, sl] += jnp.sum(bk * gated * rescale, axis=0, keepdims=True)
        colsum_out[6:7, sl] += jnp.sum(dy * xp, axis=0, keepdims=True)
        dstart_out[:, sl] += tn(cc, (dy * pick(lo, dec, 2 * p)).astype(BF16))
        rowterm = rowterm + split_dot(dyb.astype(F32) * (s_ssd - taps[6:7, sl] * xp), head_map(p))
    row_out[...] = rowterm


def conv_back(dout, pre, shifts, links, taps, sl, carry, carry_links, par_out):
    length = dout.shape[0]
    s = sigmoid(pre)
    dconv = dout * (s * (1.0 + pre * (1.0 - s)))
    nxt = carry[:, sl]
    grad = taps[3:4, sl] * dconv
    above = jnp.zeros((8, dout.shape[1]), F32)
    par_out[3:4, sl] += jnp.sum(dconv * shifts[0], axis=0, keepdims=True)
    par_out[4:5, sl] += jnp.sum(dconv, axis=0, keepdims=True)
    for j in range(1, 4):
        z = dconv * links[j - 1]
        w = taps[3 - j : 4 - j, sl]
        low = jnp.concatenate([z, nxt * carry_links[:, j - 1 : j]], axis=0)
        grad = grad + w * low[j : j + length]
        high = jnp.concatenate([above * 0.0, z[0:8]], axis=0)
        above = above + w * high[j : j + 8]
        par_out[3 - j : 4 - j, sl] += jnp.sum(dconv * shifts[j], axis=0, keepdims=True)
    carry[:, sl] = dconv[0:8]
    return grad, above


def backward_body(
    k, chunks,
    inner, inner_halo, shared, shared_halo, step_raw, seg_row, seg_prev, seg_tail, taps, taps_s, heads,
    dy, x, bc, dt_in, c_in, ct_in, dec_halo, enter, start, row_in,
    ginner_out, gsmall_out, par_out, par_s_out, par_h_out, edge_out, last_out,
    dstate, carry, carry_s, carry_links, grads_bc,
):
    length, width = x.shape
    state_dim = dstate.shape[0]

    segr, seg, seg_halo, tail_seg = segments(seg_row, seg_prev, seg_tail)
    links = chunk_links(seg, seg_halo)
    closing = (seg == seg[length - 1 :]).astype(F32)
    entering = (seg == seg_halo[7:]).astype(F32)
    kept = (seg[length - 1 :] == seg_halo[7:]).astype(F32)
    next_links = carry_links[...]
    dt = dt_in[...]
    c = c_in[...]
    ct = ct_in[...]
    first = jnp.where(k == 0, 1.0, 0.0)
    reach = dec_halo[7:8] * (1.0 - first) + first
    b = bc[:, :state_dim]
    cc = bc[:, state_dim:]
    rows, cols = iota((length, length), 0), iota((length, length), 1)
    allowed = (rows <= cols) & (seg == segr)
    scores = jnp.where(allowed, nt(b, cc), 0.0)
    lo = iota((length, 128), 1) < 64
    lo1 = lo[0:1]
    dscores = jnp.zeros((length, length), F32)
    db = jnp.zeros((length, state_dim), F32)
    dc_mat = jnp.zeros((length, state_dim), F32)
    direct = jnp.zeros((length, 128), F32)
    matched = jnp.zeros((length, 128), F32)
    closing_term = jnp.zeros((1, 128), F32)
    for p in range(width // 128):
        sl = slice(p * 128, (p + 1) * 128)
        pre, shifts = conv_tile(inner, inner_halo, links, taps, sl)
        dyb = dy[:, sl]
        dyf = dyb.astype(F32)
        xp = x[:, sl].astype(F32)
        dtb = pick(lo, dt, 2 * p)
        xdt = xp * dtb
        cb = pick(lo, c, 2 * p)
        hm = head_map(p)
        last = cb[length - 1 :]
        entry = enter[:, sl].astype(F32) + start[:, sl] * pick(lo1, reach, 2 * p)
        entryb = entry.astype(BF16)
        ds = dstate[:, sl]
        dsb = ds.astype(BF16)
        leaving = jnp.exp(last - cb) * closing
        bds = nn(b, dsb)
        dxdt = jnp.zeros((length, 128), F32)
        for a in range(2):
            h = 2 * p + a
            mine = lo if a == 0 else ~lo
            decay = jnp.exp(jnp.minimum(ct[h : h + 1] - c[:, h : h + 1], 0.0))
            dscores = dscores + decay * nt(jnp.where(mine, xdt, 0.0).astype(BF16), dyb)
            dxdt = dxdt + nn((decay * scores).astype(BF16), jnp.where(mine, dyf, 0.0).astype(BF16))
        spread = leaving * xdt
        moved = spread * bds
        matched = matched + split_dot(xdt.astype(BF16).astype(F32) * dxdt + moved, hm)
        dxdt = dxdt + leaving * bds
        held = jnp.exp(last) * kept
        col = jnp.sum(moved, axis=0, keepdims=True) + held * jnp.sum(entry * ds, axis=0, keepdims=True)
        closing_term = closing_term + split_dot(jnp.broadcast_to(col, (8, 128)), hm)[0:1]
        direct = direct + split_dot(xp * dxdt, hm)
        edy = (jnp.exp(cb) * entering * dyf).astype(BF16)
        db = db + nt(spread.astype(BF16), dsb)
        dc_mat = dc_mat + nt(edy, entryb)
        dstate[:, sl] = ds * held + tn(cc, edy)
        dx = dtb * dxdt + taps[6:7, sl] * dyf
        grad, above = conv_back(dx, pre, shifts, links, taps, sl, carry, next_links, par_out)
        ginner_out[:, sl] = grad.astype(BF16)
        edge_out[:, sl] = above

        @pl.when(k == chunks - 1)
        def _():
            last_out[:, sl] = grad[length - 8 :]

    dsc = jnp.where(allowed, dscores, 0.0).astype(BF16)
    grads_bc[:, :state_dim] = db + nn(dsc, cc)
    grads_bc[:, state_dim:] = dc_mat + tn(dsc, b)
    for half in range(2):
        sl = slice(half * state_dim, (half + 1) * state_dim)
        pre, shifts = conv_tile(shared, shared_halo, links, taps_s, sl)
        grad, above = conv_back(grads_bc[:, sl], pre, shifts, links, taps_s, sl, carry_s, next_links, par_s_out)
        gsmall_out[:, sl] = grad.astype(BF16)
        at = slice(width + half * state_dim, width + (half + 1) * state_dim)
        edge_out[:, at] = above

        @pl.when(k == chunks - 1)
        def _():
            last_out[:, at] = grad[length - 8 :]

    for j in range(3):
        carry_links[:, j : j + 1] = links[j][0:8]
    dcum = row_in[...] - matched
    upper = (rows <= cols).astype(F32)
    dlog = jnp.dot(upper, dcum, precision=HIGH, preferred_element_type=F32) + closing_term
    rate = -jnp.exp(heads[1:2])
    dstep = (direct + dlog * rate) * sigmoid(step_raw[...] + heads[0:1])
    gsmall_out[:, 2 * state_dim :] = dstep.astype(BF16)
    par_h_out[0:1] += jnp.sum(dstep, axis=0, keepdims=True)
    par_h_out[1:2] += jnp.sum(dlog * (rate * dt), axis=0, keepdims=True)


def spread_body(ggate, ginner, gsmall, w_in, w_small, normed, part_out, gain_out):
    width = ggate.shape[1]
    part = nt(ggate[...], w_in[:, :width]) + nt(ginner[...], w_in[:, width:]) + nt(gsmall[...], w_small[...])
    part_out[...] = part.astype(BF16)
    gain_out[...] = first_rows(jnp.broadcast_to(
        jnp.sum(part * normed[...].astype(F32), axis=0, keepdims=True), gain_out.shape))


PIECES = 2
MESH = pl.DeviceIdType.MESH
ANY = pl.BlockSpec(memory_space=pl.ANY)


def remote(src, dst, send, recv, **to):
    return pltpu.make_async_remote_copy(
        src_ref=src, dst_ref=dst, send_sem=send, recv_sem=recv, device_id=to, device_id_type=MESH
    )


def greet(barrier, when, **to):
    @pl.when(when)
    def _():
        pl.semaphore_signal(barrier, inc=1, device_id=to, device_id_type=MESH)


def start(copies):
    for copy in copies:
        copy.start()


def guarded(when, action):
    @pl.when(when)
    def _():
        action()


class LineGather:
    def __init__(self, ncol, z, first, second, extra, sems):
        self.ncol, self.z, self.last = ncol, z, ncol - 1
        self.parts = (first, second)
        self.extra = extra
        self.sems = sems
        self.tokens = second[1].shape[0] // ncol
        self.part = self.tokens // PIECES

    def copies(self, kind, s, way, pieces, mine=False):
        source, dest = self.parts[kind]
        send, recv = self.sems[2 * kind : 2 * kind + 2]
        to = self.z + 1 if way == 0 else self.z - 1
        made = []
        for p in pieces:
            at = pl.ds(pl.multiple_of(s * self.tokens + p * self.part, self.part), self.part)
            src = source.at[pl.ds(p * self.part, self.part)] if mine and source is not None else dest.at[at]
            made.append(remote(src, dest.at[at], send.at[way, s, p], recv.at[s, p], col=to))
            if kind == 0 and p == PIECES - 1:
                place = self.extra.at[pl.ds(pl.multiple_of(s * 8, 8), 8)]
                made.append(remote(place, place, send.at[way, s, PIECES], recv.at[s, PIECES], col=to))
        return made

    def exit(self, way):
        return self.z < self.last if way == 0 else self.z > 0

    def depth(self, way):
        return self.z if way == 0 else self.last - self.z

    def begin(self):
        every = range(PIECES)
        for way in range(2):
            guarded(self.exit(way), lambda way=way: start(self.copies(0, self.z, way, every, True)))
        for way in range(2):
            guarded(self.depth(way) == 0, lambda way=way: start(self.copies(1, self.z, way, every, True)))

    ticks = property(lambda self: 2 * self.last * PIECES)

    def tick(self, tau):
        j, p = (tau - 1) // PIECES, (tau - 1) % PIECES
        for way in range(2):
            depth = self.depth(way)
            sign = -1 if way == 0 else 1

            def relay(kind, s, way=way, depth=depth):
                for copy in self.copies(kind, s, way, (p,)):
                    copy.wait_recv()
                guarded(self.exit(way), lambda: start(self.copies(kind, s, way, (p,))))
                if kind == 0 and p == PIECES - 1:
                    guarded(self.exit(way) & (j == depth - 1),
                            lambda: start(self.copies(1, self.z, way, range(PIECES), True)))

            guarded(j < depth, lambda s=self.z + sign * (j + 1), relay=relay: relay(0, s))
            guarded((j >= depth) & (j < 2 * depth),
                    lambda s=self.z + sign * (j - depth + 1), relay=relay: relay(1, s))

    def drain(self):
        for kind in range(2):
            for way in range(2):
                sign = -1 if way == 0 else 1
                for s in range(self.ncol):

                    def wait(kind=kind, way=way, s=s, sign=sign):
                        for copy in self.copies(kind, self.z + sign * s, way, range(PIECES)):
                            copy.wait_send()

                    guarded(self.exit(way) & (s <= self.depth(way)), wait)


def mixer_kernel(ncol, ndp, full_width, *refs):
    refs = list(refs)

    def take(number):
        taken = refs[:number]
        del refs[:number]
        return taken

    tokens_in, gain, seg_in, ci, cib, gg, cs, csb, sb, rl, sg = take(11)
    w0, w1, w2, cot_in = take(4)
    normed_hbm, gsmall_hbm, ggate_hbm, cot_hbm, gnorm_hbm, ginner_hbm, part_hbm = take(7)
    par, par_s, par_h, gain_out, total_out = take(5)
    normed, seg, w_in, w_small, out_t, cot = take(6)
    taps, taps_s, heads = take(3)
    both, shared, step = take(3)
    ssd, x, bc, dt, c, ct, dec, enter, state, start_state, total = take(11)
    gated, gnorm, projected, back, dy, ggate, rowterm, dstart, dend = take(9)
    ginner, gsmall, part, edge, edge_in, last_rows = take(6)
    dstate, carry, carry_s, carry_links, grads_bc = take(5)
    squares, squares_all, inner, inner_all, slots = take(5)
    line_box, line_send, line_recv = take(3)
    xs_send, xs_recv, cs_send, cs_recv, w_send, c_send, w_recv, t_send, t_recv = take(9)
    sum_send, sum_recv, row_send, row_recv, here = take(5)

    dp, row, z = lax.axis_index("dp"), lax.axis_index("row"), lax.axis_index("col")
    other = 1 - row
    last = ncol - 1
    tokens = tokens_in.shape[0]
    tail = HALO
    length = ncol * tokens
    width = taps.shape[1]
    scols = taps_s.shape[1]
    state_dim = scols // 2
    chunks = length // SPAN
    rows = w0.shape[0]
    me = dp * 2 + row
    sends_tail = (row == 0) & (z == last)

    barrier = pltpu.get_barrier_semaphore()
    for s in range(1, ncol):
        greet(barrier, row >= 0, col=lax.rem(z + s, ncol))
    greet(barrier, row >= 0, row=other)
    for m in range(1, ndp):
        greet(barrier, row >= 0, dp=dp ^ m)
    greet(barrier, row == 1, row=0, col=last)
    for s in range(ncol):
        greet(barrier, sends_tail, row=1, col=s)

    seg[pl.ds(pl.multiple_of(z * 8, 8), 8)] = jnp.broadcast_to(seg_in[...], (8, tokens))
    base = pl.multiple_of(z * tokens, 32)

    def normalize(n, carried):
        at = pl.multiple_of(n * 32, 32)
        wide = tokens_in[pl.ds(at, 32)].astype(F32)
        scale = lax.rsqrt(jnp.sum(wide * wide, axis=1, keepdims=True) / wide.shape[1] + EPS)
        normed[pl.ds(pl.multiple_of(base + at, 32), 32)] = (wide * scale * gain[...]).astype(BF16)
        return carried

    lax.fori_loop(0, tokens // 32, normalize, 0)

    @pl.when(row == 0)
    def _():
        seg[pl.ds(ncol * 8, 8)] = jnp.full((8, tokens), -1, jnp.int32)
        normed[pl.ds(length, tail)] = jnp.zeros((tail, normed.shape[1]), BF16)
        start_state[...] = jnp.zeros_like(start_state)

    @pl.when(row == 1)
    def _():
        dend[...] = jnp.zeros_like(dend)
        edge_in[...] = jnp.zeros_like(edge_in)

    taps[0:4] = ci[...]
    taps[4:5] = cib[...]
    taps[5:6] = gg[...]
    lo1 = iota((1, 128), 1) < 64
    for p in range(width // 128):
        taps[6:7, p * 128 : (p + 1) * 128] = pick(lo1, sg, 2 * p)
    taps_s[0:4] = cs[...]
    taps_s[4:5] = csb[...]
    heads[...] = jnp.zeros_like(heads)
    heads[0:1, : sb.shape[1]] = sb[...]
    heads[1:2, : rl.shape[1]] = rl[...]
    for ref in (state, total, dstart, carry, carry_s, carry_links, par, par_s, par_h):
        ref[...] = jnp.zeros_like(ref)

    count = ncol - 1 + ndp + row + jnp.where(sends_tail, ncol, 0)
    pl.semaphore_wait(barrier, count)

    weights = ((w0, w_in), (w1, w_small), (w2, out_t))

    def weight_copies(j, mine, send, **to):
        copies = []
        for i, (src, dst) in enumerate(weights):
            place = dst.at[pl.ds(pl.multiple_of(j * rows, 16), rows)]
            copies.append(remote(src if mine else place, place, send.at[i], w_recv.at[j, i], **to))
        return copies

    def tail_copies(s):
        place = seg.at[pl.ds(pl.multiple_of(z * 8, 8), 8)]
        end = pl.multiple_of(z * tokens + tokens - tail, 16)
        return [
            remote(normed.at[pl.ds(end, tail)], normed.at[pl.ds(length, tail)],
                   t_send.at[s, 0], t_recv.at[0], row=1, col=s),
            remote(place, seg.at[pl.ds(ncol * 8, 8)], t_send.at[s, 1], t_recv.at[1], row=1, col=s),
        ]

    for s in range(ncol):
        guarded(sends_tail, lambda s=s: start(tail_copies(s)))
    gather = LineGather(ncol, z, (None, normed), (cot_in, cot), seg, (xs_send, xs_recv, cs_send, cs_recv))
    gather.begin()
    for m in range(1, ndp):
        start(weight_copies(me, True, w_send.at[m], dp=dp ^ m))
    start(weight_copies(me, True, c_send.at[0], row=other))
    local = [pltpu.make_async_copy(cot_in, cot.at[pl.ds(base, tokens)], here.at[0])]
    for i, (src, dst) in enumerate(weights):
        local.append(pltpu.make_async_copy(src, dst.at[pl.ds(pl.multiple_of(me * rows, 16), rows)], here.at[1 + i]))
    start(local)

    def pass_weights(m):
        j = (dp ^ m) * 2 + row
        for copy in weight_copies(j, False, w_send.at[m], dp=dp ^ m):
            copy.wait_recv()
        start(weight_copies(j, False, c_send.at[m], row=other))

    half = gather.ticks // 2
    due = {tau: [] for tau in range(1, half + 1)}
    for m in range(1, ndp):
        due[min(half - 1, 2 + (3 * (m - 1)) // (ndp - 1) * (half - 3) // 2)].append(m)
    for tau in range(1, half):
        gather.tick(tau)
        for m in due[tau]:
            pass_weights(m)
    for m in range(ndp):
        for copy in weight_copies((dp ^ m) * 2 + other, False, c_send.at[m], row=other):
            copy.wait_recv()
    guarded(row == 1, lambda: [copy.wait_recv() for copy in tail_copies(0)])
    for copy in local:
        copy.wait()

    def nth(n):
        return pl.multiple_of(jnp.where(z * 2 < ncol, n, last - n) * tokens, tokens)

    def put(at, size, value, small):
        both[pl.ds(at, size)] = value.astype(BF16)
        shared[pl.ds(at, size)] = small[:, :scols].astype(BF16)
        step[pl.ds(at, size)] = small[:, scols:]

    def project_tokens(n, with_tail):
        at = nth(n)
        lhs = normed[pl.ds(at, tokens)]
        if with_tail:
            lhs = jnp.concatenate([lhs, normed[pl.ds(length, tail)]], axis=0)
        value, small = nn(lhs, w_in[...]), nn(lhs, w_small[...])
        put(at, tokens, value[:tokens], small[:tokens])
        if with_tail:
            put(length, tail, value[tokens:], small[tokens:])

    for n in range(ncol - 1):
        project_tokens(n, n == 0)
    gather.tick(half)
    project_tokens(ncol - 1, False)
    outs = [pltpu.make_async_copy(normed, normed_hbm, here.at[4])]
    outs[0].start()

    def at_rows(k):
        return pl.ds(pl.multiple_of(k * SPAN, SPAN), SPAN)

    def common(k):
        this = at_rows(k)
        above = pl.ds(pl.multiple_of(jnp.where(k == 0, length, k * SPAN - HALO), HALO), HALO)
        prev = pl.ds(pl.multiple_of(jnp.where(k == 0, chunks, k - 1) * 8, 8), 8)
        side = pl.ds(width, width)
        return (
            both.at[this, side], both.at[above, side], shared.at[this], shared.at[above], step.at[this],
            seg.at[pl.ds(pl.multiple_of(k * 8, 8), 8)], seg.at[prev], seg.at[pl.ds(chunks * 8, 8)], taps, taps_s, heads,
        )

    later = list(range(half + 1, gather.ticks + 1))

    def forward(k, carried):
        this = at_rows(k)
        forward_body(*common(k), ssd.at[this], x.at[this], bc.at[this], dt.at[this], c.at[this],
                     ct.at[:, this], dec.at[this], enter.at[k], state, total)
        guarded(k == chunks // 2, lambda: gather.tick(half + 1))
        return carried

    lax.fori_loop(0, chunks, forward, 0)
    later.pop(0)

    def row_copy(n, src, dst):
        return remote(src, dst, row_send.at[n], row_recv.at[n], row=other)

    guarded(row == 0, lambda: row_copy(0, state, start_state).start())
    gather.tick(later.pop(0))
    guarded(row == 1, lambda: row_copy(0, state, start_state).wait_recv())

    def gating(k, carried):
        this = at_rows(k)
        gate_body(ssd.at[this], x.at[this], bc.at[this], dec.at[this], start_state, both.at[this, pl.ds(0, width)],
                  taps, ssd.at[this], gated.at[this], squares.at[:, this])
        return carried

    lax.fori_loop(0, chunks, gating, 0)

    def sum_copy(n, value, s, source):
        return remote(value, slots.at[n, source], sum_send.at[n, s], sum_recv.at[n, source],
                      col=lax.rem(z + s, ncol))

    def sum_begin(n, value):
        for s in range(1, ncol):
            sum_copy(n, value, s, z).start()

    def sum_end(n, value, out):
        result = value[...]
        for s in range(1, ncol):
            source = lax.rem(z + s, ncol)
            sum_copy(n, value, s, source).wait_recv()
            result = result + slots[n, source]
        out[...] = result

    sum_begin(0, squares)
    gather.tick(later.pop(0))
    sum_end(0, squares, squares_all)

    def projecting(k, carried):
        this = at_rows(k)
        project_body(full_width, gated.at[this], squares_all.at[:, this], taps, out_t, gnorm.at[this], projected.at[this])
        return carried

    lax.fori_loop(0, chunks, projecting, 0)
    line = LineReduce(ncol, z, projected, projected, line_box, line_send, line_recv)
    while len(later) > 2:
        gather.tick(later.pop(0))

    def pulling(n):
        this = pl.ds(nth(n), tokens)
        pull_body(cot.at[this], out_t, gated.at[this], taps, back.at[this], inner.at[:, this])

    for n in range(ncol - 1):
        pulling(n)
        if n == 0:
            gather.tick(later.pop(0))
    gather.tick(later.pop(0))
    ticks = list(range(1, line.ticks + 1))
    pulling(ncol - 1)
    outs.append(pltpu.make_async_copy(cot, cot_hbm, here.at[5]))
    outs.append(pltpu.make_async_copy(gnorm, gnorm_hbm, here.at[6]))
    start(outs[1:])
    sum_begin(1, inner)
    sum_end(1, inner, inner_all)
    line.start()

    def pull_gate(k, carried):
        this = at_rows(k)
        back_body(full_width, ssd.at[this], x.at[this], bc.at[this], dec.at[this], both.at[this, pl.ds(0, width)],
                  back.at[this], squares_all.at[:, this], inner_all.at[:, this], taps,
                  dy.at[this], ggate.at[this], rowterm.at[this], par, dstart)
        return carried

    lax.fori_loop(0, chunks, pull_gate, 0)
    guarded(row == 1, lambda: row_copy(1, dstart, dend).start())
    outs.append(pltpu.make_async_copy(ggate, ggate_hbm, here.at[7]))
    outs[-1].start()
    line.tick(ticks.pop(0))
    guarded(row == 0, lambda: row_copy(1, dstart, dend).wait_recv())
    dstate[...] = dend[...]

    spaced = {n: [tau] for n, tau in enumerate(ticks[:chunks])}
    ticks = ticks[chunks:]

    def backward(n, carried):
        k = chunks - 1 - n
        this = at_rows(k)
        before = pl.ds(pl.multiple_of(jnp.maximum(k * SPAN - 8, 0), 8), 8)
        backward_body(k, chunks, *common(k), dy.at[this], x.at[this], bc.at[this], dt.at[this], c.at[this],
                      ct.at[:, this], dec.at[before], enter.at[k], start_state, rowterm.at[this],
                      ginner.at[this], gsmall.at[this], par, par_s, par_h, edge, last_rows,
                      dstate, carry, carry_s, carry_links, grads_bc)
        for turn, taus in spaced.items():
            if turn < chunks - 1:
                for tau in taus:
                    guarded(n == turn, lambda tau=tau: line.tick(tau))
        return carried

    lax.fori_loop(0, chunks, backward, 0)
    guarded(row == 1, lambda: row_copy(2, edge, edge_in).start())
    for tau in spaced.get(chunks - 1, []):
        line.tick(tau)
    guarded(row == 0, lambda: row_copy(2, edge, edge_in).wait_recv())
    fixed = (last_rows[...] + edge_in[...]).astype(BF16)
    ginner[length - 8 :] = fixed[:, :width]
    gsmall[length - 8 :, : fixed.shape[1] - width] = fixed[:, width:]
    outs.append(pltpu.make_async_copy(ginner, ginner_hbm, here.at[8]))
    outs.append(pltpu.make_async_copy(gsmall, gsmall_hbm, here.at[9]))
    start(outs[-2:])

    tile = 256
    tiles = part.shape[1] // tile

    def part_copy(n):
        at = pl.ds(pl.multiple_of(n * tile, tile), tile)
        return pltpu.make_async_copy(part.at[:, at], part_hbm.at[:, at], here.at[10 + n])

    def spreading(n, carried):
        at = pl.ds(pl.multiple_of(n * tile, tile), tile)
        spread_body(ggate, ginner, gsmall, w_in.at[at], w_small.at[at], normed.at[pl.ds(0, length), at],
                    part.at[:, at], gain_out.at[:, at])
        guarded(n > 0, lambda: part_copy(jnp.maximum(n - 1, 0)).start())
        for tau in ticks:
            guarded(n == tiles // 2, lambda tau=tau: line.tick(tau))
        return carried

    lax.fori_loop(0, tiles, spreading, 0)
    part_copy(tiles - 1).start()

    def keep(at, value):
        total_out[pl.ds(pl.multiple_of(at, 16), 16)] = value.astype(BF16)

    line.total(keep)

    gather.drain()
    line.drain()
    for m in range(ndp):
        if m:
            for copy in weight_copies(me, True, w_send.at[m], dp=dp ^ m):
                copy.wait_send()
        for copy in weight_copies((dp ^ m) * 2 + row, m == 0, c_send.at[m], row=other):
            copy.wait_send()
    for s in range(ncol):
        guarded(sends_tail, lambda s=s: [copy.wait_send() for copy in tail_copies(s)])
    for n, value in ((0, squares), (1, inner)):
        for s in range(1, ncol):
            sum_copy(n, value, s, z).wait_send()
    guarded(row == 0, lambda: row_copy(0, state, start_state).wait_send())
    guarded(row == 1, lambda: row_copy(1, dstart, dend).wait_send())
    guarded(row == 1, lambda: row_copy(2, edge, edge_in).wait_send())
    for copy in outs:
        copy.wait()
    for n in range(tiles):
        part_copy(n).wait()


def run_mixer(full_width, tokens_in, gain, seg, ci, cib, gg, cs, csb, sb, rl, sg, w0, w1, w2, cot):
    ncol, ndp = lax.axis_size("col"), lax.axis_size("dp")
    tokens, model = tokens_in.shape
    width, scols = ci.shape[1], cs.shape[1]
    length = ncol * tokens
    chunks = length // SPAN
    state_dim = scols // 2
    small = w1.shape[1]
    shards = 2 * ndp
    S = jax.ShapeDtypeStruct
    V = pltpu.VMEM
    dma = pltpu.SemaphoreType.DMA
    vmem = pl.BlockSpec(memory_space=V)
    return pl.pallas_call(
        functools.partial(mixer_kernel, ncol, ndp, full_width),
        in_specs=[vmem] * 11 + [ANY] * 4,
        out_specs=[ANY] * 7 + [vmem] * 5,
        out_shape=[
            S((length + HALO, model), BF16), S((length, small), BF16), S((length, width), BF16), S((length, model), BF16),
            S((length, width), BF16), S((length, width), BF16), S((length, model), BF16),
            S((8, width), F32), S((8, scols), F32), S((8, 128), F32), S((8, model), F32), S((tokens, model), BF16),
        ],
        scratch_shapes=[
            V((length + HALO, model), BF16), V(((ncol + 1) * 8, tokens), jnp.int32), V((model, 2 * width), BF16),
            V((model, small), BF16), V((model, width), BF16), V((length, model), BF16),
            V((8, width), F32), V((8, scols), F32), V((8, 128), F32),
            V((length + HALO, 2 * width), BF16), V((length + HALO, scols), BF16), V((length + HALO, 128), F32),
            V((length, width), F32), V((length, width), BF16), V((length, scols), BF16), V((length, 128), F32),
            V((length, 128), F32), V((16, length), F32), V((length, 128), F32), V((chunks, state_dim, width), BF16),
            V((state_dim, width), F32), V((state_dim, width), F32), V((8, 128), F32),
            V((length, width), BF16), V((length, width), BF16), V((length, model), BF16), V((length, width), BF16),
            V((length, width), BF16), V((length, width), BF16), V((length, 128), F32), V((state_dim, width), F32),
            V((state_dim, width), F32),
            V((length, width), BF16), V((length, small), BF16), V((length, model), BF16),
            V((8, width + scols), F32), V((8, width + scols), F32), V((8, width + scols), F32),
            V((state_dim, width), F32), V((8, width), F32), V((8, scols), F32), V((8, 128), F32), V((SPAN, scols), F32),
            V((8, length), F32), V((8, length), F32), V((8, length), F32), V((8, length), F32),
            V((2, ncol, 8, length), F32),
            *line_scratch(ncol, tokens, model),
            dma((2, ncol, PIECES + 1)), dma((ncol, PIECES + 1)), dma((2, ncol, PIECES)), dma((ncol, PIECES)),
            dma((ndp, 3)), dma((ndp, 3)), dma((shards, 3)), dma((ncol, 2)), dma((2,)),
            dma((2, ncol)), dma((2, ncol)), dma((3,)), dma((3,)), dma((10 + model // 256,)),
        ],
        compiler_params=pltpu.CompilerParams(
            collective_id=1, has_side_effects=True, vmem_limit_bytes=63 * 1024 * 1024
        ),
        cost_estimate=pl.CostEstimate(flops=0, bytes_accessed=500_000_000, transcendentals=0),
        name="mixer",
    )(tokens_in, gain[None], seg[None], ci, cib[None], gg[None], cs, csb[None], sb[None], rl[None], sg[None], w0, w1, w2, cot)
class LineReduce:
    def __init__(self, ncol, z, source, local, inbox, send, recv):
        self.ncol, self.z, self.last = ncol, z, ncol - 1
        self.source, self.local, self.inbox = source, local, inbox
        self.send, self.recv = send, recv
        self.tokens = local.shape[0] // ncol
        self.part = self.tokens // PIECES

    def rows(self, way, t, p):
        d = self.last - t if way == 0 else t
        return pl.multiple_of(d * self.tokens + p * self.part, self.part)

    def copy(self, way, t, p, first):
        src = self.source.at[pl.ds(self.rows(way, t, p), self.part)] if first else self.inbox.at[way, t, p]
        to = self.z + 1 if way == 0 else self.z - 1
        return remote(src, self.inbox.at[way, t, p], self.send.at[way, t, p], self.recv.at[way, t, p], col=to)

    def edge(self, way):
        return self.z == (0 if way == 0 else self.last)

    def depth(self, way):
        return self.z if way == 0 else self.last - self.z

    def start(self):
        for way in range(2):

            @pl.when(self.edge(way))
            def _(way=way):
                for t in range(self.last):
                    for p in range(PIECES):
                        self.copy(way, t, p, True).start()

    ticks = property(lambda self: self.last * PIECES)

    def tick(self, tau):
        for stage in range(2):
            for way in range(2):
                depth = self.depth(way)
                index = tau - depth
                t, p = index // PIECES, lax.rem(index, PIECES)

                @pl.when((depth > 0) & (index >= 0) & (index < (self.ncol - depth) * PIECES))
                def _(way=way, depth=depth, t=t, p=p, stage=stage):
                    onward = t < self.last - depth
                    if stage == 0:
                        self.copy(way, t, p, False).wait_recv()

                        @pl.when(onward)
                        def _():
                            base = self.rows(way, t, p)

                            def add(k, carry):
                                at = pl.multiple_of(k * 16, 16)
                                mine = self.local[pl.ds(pl.multiple_of(base + at, 16), 16)].astype(F32)
                                here = pl.ds(at, 16)
                                self.inbox[way, t, p, here] = (self.inbox[way, t, p, here].astype(F32) + mine).astype(BF16)
                                return carry

                            lax.fori_loop(0, self.part // 16, add, 0)
                    else:

                        @pl.when(onward)
                        def _():
                            self.copy(way, t, p, False).start()

    def total(self, store):
        z, last = self.z, self.last
        for p in range(PIECES):

            def add(k, carry, p=p):
                at = pl.multiple_of(k * 16, 16)
                here = pl.ds(at, 16)
                row = p * self.part + at
                value = self.local[pl.ds(pl.multiple_of(z * self.tokens + row, 16), 16)].astype(F32)
                low = self.inbox[0, jnp.minimum(last - z, last - 1), p, here].astype(F32)
                high = self.inbox[1, jnp.minimum(z, last - 1), p, here].astype(F32)
                value = value + jnp.where(z > 0, low, 0.0) + jnp.where(z < last, high, 0.0)
                store(row, value)
                return carry

            lax.fori_loop(0, self.part // 16, add, 0)

    def drain(self):
        for way in range(2):
            depth = self.depth(way)
            for t in range(self.last):

                @pl.when((depth < self.last) & (t < self.last - depth))
                def _(way=way, t=t):
                    for p in range(PIECES):
                        self.copy(way, t, p, False).wait_send()


def line_scratch(ncol, tokens, width):
    shape = (2, ncol - 1, PIECES)
    dma = pltpu.SemaphoreType.DMA
    return [pltpu.VMEM(shape + (tokens // PIECES, width), BF16), dma(shape), dma(shape)]


def reduce_kernel(ncol, ndp, scols, *refs):
    count = 4
    refs = list(refs)

    def take(number):
        taken = refs[:number]
        del refs[:number]
        return taken

    sources = take(7)
    vecs = take(4)
    r, vec_outs, gsum_out = take(count), take(4), refs.pop(0)
    held = take(7)
    (line_box, line_send, line_recv) = take(3)
    g, near, sent, far = take(count), take(count), take(count), take(count)
    vec_slots, col_slots = take(4), take(2)
    bc_slots, load, c_send, c_recv, p_send, p_recv, v_send, v_recv, u_send, u_recv, b_send, b_recv = refs
    dp, row, z = lax.axis_index("dp"), lax.axis_index("row"), lax.axis_index("col")
    other = 1 - row
    me = dp * 2 + row
    rows = [out.shape[0] for out in r]
    barrier = pltpu.get_barrier_semaphore()
    for q in range(1, 2 * ndp):
        greet(barrier, row >= 0, dp=dp ^ (q >> 1), row=row ^ (q & 1))
    for s in range(1, ncol):
        greet(barrier, row >= 0, col=lax.rem(z + s, ncol))
    loads = []
    for i, (src, dst) in enumerate(zip(sources, held)):
        src = src.at[pl.ds(0, dst.shape[0])]
        loads.append(pltpu.make_async_copy(src, dst, load.at[i]))
        loads[-1].start()
    normed, gsmall, ggate, cot, gnorm, ginner, part = held
    pl.semaphore_wait(barrier, 2 * ndp + ncol - 2)
    line = LineReduce(ncol, z, sources[6], part, line_box, line_send, line_recv)
    line.start()

    order = (0, 1, 2, 3)
    turns = [3, 1, 2, 0] if ndp == 4 else list(range(1, ndp)) + [0]

    def core_copy(i, d):
        return remote(g[i].at[pl.ds((d * 2 + other) * rows[i], rows[i])], near[i].at[d],
                      c_send.at[i, d], c_recv.at[i, d], row=other)

    def vec_copy(q, i, j):
        return remote(vecs[i], vec_slots[i].at[j], v_send.at[q, i], v_recv.at[j, i],
                      dp=dp ^ (q >> 1), row=row ^ (q & 1))

    for q in range(1, 2 * ndp):
        for i in range(4):
            vec_copy(q, i, me).start()

    waiting = []

    def later(copy):
        if waiting:
            waiting.pop().start()
        if copy is not None:
            waiting.append(copy)

    def accumulate(i, first, number, terms, store):
        def step(k, carry):
            at = first + pl.multiple_of(k * 16, 16)
            total = terms[0](at)
            for term in terms[1:]:
                total = total + term(at)
            store(at, total)
            return carry

        lax.fori_loop(0, number // 16, step, 0)

    def read(ref, index, shift=0):
        return lambda at: ref[index, pl.ds(at - shift, 16)].astype(F32)

    def mine(i, d):
        return lambda at: g[i][pl.ds(pl.multiple_of((d * 2 + row) * rows[i] + at, 16), 16)].astype(F32)

    def write(ref, index, shift):
        def store(at, total):
            ref[index, pl.ds(at - shift, 16)] = total.astype(BF16)

        return store

    def arrived(i, d):
        core_copy(i, d).wait_recv()

    model = normed.shape[1]
    block = model // 4
    ends = [[] for _ in range(4)]
    products = ((normed, gsmall), (normed, ggate), (cot, gnorm), (normed, ginner))
    ready = {0: (0, 1), 1: (2,), 2: (3, 4), 3: (5,)}
    ticks = list(range(1, line.ticks + 1))
    loaded = [False]
    for i in order:
        for at in ready[i]:
            loads[at].wait()
        left, right = products[i]
        for m in ([3, 1, 2, 0] if ndp == 4 else range(4)):
            b = dp ^ m if ndp == 4 else m
            first = pl.multiple_of(b * block, 128)
            g[i][pl.ds(pl.multiple_of(b * block, 16), block)] = tn(left[:, pl.ds(first, block)], right[...]).astype(BF16)
            if ndp == 4:
                later(core_copy(i, b))
        if i == 1:
            loads[6].wait()
            line.tick(ticks.pop(0))
        if i == 3 and ticks:
            line.tick(ticks.pop(0))
    later(None)
    if ndp != 4:
        for i in order:
            for m in turns:
                core_copy(i, dp ^ m).start()

    def tick():
        if ticks:
            line.tick(ticks.pop(0))

    if ndp == 4:
        halves = ((0, 1, 2), (1, 2, 1))

        def leg(i, slot, m):
            return remote(sent[i].at[slot], far[i].at[slot], p_send.at[i, slot], p_recv.at[i, slot], dp=dp ^ m)

        for i in order:
            half = rows[i] // 2
            arrived(i, dp ^ 3)
            for h, m1, m2 in halves:
                accumulate(i, h * half, half, [mine(i, dp ^ 3), read(near[i], dp ^ 3)],
                           write(sent[i], 3 * h + 1, h * half))
                later(leg(i, 3 * h + 1, m1))
            for h, m1, m2 in halves:
                arrived(i, dp ^ m1)
                accumulate(i, h * half, half, [mine(i, dp ^ m1), read(near[i], dp ^ m1)],
                           write(sent[i], 3 * h, h * half))
                later(leg(i, 3 * h, m1))
        later(None)

        def relay(i):
            half = rows[i] // 2
            for h, m1, m2 in halves:
                leg(i, 3 * h + 1, m1).wait_recv()
                accumulate(i, h * half, half,
                           [mine(i, dp ^ m2), read(near[i], dp ^ m2), read(far[i], 3 * h + 1, h * half)],
                           write(sent[i], 3 * h + 2, h * half))
                later(leg(i, 3 * h + 2, m2))

        def finish(i, store):
            half = rows[i] // 2
            for h, m1, m2 in halves:
                leg(i, 3 * h, m1).wait_recv()
                leg(i, 3 * h + 2, m2).wait_recv()
                accumulate(i, h * half, half,
                           [mine(i, dp), read(near[i], dp), read(far[i], 3 * h, h * half),
                            read(far[i], 3 * h + 2, h * half)], store)

        sends = [leg(i, 3 * h + k, m2 if k == 2 else m1) for i in order for h, m1, m2 in halves for k in range(3)]
    else:

        def peer(i, m):
            return remote(sent[i].at[m], far[i].at[m], p_send.at[i, m], p_recv.at[i, m], dp=dp ^ m)

        for i in order:
            for m in turns[:-1]:
                arrived(i, dp ^ m)
                accumulate(i, 0, rows[i], [mine(i, dp ^ m), read(near[i], dp ^ m)], write(sent[i], m, 0))
                later(peer(i, m))
        later(None)

        def relay(i):
            pass

        def finish(i, store):
            for m in range(1, ndp):
                peer(i, m).wait_recv()
            accumulate(i, 0, rows[i],
                       [mine(i, dp), read(near[i], dp)] + [read(far[i], m) for m in range(1, ndp)], store)

        sends = [peer(i, m) for i in order for m in range(1, ndp)]

    for i in order:
        arrived(i, dp)
    tick()
    for q in range(1, 2 * ndp):
        for i in range(4):
            vec_copy(q, i, me ^ q).wait_recv()
    for i in range(4):
        vec_slots[i][me] = vecs[i][...]
        total = vec_slots[i][0]
        for j in range(1, 2 * ndp):
            total = total + vec_slots[i][j]
        if i < 2:
            vec_outs[i][...] = total
        else:
            col_slots[i - 2][z] = total

    def plain(i):
        def store(at, total):
            r[i][pl.ds(at, 16)] = total

        return store

    def shared_rows(at, total):
        r[0][pl.ds(at, 16)] = total
        bc_slots[z, pl.ds(at, 16)] = total[:, : bc_slots.shape[2]].astype(BF16)

    def col_copies(s, source):
        to = lax.rem(z + s, ncol)
        copies = [remote(col_slots[i].at[source], col_slots[i].at[source], u_send.at[s, i], u_recv.at[source, i], col=to)
                  for i in range(2)]
        return copies + [remote(bc_slots.at[source], bc_slots.at[source], b_send.at[s], b_recv.at[source], col=to)]

    relay(0)
    relay(1)
    tick()
    relay(2)
    relay(3)
    later(None)
    finish(0, shared_rows)
    for s in range(1, ncol):
        for copy in col_copies(s, z):
            copy.start()
    while len(ticks) > 1:
        tick()
    finish(1, plain(1))
    finish(2, plain(2))
    finish(3, plain(3))
    while ticks:
        tick()

    def keep(at, value):
        gsum_out[pl.ds(pl.multiple_of(at, 16), 16)] = value.astype(BF16)

    line.total(keep)
    for s in range(1, ncol):
        for copy in col_copies(s, lax.rem(z + s, ncol)):
            copy.wait_recv()
    for i in range(2):
        total = col_slots[i][0]
        for j in range(1, ncol):
            total = total + col_slots[i][j]
        vec_outs[2 + i][...] = total
    total = bc_slots[0].astype(F32)
    for j in range(1, ncol):
        total = total + bc_slots[j].astype(F32)
    r[0][:, : bc_slots.shape[2]] = total

    for q in range(1, 2 * ndp):
        for i in range(4):
            vec_copy(q, i, me).wait_send()
    for i in order:
        for m in turns:
            core_copy(i, dp ^ m).wait_send()
    for copy in sends:
        copy.wait_send()
    for s in range(1, ncol):
        for copy in col_copies(s, z):
            copy.wait_send()
    line.drain()


def reduce_grads(sources, vecs, scols):
    ncol, ndp = lax.axis_size("col"), lax.axis_size("dp")
    dma = pltpu.SemaphoreType.DMA
    vmem = pl.BlockSpec(memory_space=pltpu.VMEM)
    S = jax.ShapeDtypeStruct
    length = sources[1].shape[0]
    model = sources[0].shape[1]
    widths = [sources[1].shape[1], sources[2].shape[1], sources[4].shape[1], sources[5].shape[1]]
    count = len(widths)
    blocks = [(model // (2 * ndp), w) for w in widths]
    near = [pltpu.VMEM((ndp,) + b, BF16) for b in blocks]
    slots = 6 if ndp == 4 else ndp
    legs = [pltpu.VMEM((6, b[0] // 2, b[1]) if ndp == 4 else (ndp,) + b, BF16) for b in blocks]
    tokens = length // ncol
    return pl.pallas_call(
        functools.partial(reduce_kernel, ncol, ndp, scols),
        in_specs=[ANY] * 7 + [vmem] * 4,
        out_specs=[vmem] * (count + 5),
        out_shape=[S(b, F32) for b in blocks] + [S(v.shape, F32) for v in vecs] + [S((tokens, model), BF16)],
        scratch_shapes=[pltpu.VMEM((length, s.shape[1]), BF16) for s in sources]
        + line_scratch(ncol, tokens, model)
        + [pltpu.VMEM((model, w), BF16) for w in widths]
        + near + legs * 2
        + [pltpu.VMEM((2 * ndp,) + v.shape, F32) for v in vecs]
        + [pltpu.VMEM((ncol,) + v.shape, F32) for v in vecs[2:]]
        + [pltpu.VMEM((ncol, blocks[0][0], scols), BF16)]
        + [dma((7,))]
        + [dma((count, ndp))] * 2
        + [dma((count, slots))] * 2
        + [dma((2 * ndp, 4))] * 2
        + [dma((ncol, 2))] * 2
        + [dma((ncol,))] * 2,
        compiler_params=pltpu.CompilerParams(
            collective_id=2, has_side_effects=True, vmem_limit_bytes=60 * 1024 * 1024
        ),
        cost_estimate=pl.CostEstimate(flops=0, bytes_accessed=200_000_000, transcendentals=0),
        name="reduce_grads",
    )(*sources, *vecs)


def finish_kernel(
    nheads, small, gate, inner, out, par, par_h, par_s, gain_sum, gain, tokens, cot, gnormed, projected,
    zx_out, bc_out, dt_out, out_out, ci_out, cib_out, cs_out, csb_out, sb_out, rl_out, sg_out, gg_out, ng_out, gin_out, block_out,
):
    width = par.shape[1]
    scols = par_s.shape[1]
    zx_out[:, 0, :] = gate[...]
    zx_out[:, 1, :] = inner[...]
    bc_out[...] = small[:, :scols]
    dt_out[...] = small[:, scols:].T[:nheads]
    out_out[...] = out[...]
    ci_out[...] = par[0:4]
    cib_out[...] = par[4:5]
    gg_out[...] = par[5:6]
    cs_out[...] = par_s[0:4]
    csb_out[...] = par_s[4:5]
    sb_out[...] = par_h[0:1, :nheads]
    rl_out[...] = par_h[1:2, :nheads]
    skip = jnp.zeros((8, 128), F32)
    for p in range(width // 128):
        skip = skip + split_dot(jnp.broadcast_to(par[6:7, p * 128 : (p + 1) * 128], (8, 128)), head_map(p))
    sg_out[...] = skip[0:1, :nheads]
    ng_out[...] = gain_sum[0:1] / gain[...]

    def rows(step, carry):
        at = pl.ds(pl.multiple_of(step * 32, 32), 32)
        wide = tokens[at].astype(F32)
        scale = lax.rsqrt(jnp.sum(wide * wide, axis=1, keepdims=True) / wide.shape[1] + EPS)
        pushed = gnormed[at].astype(F32) * gain[...]
        mean = jnp.sum(pushed * wide, axis=1, keepdims=True) / wide.shape[1]
        grad = scale * pushed - wide * (scale * scale * scale * mean)
        gin_out[at] = (cot[at].astype(F32) + grad).astype(BF16)
        block_out[at] = (wide + projected[at].astype(F32)).astype(BF16)
        return carry

    lax.fori_loop(0, tokens.shape[0] // 32, rows, 0)


def run_finish(nheads, small, gate, inner, out, par, par_h, par_s, gain_sum, gain, tokens, cot, gnormed, projected):
    rows, width = gate.shape
    scols = par_s.shape[1]
    model = gain.shape[0]
    S = jax.ShapeDtypeStruct
    shapes = [
        (rows, 2, width), (rows, scols), (nheads, rows), (rows, width), (4, width), (1, width), (4, scols), (1, scols),
        (1, nheads), (1, nheads), (1, nheads), (1, width), (1, model),
    ]
    return pl.pallas_call(
        functools.partial(finish_kernel, nheads),
        out_shape=[S(shape, F32) for shape in shapes] + [S(tokens.shape, BF16)] * 2,
        name="finish",
    )(small, gate, inner, out, par, par_h, par_s, gain_sum, gain[None], tokens, cot, gnormed, projected)


def per_device(
    block_input, segment_ids, norm_gain, proj_zx, proj_bc, proj_dt, conv_inner, conv_inner_bias,
    conv_shared, conv_shared_bias, step_bias, rate_log, skip_gain, gated_gain, proj_out, cotangent,
):
    width = proj_zx.shape[2]
    scols = proj_bc.shape[1]
    nheads = proj_dt.shape[1]
    full_width = float(width * lax.axis_size("col"))
    small_own = jnp.concatenate([proj_bc, jnp.pad(proj_dt, ((0, 0), (0, 128 - nheads)))], axis=1)
    (normed, gsmall, ggate, cot_all, gated_normed, ginner, part, par, par_s, par_h, gain_part, projected) = run_mixer(
        full_width, block_input, norm_gain, segment_ids, conv_inner, conv_inner_bias, gated_gain, conv_shared,
        conv_shared_bias, step_bias, rate_log, skip_gain, proj_zx.reshape(-1, 2 * width), small_own, proj_out.T, cotangent,
    )
    gsm, gz, gout, gx, par, par_h, par_s, gain_sum, grad_normed = reduce_grads(
        (normed, gsmall, ggate, cot_all, gated_normed, ginner, part), (par, par_h, par_s, gain_part), scols
    )
    zx, gbc, gdt, gout, ci, cib, cs, csb, sb, rl, sg, gg, ng, grad_input, block_output = run_finish(
        nheads, gsm, gz, gx, gout, par, par_h, par_s, gain_sum, norm_gain, block_input, cotangent, grad_normed, projected
    )
    return (
        block_output, grad_input, ng[0], zx, gbc, gdt.T, ci, cib[0], cs, csb[0], sb[0], rl[0], sg[0], gg[0], gout.T,
    )


def solution(mesh):
    shards = ("dp", "row")
    tokens = P(("dp", "row", "col"), None)
    zx = P(shards, None, "col")
    in_specs = (
        tokens, P(("dp", "row", "col")), P(), zx, P(shards, None), P(shards, "col"), P(None, "col"), P("col"),
        P(), P(), P("col"), P("col"), P("col"), P("col"), P("col", shards), tokens,
    )
    out_specs = (
        tokens, tokens, P(), zx, P(shards, None), P(shards, "col"), P(None, "col"), P("col"),
        P(), P(), P("col"), P("col"), P("col"), P("col"), P("col", shards),
    )
    return jax.shard_map(per_device, mesh=mesh, in_specs=in_specs, out_specs=out_specs, check_vma=False)
```

```python
import functools
import jax, jax.numpy as jnp
from jax import lax
from jax.experimental import pallas as pl
from jax.experimental.pallas import tpu as pltpu
from jax.sharding import PartitionSpec as P

F32, BF16 = jnp.float32, jnp.bfloat16
HIGH = lax.Precision.HIGHEST
SPAN = 256
HALO = 16
EPS = 1e-5


def nn(a, b):
    return lax.dot_general(a, b, (((1,), (0,)), ((), ())), preferred_element_type=F32)


def nt(a, b):
    return lax.dot_general(a, b, (((1,), (1,)), ((), ())), preferred_element_type=F32)


def tn(a, b):
    return lax.dot_general(a, b, (((0,), (0,)), ((), ())), preferred_element_type=F32)


def iota(shape, axis):
    return lax.broadcasted_iota(jnp.int32, shape, axis)


def split_dot(a, b01):
    hi = a.astype(BF16)
    lo = (a - hi.astype(F32)).astype(BF16)
    return nn(hi, b01) + nn(lo, b01)


def sigmoid(v):
    return 0.5 * jnp.tanh(0.5 * v) + 0.5


def softplus(v):
    return jnp.maximum(v, 0.0) + jnp.log1p(jnp.exp(-jnp.abs(v)))


def columns(row):
    return jnp.broadcast_to(row, (128, row.shape[1])).T


def segments(seg_row, prev_row, tail_row):
    row = seg_row[0:1].astype(F32)
    seg = columns(row)[:, 0:1]
    length = row.shape[1]
    prev = columns(prev_row[0:1].astype(F32))[length - 8 :, 0:1]
    tail = tail_row[0:1, length - 1 :].astype(F32)
    return row, seg, prev, tail


def chunk_links(segc, halo):
    ext = jnp.concatenate([halo, segc], axis=0)
    length = segc.shape[0]
    return [(ext[8 - j : 8 - j + length] == segc).astype(F32) for j in range(1, 4)]


def conv_tile(cur, halo, links, taps, sl):
    v = jnp.concatenate([halo[HALO - 8 :, sl].astype(F32), cur[:, sl].astype(F32)], axis=0)
    length = cur.shape[0]
    pre = taps[4:5, sl] + taps[3:4, sl] * v[8:]
    for j in range(1, 4):
        pre = pre + taps[3 - j : 4 - j, sl] * (v[8 - j : 8 - j + length] * links[j - 1])
    return pre


def silu_and_slope(pre):
    s = sigmoid(pre)
    value = pre * s
    return value, s + value * (1.0 - s)


def pick(lo, cols, h):
    return jnp.where(lo, cols[:, h : h + 1], cols[:, h + 1 : h + 2])


def forward_body(
    inner, inner_halo, shared, shared_halo, step_raw, seg_row, seg_prev, seg_tail, taps, taps_s, heads,
    y_out, x_out, bc_out, dt_out, c_out, ct_out, dec_out, enter_out, slope_out, slope_s_out, state, total,
):
    length, width = inner.shape
    pairs = width // 128
    state_dim = state.shape[0]

    segr, seg, seg_halo, tail_seg = segments(seg_row, seg_prev, seg_tail)
    links = chunk_links(seg, seg_halo)
    closing = (seg == seg[length - 1 :]).astype(F32)
    entering = (seg == seg_halo[7:]).astype(F32)
    kept = (seg[length - 1 :] == seg_halo[7:]).astype(F32)
    dt = softplus(step_raw[...] + heads[0:1])
    log_decay = -jnp.exp(heads[1:2]) * dt
    rows, cols = iota((length, length), 0), iota((length, length), 1)
    lower = (rows >= cols).astype(F32)
    c = jnp.dot(lower, log_decay, precision=HIGH, preferred_element_type=F32)
    ct = c.T
    dt_out[...] = dt
    c_out[...] = c
    ct_out[...] = ct[: ct_out.shape[0]]
    whole = c + total[0:1]
    dec_out[...] = jnp.exp(whole) * (seg == tail_seg).astype(F32)
    total[0:1] = whole[length - 1 :]
    for half in range(2):
        sl = slice(half * state_dim, (half + 1) * state_dim)
        value, slope = silu_and_slope(conv_tile(shared, shared_halo, links, taps_s, sl))
        bc_out[:, sl] = value.astype(BF16)
        slope_s_out[:, sl] = slope.astype(BF16)
    b = bc_out[:, :state_dim]
    cc = bc_out[:, state_dim:]
    scores = jnp.where((rows >= cols) & (seg == segr), nt(cc, b), 0.0)
    lo = iota((length, 128), 1) < 64
    lo1 = lo[0:1]
    sides = [jnp.where(lo, 1.0, 0.0).astype(BF16), jnp.where(lo, 0.0, 1.0).astype(BF16)]
    arriving = jnp.exp(c) * entering
    leaving = jnp.exp(c[length - 1 :] - c) * closing
    held = jnp.exp(c[length - 1 :]) * kept
    enter_out[...] = state[...].astype(BF16)
    for p in range(pairs):
        sl = slice(p * 128, (p + 1) * 128)
        xp, slope = silu_and_slope(conv_tile(inner, inner_halo, links, taps, sl))
        xb = xp.astype(BF16)
        x_out[:, sl] = xb
        slope_out[:, sl] = slope.astype(BF16)
        xdt = xb.astype(F32) * pick(lo, dt, 2 * p)
        xdtb = xdt.astype(BF16)
        acc = nn(cc, state[:, sl].astype(BF16)) * pick(lo, arriving, 2 * p)
        for a in range(2):
            h = 2 * p + a
            weights = jnp.exp(jnp.minimum(c[:, h : h + 1] - ct[h : h + 1], 0.0)) * scores
            acc = acc + nn(weights.astype(BF16), xdtb * sides[a])
        y_out[:, sl] = acc
        moved = pick(lo, leaving, 2 * p) * xdt
        state[:, sl] = state[:, sl] * pick(lo1, held, 2 * p) + tn(b, moved.astype(BF16))


def row_sums(value):
    hi = value.astype(BF16)
    lo = (value - hi.astype(F32)).astype(BF16)
    ones = jnp.ones((8, value.shape[1]), BF16)
    return nt(ones, hi) + nt(ones, lo)


def first_rows(value):
    return jnp.where(iota(value.shape, 0) == 0, value, 0.0)


def head_map(p):
    lane, head = iota((128, 128), 0), iota((128, 128), 1)
    return (head == 2 * p + lane // 64).astype(BF16)


def gate_body(y, x, bc, dec, start, gate, taps, ssd_out, gated_out, sums_out):
    length, width = x.shape
    state_dim = start.shape[0]
    cc = bc[:, state_dim:]
    lo = iota((length, 128), 1) < 64
    squares = jnp.zeros((length, 128), F32)
    for p in range(width // 128):
        sl = slice(p * 128, (p + 1) * 128)
        corr = nn(cc, start[:, sl].astype(BF16)) * pick(lo, dec, 2 * p)
        ssd = y[:, sl] + corr + taps[6:7, sl] * x[:, sl].astype(F32)
        ssd_out[:, sl] = ssd
        g = gate[:, sl].astype(F32)
        gated = ssd * (g * sigmoid(g))
        gated_out[:, sl] = gated.astype(BF16)
        squares = squares + gated * gated
    sums_out[...] = row_sums(squares)


def project_body(full_width, gated, sums, taps, out_t, normed_out, proj_out):
    rescale = columns(lax.rsqrt(sums[0:1] / full_width + EPS))
    for p in range(gated.shape[1] // 128):
        sl = slice(p * 128, (p + 1) * 128)
        normed_out[:, sl] = (gated[:, sl].astype(F32) * rescale * taps[5:6, sl]).astype(BF16)
    proj_out[...] = nt(normed_out[...], out_t[...]).astype(BF16)


def pull_body(cot, out_t, gated, taps, back_out, sums_out):
    back = nn(cot[...], out_t[...])
    back_out[...] = back.astype(BF16)
    inner = jnp.zeros((cot.shape[0], 128), F32)
    for p in range(back.shape[1] // 128):
        sl = slice(p * 128, (p + 1) * 128)
        inner = inner + back[:, sl] * taps[5:6, sl] * gated[:, sl].astype(F32)
    sums_out[...] = row_sums(inner)


def back_body(
    full_width, ssd, x, bc, dec, gate, back, squares, inner, taps,
    dy_out, ggate_out, row_out, colsum_out, dstart_out,
):
    length, width = x.shape
    state_dim = dstart_out.shape[0]

    cc = bc[:, state_dim:]
    lo = iota((length, 128), 1) < 64
    rescale = columns(lax.rsqrt(squares[0:1] / full_width + EPS))
    pull = columns(inner[0:1]) * (rescale * rescale * rescale / full_width)
    rowterm = jnp.zeros((length, 128), F32)
    for p in range(width // 128):
        sl = slice(p * 128, (p + 1) * 128)
        s_ssd = ssd[:, sl]
        xp = x[:, sl].astype(F32)
        g = gate[:, sl].astype(F32)
        s = sigmoid(g)
        gated = s_ssd * (g * s)
        bk = back[:, sl].astype(F32)
        gain = taps[5:6, sl]
        gg = rescale * (bk * gain) - gated * pull
        dy = gg * (g * s)
        dyb = dy.astype(BF16)
        dy_out[:, sl] = dyb
        ggate_out[:, sl] = (gg * s_ssd * s * (1.0 + g * (1.0 - s))).astype(BF16)
        colsum_out[5:6, sl] += jnp.sum(bk * gated * rescale, axis=0, keepdims=True)
        colsum_out[6:7, sl] += jnp.sum(dy * xp, axis=0, keepdims=True)
        dstart_out[:, sl] += tn(cc, (dy * pick(lo, dec, 2 * p)).astype(BF16))
        rowterm = rowterm + split_dot(dyb.astype(F32) * (s_ssd - taps[6:7, sl] * xp), head_map(p))
    row_out[...] = rowterm


def conv_back(dout, slope, cur, halo, links, taps, sl, carry, carry_links, par_out, first):
    length = dout.shape[0]
    dconv = dout * slope[:, sl].astype(F32)
    v = cur[:, sl].astype(F32)
    v_above = halo[HALO - 8 :, sl].astype(F32) * first
    nxt = carry[:, sl]
    grad = taps[3:4, sl] * dconv
    above = jnp.zeros((8, dout.shape[1]), F32)
    par_out[3:4, sl] += jnp.sum(dconv * v, axis=0, keepdims=True)
    par_out[4:5, sl] += jnp.sum(dconv, axis=0, keepdims=True)
    for j in range(1, 4):
        z = dconv * links[j - 1]
        w = taps[3 - j : 4 - j, sl]
        low = jnp.concatenate([z, nxt * carry_links[:, j - 1 : j]], axis=0)[j : j + length]
        high = jnp.concatenate([jnp.zeros_like(nxt), z[0:8]], axis=0)[j : j + 8]
        grad = grad + w * low
        above = above + w * high
        par_out[3 - j : 4 - j, sl] += jnp.sum(low * v, axis=0, keepdims=True) + jnp.sum(
            high * v_above, axis=0, keepdims=True
        )
    carry[:, sl] = dconv[0:8]
    return grad, above


def backward_body(
    k, chunks,
    inner, inner_halo, shared, shared_halo, step_raw, seg_row, seg_prev, seg_tail, taps, taps_s, heads,
    dy, x, bc, dt_in, c_in, ct_in, dec_halo, enter, slope, slope_s, start, row_in,
    ginner_out, gsmall_out, par_out, par_s_out, par_h_out, edge_out, last_out,
    dstate, carry, carry_s, carry_links, grads_bc,
):
    length, width = x.shape
    state_dim = dstate.shape[0]

    segr, seg, seg_halo, tail_seg = segments(seg_row, seg_prev, seg_tail)
    links = chunk_links(seg, seg_halo)
    closing = (seg == seg[length - 1 :]).astype(F32)
    entering = (seg == seg_halo[7:]).astype(F32)
    kept = (seg[length - 1 :] == seg_halo[7:]).astype(F32)
    next_links = carry_links[...]
    dt = dt_in[...]
    c = c_in[...]
    ct = ct_in[...]
    first = jnp.where(k == 0, 1.0, 0.0)
    reach = dec_halo[7:8] * (1.0 - first) + first
    b = bc[:, :state_dim]
    cc = bc[:, state_dim:]
    rows, cols = iota((length, length), 0), iota((length, length), 1)
    allowed = (rows <= cols) & (seg == segr)
    scores = jnp.where(allowed, nt(b, cc), 0.0)
    lo = iota((length, 128), 1) < 64
    lo1 = lo[0:1]
    sides = [jnp.where(lo, 1.0, 0.0).astype(BF16), jnp.where(lo, 0.0, 1.0).astype(BF16)]
    arriving = jnp.exp(c) * entering
    leaving_all = jnp.exp(c[length - 1 :] - c) * closing
    held_all = jnp.exp(c[length - 1 :]) * kept
    dscores = jnp.zeros((length, length), F32)
    db = jnp.zeros((length, state_dim), F32)
    dc_mat = jnp.zeros((length, state_dim), F32)
    direct = jnp.zeros((length, 128), F32)
    matched = jnp.zeros((length, 128), F32)
    closing_term = jnp.zeros((1, 128), F32)
    for p in range(width // 128):
        sl = slice(p * 128, (p + 1) * 128)
        dyb = dy[:, sl]
        dyf = dyb.astype(F32)
        xp = x[:, sl].astype(F32)
        dtb = pick(lo, dt, 2 * p)
        xdt = xp * dtb
        xdtb = xdt.astype(BF16)
        hm = head_map(p)
        entry = enter[:, sl].astype(F32) + start[:, sl] * pick(lo1, reach, 2 * p)
        entryb = entry.astype(BF16)
        ds = dstate[:, sl]
        dsb = ds.astype(BF16)
        leaving = pick(lo, leaving_all, 2 * p)
        bds = nn(b, dsb)
        dxdt = jnp.zeros((length, 128), F32)
        for a in range(2):
            h = 2 * p + a
            decay = jnp.exp(jnp.minimum(ct[h : h + 1] - c[:, h : h + 1], 0.0))
            dscores = dscores + decay * nt(xdtb * sides[a], dyb)
            dxdt = dxdt + nn((decay * scores).astype(BF16), dyb * sides[a])
        spread = leaving * xdt
        moved = spread * bds
        matched = matched + split_dot(xdtb.astype(F32) * dxdt + moved, hm)
        dxdt = dxdt + leaving * bds
        held = pick(lo1, held_all, 2 * p)
        col = jnp.sum(moved, axis=0, keepdims=True) + held * jnp.sum(entry * ds, axis=0, keepdims=True)
        closing_term = closing_term + split_dot(jnp.broadcast_to(col, (8, 128)), hm)[0:1]
        direct = direct + nn((xp * dxdt).astype(BF16), hm)
        edy = (pick(lo, arriving, 2 * p) * dyf).astype(BF16)
        db = db + nt(spread.astype(BF16), dsb)
        dc_mat = dc_mat + nt(edy, entryb)
        dstate[:, sl] = ds * held + tn(cc, edy)
        dx = dtb * dxdt + taps[6:7, sl] * dyf
        grad, above = conv_back(dx, slope, inner, inner_halo, links, taps, sl, carry, next_links, par_out, first)
        ginner_out[:, sl] = grad.astype(BF16)
        edge_out[:, sl] = above

        @pl.when(k == chunks - 1)
        def _():
            last_out[:, sl] = grad[length - 8 :]

    dsc = jnp.where(allowed, dscores, 0.0).astype(BF16)
    grads_bc[:, :state_dim] = db + nn(dsc, cc)
    grads_bc[:, state_dim:] = dc_mat + tn(dsc, b)
    for half in range(2):
        sl = slice(half * state_dim, (half + 1) * state_dim)
        grad, above = conv_back(
            grads_bc[:, sl], slope_s, shared, shared_halo, links, taps_s, sl, carry_s, next_links, par_s_out, first
        )
        gsmall_out[:, sl] = grad.astype(BF16)
        at = slice(width + half * state_dim, width + (half + 1) * state_dim)
        edge_out[:, at] = above

        @pl.when(k == chunks - 1)
        def _():
            last_out[:, at] = grad[length - 8 :]

    for j in range(3):
        carry_links[:, j : j + 1] = links[j][0:8]
    dcum = row_in[...] - matched
    upper = (rows <= cols).astype(F32)
    dlog = jnp.dot(upper, dcum, precision=HIGH, preferred_element_type=F32) + closing_term
    rate = -jnp.exp(heads[1:2])
    dstep = (direct + dlog * rate) * sigmoid(step_raw[...] + heads[0:1])
    gsmall_out[:, 2 * state_dim :] = dstep.astype(BF16)
    par_h_out[0:1] += jnp.sum(dstep, axis=0, keepdims=True)
    par_h_out[1:2] += jnp.sum(dlog * (rate * dt), axis=0, keepdims=True)


def spread_body(ggate, ginner, gsmall, w_in, w_small, normed, part_out, gain_out):
    width = ggate.shape[1]
    part = nt(ggate[...], w_in[:, :width]) + nt(ginner[...], w_in[:, width:]) + nt(gsmall[...], w_small[...])
    part_out[...] = part.astype(BF16)
    gain_out[...] = jnp.sum(part * normed[...].astype(F32), axis=0, keepdims=True)


PIECES = 2
MESH = pl.DeviceIdType.MESH
ANY = pl.BlockSpec(memory_space=pl.ANY)


def remote(src, dst, send, recv, **to):
    return pltpu.make_async_remote_copy(
        src_ref=src, dst_ref=dst, send_sem=send, recv_sem=recv, device_id=to, device_id_type=MESH
    )


def greet(barrier, when, **to):
    @pl.when(when)
    def _():
        pl.semaphore_signal(barrier, inc=1, device_id=to, device_id_type=MESH)


def line_of(ref):
    return ref[...].reshape(1, ref.shape[0])


def start(copies):
    for copy in copies:
        copy.start()


def guarded(when, action):
    @pl.when(when)
    def _():
        action()


class LineGather:
    def __init__(self, ncol, z, first, second, extra, sems):
        self.ncol, self.z, self.last = ncol, z, ncol - 1
        self.parts = (first, second)
        self.extra = extra
        self.sems = sems
        self.tokens = second[1].shape[0] // ncol
        self.part = self.tokens // PIECES

    def copies(self, kind, s, way, pieces, mine=False):
        source, dest = self.parts[kind]
        send, recv = self.sems[2 * kind : 2 * kind + 2]
        to = self.z + 1 if way == 0 else self.z - 1
        made = []
        for p in pieces:
            at = pl.ds(pl.multiple_of(s * self.tokens + p * self.part, self.part), self.part)
            src = source.at[pl.ds(p * self.part, self.part)] if mine and source is not None else dest.at[at]
            made.append(remote(src, dest.at[at], send.at[way, s, p], recv.at[s, p], col=to))
            if kind == 0 and p == PIECES - 1:
                place = self.extra.at[pl.ds(pl.multiple_of(s * 8, 8), 8)]
                made.append(remote(place, place, send.at[way, s, PIECES], recv.at[s, PIECES], col=to))
        return made

    def exit(self, way):
        return self.z < self.last if way == 0 else self.z > 0

    def depth(self, way):
        return self.z if way == 0 else self.last - self.z

    def begin(self):
        every = range(PIECES)
        for way in range(2):
            guarded(self.exit(way), lambda way=way: start(self.copies(0, self.z, way, every, True)))
        for way in range(2):
            guarded(self.depth(way) == 0, lambda way=way: start(self.copies(1, self.z, way, every, True)))

    ticks = property(lambda self: 2 * self.last * PIECES)

    def tick(self, tau):
        j, p = (tau - 1) // PIECES, (tau - 1) % PIECES
        for way in range(2):
            depth = self.depth(way)
            sign = -1 if way == 0 else 1

            def relay(kind, s, way=way, depth=depth):
                for copy in self.copies(kind, s, way, (p,)):
                    copy.wait_recv()
                guarded(self.exit(way), lambda: start(self.copies(kind, s, way, (p,))))
                if kind == 0 and p == PIECES - 1:
                    guarded(self.exit(way) & (j == depth - 1),
                            lambda: start(self.copies(1, self.z, way, range(PIECES), True)))

            guarded(j < depth, lambda s=self.z + sign * (j + 1), relay=relay: relay(0, s))
            guarded((j >= depth) & (j < 2 * depth),
                    lambda s=self.z + sign * (j - depth + 1), relay=relay: relay(1, s))

    def drain(self):
        for kind in range(2):
            for way in range(2):
                sign = -1 if way == 0 else 1
                for s in range(self.ncol):

                    def wait(kind=kind, way=way, s=s, sign=sign):
                        for copy in self.copies(kind, self.z + sign * s, way, range(PIECES)):
                            copy.wait_send()

                    guarded(self.exit(way) & (s <= self.depth(way)), wait)


def mixer_kernel(ncol, ndp, full_width, *refs):
    refs = list(refs)

    def take(number):
        taken = refs[:number]
        del refs[:number]
        return taken

    tokens_in, gain, seg_in, ci, cib, gg, cs, csb, sb, rl, sg = take(11)
    zx, bc_in, dt_in, w2, cot_in = take(5)
    normed_hbm, gsmall_hbm, ggate_hbm, cot_hbm, gnorm_hbm, ginner_hbm, part_hbm = take(7)
    par, par_s, par_h, gain_out, total_out = take(5)
    normed, seg, w_in, w_small, out_t, cot = take(6)
    taps, taps_s, heads = take(3)
    both, shared, step = take(3)
    ssd, x, bc, dt, c, ct, dec, enter, slope, slope_s, state, start_state, total = take(13)
    gated, gnorm, projected, back, dy, ggate, rowterm, dstart, dend = take(9)
    ginner, gsmall, part, edge, edge_in, last_rows = take(6)
    dstate, carry, carry_s, carry_links, grads_bc = take(5)
    squares, squares_all, inner, inner_all, slots = take(5)
    line_box, line_send, line_recv = take(3)
    xs_send, xs_recv, cs_send, cs_recv, w_send, c_send, w_recv, t_send, t_recv = take(9)
    sum_send, sum_recv, row_send, row_recv, here = take(5)

    dp, row, z = lax.axis_index("dp"), lax.axis_index("row"), lax.axis_index("col")
    other = 1 - row
    last = ncol - 1
    tokens = tokens_in.shape[0]
    tail = HALO
    length = ncol * tokens
    width = taps.shape[1]
    scols = taps_s.shape[1]
    state_dim = scols // 2
    chunks = length // SPAN
    rows = bc_in.shape[0]
    me = dp * 2 + row
    sends_tail = (row == 0) & (z == last)

    barrier = pltpu.get_barrier_semaphore()
    for s in range(1, ncol):
        greet(barrier, row >= 0, col=lax.rem(z + s, ncol))
    greet(barrier, row >= 0, row=other)
    for m in range(1, ndp):
        greet(barrier, row >= 0, dp=dp ^ m)
    greet(barrier, row == 1, row=0, col=last)
    for s in range(ncol):
        greet(barrier, sends_tail, row=1, col=s)

    seg[pl.ds(pl.multiple_of(z * 8, 8), 8)] = jnp.broadcast_to(line_of(seg_in), (8, tokens))
    base = pl.multiple_of(z * tokens, 32)
    gain_row = line_of(gain)

    def normalize(n, carried):
        at = pl.multiple_of(n * 32, 32)
        wide = tokens_in[pl.ds(at, 32)].astype(F32)
        scale = lax.rsqrt(jnp.sum(wide * wide, axis=1, keepdims=True) / wide.shape[1] + EPS)
        normed[pl.ds(pl.multiple_of(base + at, 32), 32)] = (wide * scale * gain_row).astype(BF16)
        return carried

    lax.fori_loop(0, tokens // 32, normalize, 0)

    @pl.when(row == 0)
    def _():
        seg[pl.ds(ncol * 8, 8)] = jnp.full((8, tokens), -1, jnp.int32)
        normed[pl.ds(length, tail)] = jnp.zeros((tail, normed.shape[1]), BF16)
        start_state[...] = jnp.zeros_like(start_state)

    @pl.when(row == 1)
    def _():
        dend[...] = jnp.zeros_like(dend)
        edge_in[...] = jnp.zeros_like(edge_in)

    count = ncol - 1 + ndp + row + jnp.where(sends_tail, ncol, 0)
    pl.semaphore_wait(barrier, count)

    weights = ((None, w_in), (None, w_small), (w2, out_t))

    def weight_rows(j):
        return pl.ds(pl.multiple_of(j * rows, 16), rows)

    def weight_copies(j, mine, send, **to):
        copies = []
        for i, (src, dst) in enumerate(weights):
            place = dst.at[weight_rows(j)]
            from_input = mine and src is not None
            copies.append(remote(src if from_input else place, place, send.at[i], w_recv.at[j, i], **to))
        return copies

    def tail_copies(s):
        place = seg.at[pl.ds(pl.multiple_of(z * 8, 8), 8)]
        end = pl.multiple_of(z * tokens + tokens - tail, 16)
        return [
            remote(normed.at[pl.ds(end, tail)], normed.at[pl.ds(length, tail)],
                   t_send.at[s, 0], t_recv.at[0], row=1, col=s),
            remote(place, seg.at[pl.ds(ncol * 8, 8)], t_send.at[s, 1], t_recv.at[1], row=1, col=s),
        ]

    for s in range(ncol):
        guarded(sends_tail, lambda s=s: start(tail_copies(s)))
    gather = LineGather(ncol, z, (None, normed), (cot_in, cot), seg, (xs_send, xs_recv, cs_send, cs_recv))
    gather.begin()
    w_in[weight_rows(me), 0:width] = zx[:, 0, :]
    w_in[weight_rows(me), width : 2 * width] = zx[:, 1, :]
    w_small[weight_rows(me), 0:scols] = bc_in[...]
    dt_rows = jnp.concatenate([dt_in[...].astype(F32), jnp.zeros((128 - dt_in.shape[0], rows), F32)], axis=0)
    w_small[weight_rows(me), scols : scols + 128] = dt_rows.T.astype(BF16)
    local = [
        pltpu.make_async_copy(cot_in, cot.at[pl.ds(base, tokens)], here.at[0]),
        pltpu.make_async_copy(w2, out_t.at[weight_rows(me)], here.at[1]),
    ]
    start(local)
    taps[0:4] = ci[...]
    taps[4:5] = line_of(cib)
    taps[5:6] = line_of(gg)
    sg_row = line_of(sg)
    lo1 = iota((1, 128), 1) < 64
    for p in range(width // 128):
        taps[6:7, p * 128 : (p + 1) * 128] = pick(lo1, sg_row, 2 * p)
    taps_s[0:4] = cs[...]
    taps_s[4:5] = line_of(csb)
    heads[...] = jnp.zeros_like(heads)
    heads[0:1, : sb.shape[0]] = line_of(sb)
    heads[1:2, : rl.shape[0]] = line_of(rl)
    for ref in (state, total, dstart, carry, carry_s, carry_links, par, par_s, par_h):
        ref[...] = jnp.zeros_like(ref)

    for m in range(1, ndp):
        start(weight_copies(me, True, w_send.at[m], dp=dp ^ m))
    start(weight_copies(me, True, c_send.at[0], row=other))

    def pass_weights(m):
        j = (dp ^ m) * 2 + row
        for copy in weight_copies(j, False, w_send.at[m], dp=dp ^ m):
            copy.wait_recv()
        start(weight_copies(j, False, c_send.at[m], row=other))

    half = gather.ticks // 2
    due = {tau: [] for tau in range(1, half + 1)}
    for m in range(1, ndp):
        due[min(half - 1, 2 + (3 * (m - 1)) // (ndp - 1) * (half - 3) // 2)].append(m)
    for tau in range(1, half):
        gather.tick(tau)
        for m in due[tau]:
            pass_weights(m)
    for m in range(ndp):
        for copy in weight_copies((dp ^ m) * 2 + other, False, c_send.at[m], row=other):
            copy.wait_recv()
    guarded(row == 1, lambda: [copy.wait_recv() for copy in tail_copies(0)])
    for copy in local:
        copy.wait()

    def nth(n):
        return pl.multiple_of(jnp.where(z * 2 < ncol, n, last - n) * tokens, tokens)

    def put(at, size, value, small):
        both[pl.ds(at, size)] = value.astype(BF16)
        shared[pl.ds(at, size)] = small[:, :scols].astype(BF16)
        step[pl.ds(at, size)] = small[:, scols:]

    def project_tokens(n, with_tail):
        at = nth(n)
        lhs = normed[pl.ds(at, tokens)]
        if with_tail:
            lhs = jnp.concatenate([lhs, normed[pl.ds(length, tail)]], axis=0)
        value, small = nn(lhs, w_in[...]), nn(lhs, w_small[...])
        put(at, tokens, value[:tokens], small[:tokens])
        if with_tail:
            put(length, tail, value[tokens:], small[tokens:])

    for n in range(ncol - 1):
        project_tokens(n, n == 0)
    gather.tick(half)
    project_tokens(ncol - 1, False)
    outs = [pltpu.make_async_copy(normed, normed_hbm, here.at[4])]
    outs[0].start()

    def at_rows(k):
        return pl.ds(pl.multiple_of(k * SPAN, SPAN), SPAN)

    def common(k):
        this = at_rows(k)
        above = pl.ds(pl.multiple_of(jnp.where(k == 0, length, k * SPAN - HALO), HALO), HALO)
        prev = pl.ds(pl.multiple_of(jnp.where(k == 0, chunks, k - 1) * 8, 8), 8)
        side = pl.ds(width, width)
        return (
            both.at[this, side], both.at[above, side], shared.at[this], shared.at[above], step.at[this],
            seg.at[pl.ds(pl.multiple_of(k * 8, 8), 8)], seg.at[prev], seg.at[pl.ds(chunks * 8, 8)], taps, taps_s, heads,
        )

    later = list(range(half + 1, gather.ticks + 1))

    def forward(k, carried):
        this = at_rows(k)
        forward_body(*common(k), ssd.at[this], x.at[this], bc.at[this], dt.at[this], c.at[this],
                     ct.at[:, this], dec.at[this], enter.at[k], slope.at[this], slope_s.at[this], state, total)
        guarded(k == chunks // 2, lambda: gather.tick(half + 1))
        return carried

    lax.fori_loop(0, chunks, forward, 0)
    later.pop(0)

    def row_copy(n, src, dst):
        return remote(src, dst, row_send.at[n], row_recv.at[n], row=other)

    guarded(row == 0, lambda: row_copy(0, state, start_state).start())
    gather.tick(later.pop(0))
    guarded(row == 1, lambda: row_copy(0, state, start_state).wait_recv())

    def gating(k, carried):
        this = at_rows(k)
        gate_body(ssd.at[this], x.at[this], bc.at[this], dec.at[this], start_state, both.at[this, pl.ds(0, width)],
                  taps, ssd.at[this], gated.at[this], squares.at[:, this])
        return carried

    lax.fori_loop(0, chunks, gating, 0)

    def sum_copy(n, value, s, source):
        return remote(value, slots.at[n, source], sum_send.at[n, s], sum_recv.at[n, source],
                      col=lax.rem(z + s, ncol))

    def sum_begin(n, value):
        for s in range(1, ncol):
            sum_copy(n, value, s, z).start()

    def sum_end(n, value, out):
        result = value[...]
        for s in range(1, ncol):
            source = lax.rem(z + s, ncol)
            sum_copy(n, value, s, source).wait_recv()
            result = result + slots[n, source]
        out[...] = result

    sum_begin(0, squares)
    gather.tick(later.pop(0))
    sum_end(0, squares, squares_all)

    def projecting(k, carried):
        this = at_rows(k)
        project_body(full_width, gated.at[this], squares_all.at[:, this], taps, out_t, gnorm.at[this], projected.at[this])
        return carried

    lax.fori_loop(0, chunks, projecting, 0)
    line = LineReduce(ncol, z, projected, projected, line_box, line_send, line_recv, False)
    while len(later) > 2:
        gather.tick(later.pop(0))

    def pulling(n):
        this = pl.ds(nth(n), tokens)
        pull_body(cot.at[this], out_t, gated.at[this], taps, back.at[this], inner.at[:, this])

    for n in range(ncol - 1):
        pulling(n)
        if n == 0:
            gather.tick(later.pop(0))
    gather.tick(later.pop(0))
    ticks = list(range(1, line.ticks + 1))
    pulling(ncol - 1)
    outs.append(pltpu.make_async_copy(cot, cot_hbm, here.at[5]))
    outs.append(pltpu.make_async_copy(gnorm, gnorm_hbm, here.at[6]))
    start(outs[1:])
    sum_begin(1, inner)
    sum_end(1, inner, inner_all)
    line.start(0, line.ticks)

    def pull_gate(k, carried):
        this = at_rows(k)
        back_body(full_width, ssd.at[this], x.at[this], bc.at[this], dec.at[this], both.at[this, pl.ds(0, width)],
                  back.at[this], squares_all.at[:, this], inner_all.at[:, this], taps,
                  dy.at[this], ggate.at[this], rowterm.at[this], par, dstart)
        return carried

    lax.fori_loop(0, chunks, pull_gate, 0)
    guarded(row == 1, lambda: row_copy(1, dstart, dend).start())
    outs.append(pltpu.make_async_copy(ggate, ggate_hbm, here.at[7]))
    outs[-1].start()
    guarded(row == 0, lambda: row_copy(1, dstart, dend).wait_recv())
    dstate[...] = dend[...]

    spaced = {n: [tau] for n, tau in enumerate(ticks[:chunks])}
    ticks = ticks[chunks:]

    def backward(n, carried):
        k = chunks - 1 - n
        this = at_rows(k)
        before = pl.ds(pl.multiple_of(jnp.maximum(k * SPAN - 8, 0), 8), 8)
        backward_body(k, chunks, *common(k), dy.at[this], x.at[this], bc.at[this], dt.at[this], c.at[this],
                      ct.at[:, this], dec.at[before], enter.at[k], slope.at[this], slope_s.at[this], start_state, rowterm.at[this],
                      ginner.at[this], gsmall.at[this], par, par_s, par_h, edge, last_rows,
                      dstate, carry, carry_s, carry_links, grads_bc)
        for turn, taus in spaced.items():
            if turn < chunks - 1:
                for tau in taus:
                    guarded(n == turn, lambda tau=tau: line.tick(tau))
        return carried

    lax.fori_loop(0, chunks, backward, 0)
    guarded(row == 1, lambda: row_copy(2, edge, edge_in).start())
    for tau in spaced.get(chunks - 1, []):
        line.tick(tau)
    guarded(row == 0, lambda: row_copy(2, edge, edge_in).wait_recv())
    fixed = (last_rows[...] + edge_in[...]).astype(BF16)
    ginner[length - 8 :] = fixed[:, :width]
    gsmall[length - 8 :, : fixed.shape[1] - width] = fixed[:, width:]
    outs.append(pltpu.make_async_copy(ginner, ginner_hbm, here.at[8]))
    outs.append(pltpu.make_async_copy(gsmall, gsmall_hbm, here.at[9]))
    start(outs[-2:])

    tile = 256
    tiles = part.shape[1] // tile

    def part_copy(n):
        at = pl.ds(pl.multiple_of(n * tile, tile), tile)
        return pltpu.make_async_copy(part.at[:, at], part_hbm.at[:, at], here.at[10 + n])

    def spreading(n, carried):
        at = pl.ds(pl.multiple_of(n * tile, tile), tile)
        spread_body(ggate, ginner, gsmall, w_in.at[at], w_small.at[at], normed.at[pl.ds(0, length), at],
                    part.at[:, at], gain_out.at[:, at])
        guarded(n > 0, lambda: part_copy(jnp.maximum(n - 1, 0)).start())
        for tau in ticks[:-1]:
            guarded(n == tiles // 2, lambda tau=tau: line.tick(tau))
        return carried

    lax.fori_loop(0, tiles, spreading, 0)
    part_copy(tiles - 1).start()
    for tau in ticks[-1:]:
        line.tick(tau)

    def keep(at, value):
        total_out[pl.ds(pl.multiple_of(at, 16), 16)] = value.astype(BF16)

    line.total(keep)

    gather.drain()
    line.drain()
    for m in range(ndp):
        if m:
            for copy in weight_copies(me, True, w_send.at[m], dp=dp ^ m):
                copy.wait_send()
        for copy in weight_copies((dp ^ m) * 2 + row, m == 0, c_send.at[m], row=other):
            copy.wait_send()
    for s in range(ncol):
        guarded(sends_tail, lambda s=s: [copy.wait_send() for copy in tail_copies(s)])
    for n, value in ((0, squares), (1, inner)):
        for s in range(1, ncol):
            sum_copy(n, value, s, z).wait_send()
    guarded(row == 0, lambda: row_copy(0, state, start_state).wait_send())
    guarded(row == 1, lambda: row_copy(1, dstart, dend).wait_send())
    guarded(row == 1, lambda: row_copy(2, edge, edge_in).wait_send())
    for copy in outs:
        copy.wait()
    for n in range(tiles):
        part_copy(n).wait()


def run_mixer(full_width, tokens_in, gain, seg, ci, cib, gg, cs, csb, sb, rl, sg, zx, bc, dt, w2, cot):
    ncol, ndp = lax.axis_size("col"), lax.axis_size("dp")
    tokens, model = tokens_in.shape
    width, scols = ci.shape[1], cs.shape[1]
    length = ncol * tokens
    chunks = length // SPAN
    state_dim = scols // 2
    small = scols + 128
    shards = 2 * ndp
    S = jax.ShapeDtypeStruct
    V = pltpu.VMEM
    dma = pltpu.SemaphoreType.DMA
    vmem = pl.BlockSpec(memory_space=V)
    return pl.pallas_call(
        functools.partial(mixer_kernel, ncol, ndp, full_width),
        in_specs=[vmem] * 14 + [ANY] * 2,
        out_specs=[ANY] * 7 + [vmem] * 5,
        out_shape=[
            S((length + HALO, model), BF16), S((length, small), BF16), S((length, width), BF16), S((length, model), BF16),
            S((length, width), BF16), S((length, width), BF16), S((length, model), BF16),
            S((8, width), F32), S((8, scols), F32), S((8, 128), F32), S((1, model), F32), S((tokens, model), BF16),
        ],
        scratch_shapes=[
            V((length + HALO, model), BF16), V(((ncol + 1) * 8, tokens), jnp.int32), V((model, 2 * width), BF16),
            V((model, small), BF16), V((model, width), BF16), V((length, model), BF16),
            V((8, width), F32), V((8, scols), F32), V((8, 128), F32),
            V((length + HALO, 2 * width), BF16), V((length + HALO, scols), BF16), V((length + HALO, 128), F32),
            V((length, width), F32), V((length, width), BF16), V((length, scols), BF16), V((length, 128), F32),
            V((length, 128), F32), V((16, length), F32), V((length, 128), F32), V((chunks, state_dim, width), BF16),
            V((length, width), BF16), V((length, scols), BF16),
            V((state_dim, width), F32), V((state_dim, width), F32), V((8, 128), F32),
            V((length, width), BF16), V((length, width), BF16), V((length, model), BF16), V((length, width), BF16),
            V((length, width), BF16), V((length, width), BF16), V((length, 128), F32), V((state_dim, width), F32),
            V((state_dim, width), F32),
            V((length, width), BF16), V((length, small), BF16), V((length, model), BF16),
            V((8, width + scols), F32), V((8, width + scols), F32), V((8, width + scols), F32),
            V((state_dim, width), F32), V((8, width), F32), V((8, scols), F32), V((8, 128), F32), V((SPAN, scols), F32),
            V((8, length), F32), V((8, length), F32), V((8, length), F32), V((8, length), F32),
            V((2, ncol, 8, length), F32),
            *line_scratch(ncol, tokens, model),
            dma((2, ncol, PIECES + 1)), dma((ncol, PIECES + 1)), dma((2, ncol, PIECES)), dma((ncol, PIECES)),
            dma((ndp, 3)), dma((ndp, 3)), dma((shards, 3)), dma((ncol, 2)), dma((2,)),
            dma((2, ncol)), dma((2, ncol)), dma((3,)), dma((3,)), dma((10 + model // 256,)),
        ],
        compiler_params=pltpu.CompilerParams(
            collective_id=1, has_side_effects=True, vmem_limit_bytes=63 * 1024 * 1024
        ),
        cost_estimate=pl.CostEstimate(flops=0, bytes_accessed=500_000_000, transcendentals=0),
        name="mixer",
    )(tokens_in, gain, seg, ci, cib, gg, cs, csb, sb, rl, sg, zx, bc, dt, w2, cot)
class LineReduce:
    def __init__(self, ncol, z, source, local, inbox, send, recv, paced):
        self.paced = paced
        self.ncol, self.z, self.last = ncol, z, ncol - 1
        self.source, self.local, self.inbox = source, local, inbox
        self.send, self.recv = send, recv
        self.tokens = local.shape[0] // ncol
        self.part = self.tokens // PIECES

    def rows(self, way, t, p):
        d = self.last - t if way == 0 else t
        return pl.multiple_of(d * self.tokens + p * self.part, self.part)

    def copy(self, way, t, p, first):
        src = self.source.at[pl.ds(self.rows(way, t, p), self.part)] if first else self.inbox.at[way, t, p]
        to = self.z + 1 if way == 0 else self.z - 1
        return remote(src, self.inbox.at[way, t, p], self.send.at[way, t, p], self.recv.at[way, t, p], col=to)

    def edge(self, way):
        return self.z == (0 if way == 0 else self.last)

    def depth(self, way):
        return self.z if way == 0 else self.last - self.z

    def start(self, first=0, stop=2):
        for way in range(2):

            @pl.when(self.edge(way))
            def _(way=way):
                for i in range(first, min(stop, self.ticks)):
                    self.copy(way, i // PIECES, i % PIECES, True).start()

    ticks = property(lambda self: self.last * PIECES)

    def tick(self, tau):
        for way in range(2):

            @pl.when(self.edge(way) & (self.paced and tau + 1 < self.ticks))
            def _(way=way):
                self.copy(way, (tau - 1) // PIECES, (tau - 1) % PIECES, True).wait_send()
                self.copy(way, (tau + 1) // PIECES, (tau + 1) % PIECES, True).start()

        for stage in range(2):
            for way in range(2):
                depth = self.depth(way)
                index = tau - (2 * depth - 1)
                t, p = index // PIECES, lax.rem(index, PIECES)

                @pl.when((depth > 0) & (index >= 0) & (index < (self.ncol - depth) * PIECES))
                def _(way=way, depth=depth, t=t, p=p, stage=stage):
                    onward = t < self.last - depth
                    if stage == 0:
                        self.copy(way, t, p, False).wait_recv()

                        @pl.when(onward)
                        def _():
                            base = self.rows(way, t, p)

                            def add(k, carry):
                                at = pl.multiple_of(k * 16, 16)
                                mine = self.local[pl.ds(pl.multiple_of(base + at, 16), 16)].astype(F32)
                                here = pl.ds(at, 16)
                                self.inbox[way, t, p, here] = (self.inbox[way, t, p, here].astype(F32) + mine).astype(BF16)
                                return carry

                            lax.fori_loop(0, self.part // 16, add, 0)
                    else:

                        @pl.when(onward)
                        def _():
                            self.copy(way, t, p, False).start()

    def total(self, store):
        z, last = self.z, self.last
        for p in range(PIECES):

            def add(k, carry, p=p):
                at = pl.multiple_of(k * 16, 16)
                here = pl.ds(at, 16)
                row = p * self.part + at
                value = self.local[pl.ds(pl.multiple_of(z * self.tokens + row, 16), 16)].astype(F32)
                low = self.inbox[0, jnp.minimum(last - z, last - 1), p, here].astype(F32)
                high = self.inbox[1, jnp.minimum(z, last - 1), p, here].astype(F32)
                value = value + jnp.where(z > 0, low, 0.0) + jnp.where(z < last, high, 0.0)
                store(row, value)
                return carry

            lax.fori_loop(0, self.part // 16, add, 0)

    def drain(self):
        for way in range(2):
            depth = self.depth(way)

            @pl.when(self.edge(way))
            def _(way=way):
                for i in range(self.ticks - 2 if self.paced else 0, self.ticks):
                    self.copy(way, i // PIECES, i % PIECES, True).wait_send()

            for t in range(self.last):

                @pl.when((depth > 0) & (t < self.last - depth))
                def _(way=way, t=t):
                    for p in range(PIECES):
                        self.copy(way, t, p, False).wait_send()


def line_scratch(ncol, tokens, width):
    shape = (2, ncol - 1, PIECES)
    dma = pltpu.SemaphoreType.DMA
    return [pltpu.VMEM(shape + (tokens // PIECES, width), BF16), dma(shape), dma(shape)]


def reduce_kernel(ncol, ndp, scols, *refs):
    count = 4
    refs = list(refs)

    def take(number):
        taken = refs[:number]
        del refs[:number]
        return taken

    sources = take(7)
    vecs = take(4)
    r, vec_outs, gsum_out = take(count), take(4), refs.pop(0)
    held = take(7)
    (line_box, line_send, line_recv) = take(3)
    g, near, sent, far = take(count), take(count), take(count), take(count)
    vec_slots, col_slots = take(4), take(2)
    col_sums = take(2)
    bc_slots, bc_sum, load, c_send, c_recv, p_send, p_recv, v_send, v_recv, u_send, u_recv, b_send, b_recv = refs
    dp, row, z = lax.axis_index("dp"), lax.axis_index("row"), lax.axis_index("col")
    other = 1 - row
    me = dp * 2 + row
    rows = [out.shape[0] for out in r]
    barrier = pltpu.get_barrier_semaphore()
    for q in range(1, 2 * ndp):
        greet(barrier, row >= 0, dp=dp ^ (q >> 1), row=row ^ (q & 1))
    for s in range(1, ncol):
        greet(barrier, row >= 0, col=lax.rem(z + s, ncol))
    loads = []
    for i, (src, dst) in enumerate(zip(sources, held)):
        src = src.at[pl.ds(0, dst.shape[0])]
        loads.append(pltpu.make_async_copy(src, dst, load.at[i]))
        loads[-1].start()
    normed, gsmall, ggate, cot, gnorm, ginner, part = held
    pl.semaphore_wait(barrier, 2 * ndp + ncol - 2)
    line = LineReduce(ncol, z, sources[6], part, line_box, line_send, line_recv, True)
    line.start()

    order = (0, 1, 2, 3)
    turns = [3, 1, 2, 0] if ndp == 4 else list(range(1, ndp)) + [0]

    def core_copy(i, d):
        return remote(g[i].at[pl.ds((d * 2 + other) * rows[i], rows[i])], near[i].at[d],
                      c_send.at[i, d], c_recv.at[i, d], row=other)

    def vec_copy(q, i, j):
        return remote(vecs[i], vec_slots[i].at[j], v_send.at[q, i], v_recv.at[j, i],
                      dp=dp ^ (q >> 1), row=row ^ (q & 1))

    for q in range(1, 2 * ndp):
        for i in range(4):
            vec_copy(q, i, me).start()

    waiting = []

    def later(copy):
        if waiting:
            waiting.pop().start()
        if copy is not None:
            waiting.append(copy)

    def accumulate(i, first, number, terms, store):
        def step(k, carry):
            at = first + pl.multiple_of(k * 16, 16)
            total = terms[0](at)
            for term in terms[1:]:
                total = total + term(at)
            store(at, total)
            return carry

        lax.fori_loop(0, number // 16, step, 0)

    def read(ref, index, shift=0):
        return lambda at: ref[index, pl.ds(at - shift, 16)].astype(F32)

    def mine(i, d):
        return lambda at: g[i][pl.ds(pl.multiple_of((d * 2 + row) * rows[i] + at, 16), 16)].astype(F32)

    def write(ref, index, shift):
        def store(at, total):
            ref[index, pl.ds(at - shift, 16)] = total.astype(BF16)

        return store

    def arrived(i, d):
        core_copy(i, d).wait_recv()

    def tick():
        if ticks:
            line.tick(ticks.pop(0))

    if ndp == 4:
        halves = ((0, 1, 2), (1, 2, 1))

        def leg(i, slot, m):
            return remote(sent[i].at[slot], far[i].at[slot], p_send.at[i, slot], p_recv.at[i, slot], dp=dp ^ m)

        def step_one(i):
            half = rows[i] // 2
            arrived(i, dp ^ 3)
            for h, m1, m2 in halves:
                accumulate(i, h * half, half, [mine(i, dp ^ 3), read(near[i], dp ^ 3)],
                           write(sent[i], 3 * h + 1, h * half))
                later(leg(i, 3 * h + 1, m1))
            for h, m1, m2 in halves:
                arrived(i, dp ^ m1)
                accumulate(i, h * half, half, [mine(i, dp ^ m1), read(near[i], dp ^ m1)],
                           write(sent[i], 3 * h, h * half))
                later(leg(i, 3 * h, m1))
            later(None)
            arrived(i, dp)

        def relay(i):
            half = rows[i] // 2
            for h, m1, m2 in halves:
                leg(i, 3 * h + 1, m1).wait_recv()
                accumulate(i, h * half, half,
                           [mine(i, dp ^ m2), read(near[i], dp ^ m2), read(far[i], 3 * h + 1, h * half)],
                           write(sent[i], 3 * h + 2, h * half))
                later(leg(i, 3 * h + 2, m2))
            later(None)

        def finish(i, store):
            half = rows[i] // 2
            for h, m1, m2 in halves:
                leg(i, 3 * h, m1).wait_recv()
                leg(i, 3 * h + 2, m2).wait_recv()
                accumulate(i, h * half, half,
                           [mine(i, dp), read(near[i], dp), read(far[i], 3 * h, h * half),
                            read(far[i], 3 * h + 2, h * half)], store)

        sends = [leg(i, 3 * h + k, m2 if k == 2 else m1) for i in order for h, m1, m2 in halves for k in range(3)]
    else:

        def peer(i, m):
            return remote(sent[i].at[m], far[i].at[m], p_send.at[i, m], p_recv.at[i, m], dp=dp ^ m)

        def step_one(i):
            for m in turns[:-1]:
                arrived(i, dp ^ m)
                accumulate(i, 0, rows[i], [mine(i, dp ^ m), read(near[i], dp ^ m)], write(sent[i], m, 0))
                later(peer(i, m))
            later(None)
            arrived(i, dp)

        def relay(i):
            pass

        def finish(i, store):
            for m in range(1, ndp):
                peer(i, m).wait_recv()
            accumulate(i, 0, rows[i],
                       [mine(i, dp), read(near[i], dp)] + [read(far[i], m) for m in range(1, ndp)], store)

        sends = [peer(i, m) for i in order for m in range(1, ndp)]

    def plain(i):
        def store(at, total):
            r[i][pl.ds(at, 16)] = total

        return store

    def shared_rows(at, total):
        r[0][pl.ds(at, 16)] = total
        bc_slots[z, pl.ds(at, 16)] = total[:, : bc_slots.shape[2]].astype(BF16)

    root = ncol // 2
    at_root = z == root

    def to_root(source):
        pairs = [(col_slots[i].at[source], u_send.at[0, i], u_recv.at[source, i]) for i in range(2)]
        pairs.append((bc_slots.at[source], b_send.at[0], b_recv.at[source]))
        return [remote(ref, ref, send, recv, col=root) for ref, send, recv in pairs]

    def from_root(target):
        pairs = [(col_sums[i], u_send.at[target, i], u_recv.at[root, i]) for i in range(2)]
        pairs.append((bc_sum, b_send.at[target], b_recv.at[root]))
        return [remote(ref, ref, send, recv, col=target) for ref, send, recv in pairs]

    others = [s for s in range(ncol) if s != root]

    def sum_at_root():
        @pl.when(at_root)
        def _():
            for s in others:
                for copy in to_root(s):
                    copy.wait_recv()
            for i in range(2):
                total = col_slots[i][0]
                for j in range(1, ncol):
                    total = total + col_slots[i][j]
                col_sums[i][...] = total
            total = bc_slots[0].astype(F32)
            for j in range(1, ncol):
                total = total + bc_slots[j].astype(F32)
            bc_sum[...] = total.astype(BF16)
            for s in others:
                for copy in from_root(s):
                    copy.start()

    model = normed.shape[1]
    block = model // 4
    products = ((normed, gsmall), (normed, ggate), (cot, gnorm), (normed, ginner))
    ready = {0: (0, 1), 1: (2,), 2: (3, 4), 3: (5,)}
    ticks = list(range(1, line.ticks + 1))
    for i in order:
        for at in ready[i]:
            loads[at].wait()
        left, right = products[i]
        for n, m in enumerate([3, 1, 2, 0] if ndp == 4 else range(4)):
            b = dp ^ m if ndp == 4 else m
            first = pl.multiple_of(b * block, 128)
            g[i][pl.ds(pl.multiple_of(b * block, 16), block)] = tn(left[:, pl.ds(first, block)], right[...]).astype(BF16)
            if ndp == 4:
                later(core_copy(i, b))
        if ndp != 4:
            for m in turns:
                later(core_copy(i, dp ^ m))
        if i == 1:
            loads[6].wait()
        if i > 0:
            step_one(i - 1)
        if i > 1:
            relay(i - 2)
        if i % 2:
            tick()
    later(None)
    step_one(3)
    relay(2)
    finish(0, shared_rows)
    for q in range(1, 2 * ndp):
        for i in range(4):
            vec_copy(q, i, me ^ q).wait_recv()
    for i in range(4):
        vec_slots[i][me] = vecs[i][...]
        total = vec_slots[i][0]
        for j in range(1, 2 * ndp):
            total = total + vec_slots[i][j]
        if i < 2:
            vec_outs[i][...] = total
        else:
            col_slots[i - 2][z] = total

    @pl.when(~at_root)
    def _():
        for copy in to_root(z):
            copy.start()

    tick()
    relay(3)
    while len(ticks) > 1:
        tick()
    sum_at_root()
    finish(1, plain(1))
    finish(2, plain(2))
    finish(3, plain(3))
    while ticks:
        tick()

    def keep(at, value):
        gsum_out[pl.ds(pl.multiple_of(at, 16), 16)] = value.astype(BF16)

    line.total(keep)
    @pl.when(~at_root)
    def _():
        for copy in from_root(z):
            copy.wait_recv()

    for i in range(2):
        vec_outs[2 + i][...] = col_sums[i][...]
    r[0][:, : bc_slots.shape[2]] = bc_sum[...].astype(F32)

    for q in range(1, 2 * ndp):
        for i in range(4):
            vec_copy(q, i, me).wait_send()
    for i in order:
        for m in turns:
            core_copy(i, dp ^ m).wait_send()
    for copy in sends:
        copy.wait_send()
    @pl.when(~at_root)
    def _():
        for copy in to_root(z):
            copy.wait_send()

    @pl.when(at_root)
    def _():
        for s in others:
            for copy in from_root(s):
                copy.wait_send()

    line.drain()


def reduce_grads(sources, vecs, scols):
    ncol, ndp = lax.axis_size("col"), lax.axis_size("dp")
    dma = pltpu.SemaphoreType.DMA
    vmem = pl.BlockSpec(memory_space=pltpu.VMEM)
    S = jax.ShapeDtypeStruct
    length = sources[1].shape[0]
    model = sources[0].shape[1]
    widths = [sources[1].shape[1], sources[2].shape[1], sources[4].shape[1], sources[5].shape[1]]
    count = len(widths)
    blocks = [(model // (2 * ndp), w) for w in widths]
    near = [pltpu.VMEM((ndp,) + b, BF16) for b in blocks]
    slots = 6 if ndp == 4 else ndp
    legs = [pltpu.VMEM((6, b[0] // 2, b[1]) if ndp == 4 else (ndp,) + b, BF16) for b in blocks]
    tokens = length // ncol
    return pl.pallas_call(
        functools.partial(reduce_kernel, ncol, ndp, scols),
        in_specs=[ANY] * 7 + [vmem] * 4,
        out_specs=[vmem] * (count + 5),
        out_shape=[S(b, F32) for b in blocks] + [S(v.shape, F32) for v in vecs] + [S((tokens, model), BF16)],
        scratch_shapes=[pltpu.VMEM((length, s.shape[1]), BF16) for s in sources]
        + line_scratch(ncol, tokens, model)
        + [pltpu.VMEM((model, w), BF16) for w in widths]
        + near + legs * 2
        + [pltpu.VMEM((2 * ndp,) + v.shape, F32) for v in vecs]
        + [pltpu.VMEM((ncol,) + v.shape, F32) for v in vecs[2:]]
        + [pltpu.VMEM(v.shape, F32) for v in vecs[2:]]
        + [pltpu.VMEM((ncol, blocks[0][0], scols), BF16), pltpu.VMEM((blocks[0][0], scols), BF16)]
        + [dma((7,))]
        + [dma((count, ndp))] * 2
        + [dma((count, slots))] * 2
        + [dma((2 * ndp, 4))] * 2
        + [dma((ncol, 2))] * 2
        + [dma((ncol,))] * 2,
        compiler_params=pltpu.CompilerParams(
            collective_id=2, has_side_effects=True, vmem_limit_bytes=60 * 1024 * 1024
        ),
        cost_estimate=pl.CostEstimate(flops=0, bytes_accessed=200_000_000, transcendentals=0),
        name="reduce_grads",
    )(*sources, *vecs)


def finish_kernel(
    nheads, small, gate, inner, out, par, par_h, par_s, gain_sum, gain, tokens, cot, gnormed, projected,
    zx_out, bc_out, dt_out, out_out, ci_out, cib_out, cs_out, csb_out, sb_out, rl_out, sg_out, gg_out, ng_out, gin_out, block_out,
):
    width = par.shape[1]
    scols = par_s.shape[1]
    gain_row = gain[...].reshape(1, gain.shape[0])
    zx_out[:, 0, :] = gate[...]
    zx_out[:, 1, :] = inner[...]
    bc_out[...] = small[:, :scols]
    dt_out[...] = small[:, scols:].T[:nheads]
    out_out[...] = out[...]
    ci_out[...] = par[0:4]
    cib_out[...] = par[4:5].reshape(width)
    gg_out[...] = par[5:6].reshape(width)
    cs_out[...] = par_s[0:4]
    csb_out[...] = par_s[4:5].reshape(scols)
    sb_out[...] = par_h[0:1, :nheads].reshape(nheads)
    rl_out[...] = par_h[1:2, :nheads].reshape(nheads)
    skip = jnp.zeros((8, 128), F32)
    for p in range(width // 128):
        skip = skip + split_dot(jnp.broadcast_to(par[6:7, p * 128 : (p + 1) * 128], (8, 128)), head_map(p))
    sg_out[...] = skip[0:1, :nheads].reshape(nheads)
    ng_out[...] = (gain_sum[0:1] / gain_row).reshape(gain.shape[0])

    def rows(step, carry):
        at = pl.ds(pl.multiple_of(step * 32, 32), 32)
        wide = tokens[at].astype(F32)
        scale = lax.rsqrt(jnp.sum(wide * wide, axis=1, keepdims=True) / wide.shape[1] + EPS)
        pushed = gnormed[at].astype(F32) * gain_row
        mean = jnp.sum(pushed * wide, axis=1, keepdims=True) / wide.shape[1]
        grad = scale * pushed - wide * (scale * scale * scale * mean)
        gin_out[at] = (cot[at].astype(F32) + grad).astype(BF16)
        block_out[at] = (wide + projected[at].astype(F32)).astype(BF16)
        return carry

    lax.fori_loop(0, tokens.shape[0] // 32, rows, 0)


def run_finish(nheads, small, gate, inner, out, par, par_h, par_s, gain_sum, gain, tokens, cot, gnormed, projected):
    rows, width = gate.shape
    scols = par_s.shape[1]
    model = gain.shape[0]
    S = jax.ShapeDtypeStruct
    shapes = [
        (rows, 2, width), (rows, scols), (nheads, rows), (rows, width), (4, width), (width,), (4, scols), (scols,),
        (nheads,), (nheads,), (nheads,), (width,), (model,),
    ]
    return pl.pallas_call(
        functools.partial(finish_kernel, nheads),
        out_shape=[S(shape, F32) for shape in shapes] + [S(tokens.shape, BF16)] * 2,
        name="finish",
    )(small, gate, inner, out, par, par_h, par_s, gain_sum, gain, tokens, cot, gnormed, projected)


def per_device(
    block_input, segment_ids, norm_gain, proj_zx, proj_bc, proj_dt, conv_inner, conv_inner_bias,
    conv_shared, conv_shared_bias, step_bias, rate_log, skip_gain, gated_gain, proj_out, cotangent,
):
    width = proj_zx.shape[2]
    scols = proj_bc.shape[1]
    nheads = proj_dt.shape[1]
    full_width = float(width * lax.axis_size("col"))
    (normed, gsmall, ggate, cot_all, gated_normed, ginner, part, par, par_s, par_h, gain_part, projected) = run_mixer(
        full_width, block_input, norm_gain, segment_ids, conv_inner, conv_inner_bias, gated_gain, conv_shared,
        conv_shared_bias, step_bias, rate_log, skip_gain, proj_zx, proj_bc, proj_dt.T, proj_out.T, cotangent,
    )
    gsm, gz, gout, gx, par, par_h, par_s, gain_sum, grad_normed = reduce_grads(
        (normed, gsmall, ggate, cot_all, gated_normed, ginner, part), (par, par_h, par_s, gain_part), scols
    )
    zx, gbc, gdt, gout, ci, cib, cs, csb, sb, rl, sg, gg, ng, grad_input, block_output = run_finish(
        nheads, gsm, gz, gx, gout, par, par_h, par_s, gain_sum, norm_gain, block_input, cotangent, grad_normed, projected
    )
    return (
        block_output, grad_input, ng, zx, gbc, gdt.T, ci, cib, cs, csb, sb, rl, sg, gg, gout.T,
    )


def solution(mesh):
    shards = ("dp", "row")
    tokens = P(("dp", "row", "col"), None)
    zx = P(shards, None, "col")
    in_specs = (
        tokens, P(("dp", "row", "col")), P(), zx, P(shards, None), P(shards, "col"), P(None, "col"), P("col"),
        P(), P(), P("col"), P("col"), P("col"), P("col"), P("col", shards), tokens,
    )
    out_specs = (
        tokens, tokens, P(), zx, P(shards, None), P(shards, "col"), P(None, "col"), P("col"),
        P(), P(), P("col"), P("col"), P("col"), P("col"), P("col", shards),
    )
    return jax.shard_map(per_device, mesh=mesh, in_specs=in_specs, out_specs=out_specs, check_vma=False)
```

```python
import functools
import jax, jax.numpy as jnp
from jax import lax
from jax.experimental import pallas as pl
from jax.experimental.pallas import tpu as pltpu
from jax.sharding import PartitionSpec as P

F32, BF16 = jnp.float32, jnp.bfloat16
HIGH = lax.Precision.HIGHEST
SPAN = 256
HALO = 16
EPS = 1e-5


def nn(a, b):
    return lax.dot_general(a, b, (((1,), (0,)), ((), ())), preferred_element_type=F32)


def nt(a, b):
    return lax.dot_general(a, b, (((1,), (1,)), ((), ())), preferred_element_type=F32)


def tn(a, b):
    return lax.dot_general(a, b, (((0,), (0,)), ((), ())), preferred_element_type=F32)


def iota(shape, axis):
    return lax.broadcasted_iota(jnp.int32, shape, axis)


def split_dot(a, b01):
    hi = a.astype(BF16)
    lo = (a - hi.astype(F32)).astype(BF16)
    return nn(hi, b01) + nn(lo, b01)


def sigmoid(v):
    return 0.5 * jnp.tanh(0.5 * v) + 0.5


def softplus(v):
    return jnp.maximum(v, 0.0) + jnp.log1p(jnp.exp(-jnp.abs(v)))


def columns(row):
    return jnp.broadcast_to(row, (128, row.shape[1])).T


def segments(seg_row, prev_row, tail_row):
    row = seg_row[0:1].astype(F32)
    seg = columns(row)[:, 0:1]
    length = row.shape[1]
    prev = columns(prev_row[0:1].astype(F32))[length - 8 :, 0:1]
    tail = tail_row[0:1, length - 1 :].astype(F32)
    return row, seg, prev, tail


def chunk_links(segc, halo):
    ext = jnp.concatenate([halo, segc], axis=0)
    length = segc.shape[0]
    return [(ext[8 - j : 8 - j + length] == segc).astype(F32) for j in range(1, 4)]


def conv_tile(cur, halo, links, taps, sl):
    v = jnp.concatenate([halo[HALO - 8 :, sl].astype(F32), cur[:, sl].astype(F32)], axis=0)
    length = cur.shape[0]
    pre = taps[4:5, sl] + taps[3:4, sl] * v[8:]
    for j in range(1, 4):
        pre = pre + taps[3 - j : 4 - j, sl] * (v[8 - j : 8 - j + length] * links[j - 1])
    return pre


def silu_and_slope(pre):
    s = sigmoid(pre)
    value = pre * s
    return value, s + value * (1.0 - s)


def pick(lo, cols, h):
    return jnp.where(lo, cols[:, h : h + 1], cols[:, h + 1 : h + 2])


def forward_body(
    inner, inner_halo, shared, shared_halo, step_raw, seg_row, seg_prev, seg_tail, taps, taps_s, heads,
    y_out, x_out, bc_out, dt_out, c_out, ct_out, dec_out, enter_out, slope_out, slope_s_out, state, total,
):
    length, width = inner.shape
    pairs = width // 128
    state_dim = state.shape[0]

    segr, seg, seg_halo, tail_seg = segments(seg_row, seg_prev, seg_tail)
    links = chunk_links(seg, seg_halo)
    closing = (seg == seg[length - 1 :]).astype(F32)
    entering = (seg == seg_halo[7:]).astype(F32)
    kept = (seg[length - 1 :] == seg_halo[7:]).astype(F32)
    dt = softplus(step_raw[...] + heads[0:1])
    log_decay = -jnp.exp(heads[1:2]) * dt
    rows, cols = iota((length, length), 0), iota((length, length), 1)
    lower = (rows >= cols).astype(F32)
    c = jnp.dot(lower, log_decay, precision=HIGH, preferred_element_type=F32)
    ct = c.T
    dt_out[...] = dt
    c_out[...] = c
    ct_out[...] = ct[: ct_out.shape[0]]
    whole = c + total[0:1]
    dec_out[...] = jnp.exp(whole) * (seg == tail_seg).astype(F32)
    total[0:1] = whole[length - 1 :]
    for half in range(2):
        sl = slice(half * state_dim, (half + 1) * state_dim)
        value, slope = silu_and_slope(conv_tile(shared, shared_halo, links, taps_s, sl))
        bc_out[:, sl] = value.astype(BF16)
        slope_s_out[:, sl] = slope.astype(BF16)
    b = bc_out[:, :state_dim]
    cc = bc_out[:, state_dim:]
    scores = jnp.where((rows >= cols) & (seg == segr), nt(cc, b), 0.0)
    lo = iota((length, 128), 1) < 64
    lo1 = lo[0:1]
    sides = [jnp.where(lo, 1.0, 0.0).astype(BF16), jnp.where(lo, 0.0, 1.0).astype(BF16)]
    arriving = jnp.exp(c) * entering
    leaving = jnp.exp(c[length - 1 :] - c) * closing
    held = jnp.exp(c[length - 1 :]) * kept
    enter_out[...] = state[...].astype(BF16)
    for p in range(pairs):
        sl = slice(p * 128, (p + 1) * 128)
        xp, slope = silu_and_slope(conv_tile(inner, inner_halo, links, taps, sl))
        xb = xp.astype(BF16)
        x_out[:, sl] = xb
        slope_out[:, sl] = slope.astype(BF16)
        xdt = xb.astype(F32) * pick(lo, dt, 2 * p)
        xdtb = xdt.astype(BF16)
        acc = nn(cc, state[:, sl].astype(BF16)) * pick(lo, arriving, 2 * p)
        for a in range(2):
            h = 2 * p + a
            weights = jnp.exp(jnp.minimum(c[:, h : h + 1] - ct[h : h + 1], 0.0)) * scores
            acc = acc + nn(weights.astype(BF16), xdtb * sides[a])
        y_out[:, sl] = acc
        moved = pick(lo, leaving, 2 * p) * xdt
        state[:, sl] = state[:, sl] * pick(lo1, held, 2 * p) + tn(b, moved.astype(BF16))


def row_sums(value):
    hi = value.astype(BF16)
    lo = (value - hi.astype(F32)).astype(BF16)
    ones = jnp.ones((8, value.shape[1]), BF16)
    return nt(ones, hi) + nt(ones, lo)


def first_rows(value):
    return jnp.where(iota(value.shape, 0) == 0, value, 0.0)


def head_map(p):
    lane, head = iota((128, 128), 0), iota((128, 128), 1)
    return (head == 2 * p + lane // 64).astype(BF16)


def gate_body(y, x, bc, dec, start, gate, taps, ssd_out, gained_out, sums_out):
    length, width = x.shape
    state_dim = start.shape[0]
    cc = bc[:, state_dim:]
    lo = iota((length, 128), 1) < 64
    squares = jnp.zeros((length, 128), F32)
    for p in range(width // 128):
        sl = slice(p * 128, (p + 1) * 128)
        corr = nn(cc, start[:, sl].astype(BF16)) * pick(lo, dec, 2 * p)
        ssd = y[:, sl] + corr + taps[6:7, sl] * x[:, sl].astype(F32)
        ssd_out[:, sl] = ssd
        g = gate[:, sl].astype(F32)
        gated = ssd * (g * sigmoid(g))
        gained_out[:, sl] = (gated * taps[5:6, sl]).astype(BF16)
        squares = squares + gated * gated
    sums_out[0:1] = row_sums(squares)[0:1]


def pull_body(cot, out_t, gained, back_out, sums_out):
    back = nn(cot[...], out_t[...])
    back_out[...] = back.astype(BF16)
    inner = jnp.zeros((cot.shape[0], 128), F32)
    for p in range(back.shape[1] // 128):
        sl = slice(p * 128, (p + 1) * 128)
        inner = inner + back[:, sl] * gained[:, sl].astype(F32)
    sums_out[1:2] = row_sums(inner)[0:1]


def back_body(
    full_width, ssd, x, bc, dec, gate, back, sums, taps,
    normed_out, dy_out, ggate_out, row_out, colsum_out, dstart_out,
):
    length, width = x.shape
    state_dim = dstart_out.shape[0]

    cc = bc[:, state_dim:]
    lo = iota((length, 128), 1) < 64
    rescale = columns(lax.rsqrt(sums[0:1] / full_width + EPS))
    pull = columns(sums[1:2]) * (rescale * rescale * rescale / full_width)
    rowterm = jnp.zeros((length, 128), F32)
    for p in range(width // 128):
        sl = slice(p * 128, (p + 1) * 128)
        s_ssd = ssd[:, sl]
        xp = x[:, sl].astype(F32)
        g = gate[:, sl].astype(F32)
        s = sigmoid(g)
        gated = s_ssd * (g * s)
        bk = back[:, sl].astype(F32)
        gain = taps[5:6, sl]
        normed_out[:, sl] = (gated * rescale * gain).astype(BF16)
        gg = rescale * (bk * gain) - gated * pull
        dy = gg * (g * s)
        dyb = dy.astype(BF16)
        dy_out[:, sl] = dyb
        ggate_out[:, sl] = (gg * s_ssd * s * (1.0 + g * (1.0 - s))).astype(BF16)
        colsum_out[5:6, sl] += jnp.sum(bk * gated * rescale, axis=0, keepdims=True)
        colsum_out[6:7, sl] += jnp.sum(dy * xp, axis=0, keepdims=True)
        dstart_out[:, sl] += tn(cc, (dy * pick(lo, dec, 2 * p)).astype(BF16))
        rowterm = rowterm + split_dot(dyb.astype(F32) * (s_ssd - taps[6:7, sl] * xp), head_map(p))
    row_out[...] = rowterm


def conv_back(dout, slope, cur, halo, links, taps, sl, carry, carry_links, par_out, first):
    length = dout.shape[0]
    dconv = dout * slope[:, sl].astype(F32)
    v = cur[:, sl].astype(F32)
    v_above = halo[HALO - 8 :, sl].astype(F32) * first
    nxt = carry[:, sl]
    grad = taps[3:4, sl] * dconv
    above = jnp.zeros((8, dout.shape[1]), F32)
    par_out[3:4, sl] += jnp.sum(dconv * v, axis=0, keepdims=True)
    par_out[4:5, sl] += jnp.sum(dconv, axis=0, keepdims=True)
    for j in range(1, 4):
        z = dconv * links[j - 1]
        w = taps[3 - j : 4 - j, sl]
        low = jnp.concatenate([z, nxt * carry_links[:, j - 1 : j]], axis=0)[j : j + length]
        high = jnp.concatenate([jnp.zeros_like(nxt), z[0:8]], axis=0)[j : j + 8]
        grad = grad + w * low
        above = above + w * high
        par_out[3 - j : 4 - j, sl] += jnp.sum(low * v, axis=0, keepdims=True) + jnp.sum(
            high * v_above, axis=0, keepdims=True
        )
    carry[:, sl] = dconv[0:8]
    return grad, above


def backward_body(
    k, chunks,
    inner, inner_halo, shared, shared_halo, step_raw, seg_row, seg_prev, seg_tail, taps, taps_s, heads,
    dy, x, bc, dt_in, c_in, ct_in, dec_halo, enter, slope, slope_s, start, row_in,
    ginner_out, gsmall_out, par_out, par_s_out, par_h_out, edge_out, last_out,
    dstate, carry, carry_s, carry_links, grads_bc,
):
    length, width = x.shape
    state_dim = dstate.shape[0]

    segr, seg, seg_halo, tail_seg = segments(seg_row, seg_prev, seg_tail)
    links = chunk_links(seg, seg_halo)
    closing = (seg == seg[length - 1 :]).astype(F32)
    entering = (seg == seg_halo[7:]).astype(F32)
    kept = (seg[length - 1 :] == seg_halo[7:]).astype(F32)
    next_links = carry_links[...]
    dt = dt_in[...]
    c = c_in[...]
    ct = ct_in[...]
    first = jnp.where(k == 0, 1.0, 0.0)
    reach = dec_halo[7:8] * (1.0 - first) + first
    b = bc[:, :state_dim]
    cc = bc[:, state_dim:]
    rows, cols = iota((length, length), 0), iota((length, length), 1)
    allowed = (rows <= cols) & (seg == segr)
    scores = jnp.where(allowed, nt(b, cc), 0.0)
    lo = iota((length, 128), 1) < 64
    lo1 = lo[0:1]
    sides = [jnp.where(lo, 1.0, 0.0).astype(BF16), jnp.where(lo, 0.0, 1.0).astype(BF16)]
    arriving = jnp.exp(c) * entering
    leaving_all = jnp.exp(c[length - 1 :] - c) * closing
    held_all = jnp.exp(c[length - 1 :]) * kept
    dscores = jnp.zeros((length, length), F32)
    db = jnp.zeros((length, state_dim), F32)
    dc_mat = jnp.zeros((length, state_dim), F32)
    direct = jnp.zeros((length, 128), F32)
    matched = jnp.zeros((length, 128), F32)
    closing_term = jnp.zeros((1, 128), F32)
    for p in range(width // 128):
        sl = slice(p * 128, (p + 1) * 128)
        dyb = dy[:, sl]
        dyf = dyb.astype(F32)
        xp = x[:, sl].astype(F32)
        dtb = pick(lo, dt, 2 * p)
        xdt = xp * dtb
        xdtb = xdt.astype(BF16)
        hm = head_map(p)
        entry = enter[:, sl].astype(F32) + start[:, sl] * pick(lo1, reach, 2 * p)
        entryb = entry.astype(BF16)
        ds = dstate[:, sl]
        dsb = ds.astype(BF16)
        leaving = pick(lo, leaving_all, 2 * p)
        bds = nn(b, dsb)
        dxdt = jnp.zeros((length, 128), F32)
        for a in range(2):
            h = 2 * p + a
            decay = jnp.exp(jnp.minimum(ct[h : h + 1] - c[:, h : h + 1], 0.0))
            dscores = dscores + decay * nt(xdtb * sides[a], dyb)
            dxdt = dxdt + nn((decay * scores).astype(BF16), dyb * sides[a])
        spread = leaving * xdt
        moved = spread * bds
        matched = matched + split_dot(xdtb.astype(F32) * dxdt + moved, hm)
        dxdt = dxdt + leaving * bds
        held = pick(lo1, held_all, 2 * p)
        col = jnp.sum(moved, axis=0, keepdims=True) + held * jnp.sum(entry * ds, axis=0, keepdims=True)
        closing_term = closing_term + split_dot(jnp.broadcast_to(col, (8, 128)), hm)[0:1]
        direct = direct + nn((xp * dxdt).astype(BF16), hm)
        edy = (pick(lo, arriving, 2 * p) * dyf).astype(BF16)
        db = db + nt(spread.astype(BF16), dsb)
        dc_mat = dc_mat + nt(edy, entryb)
        dstate[:, sl] = ds * held + tn(cc, edy)
        dx = dtb * dxdt + taps[6:7, sl] * dyf
        grad, above = conv_back(dx, slope, inner, inner_halo, links, taps, sl, carry, next_links, par_out, first)
        ginner_out[:, sl] = grad.astype(BF16)
        edge_out[:, sl] = above

        @pl.when(k == chunks - 1)
        def _():
            last_out[:, sl] = grad[length - 8 :]

    dsc = jnp.where(allowed, dscores, 0.0).astype(BF16)
    grads_bc[:, :state_dim] = db + nn(dsc, cc)
    grads_bc[:, state_dim:] = dc_mat + tn(dsc, b)
    for half in range(2):
        sl = slice(half * state_dim, (half + 1) * state_dim)
        grad, above = conv_back(
            grads_bc[:, sl], slope_s, shared, shared_halo, links, taps_s, sl, carry_s, next_links, par_s_out, first
        )
        gsmall_out[:, sl] = grad.astype(BF16)
        at = slice(width + half * state_dim, width + (half + 1) * state_dim)
        edge_out[:, at] = above

        @pl.when(k == chunks - 1)
        def _():
            last_out[:, at] = grad[length - 8 :]

    for j in range(3):
        carry_links[:, j : j + 1] = links[j][0:8]
    dcum = row_in[...] - matched
    upper = (rows <= cols).astype(F32)
    dlog = jnp.dot(upper, dcum, precision=HIGH, preferred_element_type=F32) + closing_term
    rate = -jnp.exp(heads[1:2])
    dstep = (direct + dlog * rate) * sigmoid(step_raw[...] + heads[0:1])
    gsmall_out[:, 2 * state_dim :] = dstep.astype(BF16)
    par_h_out[0:1] += jnp.sum(dstep, axis=0, keepdims=True)
    par_h_out[1:2] += jnp.sum(dlog * (rate * dt), axis=0, keepdims=True)


def spread_body(ggate, ginner, gsmall, w_in, w_small, normed, part_out, gain_out):
    width = ggate.shape[1]
    part = nt(ggate[...], w_in[:, :width]) + nt(ginner[...], w_in[:, width:]) + nt(gsmall[...], w_small[...])
    part_out[...] = part.astype(BF16)
    gain_out[...] = jnp.sum(part * normed[...].astype(F32), axis=0, keepdims=True)


PIECES = 2
MESH = pl.DeviceIdType.MESH
ANY = pl.BlockSpec(memory_space=pl.ANY)


def remote(src, dst, send, recv, **to):
    return pltpu.make_async_remote_copy(
        src_ref=src, dst_ref=dst, send_sem=send, recv_sem=recv, device_id=to, device_id_type=MESH
    )


def greet(barrier, when, **to):
    @pl.when(when)
    def _():
        pl.semaphore_signal(barrier, inc=1, device_id=to, device_id_type=MESH)


def line_of(ref):
    return ref[...].reshape(1, ref.shape[0])


def start(copies):
    for copy in copies:
        copy.start()


def guarded(when, action):
    @pl.when(when)
    def _():
        action()


class LineGather:
    def __init__(self, ncol, z, first, second, extra, sems):
        self.ncol, self.z, self.last = ncol, z, ncol - 1
        self.parts = (first, second)
        self.extra = extra
        self.sems = sems
        self.tokens = second[1].shape[0] // ncol
        self.part = self.tokens // PIECES

    def copies(self, kind, s, way, pieces, mine=False):
        source, dest = self.parts[kind]
        send, recv = self.sems[2 * kind : 2 * kind + 2]
        to = self.z + 1 if way == 0 else self.z - 1
        made = []
        for p in pieces:
            at = pl.ds(pl.multiple_of(s * self.tokens + p * self.part, self.part), self.part)
            src = source.at[pl.ds(p * self.part, self.part)] if mine and source is not None else dest.at[at]
            made.append(remote(src, dest.at[at], send.at[way, s, p], recv.at[s, p], col=to))
            if kind == 0 and p == PIECES - 1:
                place = self.extra.at[pl.ds(pl.multiple_of(s * 8, 8), 8)]
                made.append(remote(place, place, send.at[way, s, PIECES], recv.at[s, PIECES], col=to))
        return made

    def exit(self, way):
        return self.z < self.last if way == 0 else self.z > 0

    def depth(self, way):
        return self.z if way == 0 else self.last - self.z

    def begin(self):
        every = range(PIECES)
        for way in range(2):
            guarded(self.exit(way), lambda way=way: start(self.copies(0, self.z, way, every, True)))
        for way in range(2):
            guarded(self.depth(way) == 0, lambda way=way: start(self.copies(1, self.z, way, every, True)))

    ticks = property(lambda self: 2 * self.last * PIECES)

    def tick(self, tau):
        j, p = (tau - 1) // PIECES, (tau - 1) % PIECES
        for way in range(2):
            depth = self.depth(way)
            sign = -1 if way == 0 else 1

            def relay(kind, s, way=way, depth=depth):
                for copy in self.copies(kind, s, way, (p,)):
                    copy.wait_recv()
                guarded(self.exit(way), lambda: start(self.copies(kind, s, way, (p,))))
                if kind == 0 and p == PIECES - 1:
                    guarded(self.exit(way) & (j == depth - 1),
                            lambda: start(self.copies(1, self.z, way, range(PIECES), True)))

            guarded(j < depth, lambda s=self.z + sign * (j + 1), relay=relay: relay(0, s))
            guarded((j >= depth) & (j < 2 * depth),
                    lambda s=self.z + sign * (j - depth + 1), relay=relay: relay(1, s))

    def drain(self):
        for kind in range(2):
            for way in range(2):
                sign = -1 if way == 0 else 1
                for s in range(self.ncol):

                    def wait(kind=kind, way=way, s=s, sign=sign):
                        for copy in self.copies(kind, self.z + sign * s, way, range(PIECES)):
                            copy.wait_send()

                    guarded(self.exit(way) & (s <= self.depth(way)), wait)


def mixer_kernel(ncol, ndp, full_width, *refs):
    refs = list(refs)

    def take(number):
        taken = refs[:number]
        del refs[:number]
        return taken

    tokens_in, gain, seg_in, ci, cib, gg, cs, csb, sb, rl, sg = take(11)
    zx, bc_in, dt_in, w2, cot_in = take(5)
    normed_hbm, gsmall_hbm, ggate_hbm, cot_hbm, gnorm_hbm, ginner_hbm, part_hbm = take(7)
    par, par_s, par_h, gain_out, total_out = take(5)
    normed, seg, w_in, w_small, out_t, cot = take(6)
    taps, taps_s, heads = take(3)
    both, shared, step = take(3)
    ssd, x, bc, dt, c, ct, dec, enter, slope, slope_s, state, start_state, total = take(13)
    gained, gnorm, projected, back, dy, ggate, rowterm, dstart, dend = take(9)
    ginner, gsmall, part, edge, edge_in, last_rows = take(6)
    dstate, carry, carry_s, carry_links, grads_bc = take(5)
    sums, sums_all, own_scale, slots = take(4)
    line_box, line_send, line_recv = take(3)
    xs_send, xs_recv, cs_send, cs_recv, w_send, c_send, w_recv, t_send, t_recv = take(9)
    sum_send, sum_recv, row_send, row_recv, here = take(5)

    dp, row, z = lax.axis_index("dp"), lax.axis_index("row"), lax.axis_index("col")
    other = 1 - row
    last = ncol - 1
    tokens = tokens_in.shape[0]
    tail = HALO
    length = ncol * tokens
    width = taps.shape[1]
    scols = taps_s.shape[1]
    state_dim = scols // 2
    chunks = length // SPAN
    rows = bc_in.shape[0]
    me = dp * 2 + row
    sends_tail = (row == 0) & (z == last)

    barrier = pltpu.get_barrier_semaphore()
    for s in range(1, ncol):
        greet(barrier, row >= 0, col=lax.rem(z + s, ncol))
    greet(barrier, row >= 0, row=other)
    for m in range(1, ndp):
        greet(barrier, row >= 0, dp=dp ^ m)
    greet(barrier, row == 1, row=0, col=last)
    for s in range(ncol):
        greet(barrier, sends_tail, row=1, col=s)

    seg[pl.ds(pl.multiple_of(z * 8, 8), 8)] = jnp.broadcast_to(line_of(seg_in), (8, tokens))
    base = pl.multiple_of(z * tokens, 32)
    gain_row = line_of(gain)

    def normalize(n, carried):
        at = pl.multiple_of(n * 32, 32)
        wide = tokens_in[pl.ds(at, 32)].astype(F32)
        scale = lax.rsqrt(jnp.sum(wide * wide, axis=1, keepdims=True) / wide.shape[1] + EPS)
        normed[pl.ds(pl.multiple_of(base + at, 32), 32)] = (wide * scale * gain_row).astype(BF16)
        return carried

    lax.fori_loop(0, tokens // 32, normalize, 0)

    @pl.when(row == 0)
    def _():
        seg[pl.ds(ncol * 8, 8)] = jnp.full((8, tokens), -1, jnp.int32)
        normed[pl.ds(length, tail)] = jnp.zeros((tail, normed.shape[1]), BF16)
        start_state[...] = jnp.zeros_like(start_state)

    @pl.when(row == 1)
    def _():
        dend[...] = jnp.zeros_like(dend)
        edge_in[...] = jnp.zeros_like(edge_in)

    count = ncol - 1 + ndp + row + jnp.where(sends_tail, ncol, 0)
    pl.semaphore_wait(barrier, count)

    weights = ((None, w_in), (None, w_small), (w2, out_t))

    def weight_rows(j):
        return pl.ds(pl.multiple_of(j * rows, 16), rows)

    def weight_copies(j, mine, send, **to):
        copies = []
        for i, (src, dst) in enumerate(weights):
            place = dst.at[weight_rows(j)]
            from_input = mine and src is not None
            copies.append(remote(src if from_input else place, place, send.at[i], w_recv.at[j, i], **to))
        return copies

    def tail_copies(s):
        place = seg.at[pl.ds(pl.multiple_of(z * 8, 8), 8)]
        end = pl.multiple_of(z * tokens + tokens - tail, 16)
        return [
            remote(normed.at[pl.ds(end, tail)], normed.at[pl.ds(length, tail)],
                   t_send.at[s, 0], t_recv.at[0], row=1, col=s),
            remote(place, seg.at[pl.ds(ncol * 8, 8)], t_send.at[s, 1], t_recv.at[1], row=1, col=s),
        ]

    for s in range(ncol):
        guarded(sends_tail, lambda s=s: start(tail_copies(s)))
    gather = LineGather(ncol, z, (None, normed), (cot_in, cot), seg, (xs_send, xs_recv, cs_send, cs_recv))
    gather.begin()
    w_in[weight_rows(me), 0:width] = zx[:, 0, :]
    w_in[weight_rows(me), width : 2 * width] = zx[:, 1, :]
    w_small[weight_rows(me), 0:scols] = bc_in[...]
    dt_rows = jnp.concatenate([dt_in[...].astype(F32), jnp.zeros((128 - dt_in.shape[0], rows), F32)], axis=0)
    w_small[weight_rows(me), scols : scols + 128] = dt_rows.T.astype(BF16)
    local = [
        pltpu.make_async_copy(cot_in, cot.at[pl.ds(base, tokens)], here.at[0]),
        pltpu.make_async_copy(w2, out_t.at[weight_rows(me)], here.at[1]),
    ]
    start(local)
    taps[0:4] = ci[...]
    taps[4:5] = line_of(cib)
    taps[5:6] = line_of(gg)
    sg_row = line_of(sg)
    lo1 = iota((1, 128), 1) < 64
    for p in range(width // 128):
        taps[6:7, p * 128 : (p + 1) * 128] = pick(lo1, sg_row, 2 * p)
    taps_s[0:4] = cs[...]
    taps_s[4:5] = line_of(csb)
    heads[...] = jnp.zeros_like(heads)
    heads[0:1, : sb.shape[0]] = line_of(sb)
    heads[1:2, : rl.shape[0]] = line_of(rl)
    for ref in (state, total, dstart, carry, carry_s, carry_links, par, par_s, par_h, sums):
        ref[...] = jnp.zeros_like(ref)

    for m in range(1, ndp):
        start(weight_copies(me, True, w_send.at[m], dp=dp ^ m))
    start(weight_copies(me, True, c_send.at[0], row=other))

    def pass_weights(m):
        j = (dp ^ m) * 2 + row
        for copy in weight_copies(j, False, w_send.at[m], dp=dp ^ m):
            copy.wait_recv()
        start(weight_copies(j, False, c_send.at[m], row=other))

    half = gather.ticks // 2
    due = {tau: [] for tau in range(1, half + 1)}
    for m in range(1, ndp):
        due[min(half - 1, 2 + (3 * (m - 1)) // (ndp - 1) * (half - 3) // 2)].append(m)
    for tau in range(1, half):
        gather.tick(tau)
        for m in due[tau]:
            pass_weights(m)
    for m in range(ndp):
        for copy in weight_copies((dp ^ m) * 2 + other, False, c_send.at[m], row=other):
            copy.wait_recv()
    guarded(row == 1, lambda: [copy.wait_recv() for copy in tail_copies(0)])
    for copy in local:
        copy.wait()

    def nth(n):
        return pl.multiple_of(jnp.where(z * 2 < ncol, n, last - n) * tokens, tokens)

    def put(at, size, value, small):
        both[pl.ds(at, size)] = value.astype(BF16)
        shared[pl.ds(at, size)] = small[:, :scols].astype(BF16)
        step[pl.ds(at, size)] = small[:, scols:]

    def project_tokens(n, with_tail):
        at = nth(n)
        lhs = normed[pl.ds(at, tokens)]
        if with_tail:
            lhs = jnp.concatenate([lhs, normed[pl.ds(length, tail)]], axis=0)
        value, small = nn(lhs, w_in[...]), nn(lhs, w_small[...])
        put(at, tokens, value[:tokens], small[:tokens])
        if with_tail:
            put(length, tail, value[tokens:], small[tokens:])

    for n in range(ncol - 1):
        project_tokens(n, n == 0)
    gather.tick(half)
    project_tokens(ncol - 1, False)
    outs = [pltpu.make_async_copy(normed, normed_hbm, here.at[4])]
    outs[0].start()

    def at_rows(k):
        return pl.ds(pl.multiple_of(k * SPAN, SPAN), SPAN)

    def common(k):
        this = at_rows(k)
        above = pl.ds(pl.multiple_of(jnp.where(k == 0, length, k * SPAN - HALO), HALO), HALO)
        prev = pl.ds(pl.multiple_of(jnp.where(k == 0, chunks, k - 1) * 8, 8), 8)
        side = pl.ds(width, width)
        return (
            both.at[this, side], both.at[above, side], shared.at[this], shared.at[above], step.at[this],
            seg.at[pl.ds(pl.multiple_of(k * 8, 8), 8)], seg.at[prev], seg.at[pl.ds(chunks * 8, 8)], taps, taps_s, heads,
        )

    later = list(range(half + 1, gather.ticks + 1))

    def forward(k, carried):
        this = at_rows(k)
        forward_body(*common(k), ssd.at[this], x.at[this], bc.at[this], dt.at[this], c.at[this],
                     ct.at[:, this], dec.at[this], enter.at[k], slope.at[this], slope_s.at[this], state, total)
        guarded(k == chunks // 2, lambda: gather.tick(half + 1))
        return carried

    lax.fori_loop(0, chunks, forward, 0)
    later.pop(0)

    def row_copy(n, src, dst):
        return remote(src, dst, row_send.at[n], row_recv.at[n], row=other)

    guarded(row == 0, lambda: row_copy(0, state, start_state).start())
    gather.tick(later.pop(0))
    guarded(row == 1, lambda: row_copy(0, state, start_state).wait_recv())

    def gating(k, carried):
        this = at_rows(k)
        gate_body(ssd.at[this], x.at[this], bc.at[this], dec.at[this], start_state, both.at[this, pl.ds(0, width)],
                  taps, ssd.at[this], gained.at[this], sums.at[:, this])
        return carried

    lax.fori_loop(0, chunks, gating, 0)

    def sum_copy(s, source):
        return remote(sums, slots.at[source], sum_send.at[s], sum_recv.at[source], col=lax.rem(z + s, ncol))

    def sum_end():
        result = sums[...]
        for s in range(1, ncol):
            source = lax.rem(z + s, ncol)
            sum_copy(s, source).wait_recv()
            result = result + slots[source]
        sums_all[...] = result

    gather.tick(later.pop(0))

    def projecting(k, carried):
        this = at_rows(k)
        projected[this] = nt(gained[this], out_t[...]).astype(BF16)
        return carried

    lax.fori_loop(0, chunks, projecting, 0)
    line = LineReduce(ncol, z, projected, projected, line_box, line_send, line_recv, False)
    line.start()
    while len(later) > 2:
        gather.tick(later.pop(0))

    def pulling(n):
        this = pl.ds(nth(n), tokens)
        pull_body(cot.at[this], out_t, gained.at[this], back.at[this], sums.at[:, this])

    for n in range(ncol - 1):
        pulling(n)
        if n == 0:
            gather.tick(later.pop(0))
    gather.tick(later.pop(0))
    ticks = list(range(1, line.ticks + 1))
    pulling(ncol - 1)
    outs.append(pltpu.make_async_copy(cot, cot_hbm, here.at[5]))
    outs[-1].start()
    for s in range(1, ncol):
        sum_copy(s, z).start()
    line.start(2, line.ticks)
    line.tick(ticks.pop(0))
    sum_end()
    own_scale[...] = columns(lax.rsqrt(sums_all[0:1, pl.ds(pl.multiple_of(z * tokens, tokens), tokens)] / full_width + EPS))

    def pull_gate(k, carried):
        this = at_rows(k)
        back_body(full_width, ssd.at[this], x.at[this], bc.at[this], dec.at[this], both.at[this, pl.ds(0, width)],
                  back.at[this], sums_all.at[:, this], taps,
                  gnorm.at[this], dy.at[this], ggate.at[this], rowterm.at[this], par, dstart)
        return carried

    lax.fori_loop(0, chunks, pull_gate, 0)
    guarded(row == 1, lambda: row_copy(1, dstart, dend).start())
    outs.append(pltpu.make_async_copy(ggate, ggate_hbm, here.at[7]))
    outs.append(pltpu.make_async_copy(gnorm, gnorm_hbm, here.at[6]))
    start(outs[-2:])
    line.tick(ticks.pop(0))
    guarded(row == 0, lambda: row_copy(1, dstart, dend).wait_recv())
    dstate[...] = dend[...]

    spaced = {n: [tau] for n, tau in enumerate(ticks[:chunks])}
    ticks = ticks[chunks:]

    def backward(n, carried):
        k = chunks - 1 - n
        this = at_rows(k)
        before = pl.ds(pl.multiple_of(jnp.maximum(k * SPAN - 8, 0), 8), 8)
        backward_body(k, chunks, *common(k), dy.at[this], x.at[this], bc.at[this], dt.at[this], c.at[this],
                      ct.at[:, this], dec.at[before], enter.at[k], slope.at[this], slope_s.at[this], start_state, rowterm.at[this],
                      ginner.at[this], gsmall.at[this], par, par_s, par_h, edge, last_rows,
                      dstate, carry, carry_s, carry_links, grads_bc)
        for turn, taus in spaced.items():
            if turn < chunks - 1:
                for tau in taus:
                    guarded(n == turn, lambda tau=tau: line.tick(tau))
        return carried

    lax.fori_loop(0, chunks, backward, 0)
    guarded(row == 1, lambda: row_copy(2, edge, edge_in).start())
    for tau in spaced.get(chunks - 1, []):
        line.tick(tau)
    guarded(row == 0, lambda: row_copy(2, edge, edge_in).wait_recv())
    fixed = (last_rows[...] + edge_in[...]).astype(BF16)
    ginner[length - 8 :] = fixed[:, :width]
    gsmall[length - 8 :, : fixed.shape[1] - width] = fixed[:, width:]
    outs.append(pltpu.make_async_copy(ginner, ginner_hbm, here.at[8]))
    outs.append(pltpu.make_async_copy(gsmall, gsmall_hbm, here.at[9]))
    start(outs[-2:])

    tile = 256
    tiles = part.shape[1] // tile

    def part_copy(n):
        at = pl.ds(pl.multiple_of(n * tile, tile), tile)
        return pltpu.make_async_copy(part.at[:, at], part_hbm.at[:, at], here.at[10 + n])

    def spreading(n, carried):
        at = pl.ds(pl.multiple_of(n * tile, tile), tile)
        spread_body(ggate, ginner, gsmall, w_in.at[at], w_small.at[at], normed.at[pl.ds(0, length), at],
                    part.at[:, at], gain_out.at[:, at])
        guarded(n > 0, lambda: part_copy(jnp.maximum(n - 1, 0)).start())
        for tau in ticks[:-1]:
            guarded(n == tiles // 2, lambda tau=tau: line.tick(tau))
        return carried

    lax.fori_loop(0, tiles, spreading, 0)
    part_copy(tiles - 1).start()
    for tau in ticks[-1:]:
        line.tick(tau)

    def keep(at, value):
        here_rows = pl.ds(pl.multiple_of(at, 16), 16)
        total_out[here_rows] = (value * own_scale[here_rows, 0:1]).astype(BF16)

    line.total(keep)

    gather.drain()
    line.drain()
    for m in range(ndp):
        if m:
            for copy in weight_copies(me, True, w_send.at[m], dp=dp ^ m):
                copy.wait_send()
        for copy in weight_copies((dp ^ m) * 2 + row, m == 0, c_send.at[m], row=other):
            copy.wait_send()
    for s in range(ncol):
        guarded(sends_tail, lambda s=s: [copy.wait_send() for copy in tail_copies(s)])
    for s in range(1, ncol):
        sum_copy(s, z).wait_send()
    guarded(row == 0, lambda: row_copy(0, state, start_state).wait_send())
    guarded(row == 1, lambda: row_copy(1, dstart, dend).wait_send())
    guarded(row == 1, lambda: row_copy(2, edge, edge_in).wait_send())
    for copy in outs:
        copy.wait()
    for n in range(tiles):
        part_copy(n).wait()


def run_mixer(full_width, tokens_in, gain, seg, ci, cib, gg, cs, csb, sb, rl, sg, zx, bc, dt, w2, cot):
    ncol, ndp = lax.axis_size("col"), lax.axis_size("dp")
    tokens, model = tokens_in.shape
    width, scols = ci.shape[1], cs.shape[1]
    length = ncol * tokens
    chunks = length // SPAN
    state_dim = scols // 2
    small = scols + 128
    shards = 2 * ndp
    S = jax.ShapeDtypeStruct
    V = pltpu.VMEM
    dma = pltpu.SemaphoreType.DMA
    vmem = pl.BlockSpec(memory_space=V)
    return pl.pallas_call(
        functools.partial(mixer_kernel, ncol, ndp, full_width),
        in_specs=[vmem] * 14 + [ANY] * 2,
        out_specs=[ANY] * 7 + [vmem] * 5,
        out_shape=[
            S((length + HALO, model), BF16), S((length, small), BF16), S((length, width), BF16), S((length, model), BF16),
            S((length, width), BF16), S((length, width), BF16), S((length, model), BF16),
            S((8, width), F32), S((8, scols), F32), S((8, 128), F32), S((1, model), F32), S((tokens, model), BF16),
        ],
        scratch_shapes=[
            V((length + HALO, model), BF16), V(((ncol + 1) * 8, tokens), jnp.int32), V((model, 2 * width), BF16),
            V((model, small), BF16), V((model, width), BF16), V((length, model), BF16),
            V((8, width), F32), V((8, scols), F32), V((8, 128), F32),
            V((length + HALO, 2 * width), BF16), V((length + HALO, scols), BF16), V((length + HALO, 128), F32),
            V((length, width), F32), V((length, width), BF16), V((length, scols), BF16), V((length, 128), F32),
            V((length, 128), F32), V((16, length), F32), V((length, 128), F32), V((chunks, state_dim, width), BF16),
            V((length, width), BF16), V((length, scols), BF16),
            V((state_dim, width), F32), V((state_dim, width), F32), V((8, 128), F32),
            V((length, width), BF16), V((length, width), BF16), V((length, model), BF16), V((length, width), BF16),
            V((length, width), BF16), V((length, width), BF16), V((length, 128), F32), V((state_dim, width), F32),
            V((state_dim, width), F32),
            V((length, width), BF16), V((length, small), BF16), V((length, model), BF16),
            V((8, width + scols), F32), V((8, width + scols), F32), V((8, width + scols), F32),
            V((state_dim, width), F32), V((8, width), F32), V((8, scols), F32), V((8, 128), F32), V((SPAN, scols), F32),
            V((8, length), F32), V((8, length), F32), V((tokens, 128), F32), V((ncol, 8, length), F32),
            *line_scratch(ncol, tokens, model),
            dma((2, ncol, PIECES + 1)), dma((ncol, PIECES + 1)), dma((2, ncol, PIECES)), dma((ncol, PIECES)),
            dma((ndp, 3)), dma((ndp, 3)), dma((shards, 3)), dma((ncol, 2)), dma((2,)),
            dma((ncol,)), dma((ncol,)), dma((3,)), dma((3,)), dma((10 + model // 256,)),
        ],
        compiler_params=pltpu.CompilerParams(
            collective_id=1, has_side_effects=True, vmem_limit_bytes=63 * 1024 * 1024
        ),
        cost_estimate=pl.CostEstimate(flops=0, bytes_accessed=500_000_000, transcendentals=0),
        name="mixer",
    )(tokens_in, gain, seg, ci, cib, gg, cs, csb, sb, rl, sg, zx, bc, dt, w2, cot)
class LineReduce:
    def __init__(self, ncol, z, source, local, inbox, send, recv, paced):
        self.paced = paced
        self.ncol, self.z, self.last = ncol, z, ncol - 1
        self.source, self.local, self.inbox = source, local, inbox
        self.send, self.recv = send, recv
        self.tokens = local.shape[0] // ncol
        self.part = self.tokens // PIECES

    def rows(self, way, t, p):
        d = self.last - t if way == 0 else t
        return pl.multiple_of(d * self.tokens + p * self.part, self.part)

    def copy(self, way, t, p, first):
        src = self.source.at[pl.ds(self.rows(way, t, p), self.part)] if first else self.inbox.at[way, t, p]
        to = self.z + 1 if way == 0 else self.z - 1
        return remote(src, self.inbox.at[way, t, p], self.send.at[way, t, p], self.recv.at[way, t, p], col=to)

    def edge(self, way):
        return self.z == (0 if way == 0 else self.last)

    def depth(self, way):
        return self.z if way == 0 else self.last - self.z

    def start(self, first=0, stop=2):
        for way in range(2):

            @pl.when(self.edge(way))
            def _(way=way):
                for i in range(first, min(stop, self.ticks)):
                    self.copy(way, i // PIECES, i % PIECES, True).start()

    ticks = property(lambda self: self.last * PIECES)

    def tick(self, tau):
        for way in range(2):

            @pl.when(self.edge(way) & (self.paced and tau + 1 < self.ticks))
            def _(way=way):
                self.copy(way, (tau - 1) // PIECES, (tau - 1) % PIECES, True).wait_send()
                self.copy(way, (tau + 1) // PIECES, (tau + 1) % PIECES, True).start()

        for stage in range(2):
            for way in range(2):
                depth = self.depth(way)
                index = tau - (2 * depth - 1)
                t, p = index // PIECES, lax.rem(index, PIECES)

                @pl.when((depth > 0) & (index >= 0) & (index < (self.ncol - depth) * PIECES))
                def _(way=way, depth=depth, t=t, p=p, stage=stage):
                    onward = t < self.last - depth
                    if stage == 0:
                        self.copy(way, t, p, False).wait_recv()

                        @pl.when(onward)
                        def _():
                            base = self.rows(way, t, p)

                            def add(k, carry):
                                at = pl.multiple_of(k * 16, 16)
                                mine = self.local[pl.ds(pl.multiple_of(base + at, 16), 16)].astype(F32)
                                here = pl.ds(at, 16)
                                self.inbox[way, t, p, here] = (self.inbox[way, t, p, here].astype(F32) + mine).astype(BF16)
                                return carry

                            lax.fori_loop(0, self.part // 16, add, 0)
                    else:

                        @pl.when(onward)
                        def _():
                            self.copy(way, t, p, False).start()

    def total(self, store):
        z, last = self.z, self.last
        for p in range(PIECES):

            def add(k, carry, p=p):
                at = pl.multiple_of(k * 16, 16)
                here = pl.ds(at, 16)
                row = p * self.part + at
                value = self.local[pl.ds(pl.multiple_of(z * self.tokens + row, 16), 16)].astype(F32)
                low = self.inbox[0, jnp.minimum(last - z, last - 1), p, here].astype(F32)
                high = self.inbox[1, jnp.minimum(z, last - 1), p, here].astype(F32)
                value = value + jnp.where(z > 0, low, 0.0) + jnp.where(z < last, high, 0.0)
                store(row, value)
                return carry

            lax.fori_loop(0, self.part // 16, add, 0)

    def drain(self):
        for way in range(2):
            depth = self.depth(way)

            @pl.when(self.edge(way))
            def _(way=way):
                for i in range(self.ticks - 2 if self.paced else 0, self.ticks):
                    self.copy(way, i // PIECES, i % PIECES, True).wait_send()

            for t in range(self.last):

                @pl.when((depth > 0) & (t < self.last - depth))
                def _(way=way, t=t):
                    for p in range(PIECES):
                        self.copy(way, t, p, False).wait_send()


def line_scratch(ncol, tokens, width):
    shape = (2, ncol - 1, PIECES)
    dma = pltpu.SemaphoreType.DMA
    return [pltpu.VMEM(shape + (tokens // PIECES, width), BF16), dma(shape), dma(shape)]


def reduce_kernel(ncol, ndp, scols, *refs):
    count = 4
    refs = list(refs)

    def take(number):
        taken = refs[:number]
        del refs[:number]
        return taken

    sources = take(7)
    vecs = take(4)
    r, vec_outs, gsum_out = take(count), take(4), refs.pop(0)
    held = take(7)
    (line_box, line_send, line_recv) = take(3)
    g, near, sent, far = take(count), take(count), take(count), take(count)
    vec_slots, col_slots = take(4), take(2)
    col_sums = take(2)
    bc_slots, bc_sum, load, c_send, c_recv, p_send, p_recv, v_send, v_recv, u_send, u_recv, b_send, b_recv = refs
    dp, row, z = lax.axis_index("dp"), lax.axis_index("row"), lax.axis_index("col")
    other = 1 - row
    me = dp * 2 + row
    rows = [out.shape[0] for out in r]
    barrier = pltpu.get_barrier_semaphore()
    for q in range(1, 2 * ndp):
        greet(barrier, row >= 0, dp=dp ^ (q >> 1), row=row ^ (q & 1))
    for s in range(1, ncol):
        greet(barrier, row >= 0, col=lax.rem(z + s, ncol))
    loads = []
    for i, (src, dst) in enumerate(zip(sources, held)):
        src = src.at[pl.ds(0, dst.shape[0])]
        loads.append(pltpu.make_async_copy(src, dst, load.at[i]))
        loads[-1].start()
    normed, gsmall, ggate, cot, gnorm, ginner, part = held
    pl.semaphore_wait(barrier, 2 * ndp + ncol - 2)
    line = LineReduce(ncol, z, sources[6], part, line_box, line_send, line_recv, True)
    line.start()

    order = (0, 1, 2, 3)
    turns = [3, 1, 2, 0] if ndp == 4 else list(range(1, ndp)) + [0]

    def core_copy(i, d):
        return remote(g[i].at[pl.ds((d * 2 + other) * rows[i], rows[i])], near[i].at[d],
                      c_send.at[i, d], c_recv.at[i, d], row=other)

    def vec_copy(q, i, j):
        return remote(vecs[i], vec_slots[i].at[j], v_send.at[q, i], v_recv.at[j, i],
                      dp=dp ^ (q >> 1), row=row ^ (q & 1))

    for q in range(1, 2 * ndp):
        for i in range(4):
            vec_copy(q, i, me).start()

    waiting = []

    def later(copy):
        if waiting:
            waiting.pop().start()
        if copy is not None:
            waiting.append(copy)

    def accumulate(i, first, number, terms, store):
        def step(k, carry):
            at = first + pl.multiple_of(k * 16, 16)
            total = terms[0](at)
            for term in terms[1:]:
                total = total + term(at)
            store(at, total)
            return carry

        lax.fori_loop(0, number // 16, step, 0)

    def read(ref, index, shift=0):
        return lambda at: ref[index, pl.ds(at - shift, 16)].astype(F32)

    def mine(i, d):
        return lambda at: g[i][pl.ds(pl.multiple_of((d * 2 + row) * rows[i] + at, 16), 16)].astype(F32)

    def write(ref, index, shift):
        def store(at, total):
            ref[index, pl.ds(at - shift, 16)] = total.astype(BF16)

        return store

    def arrived(i, d):
        core_copy(i, d).wait_recv()

    def tick():
        if ticks:
            line.tick(ticks.pop(0))

    if ndp == 4:
        halves = ((0, 1, 2), (1, 2, 1))

        def leg(i, slot, m):
            return remote(sent[i].at[slot], far[i].at[slot], p_send.at[i, slot], p_recv.at[i, slot], dp=dp ^ m)

        def step_one(i):
            half = rows[i] // 2
            arrived(i, dp ^ 3)
            for h, m1, m2 in halves:
                accumulate(i, h * half, half, [mine(i, dp ^ 3), read(near[i], dp ^ 3)],
                           write(sent[i], 3 * h + 1, h * half))
                later(leg(i, 3 * h + 1, m1))
            for h, m1, m2 in halves:
                arrived(i, dp ^ m1)
                accumulate(i, h * half, half, [mine(i, dp ^ m1), read(near[i], dp ^ m1)],
                           write(sent[i], 3 * h, h * half))
                later(leg(i, 3 * h, m1))
            later(None)
            arrived(i, dp)

        def relay(i):
            half = rows[i] // 2
            for h, m1, m2 in halves:
                leg(i, 3 * h + 1, m1).wait_recv()
                accumulate(i, h * half, half,
                           [mine(i, dp ^ m2), read(near[i], dp ^ m2), read(far[i], 3 * h + 1, h * half)],
                           write(sent[i], 3 * h + 2, h * half))
                later(leg(i, 3 * h + 2, m2))
            later(None)

        def finish(i, store):
            half = rows[i] // 2
            for h, m1, m2 in halves:
                leg(i, 3 * h, m1).wait_recv()
                leg(i, 3 * h + 2, m2).wait_recv()
                accumulate(i, h * half, half,
                           [mine(i, dp), read(near[i], dp), read(far[i], 3 * h, h * half),
                            read(far[i], 3 * h + 2, h * half)], store)

        sends = [leg(i, 3 * h + k, m2 if k == 2 else m1) for i in order for h, m1, m2 in halves for k in range(3)]
    else:

        def peer(i, m):
            return remote(sent[i].at[m], far[i].at[m], p_send.at[i, m], p_recv.at[i, m], dp=dp ^ m)

        def step_one(i):
            for m in turns[:-1]:
                arrived(i, dp ^ m)
                accumulate(i, 0, rows[i], [mine(i, dp ^ m), read(near[i], dp ^ m)], write(sent[i], m, 0))
                later(peer(i, m))
            later(None)
            arrived(i, dp)

        def relay(i):
            pass

        def finish(i, store):
            for m in range(1, ndp):
                peer(i, m).wait_recv()
            accumulate(i, 0, rows[i],
                       [mine(i, dp), read(near[i], dp)] + [read(far[i], m) for m in range(1, ndp)], store)

        sends = [peer(i, m) for i in order for m in range(1, ndp)]

    def plain(i):
        def store(at, total):
            r[i][pl.ds(at, 16)] = total

        return store

    def shared_rows(at, total):
        r[0][pl.ds(at, 16)] = total
        bc_slots[z, pl.ds(at, 16)] = total[:, : bc_slots.shape[2]].astype(BF16)

    root = ncol // 2
    at_root = z == root

    def to_root(source):
        pairs = [(col_slots[i].at[source], u_send.at[0, i], u_recv.at[source, i]) for i in range(2)]
        pairs.append((bc_slots.at[source], b_send.at[0], b_recv.at[source]))
        return [remote(ref, ref, send, recv, col=root) for ref, send, recv in pairs]

    def from_root(target):
        pairs = [(col_sums[i], u_send.at[target, i], u_recv.at[root, i]) for i in range(2)]
        pairs.append((bc_sum, b_send.at[target], b_recv.at[root]))
        return [remote(ref, ref, send, recv, col=target) for ref, send, recv in pairs]

    others = [s for s in range(ncol) if s != root]

    def sum_at_root():
        @pl.when(at_root)
        def _():
            for s in others:
                for copy in to_root(s):
                    copy.wait_recv()
            for i in range(2):
                total = col_slots[i][0]
                for j in range(1, ncol):
                    total = total + col_slots[i][j]
                col_sums[i][...] = total
            total = bc_slots[0].astype(F32)
            for j in range(1, ncol):
                total = total + bc_slots[j].astype(F32)
            bc_sum[...] = total.astype(BF16)
            for s in others:
                for copy in from_root(s):
                    copy.start()

    model = normed.shape[1]
    block = model // 4
    products = ((normed, gsmall), (normed, ggate), (cot, gnorm), (normed, ginner))
    ready = {0: (0, 1), 1: (2,), 2: (3, 4), 3: (5,)}
    ticks = list(range(1, line.ticks + 1))
    for i in order:
        for at in ready[i]:
            loads[at].wait()
        left, right = products[i]
        for n, m in enumerate([3, 1, 2, 0] if ndp == 4 else range(4)):
            b = dp ^ m if ndp == 4 else m
            first = pl.multiple_of(b * block, 128)
            g[i][pl.ds(pl.multiple_of(b * block, 16), block)] = tn(left[:, pl.ds(first, block)], right[...]).astype(BF16)
            if ndp == 4:
                later(core_copy(i, b))
        if ndp != 4:
            for m in turns:
                later(core_copy(i, dp ^ m))
        if i == 1:
            loads[6].wait()
        if i > 0:
            step_one(i - 1)
        if i > 1:
            relay(i - 2)
        if i % 2:
            tick()
    later(None)
    step_one(3)
    relay(2)
    finish(0, shared_rows)
    for q in range(1, 2 * ndp):
        for i in range(4):
            vec_copy(q, i, me ^ q).wait_recv()
    for i in range(4):
        vec_slots[i][me] = vecs[i][...]
        total = vec_slots[i][0]
        for j in range(1, 2 * ndp):
            total = total + vec_slots[i][j]
        if i < 2:
            vec_outs[i][...] = total
        else:
            col_slots[i - 2][z] = total

    @pl.when(~at_root)
    def _():
        for copy in to_root(z):
            copy.start()

    tick()
    relay(3)
    while len(ticks) > 1:
        tick()
    sum_at_root()
    finish(1, plain(1))
    finish(2, plain(2))
    finish(3, plain(3))
    while ticks:
        tick()

    def keep(at, value):
        gsum_out[pl.ds(pl.multiple_of(at, 16), 16)] = value.astype(BF16)

    line.total(keep)
    @pl.when(~at_root)
    def _():
        for copy in from_root(z):
            copy.wait_recv()

    for i in range(2):
        vec_outs[2 + i][...] = col_sums[i][...]
    r[0][:, : bc_slots.shape[2]] = bc_sum[...].astype(F32)

    for q in range(1, 2 * ndp):
        for i in range(4):
            vec_copy(q, i, me).wait_send()
    for i in order:
        for m in turns:
            core_copy(i, dp ^ m).wait_send()
    for copy in sends:
        copy.wait_send()
    @pl.when(~at_root)
    def _():
        for copy in to_root(z):
            copy.wait_send()

    @pl.when(at_root)
    def _():
        for s in others:
            for copy in from_root(s):
                copy.wait_send()

    line.drain()


def reduce_grads(sources, vecs, scols):
    ncol, ndp = lax.axis_size("col"), lax.axis_size("dp")
    dma = pltpu.SemaphoreType.DMA
    vmem = pl.BlockSpec(memory_space=pltpu.VMEM)
    S = jax.ShapeDtypeStruct
    length = sources[1].shape[0]
    model = sources[0].shape[1]
    widths = [sources[1].shape[1], sources[2].shape[1], sources[4].shape[1], sources[5].shape[1]]
    count = len(widths)
    blocks = [(model // (2 * ndp), w) for w in widths]
    near = [pltpu.VMEM((ndp,) + b, BF16) for b in blocks]
    slots = 6 if ndp == 4 else ndp
    legs = [pltpu.VMEM((6, b[0] // 2, b[1]) if ndp == 4 else (ndp,) + b, BF16) for b in blocks]
    tokens = length // ncol
    return pl.pallas_call(
        functools.partial(reduce_kernel, ncol, ndp, scols),
        in_specs=[ANY] * 7 + [vmem] * 4,
        out_specs=[vmem] * (count + 5),
        out_shape=[S(b, F32) for b in blocks] + [S(v.shape, F32) for v in vecs] + [S((tokens, model), BF16)],
        scratch_shapes=[pltpu.VMEM((length, s.shape[1]), BF16) for s in sources]
        + line_scratch(ncol, tokens, model)
        + [pltpu.VMEM((model, w), BF16) for w in widths]
        + near + legs * 2
        + [pltpu.VMEM((2 * ndp,) + v.shape, F32) for v in vecs]
        + [pltpu.VMEM((ncol,) + v.shape, F32) for v in vecs[2:]]
        + [pltpu.VMEM(v.shape, F32) for v in vecs[2:]]
        + [pltpu.VMEM((ncol, blocks[0][0], scols), BF16), pltpu.VMEM((blocks[0][0], scols), BF16)]
        + [dma((7,))]
        + [dma((count, ndp))] * 2
        + [dma((count, slots))] * 2
        + [dma((2 * ndp, 4))] * 2
        + [dma((ncol, 2))] * 2
        + [dma((ncol,))] * 2,
        compiler_params=pltpu.CompilerParams(
            collective_id=2, has_side_effects=True, vmem_limit_bytes=60 * 1024 * 1024
        ),
        cost_estimate=pl.CostEstimate(flops=0, bytes_accessed=200_000_000, transcendentals=0),
        name="reduce_grads",
    )(*sources, *vecs)


def finish_small(
    nheads, small, par, par_h, par_s, gain_sum, gain_row, bc_out, dt_out, ci_out, cib_out, cs_out,
    csb_out, sb_out, rl_out, sg_out, gg_out, ng_out,
):
    width = par.shape[1]
    scols = par_s.shape[1]
    bc_out[...] = small[:, :scols]
    dt_out[...] = small[:, scols:].T[:nheads]
    ci_out[...] = par[0:4]
    cib_out[...] = par[4:5].reshape(width)
    gg_out[...] = par[5:6].reshape(width)
    cs_out[...] = par_s[0:4]
    csb_out[...] = par_s[4:5].reshape(scols)
    sb_out[...] = par_h[0:1, :nheads].reshape(nheads)
    rl_out[...] = par_h[1:2, :nheads].reshape(nheads)
    skip = jnp.zeros((8, 128), F32)
    for p in range(width // 128):
        skip = skip + split_dot(jnp.broadcast_to(par[6:7, p * 128 : (p + 1) * 128], (8, 128)), head_map(p))
    sg_out[...] = skip[0:1, :nheads].reshape(nheads)
    ng_out[...] = (gain_sum[0:1] / gain_row).reshape(gain_row.shape[1])


def finish_kernel(
    nheads, small, gate, inner, out, par, par_h, par_s, gain_sum, gain, tokens, cot, gnormed, projected,
    zx_out, bc_out, dt_out, out_out, ci_out, cib_out, cs_out, csb_out, sb_out, rl_out, sg_out, gg_out, ng_out, gin_out, block_out,
):
    gain_row = gain[...].reshape(1, gain.shape[0])
    zx_out[:, 0, :] = gate[...]
    zx_out[:, 1, :] = inner[...]
    out_out[...] = out[...]

    @pl.when(pl.program_id(0) == 0)
    def _():
        finish_small(nheads, small, par, par_h, par_s, gain_sum, gain_row, bc_out, dt_out, ci_out, cib_out, cs_out,
                     csb_out, sb_out, rl_out, sg_out, gg_out, ng_out)

    def rows(step, carry):
        at = pl.ds(pl.multiple_of(step * 32, 32), 32)
        wide = tokens[at].astype(F32)
        scale = lax.rsqrt(jnp.sum(wide * wide, axis=1, keepdims=True) / wide.shape[1] + EPS)
        pushed = gnormed[at].astype(F32) * gain_row
        mean = jnp.sum(pushed * wide, axis=1, keepdims=True) / wide.shape[1]
        grad = scale * pushed - wide * (scale * scale * scale * mean)
        gin_out[at] = (cot[at].astype(F32) + grad).astype(BF16)
        block_out[at] = (wide + projected[at].astype(F32)).astype(BF16)
        return carry

    lax.fori_loop(0, tokens.shape[0] // 32, rows, 0)


def run_finish(nheads, small, gate, inner, out, par, par_h, par_s, gain_sum, gain, tokens, cot, gnormed, projected):
    rows, width = gate.shape
    scols = par_s.shape[1]
    model = gain.shape[0]
    S = jax.ShapeDtypeStruct
    shapes = [
        (rows, 2, width), (rows, scols), (nheads, rows), (rows, width), (4, width), (width,), (4, scols), (scols,),
        (nheads,), (nheads,), (nheads,), (width,), (model,),
    ]
    steps = 4 if rows % 32 == 0 else 2
    block = rows // steps
    some = tokens.shape[0] // steps
    down = lambda n: (n, 0)
    whole = lambda shape: pl.BlockSpec(shape, lambda n: (0,) * len(shape))
    wide_spec = pl.BlockSpec((block, width), down)
    token_spec = pl.BlockSpec((some, model), down)
    return pl.pallas_call(
        functools.partial(finish_kernel, nheads),
        grid=(steps,),
        in_specs=[whole(small.shape), wide_spec, wide_spec, wide_spec, whole(par.shape), whole(par_h.shape),
                  whole(par_s.shape), whole(gain_sum.shape), whole(gain.shape)] + [token_spec] * 4,
        out_specs=[pl.BlockSpec((block, 2, width), lambda n: (n, 0, 0)), whole(shapes[1]), whole(shapes[2]), wide_spec]
        + [whole(shape) for shape in shapes[4:]] + [token_spec] * 2,
        out_shape=[S(shape, F32) for shape in shapes] + [S(tokens.shape, BF16)] * 2,
        name="finish",
    )(small, gate, inner, out, par, par_h, par_s, gain_sum, gain, tokens, cot, gnormed, projected)


def per_device(
    block_input, segment_ids, norm_gain, proj_zx, proj_bc, proj_dt, conv_inner, conv_inner_bias,
    conv_shared, conv_shared_bias, step_bias, rate_log, skip_gain, gated_gain, proj_out, cotangent,
):
    width = proj_zx.shape[2]
    scols = proj_bc.shape[1]
    nheads = proj_dt.shape[1]
    full_width = float(width * lax.axis_size("col"))
    (normed, gsmall, ggate, cot_all, gated_normed, ginner, part, par, par_s, par_h, gain_part, projected) = run_mixer(
        full_width, block_input, norm_gain, segment_ids, conv_inner, conv_inner_bias, gated_gain, conv_shared,
        conv_shared_bias, step_bias, rate_log, skip_gain, proj_zx, proj_bc, proj_dt.T, proj_out.T, cotangent,
    )
    gsm, gz, gout, gx, par, par_h, par_s, gain_sum, grad_normed = reduce_grads(
        (normed, gsmall, ggate, cot_all, gated_normed, ginner, part), (par, par_h, par_s, gain_part), scols
    )
    zx, gbc, gdt, gout, ci, cib, cs, csb, sb, rl, sg, gg, ng, grad_input, block_output = run_finish(
        nheads, gsm, gz, gx, gout, par, par_h, par_s, gain_sum, norm_gain, block_input, cotangent, grad_normed, projected
    )
    return (
        block_output, grad_input, ng, zx, gbc, gdt.T, ci, cib, cs, csb, sb, rl, sg, gg, gout.T,
    )


def solution(mesh):
    shards = ("dp", "row")
    tokens = P(("dp", "row", "col"), None)
    zx = P(shards, None, "col")
    in_specs = (
        tokens, P(("dp", "row", "col")), P(), zx, P(shards, None), P(shards, "col"), P(None, "col"), P("col"),
        P(), P(), P("col"), P("col"), P("col"), P("col"), P("col", shards), tokens,
    )
    out_specs = (
        tokens, tokens, P(), zx, P(shards, None), P(shards, "col"), P(None, "col"), P("col"),
        P(), P(), P("col"), P("col"), P("col"), P("col"), P("col", shards),
    )
    return jax.shard_map(per_device, mesh=mesh, in_specs=in_specs, out_specs=out_specs, check_vma=False)
```

```python
import functools
import jax, jax.numpy as jnp
from jax import lax
from jax.experimental import pallas as pl
from jax.experimental.pallas import tpu as pltpu
from jax.sharding import PartitionSpec as P

F32, BF16 = jnp.float32, jnp.bfloat16
HIGH = lax.Precision.HIGHEST
SPAN = 256
HALO = 16
EPS = 1e-5


def nn(a, b):
    return lax.dot_general(a, b, (((1,), (0,)), ((), ())), preferred_element_type=F32)


def nt(a, b):
    return lax.dot_general(a, b, (((1,), (1,)), ((), ())), preferred_element_type=F32)


def tn(a, b):
    return lax.dot_general(a, b, (((0,), (0,)), ((), ())), preferred_element_type=F32)


def iota(shape, axis):
    return lax.broadcasted_iota(jnp.int32, shape, axis)


def split_dot(a, b01):
    hi = a.astype(BF16)
    lo = (a - hi.astype(F32)).astype(BF16)
    return nn(hi, b01) + nn(lo, b01)


def sigmoid(v):
    return 0.5 * jnp.tanh(0.5 * v) + 0.5


def softplus(v):
    return jnp.maximum(v, 0.0) + jnp.log1p(jnp.exp(-jnp.abs(v)))


def columns(row):
    return jnp.broadcast_to(row, (128, row.shape[1])).T


def segments(seg_row, prev_row, tail_row):
    row = seg_row[0:1].astype(F32)
    seg = columns(row)[:, 0:1]
    length = row.shape[1]
    prev = columns(prev_row[0:1].astype(F32))[length - 8 :, 0:1]
    tail = tail_row[0:1, length - 1 :].astype(F32)
    return row, seg, prev, tail


def chunk_links(segc, halo):
    ext = jnp.concatenate([halo, segc], axis=0)
    length = segc.shape[0]
    return [(ext[8 - j : 8 - j + length] == segc).astype(F32) for j in range(1, 4)]


def conv_tile(cur, halo, links, taps, sl):
    v = jnp.concatenate([halo[HALO - 8 :, sl].astype(F32), cur[:, sl].astype(F32)], axis=0)
    length = cur.shape[0]
    pre = taps[4:5, sl] + taps[3:4, sl] * v[8:]
    for j in range(1, 4):
        pre = pre + taps[3 - j : 4 - j, sl] * (v[8 - j : 8 - j + length] * links[j - 1])
    return pre


def silu_and_slope(pre):
    s = sigmoid(pre)
    value = pre * s
    return value, s + value * (1.0 - s)


def pick(lo, cols, h):
    return jnp.where(lo, cols[:, h : h + 1], cols[:, h + 1 : h + 2])


def forward_body(
    inner, inner_halo, shared, shared_halo, step_raw, seg_row, seg_prev, seg_tail, taps, taps_s, heads,
    y_out, x_out, bc_out, dt_out, c_out, ct_out, dec_out, enter_out, slope_out, slope_s_out, state, total,
):
    length, width = inner.shape
    pairs = width // 128
    state_dim = state.shape[0]

    segr, seg, seg_halo, tail_seg = segments(seg_row, seg_prev, seg_tail)
    links = chunk_links(seg, seg_halo)
    closing = (seg == seg[length - 1 :]).astype(F32)
    entering = (seg == seg_halo[7:]).astype(F32)
    kept = (seg[length - 1 :] == seg_halo[7:]).astype(F32)
    dt = softplus(step_raw[...] + heads[0:1])
    log_decay = -jnp.exp(heads[1:2]) * dt
    rows, cols = iota((length, length), 0), iota((length, length), 1)
    lower = (rows >= cols).astype(F32)
    c = jnp.dot(lower, log_decay, precision=HIGH, preferred_element_type=F32)
    ct = c.T
    dt_out[...] = dt
    c_out[...] = c
    ct_out[...] = ct[: ct_out.shape[0]]
    whole = c + total[0:1]
    dec_out[...] = jnp.exp(whole) * (seg == tail_seg).astype(F32)
    total[0:1] = whole[length - 1 :]
    for half in range(2):
        sl = slice(half * state_dim, (half + 1) * state_dim)
        value, slope = silu_and_slope(conv_tile(shared, shared_halo, links, taps_s, sl))
        bc_out[:, sl] = value.astype(BF16)
        slope_s_out[:, sl] = slope.astype(BF16)
    b = bc_out[:, :state_dim]
    cc = bc_out[:, state_dim:]
    scores = jnp.where((rows >= cols) & (seg == segr), nt(cc, b), 0.0)
    lo = iota((length, 128), 1) < 64
    lo1 = lo[0:1]
    sides = [jnp.where(lo, 1.0, 0.0).astype(BF16), jnp.where(lo, 0.0, 1.0).astype(BF16)]
    arriving = jnp.exp(c) * entering
    leaving = jnp.exp(c[length - 1 :] - c) * closing
    held = jnp.exp(c[length - 1 :]) * kept
    enter_out[...] = state[...].astype(BF16)
    for p in range(pairs):
        sl = slice(p * 128, (p + 1) * 128)
        xp, slope = silu_and_slope(conv_tile(inner, inner_halo, links, taps, sl))
        xb = xp.astype(BF16)
        x_out[:, sl] = xb
        slope_out[:, sl] = slope.astype(BF16)
        xdt = xb.astype(F32) * pick(lo, dt, 2 * p)
        xdtb = xdt.astype(BF16)
        acc = nn(cc, state[:, sl].astype(BF16)) * pick(lo, arriving, 2 * p)
        for a in range(2):
            h = 2 * p + a
            weights = jnp.exp(jnp.minimum(c[:, h : h + 1] - ct[h : h + 1], 0.0)) * scores
            acc = acc + nn(weights.astype(BF16), xdtb * sides[a])
        y_out[:, sl] = acc
        moved = pick(lo, leaving, 2 * p) * xdt
        state[:, sl] = state[:, sl] * pick(lo1, held, 2 * p) + tn(b, moved.astype(BF16))


def row_sums(value):
    hi = value.astype(BF16)
    lo = (value - hi.astype(F32)).astype(BF16)
    ones = jnp.ones((8, value.shape[1]), BF16)
    return nt(ones, hi) + nt(ones, lo)


def first_rows(value):
    return jnp.where(iota(value.shape, 0) == 0, value, 0.0)


def head_map(p):
    lane, head = iota((128, 128), 0), iota((128, 128), 1)
    return (head == 2 * p + lane // 64).astype(BF16)


def gate_body(y, x, bc, dec, start, gate, taps, ssd_out, gained_out, sums_out):
    length, width = x.shape
    state_dim = start.shape[0]
    cc = bc[:, state_dim:]
    lo = iota((length, 128), 1) < 64
    squares = jnp.zeros((length, 128), F32)
    for p in range(width // 128):
        sl = slice(p * 128, (p + 1) * 128)
        corr = nn(cc, start[:, sl].astype(BF16)) * pick(lo, dec, 2 * p)
        ssd = y[:, sl] + corr + taps[6:7, sl] * x[:, sl].astype(F32)
        ssd_out[:, sl] = ssd
        g = gate[:, sl].astype(F32)
        gated = ssd * (g * sigmoid(g))
        gained_out[:, sl] = (gated * taps[5:6, sl]).astype(BF16)
        squares = squares + gated * gated
    sums_out[0:1] = row_sums(squares)[0:1]


def pull_body(cot, out_t, gained, back_out, sums_out):
    back = nn(cot[...], out_t[...])
    back_out[...] = back.astype(BF16)
    inner = jnp.zeros((cot.shape[0], 128), F32)
    for p in range(back.shape[1] // 128):
        sl = slice(p * 128, (p + 1) * 128)
        inner = inner + back[:, sl] * gained[:, sl].astype(F32)
    sums_out[1:2] = row_sums(inner)[0:1]


def back_body(
    full_width, ssd, x, bc, dec, gate, back, sums, taps,
    normed_out, dy_out, ggate_out, row_out, colsum_out, dstart_out,
):
    length, width = x.shape
    state_dim = dstart_out.shape[0]

    cc = bc[:, state_dim:]
    lo = iota((length, 128), 1) < 64
    rescale = columns(lax.rsqrt(sums[0:1] / full_width + EPS))
    pull = columns(sums[1:2]) * (rescale * rescale * rescale / full_width)
    rowterm = jnp.zeros((length, 128), F32)
    for p in range(width // 128):
        sl = slice(p * 128, (p + 1) * 128)
        s_ssd = ssd[:, sl]
        xp = x[:, sl].astype(F32)
        g = gate[:, sl].astype(F32)
        s = sigmoid(g)
        gated = s_ssd * (g * s)
        bk = back[:, sl].astype(F32)
        gain = taps[5:6, sl]
        normed_out[:, sl] = (gated * rescale * gain).astype(BF16)
        gg = rescale * (bk * gain) - gated * pull
        dy = gg * (g * s)
        dyb = dy.astype(BF16)
        dy_out[:, sl] = dyb
        ggate_out[:, sl] = (gg * s_ssd * s * (1.0 + g * (1.0 - s))).astype(BF16)
        colsum_out[5:6, sl] += jnp.sum(bk * gated * rescale, axis=0, keepdims=True)
        colsum_out[6:7, sl] += jnp.sum(dy * xp, axis=0, keepdims=True)
        dstart_out[:, sl] += tn(cc, (dy * pick(lo, dec, 2 * p)).astype(BF16))
        rowterm = rowterm + split_dot(dyb.astype(F32) * (s_ssd - taps[6:7, sl] * xp), head_map(p))
    row_out[...] = rowterm


def conv_back(dout, slope, cur, halo, links, taps, sl, carry, carry_links, par_out, first):
    length = dout.shape[0]
    dconv = dout * slope[:, sl].astype(F32)
    v = cur[:, sl].astype(F32)
    v_above = halo[HALO - 8 :, sl].astype(F32) * first
    nxt = carry[:, sl]
    grad = taps[3:4, sl] * dconv
    above = jnp.zeros((8, dout.shape[1]), F32)
    par_out[3:4, sl] += jnp.sum(dconv * v, axis=0, keepdims=True)
    par_out[4:5, sl] += jnp.sum(dconv, axis=0, keepdims=True)
    for j in range(1, 4):
        z = dconv * links[j - 1]
        w = taps[3 - j : 4 - j, sl]
        low = jnp.concatenate([z, nxt * carry_links[:, j - 1 : j]], axis=0)[j : j + length]
        high = jnp.concatenate([jnp.zeros_like(nxt), z[0:8]], axis=0)[j : j + 8]
        grad = grad + w * low
        above = above + w * high
        par_out[3 - j : 4 - j, sl] += jnp.sum(low * v, axis=0, keepdims=True) + jnp.sum(
            high * v_above, axis=0, keepdims=True
        )
    carry[:, sl] = dconv[0:8]
    return grad, above


def backward_body(
    k, chunks,
    inner, inner_halo, shared, shared_halo, step_raw, seg_row, seg_prev, seg_tail, taps, taps_s, heads,
    dy, x, bc, dt_in, c_in, ct_in, dec_halo, enter, slope, slope_s, start, row_in,
    ginner_out, gsmall_out, par_out, par_s_out, par_h_out, edge_out, last_out,
    dstate, carry, carry_s, carry_links, grads_bc,
):
    length, width = x.shape
    state_dim = dstate.shape[0]

    segr, seg, seg_halo, tail_seg = segments(seg_row, seg_prev, seg_tail)
    links = chunk_links(seg, seg_halo)
    closing = (seg == seg[length - 1 :]).astype(F32)
    entering = (seg == seg_halo[7:]).astype(F32)
    kept = (seg[length - 1 :] == seg_halo[7:]).astype(F32)
    next_links = carry_links[...]
    dt = dt_in[...]
    c = c_in[...]
    ct = ct_in[...]
    first = jnp.where(k == 0, 1.0, 0.0)
    reach = dec_halo[7:8] * (1.0 - first) + first
    b = bc[:, :state_dim]
    cc = bc[:, state_dim:]
    rows, cols = iota((length, length), 0), iota((length, length), 1)
    allowed = (rows <= cols) & (seg == segr)
    scores = jnp.where(allowed, nt(b, cc), 0.0)
    lo = iota((length, 128), 1) < 64
    lo1 = lo[0:1]
    sides = [jnp.where(lo, 1.0, 0.0).astype(BF16), jnp.where(lo, 0.0, 1.0).astype(BF16)]
    arriving = jnp.exp(c) * entering
    leaving_all = jnp.exp(c[length - 1 :] - c) * closing
    held_all = jnp.exp(c[length - 1 :]) * kept
    half = length // 2
    scores_top, scores_low = scores[:half], scores[half:, half:]
    top = jnp.zeros((half, length), F32)
    low = jnp.zeros((half, half), F32)
    db = jnp.zeros((length, state_dim), F32)
    dc_mat = jnp.zeros((length, state_dim), F32)
    direct = jnp.zeros((length, 128), F32)
    matched = jnp.zeros((length, 128), F32)
    closing_term = jnp.zeros((1, 128), F32)
    for p in range(width // 128):
        sl = slice(p * 128, (p + 1) * 128)
        dyb = dy[:, sl]
        dyf = dyb.astype(F32)
        xp = x[:, sl].astype(F32)
        dtb = pick(lo, dt, 2 * p)
        xdt = xp * dtb
        xdtb = xdt.astype(BF16)
        hm = head_map(p)
        entry = enter[:, sl].astype(F32) + start[:, sl] * pick(lo1, reach, 2 * p)
        entryb = entry.astype(BF16)
        ds = dstate[:, sl]
        dsb = ds.astype(BF16)
        leaving = pick(lo, leaving_all, 2 * p)
        bds = nn(b, dsb)
        dx_top = jnp.zeros((half, 128), F32)
        dx_low = jnp.zeros((half, 128), F32)
        for a in range(2):
            h = 2 * p + a
            mine = dyb * sides[a]
            decay = jnp.exp(jnp.minimum(ct[h : h + 1] - c[:half, h : h + 1], 0.0))
            top = top + decay * nt(xdtb[:half], mine)
            dx_top = dx_top + nn((decay * scores_top).astype(BF16), mine)
            decay = jnp.exp(jnp.minimum(ct[h : h + 1, half:] - c[half:, h : h + 1], 0.0))
            low = low + decay * nt(xdtb[half:], mine[half:])
            dx_low = dx_low + nn((decay * scores_low).astype(BF16), mine[half:])
        dxdt = jnp.concatenate([dx_top, dx_low], axis=0)
        spread = leaving * xdt
        moved = spread * bds
        matched = matched + split_dot(xdtb.astype(F32) * dxdt + moved, hm)
        dxdt = dxdt + leaving * bds
        held = pick(lo1, held_all, 2 * p)
        col = jnp.sum(moved, axis=0, keepdims=True) + held * jnp.sum(entry * ds, axis=0, keepdims=True)
        closing_term = closing_term + split_dot(jnp.broadcast_to(col, (8, 128)), hm)[0:1]
        direct = direct + nn((xp * dxdt).astype(BF16), hm)
        edy = (pick(lo, arriving, 2 * p) * dyf).astype(BF16)
        db = db + nt(spread.astype(BF16), dsb)
        dc_mat = dc_mat + nt(edy, entryb)
        dstate[:, sl] = ds * held + tn(cc, edy)
        dx = dtb * dxdt + taps[6:7, sl] * dyf
        grad, above = conv_back(dx, slope, inner, inner_halo, links, taps, sl, carry, next_links, par_out, first)
        ginner_out[:, sl] = grad.astype(BF16)
        edge_out[:, sl] = above

        @pl.when(k == chunks - 1)
        def _():
            last_out[:, sl] = grad[length - 8 :]

    low = jnp.concatenate([jnp.zeros((half, half), F32), low], axis=1)
    dsc = jnp.where(allowed, jnp.concatenate([top, low], axis=0), 0.0).astype(BF16)
    grads_bc[:, :state_dim] = db + nn(dsc, cc)
    grads_bc[:, state_dim:] = dc_mat + tn(dsc, b)
    for half in range(2):
        sl = slice(half * state_dim, (half + 1) * state_dim)
        grad, above = conv_back(
            grads_bc[:, sl], slope_s, shared, shared_halo, links, taps_s, sl, carry_s, next_links, par_s_out, first
        )
        gsmall_out[:, sl] = grad.astype(BF16)
        at = slice(width + half * state_dim, width + (half + 1) * state_dim)
        edge_out[:, at] = above

        @pl.when(k == chunks - 1)
        def _():
            last_out[:, at] = grad[length - 8 :]

    for j in range(3):
        carry_links[:, j : j + 1] = links[j][0:8]
    dcum = row_in[...] - matched
    upper = (rows <= cols).astype(F32)
    dlog = jnp.dot(upper, dcum, precision=HIGH, preferred_element_type=F32) + closing_term
    rate = -jnp.exp(heads[1:2])
    dstep = (direct + dlog * rate) * sigmoid(step_raw[...] + heads[0:1])
    gsmall_out[:, 2 * state_dim :] = dstep.astype(BF16)
    par_h_out[0:1] += jnp.sum(dstep, axis=0, keepdims=True)
    par_h_out[1:2] += jnp.sum(dlog * (rate * dt), axis=0, keepdims=True)


def spread_body(ggate, ginner, gsmall, w_in, w_small, normed, part_out, gain_out):
    width = ggate.shape[1]
    part = nt(ggate[...], w_in[:, :width]) + nt(ginner[...], w_in[:, width:]) + nt(gsmall[...], w_small[...])
    part_out[...] = part.astype(BF16)
    gain_out[...] = jnp.sum(part * normed[...].astype(F32), axis=0, keepdims=True)


PIECES = 2
MESH = pl.DeviceIdType.MESH
ANY = pl.BlockSpec(memory_space=pl.ANY)


def remote(src, dst, send, recv, **to):
    return pltpu.make_async_remote_copy(
        src_ref=src, dst_ref=dst, send_sem=send, recv_sem=recv, device_id=to, device_id_type=MESH
    )


def greet(barrier, when, **to):
    @pl.when(when)
    def _():
        pl.semaphore_signal(barrier, inc=1, device_id=to, device_id_type=MESH)


def line_of(ref):
    return ref[...].reshape(1, ref.shape[0])


def start(copies):
    for copy in copies:
        copy.start()


def guarded(when, action):
    @pl.when(when)
    def _():
        action()


class LineGather:
    def __init__(self, ncol, z, first, second, extra, sems):
        self.ncol, self.z, self.last = ncol, z, ncol - 1
        self.parts = (first, second)
        self.extra = extra
        self.sems = sems
        self.tokens = second[1].shape[0] // ncol
        self.part = self.tokens // PIECES

    def copies(self, kind, s, way, pieces, mine=False):
        source, dest = self.parts[kind]
        send, recv = self.sems[2 * kind : 2 * kind + 2]
        to = self.z + 1 if way == 0 else self.z - 1
        made = []
        for p in pieces:
            at = pl.ds(pl.multiple_of(s * self.tokens + p * self.part, self.part), self.part)
            src = source.at[pl.ds(p * self.part, self.part)] if mine and source is not None else dest.at[at]
            made.append(remote(src, dest.at[at], send.at[way, s, p], recv.at[s, p], col=to))
            if kind == 0 and p == PIECES - 1:
                place = self.extra.at[pl.ds(pl.multiple_of(s * 8, 8), 8)]
                made.append(remote(place, place, send.at[way, s, PIECES], recv.at[s, PIECES], col=to))
        return made

    def exit(self, way):
        return self.z < self.last if way == 0 else self.z > 0

    def depth(self, way):
        return self.z if way == 0 else self.last - self.z

    def begin(self):
        every = range(PIECES)
        for way in range(2):
            guarded(self.exit(way), lambda way=way: start(self.copies(0, self.z, way, every, True)))
        for way in range(2):
            guarded(self.depth(way) == 0, lambda way=way: start(self.copies(1, self.z, way, every, True)))

    ticks = property(lambda self: 2 * self.last * PIECES)

    def tick(self, tau):
        j, p = (tau - 1) // PIECES, (tau - 1) % PIECES
        for way in range(2):
            depth = self.depth(way)
            sign = -1 if way == 0 else 1

            def relay(kind, s, way=way, depth=depth):
                for copy in self.copies(kind, s, way, (p,)):
                    copy.wait_recv()
                guarded(self.exit(way), lambda: start(self.copies(kind, s, way, (p,))))
                if kind == 0 and p == PIECES - 1:
                    guarded(self.exit(way) & (j == depth - 1),
                            lambda: start(self.copies(1, self.z, way, range(PIECES), True)))

            guarded(j < depth, lambda s=self.z + sign * (j + 1), relay=relay: relay(0, s))
            guarded((j >= depth) & (j < 2 * depth),
                    lambda s=self.z + sign * (j - depth + 1), relay=relay: relay(1, s))

    def drain(self):
        for kind in range(2):
            for way in range(2):
                sign = -1 if way == 0 else 1
                for s in range(self.ncol):

                    def wait(kind=kind, way=way, s=s, sign=sign):
                        for copy in self.copies(kind, self.z + sign * s, way, range(PIECES)):
                            copy.wait_send()

                    guarded(self.exit(way) & (s <= self.depth(way)), wait)


def mixer_kernel(ncol, ndp, full_width, *refs):
    refs = list(refs)

    def take(number):
        taken = refs[:number]
        del refs[:number]
        return taken

    tokens_in, gain, seg_in, ci, cib, gg, cs, csb, sb, rl, sg = take(11)
    zx, bc_in, dt_in, w2, cot_in = take(5)
    normed_hbm, gsmall_hbm, ggate_hbm, cot_hbm, gnorm_hbm, ginner_hbm, part_hbm = take(7)
    par, par_s, par_h, gain_out, total_out = take(5)
    normed, seg, w_in, w_small, out_t, cot = take(6)
    taps, taps_s, heads = take(3)
    both, shared, step = take(3)
    ssd, x, bc, dt, c, ct, dec, enter, slope, slope_s, state, start_state, total = take(13)
    gained, gnorm, projected, back, dy, ggate, rowterm, dstart, dend = take(9)
    ginner, gsmall, part, edge, edge_in, last_rows = take(6)
    dstate, carry, carry_s, carry_links, grads_bc = take(5)
    sums, sums_all, own_scale, slots = take(4)
    line_box, line_send, line_recv = take(3)
    xs_send, xs_recv, cs_send, cs_recv, w_send, c_send, w_recv, t_send, t_recv = take(9)
    sum_send, sum_recv, row_send, row_recv, here = take(5)

    dp, row, z = lax.axis_index("dp"), lax.axis_index("row"), lax.axis_index("col")
    other = 1 - row
    last = ncol - 1
    tokens = tokens_in.shape[0]
    tail = HALO
    length = ncol * tokens
    width = taps.shape[1]
    scols = taps_s.shape[1]
    state_dim = scols // 2
    chunks = length // SPAN
    rows = bc_in.shape[0]
    me = dp * 2 + row
    sends_tail = (row == 0) & (z == last)

    barrier = pltpu.get_barrier_semaphore()
    for s in range(1, ncol):
        greet(barrier, row >= 0, col=lax.rem(z + s, ncol))
    greet(barrier, row >= 0, row=other)
    for m in range(1, ndp):
        greet(barrier, row >= 0, dp=dp ^ m)
    greet(barrier, row == 1, row=0, col=last)
    for s in range(ncol):
        greet(barrier, sends_tail, row=1, col=s)

    seg[pl.ds(pl.multiple_of(z * 8, 8), 8)] = jnp.broadcast_to(line_of(seg_in), (8, tokens))
    base = pl.multiple_of(z * tokens, 32)
    gain_row = line_of(gain)

    def normalize(n, carried):
        at = pl.multiple_of(n * 32, 32)
        wide = tokens_in[pl.ds(at, 32)].astype(F32)
        scale = lax.rsqrt(jnp.sum(wide * wide, axis=1, keepdims=True) / wide.shape[1] + EPS)
        normed[pl.ds(pl.multiple_of(base + at, 32), 32)] = (wide * scale * gain_row).astype(BF16)
        return carried

    lax.fori_loop(0, tokens // 32, normalize, 0)

    @pl.when(row == 0)
    def _():
        seg[pl.ds(ncol * 8, 8)] = jnp.full((8, tokens), -1, jnp.int32)
        normed[pl.ds(length, tail)] = jnp.zeros((tail, normed.shape[1]), BF16)
        start_state[...] = jnp.zeros_like(start_state)

    @pl.when(row == 1)
    def _():
        dend[...] = jnp.zeros_like(dend)
        edge_in[...] = jnp.zeros_like(edge_in)

    count = ncol - 1 + ndp + row + jnp.where(sends_tail, ncol, 0)
    pl.semaphore_wait(barrier, count)

    weights = ((None, w_in), (None, w_small), (w2, out_t))

    def weight_rows(j):
        return pl.ds(pl.multiple_of(j * rows, 16), rows)

    def weight_copies(j, mine, send, **to):
        copies = []
        for i, (src, dst) in enumerate(weights):
            place = dst.at[weight_rows(j)]
            from_input = mine and src is not None
            copies.append(remote(src if from_input else place, place, send.at[i], w_recv.at[j, i], **to))
        return copies

    def tail_copies(s):
        place = seg.at[pl.ds(pl.multiple_of(z * 8, 8), 8)]
        end = pl.multiple_of(z * tokens + tokens - tail, 16)
        return [
            remote(normed.at[pl.ds(end, tail)], normed.at[pl.ds(length, tail)],
                   t_send.at[s, 0], t_recv.at[0], row=1, col=s),
            remote(place, seg.at[pl.ds(ncol * 8, 8)], t_send.at[s, 1], t_recv.at[1], row=1, col=s),
        ]

    for s in range(ncol):
        guarded(sends_tail, lambda s=s: start(tail_copies(s)))
    gather = LineGather(ncol, z, (None, normed), (cot_in, cot), seg, (xs_send, xs_recv, cs_send, cs_recv))
    gather.begin()
    w_in[weight_rows(me), 0:width] = zx[:, 0, :]
    w_in[weight_rows(me), width : 2 * width] = zx[:, 1, :]
    w_small[weight_rows(me), 0:scols] = bc_in[...]
    dt_rows = jnp.concatenate([dt_in[...].astype(F32), jnp.zeros((128 - dt_in.shape[0], rows), F32)], axis=0)
    w_small[weight_rows(me), scols : scols + 128] = dt_rows.T.astype(BF16)
    local = [
        pltpu.make_async_copy(cot_in, cot.at[pl.ds(base, tokens)], here.at[0]),
        pltpu.make_async_copy(w2, out_t.at[weight_rows(me)], here.at[1]),
    ]
    start(local)
    taps[0:4] = ci[...]
    taps[4:5] = line_of(cib)
    taps[5:6] = line_of(gg)
    sg_row = line_of(sg)
    lo1 = iota((1, 128), 1) < 64
    for p in range(width // 128):
        taps[6:7, p * 128 : (p + 1) * 128] = pick(lo1, sg_row, 2 * p)
    taps_s[0:4] = cs[...]
    taps_s[4:5] = line_of(csb)
    heads[...] = jnp.zeros_like(heads)
    heads[0:1, : sb.shape[0]] = line_of(sb)
    heads[1:2, : rl.shape[0]] = line_of(rl)
    for ref in (state, total, dstart, carry, carry_s, carry_links, par, par_s, par_h, sums):
        ref[...] = jnp.zeros_like(ref)

    for m in range(1, ndp):
        start(weight_copies(me, True, w_send.at[m], dp=dp ^ m))
    start(weight_copies(me, True, c_send.at[0], row=other))

    def pass_weights(m):
        j = (dp ^ m) * 2 + row
        for copy in weight_copies(j, False, w_send.at[m], dp=dp ^ m):
            copy.wait_recv()
        start(weight_copies(j, False, c_send.at[m], row=other))

    half = gather.ticks // 2
    due = {tau: [] for tau in range(1, half + 1)}
    for m in range(1, ndp):
        due[min(half - 1, 2 + (3 * (m - 1)) // (ndp - 1) * (half - 3) // 2)].append(m)
    for tau in range(1, half):
        gather.tick(tau)
        for m in due[tau]:
            pass_weights(m)
    for m in range(ndp):
        for copy in weight_copies((dp ^ m) * 2 + other, False, c_send.at[m], row=other):
            copy.wait_recv()
    guarded(row == 1, lambda: [copy.wait_recv() for copy in tail_copies(0)])
    for copy in local:
        copy.wait()

    def nth(n):
        return pl.multiple_of(jnp.where(z * 2 < ncol, n, last - n) * tokens, tokens)

    def put(at, size, value, small):
        both[pl.ds(at, size)] = value.astype(BF16)
        shared[pl.ds(at, size)] = small[:, :scols].astype(BF16)
        step[pl.ds(at, size)] = small[:, scols:]

    def project_tokens(n, with_tail):
        at = nth(n)
        lhs = normed[pl.ds(at, tokens)]
        if with_tail:
            lhs = jnp.concatenate([lhs, normed[pl.ds(length, tail)]], axis=0)
        value, small = nn(lhs, w_in[...]), nn(lhs, w_small[...])
        put(at, tokens, value[:tokens], small[:tokens])
        if with_tail:
            put(length, tail, value[tokens:], small[tokens:])

    for n in range(ncol - 1):
        project_tokens(n, n == 0)
    gather.tick(half)
    project_tokens(ncol - 1, False)
    outs = [pltpu.make_async_copy(normed, normed_hbm, here.at[4])]
    outs[0].start()

    def at_rows(k):
        return pl.ds(pl.multiple_of(k * SPAN, SPAN), SPAN)

    def common(k):
        this = at_rows(k)
        above = pl.ds(pl.multiple_of(jnp.where(k == 0, length, k * SPAN - HALO), HALO), HALO)
        prev = pl.ds(pl.multiple_of(jnp.where(k == 0, chunks, k - 1) * 8, 8), 8)
        side = pl.ds(width, width)
        return (
            both.at[this, side], both.at[above, side], shared.at[this], shared.at[above], step.at[this],
            seg.at[pl.ds(pl.multiple_of(k * 8, 8), 8)], seg.at[prev], seg.at[pl.ds(chunks * 8, 8)], taps, taps_s, heads,
        )

    later = list(range(half + 1, gather.ticks + 1))

    def forward(k, carried):
        this = at_rows(k)
        forward_body(*common(k), ssd.at[this], x.at[this], bc.at[this], dt.at[this], c.at[this],
                     ct.at[:, this], dec.at[this], enter.at[k], slope.at[this], slope_s.at[this], state, total)
        guarded(k == chunks // 2, lambda: gather.tick(half + 1))
        return carried

    lax.fori_loop(0, chunks, forward, 0)
    later.pop(0)

    def row_copy(n, src, dst):
        return remote(src, dst, row_send.at[n], row_recv.at[n], row=other)

    guarded(row == 0, lambda: row_copy(0, state, start_state).start())
    gather.tick(later.pop(0))
    guarded(row == 1, lambda: row_copy(0, state, start_state).wait_recv())

    def gating(k, carried):
        this = at_rows(k)
        gate_body(ssd.at[this], x.at[this], bc.at[this], dec.at[this], start_state, both.at[this, pl.ds(0, width)],
                  taps, ssd.at[this], gained.at[this], sums.at[:, this])
        return carried

    lax.fori_loop(0, chunks, gating, 0)

    def sum_copy(s, source):
        return remote(sums, slots.at[source], sum_send.at[s], sum_recv.at[source], col=lax.rem(z + s, ncol))

    def sum_end():
        result = sums[...]
        for s in range(1, ncol):
            source = lax.rem(z + s, ncol)
            sum_copy(s, source).wait_recv()
            result = result + slots[source]
        sums_all[...] = result

    gather.tick(later.pop(0))

    def projecting(k, carried):
        this = at_rows(k)
        projected[this] = nt(gained[this], out_t[...]).astype(BF16)
        return carried

    lax.fori_loop(0, chunks, projecting, 0)
    line = LineReduce(ncol, z, projected, projected, line_box, line_send, line_recv, False)
    line.start()
    while len(later) > 2:
        gather.tick(later.pop(0))

    def pulling(n):
        this = pl.ds(nth(n), tokens)
        pull_body(cot.at[this], out_t, gained.at[this], back.at[this], sums.at[:, this])

    for n in range(ncol - 1):
        pulling(n)
        if n == 0:
            gather.tick(later.pop(0))
    gather.tick(later.pop(0))
    ticks = list(range(1, line.ticks + 1))
    pulling(ncol - 1)
    outs.append(pltpu.make_async_copy(cot, cot_hbm, here.at[5]))
    outs[-1].start()
    for s in range(1, ncol):
        sum_copy(s, z).start()
    line.start(2, line.ticks)
    line.tick(ticks.pop(0))
    sum_end()
    own_scale[...] = columns(lax.rsqrt(sums_all[0:1, pl.ds(pl.multiple_of(z * tokens, tokens), tokens)] / full_width + EPS))

    def pull_gate(k, carried):
        this = at_rows(k)
        back_body(full_width, ssd.at[this], x.at[this], bc.at[this], dec.at[this], both.at[this, pl.ds(0, width)],
                  back.at[this], sums_all.at[:, this], taps,
                  gnorm.at[this], dy.at[this], ggate.at[this], rowterm.at[this], par, dstart)
        return carried

    lax.fori_loop(0, chunks, pull_gate, 0)
    guarded(row == 1, lambda: row_copy(1, dstart, dend).start())
    outs.append(pltpu.make_async_copy(ggate, ggate_hbm, here.at[7]))
    outs.append(pltpu.make_async_copy(gnorm, gnorm_hbm, here.at[6]))
    start(outs[-2:])
    line.tick(ticks.pop(0))
    guarded(row == 0, lambda: row_copy(1, dstart, dend).wait_recv())
    dstate[...] = dend[...]

    spaced = {n: [tau] for n, tau in enumerate(ticks[:chunks])}
    ticks = ticks[chunks:]

    def backward(n, carried):
        k = chunks - 1 - n
        this = at_rows(k)
        before = pl.ds(pl.multiple_of(jnp.maximum(k * SPAN - 8, 0), 8), 8)
        backward_body(k, chunks, *common(k), dy.at[this], x.at[this], bc.at[this], dt.at[this], c.at[this],
                      ct.at[:, this], dec.at[before], enter.at[k], slope.at[this], slope_s.at[this], start_state, rowterm.at[this],
                      ginner.at[this], gsmall.at[this], par, par_s, par_h, edge, last_rows,
                      dstate, carry, carry_s, carry_links, grads_bc)
        for turn, taus in spaced.items():
            if turn < chunks - 1:
                for tau in taus:
                    guarded(n == turn, lambda tau=tau: line.tick(tau))
        return carried

    lax.fori_loop(0, chunks, backward, 0)
    guarded(row == 1, lambda: row_copy(2, edge, edge_in).start())
    for tau in spaced.get(chunks - 1, []):
        line.tick(tau)
    guarded(row == 0, lambda: row_copy(2, edge, edge_in).wait_recv())
    fixed = (last_rows[...] + edge_in[...]).astype(BF16)
    ginner[length - 8 :] = fixed[:, :width]
    gsmall[length - 8 :, : fixed.shape[1] - width] = fixed[:, width:]
    outs.append(pltpu.make_async_copy(ginner, ginner_hbm, here.at[8]))
    outs.append(pltpu.make_async_copy(gsmall, gsmall_hbm, here.at[9]))
    start(outs[-2:])

    tile = 256
    tiles = part.shape[1] // tile

    def part_copy(n):
        at = pl.ds(pl.multiple_of(n * tile, tile), tile)
        return pltpu.make_async_copy(part.at[:, at], part_hbm.at[:, at], here.at[10 + n])

    def spreading(n, carried):
        at = pl.ds(pl.multiple_of(n * tile, tile), tile)
        spread_body(ggate, ginner, gsmall, w_in.at[at], w_small.at[at], normed.at[pl.ds(0, length), at],
                    part.at[:, at], gain_out.at[:, at])
        guarded(n > 0, lambda: part_copy(jnp.maximum(n - 1, 0)).start())
        for tau in ticks[:-1]:
            guarded(n == tiles // 2, lambda tau=tau: line.tick(tau))
        return carried

    lax.fori_loop(0, tiles, spreading, 0)
    part_copy(tiles - 1).start()
    for tau in ticks[-1:]:
        line.tick(tau)

    def keep(at, value):
        here_rows = pl.ds(pl.multiple_of(at, 16), 16)
        total_out[here_rows] = (value * own_scale[here_rows, 0:1]).astype(BF16)

    line.total(keep)

    gather.drain()
    line.drain()
    for m in range(ndp):
        if m:
            for copy in weight_copies(me, True, w_send.at[m], dp=dp ^ m):
                copy.wait_send()
        for copy in weight_copies((dp ^ m) * 2 + row, m == 0, c_send.at[m], row=other):
            copy.wait_send()
    for s in range(ncol):
        guarded(sends_tail, lambda s=s: [copy.wait_send() for copy in tail_copies(s)])
    for s in range(1, ncol):
        sum_copy(s, z).wait_send()
    guarded(row == 0, lambda: row_copy(0, state, start_state).wait_send())
    guarded(row == 1, lambda: row_copy(1, dstart, dend).wait_send())
    guarded(row == 1, lambda: row_copy(2, edge, edge_in).wait_send())
    for copy in outs:
        copy.wait()
    for n in range(tiles):
        part_copy(n).wait()


def run_mixer(full_width, tokens_in, gain, seg, ci, cib, gg, cs, csb, sb, rl, sg, zx, bc, dt, w2, cot):
    ncol, ndp = lax.axis_size("col"), lax.axis_size("dp")
    tokens, model = tokens_in.shape
    width, scols = ci.shape[1], cs.shape[1]
    length = ncol * tokens
    chunks = length // SPAN
    state_dim = scols // 2
    small = scols + 128
    shards = 2 * ndp
    S = jax.ShapeDtypeStruct
    V = pltpu.VMEM
    dma = pltpu.SemaphoreType.DMA
    vmem = pl.BlockSpec(memory_space=V)
    return pl.pallas_call(
        functools.partial(mixer_kernel, ncol, ndp, full_width),
        in_specs=[vmem] * 14 + [ANY] * 2,
        out_specs=[ANY] * 7 + [vmem] * 5,
        out_shape=[
            S((length + HALO, model), BF16), S((length, small), BF16), S((length, width), BF16), S((length, model), BF16),
            S((length, width), BF16), S((length, width), BF16), S((length, model), BF16),
            S((8, width), F32), S((8, scols), F32), S((8, 128), F32), S((1, model), F32), S((tokens, model), BF16),
        ],
        scratch_shapes=[
            V((length + HALO, model), BF16), V(((ncol + 1) * 8, tokens), jnp.int32), V((model, 2 * width), BF16),
            V((model, small), BF16), V((model, width), BF16), V((length, model), BF16),
            V((8, width), F32), V((8, scols), F32), V((8, 128), F32),
            V((length + HALO, 2 * width), BF16), V((length + HALO, scols), BF16), V((length + HALO, 128), F32),
            V((length, width), F32), V((length, width), BF16), V((length, scols), BF16), V((length, 128), F32),
            V((length, 128), F32), V((16, length), F32), V((length, 128), F32), V((chunks, state_dim, width), BF16),
            V((length, width), BF16), V((length, scols), BF16),
            V((state_dim, width), F32), V((state_dim, width), F32), V((8, 128), F32),
            V((length, width), BF16), V((length, width), BF16), V((length, model), BF16), V((length, width), BF16),
            V((length, width), BF16), V((length, width), BF16), V((length, 128), F32), V((state_dim, width), F32),
            V((state_dim, width), F32),
            V((length, width), BF16), V((length, small), BF16), V((length, model), BF16),
            V((8, width + scols), F32), V((8, width + scols), F32), V((8, width + scols), F32),
            V((state_dim, width), F32), V((8, width), F32), V((8, scols), F32), V((8, 128), F32), V((SPAN, scols), F32),
            V((8, length), F32), V((8, length), F32), V((tokens, 128), F32), V((ncol, 8, length), F32),
            *line_scratch(ncol, tokens, model),
            dma((2, ncol, PIECES + 1)), dma((ncol, PIECES + 1)), dma((2, ncol, PIECES)), dma((ncol, PIECES)),
            dma((ndp, 3)), dma((ndp, 3)), dma((shards, 3)), dma((ncol, 2)), dma((2,)),
            dma((ncol,)), dma((ncol,)), dma((3,)), dma((3,)), dma((10 + model // 256,)),
        ],
        compiler_params=pltpu.CompilerParams(
            collective_id=1, has_side_effects=True, vmem_limit_bytes=63 * 1024 * 1024
        ),
        cost_estimate=pl.CostEstimate(flops=0, bytes_accessed=500_000_000, transcendentals=0),
        name="mixer",
    )(tokens_in, gain, seg, ci, cib, gg, cs, csb, sb, rl, sg, zx, bc, dt, w2, cot)
class LineReduce:
    def __init__(self, ncol, z, source, local, inbox, send, recv, paced):
        self.paced = paced
        self.ncol, self.z, self.last = ncol, z, ncol - 1
        self.source, self.local, self.inbox = source, local, inbox
        self.send, self.recv = send, recv
        self.tokens = local.shape[0] // ncol
        self.part = self.tokens // PIECES

    def rows(self, way, t, p):
        d = self.last - t if way == 0 else t
        return pl.multiple_of(d * self.tokens + p * self.part, self.part)

    def copy(self, way, t, p, first):
        src = self.source.at[pl.ds(self.rows(way, t, p), self.part)] if first else self.inbox.at[way, t, p]
        to = self.z + 1 if way == 0 else self.z - 1
        return remote(src, self.inbox.at[way, t, p], self.send.at[way, t, p], self.recv.at[way, t, p], col=to)

    def edge(self, way):
        return self.z == (0 if way == 0 else self.last)

    def depth(self, way):
        return self.z if way == 0 else self.last - self.z

    def start(self, first=0, stop=2):
        for way in range(2):

            @pl.when(self.edge(way))
            def _(way=way):
                for i in range(first, min(stop, self.ticks)):
                    self.copy(way, i // PIECES, i % PIECES, True).start()

    ticks = property(lambda self: self.last * PIECES)

    def tick(self, tau):
        for way in range(2):

            @pl.when(self.edge(way) & (self.paced and tau + 1 < self.ticks))
            def _(way=way):
                self.copy(way, (tau - 1) // PIECES, (tau - 1) % PIECES, True).wait_send()
                self.copy(way, (tau + 1) // PIECES, (tau + 1) % PIECES, True).start()

        for stage in range(2):
            for way in range(2):
                depth = self.depth(way)
                index = tau - (2 * depth - 1)
                t, p = index // PIECES, lax.rem(index, PIECES)

                @pl.when((depth > 0) & (index >= 0) & (index < (self.ncol - depth) * PIECES))
                def _(way=way, depth=depth, t=t, p=p, stage=stage):
                    onward = t < self.last - depth
                    if stage == 0:
                        self.copy(way, t, p, False).wait_recv()

                        @pl.when(onward)
                        def _():
                            base = self.rows(way, t, p)

                            def add(k, carry):
                                at = pl.multiple_of(k * 16, 16)
                                mine = self.local[pl.ds(pl.multiple_of(base + at, 16), 16)].astype(F32)
                                here = pl.ds(at, 16)
                                self.inbox[way, t, p, here] = (self.inbox[way, t, p, here].astype(F32) + mine).astype(BF16)
                                return carry

                            lax.fori_loop(0, self.part // 16, add, 0)
                    else:

                        @pl.when(onward)
                        def _():
                            self.copy(way, t, p, False).start()

    def total(self, store):
        z, last = self.z, self.last
        for p in range(PIECES):

            def add(k, carry, p=p):
                at = pl.multiple_of(k * 16, 16)
                here = pl.ds(at, 16)
                row = p * self.part + at
                value = self.local[pl.ds(pl.multiple_of(z * self.tokens + row, 16), 16)].astype(F32)
                low = self.inbox[0, jnp.minimum(last - z, last - 1), p, here].astype(F32)
                high = self.inbox[1, jnp.minimum(z, last - 1), p, here].astype(F32)
                value = value + jnp.where(z > 0, low, 0.0) + jnp.where(z < last, high, 0.0)
                store(row, value)
                return carry

            lax.fori_loop(0, self.part // 16, add, 0)

    def drain(self):
        for way in range(2):
            depth = self.depth(way)

            @pl.when(self.edge(way))
            def _(way=way):
                for i in range(self.ticks - 2 if self.paced else 0, self.ticks):
                    self.copy(way, i // PIECES, i % PIECES, True).wait_send()

            for t in range(self.last):

                @pl.when((depth > 0) & (t < self.last - depth))
                def _(way=way, t=t):
                    for p in range(PIECES):
                        self.copy(way, t, p, False).wait_send()


def line_scratch(ncol, tokens, width):
    shape = (2, ncol - 1, PIECES)
    dma = pltpu.SemaphoreType.DMA
    return [pltpu.VMEM(shape + (tokens // PIECES, width), BF16), dma(shape), dma(shape)]


def reduce_kernel(ncol, ndp, scols, *refs):
    count = 4
    refs = list(refs)

    def take(number):
        taken = refs[:number]
        del refs[:number]
        return taken

    sources = take(7)
    vecs = take(4)
    r, vec_outs, gsum_out = take(count), take(4), refs.pop(0)
    held = take(7)
    (line_box, line_send, line_recv) = take(3)
    g, near, sent, far = take(count), take(count), take(count), take(count)
    vec_slots, col_slots = take(4), take(2)
    col_sums = take(2)
    bc_slots, bc_sum, load, c_send, c_recv, p_send, p_recv, v_send, v_recv, u_send, u_recv, b_send, b_recv = refs
    dp, row, z = lax.axis_index("dp"), lax.axis_index("row"), lax.axis_index("col")
    other = 1 - row
    me = dp * 2 + row
    rows = [out.shape[0] for out in r]
    barrier = pltpu.get_barrier_semaphore()
    for q in range(1, 2 * ndp):
        greet(barrier, row >= 0, dp=dp ^ (q >> 1), row=row ^ (q & 1))
    for s in range(1, ncol):
        greet(barrier, row >= 0, col=lax.rem(z + s, ncol))
    loads = []
    for i, (src, dst) in enumerate(zip(sources, held)):
        src = src.at[pl.ds(0, dst.shape[0])]
        loads.append(pltpu.make_async_copy(src, dst, load.at[i]))
        loads[-1].start()
    normed, gsmall, ggate, cot, gnorm, ginner, part = held
    pl.semaphore_wait(barrier, 2 * ndp + ncol - 2)
    line = LineReduce(ncol, z, sources[6], part, line_box, line_send, line_recv, True)
    line.start()

    order = (0, 1, 2, 3)
    turns = [3, 1, 2, 0] if ndp == 4 else list(range(1, ndp)) + [0]

    def core_copy(i, d):
        return remote(g[i].at[pl.ds((d * 2 + other) * rows[i], rows[i])], near[i].at[d],
                      c_send.at[i, d], c_recv.at[i, d], row=other)

    def vec_copy(q, i, j):
        return remote(vecs[i], vec_slots[i].at[j], v_send.at[q, i], v_recv.at[j, i],
                      dp=dp ^ (q >> 1), row=row ^ (q & 1))

    for q in range(1, 2 * ndp):
        for i in range(4):
            vec_copy(q, i, me).start()

    waiting = []

    def later(copy):
        if waiting:
            waiting.pop().start()
        if copy is not None:
            waiting.append(copy)

    def accumulate(i, first, number, terms, store):
        def step(k, carry):
            at = first + pl.multiple_of(k * 16, 16)
            total = terms[0](at)
            for term in terms[1:]:
                total = total + term(at)
            store(at, total)
            return carry

        lax.fori_loop(0, number // 16, step, 0)

    def read(ref, index, shift=0):
        return lambda at: ref[index, pl.ds(at - shift, 16)].astype(F32)

    def mine(i, d):
        return lambda at: g[i][pl.ds(pl.multiple_of((d * 2 + row) * rows[i] + at, 16), 16)].astype(F32)

    def write(ref, index, shift):
        def store(at, total):
            ref[index, pl.ds(at - shift, 16)] = total.astype(BF16)

        return store

    def arrived(i, d):
        core_copy(i, d).wait_recv()

    def tick():
        if ticks:
            line.tick(ticks.pop(0))

    if ndp == 4:
        halves = ((0, 1, 2), (1, 2, 1))

        def leg(i, slot, m):
            return remote(sent[i].at[slot], far[i].at[slot], p_send.at[i, slot], p_recv.at[i, slot], dp=dp ^ m)

        def step_one(i):
            half = rows[i] // 2
            arrived(i, dp ^ 3)
            for h, m1, m2 in halves:
                accumulate(i, h * half, half, [mine(i, dp ^ 3), read(near[i], dp ^ 3)],
                           write(sent[i], 3 * h + 1, h * half))
                later(leg(i, 3 * h + 1, m1))
            for h, m1, m2 in halves:
                arrived(i, dp ^ m1)
                accumulate(i, h * half, half, [mine(i, dp ^ m1), read(near[i], dp ^ m1)],
                           write(sent[i], 3 * h, h * half))
                later(leg(i, 3 * h, m1))
            later(None)
            arrived(i, dp)

        def relay(i):
            half = rows[i] // 2
            for h, m1, m2 in halves:
                leg(i, 3 * h + 1, m1).wait_recv()
                accumulate(i, h * half, half,
                           [mine(i, dp ^ m2), read(near[i], dp ^ m2), read(far[i], 3 * h + 1, h * half)],
                           write(sent[i], 3 * h + 2, h * half))
                later(leg(i, 3 * h + 2, m2))
            later(None)

        def finish(i, store):
            half = rows[i] // 2
            for h, m1, m2 in halves:
                leg(i, 3 * h, m1).wait_recv()
                leg(i, 3 * h + 2, m2).wait_recv()
                accumulate(i, h * half, half,
                           [mine(i, dp), read(near[i], dp), read(far[i], 3 * h, h * half),
                            read(far[i], 3 * h + 2, h * half)], store)

        sends = [leg(i, 3 * h + k, m2 if k == 2 else m1) for i in order for h, m1, m2 in halves for k in range(3)]
    else:

        def peer(i, m):
            return remote(sent[i].at[m], far[i].at[m], p_send.at[i, m], p_recv.at[i, m], dp=dp ^ m)

        def step_one(i):
            for m in turns[:-1]:
                arrived(i, dp ^ m)
                accumulate(i, 0, rows[i], [mine(i, dp ^ m), read(near[i], dp ^ m)], write(sent[i], m, 0))
                later(peer(i, m))
            later(None)
            arrived(i, dp)

        def relay(i):
            pass

        def finish(i, store):
            for m in range(1, ndp):
                peer(i, m).wait_recv()
            accumulate(i, 0, rows[i],
                       [mine(i, dp), read(near[i], dp)] + [read(far[i], m) for m in range(1, ndp)], store)

        sends = [peer(i, m) for i in order for m in range(1, ndp)]

    def plain(i):
        def store(at, total):
            r[i][pl.ds(at, 16)] = total

        return store

    def shared_rows(at, total):
        r[0][pl.ds(at, 16)] = total
        bc_slots[z, pl.ds(at, 16)] = total[:, : bc_slots.shape[2]].astype(BF16)

    root = ncol // 2
    at_root = z == root

    def to_root(source):
        pairs = [(col_slots[i].at[source], u_send.at[0, i], u_recv.at[source, i]) for i in range(2)]
        pairs.append((bc_slots.at[source], b_send.at[0], b_recv.at[source]))
        return [remote(ref, ref, send, recv, col=root) for ref, send, recv in pairs]

    def from_root(target):
        pairs = [(col_sums[i], u_send.at[target, i], u_recv.at[root, i]) for i in range(2)]
        pairs.append((bc_sum, b_send.at[target], b_recv.at[root]))
        return [remote(ref, ref, send, recv, col=target) for ref, send, recv in pairs]

    others = [s for s in range(ncol) if s != root]

    def sum_at_root():
        @pl.when(at_root)
        def _():
            for s in others:
                for copy in to_root(s):
                    copy.wait_recv()
            for i in range(2):
                total = col_slots[i][0]
                for j in range(1, ncol):
                    total = total + col_slots[i][j]
                col_sums[i][...] = total
            total = bc_slots[0].astype(F32)
            for j in range(1, ncol):
                total = total + bc_slots[j].astype(F32)
            bc_sum[...] = total.astype(BF16)
            for s in others:
                for copy in from_root(s):
                    copy.start()

    model = normed.shape[1]
    block = model // 4
    products = ((normed, gsmall), (normed, ggate), (cot, gnorm), (normed, ginner))
    ready = {0: (0, 1), 1: (2,), 2: (3, 4), 3: (5,)}
    ticks = list(range(1, line.ticks + 1))
    for i in order:
        for at in ready[i]:
            loads[at].wait()
        left, right = products[i]
        for n, m in enumerate([3, 1, 2, 0] if ndp == 4 else range(4)):
            b = dp ^ m if ndp == 4 else m
            first = pl.multiple_of(b * block, 128)
            g[i][pl.ds(pl.multiple_of(b * block, 16), block)] = tn(left[:, pl.ds(first, block)], right[...]).astype(BF16)
            if ndp == 4:
                later(core_copy(i, b))
        if ndp != 4:
            for m in turns:
                later(core_copy(i, dp ^ m))
        if i == 1:
            loads[6].wait()
        if i > 0:
            step_one(i - 1)
        if i > 1:
            relay(i - 2)
        if i % 2:
            tick()
    later(None)
    step_one(3)
    relay(2)
    finish(0, shared_rows)
    for q in range(1, 2 * ndp):
        for i in range(4):
            vec_copy(q, i, me ^ q).wait_recv()
    for i in range(4):
        vec_slots[i][me] = vecs[i][...]
        total = vec_slots[i][0]
        for j in range(1, 2 * ndp):
            total = total + vec_slots[i][j]
        if i < 2:
            vec_outs[i][...] = total
        else:
            col_slots[i - 2][z] = total

    @pl.when(~at_root)
    def _():
        for copy in to_root(z):
            copy.start()

    tick()
    relay(3)
    while len(ticks) > 1:
        tick()
    sum_at_root()
    finish(1, plain(1))
    finish(2, plain(2))
    finish(3, plain(3))
    while ticks:
        tick()

    def keep(at, value):
        gsum_out[pl.ds(pl.multiple_of(at, 16), 16)] = value.astype(BF16)

    line.total(keep)
    @pl.when(~at_root)
    def _():
        for copy in from_root(z):
            copy.wait_recv()

    for i in range(2):
        vec_outs[2 + i][...] = col_sums[i][...]
    r[0][:, : bc_slots.shape[2]] = bc_sum[...].astype(F32)

    for q in range(1, 2 * ndp):
        for i in range(4):
            vec_copy(q, i, me).wait_send()
    for i in order:
        for m in turns:
            core_copy(i, dp ^ m).wait_send()
    for copy in sends:
        copy.wait_send()
    @pl.when(~at_root)
    def _():
        for copy in to_root(z):
            copy.wait_send()

    @pl.when(at_root)
    def _():
        for s in others:
            for copy in from_root(s):
                copy.wait_send()

    line.drain()


def reduce_grads(sources, vecs, scols):
    ncol, ndp = lax.axis_size("col"), lax.axis_size("dp")
    dma = pltpu.SemaphoreType.DMA
    vmem = pl.BlockSpec(memory_space=pltpu.VMEM)
    S = jax.ShapeDtypeStruct
    length = sources[1].shape[0]
    model = sources[0].shape[1]
    widths = [sources[1].shape[1], sources[2].shape[1], sources[4].shape[1], sources[5].shape[1]]
    count = len(widths)
    blocks = [(model // (2 * ndp), w) for w in widths]
    near = [pltpu.VMEM((ndp,) + b, BF16) for b in blocks]
    slots = 6 if ndp == 4 else ndp
    legs = [pltpu.VMEM((6, b[0] // 2, b[1]) if ndp == 4 else (ndp,) + b, BF16) for b in blocks]
    tokens = length // ncol
    return pl.pallas_call(
        functools.partial(reduce_kernel, ncol, ndp, scols),
        in_specs=[ANY] * 7 + [vmem] * 4,
        out_specs=[vmem] * (count + 5),
        out_shape=[S(b, F32) for b in blocks] + [S(v.shape, F32) for v in vecs] + [S((tokens, model), BF16)],
        scratch_shapes=[pltpu.VMEM((length, s.shape[1]), BF16) for s in sources]
        + line_scratch(ncol, tokens, model)
        + [pltpu.VMEM((model, w), BF16) for w in widths]
        + near + legs * 2
        + [pltpu.VMEM((2 * ndp,) + v.shape, F32) for v in vecs]
        + [pltpu.VMEM((ncol,) + v.shape, F32) for v in vecs[2:]]
        + [pltpu.VMEM(v.shape, F32) for v in vecs[2:]]
        + [pltpu.VMEM((ncol, blocks[0][0], scols), BF16), pltpu.VMEM((blocks[0][0], scols), BF16)]
        + [dma((7,))]
        + [dma((count, ndp))] * 2
        + [dma((count, slots))] * 2
        + [dma((2 * ndp, 4))] * 2
        + [dma((ncol, 2))] * 2
        + [dma((ncol,))] * 2,
        compiler_params=pltpu.CompilerParams(
            collective_id=2, has_side_effects=True, vmem_limit_bytes=60 * 1024 * 1024
        ),
        cost_estimate=pl.CostEstimate(flops=0, bytes_accessed=200_000_000, transcendentals=0),
        name="reduce_grads",
    )(*sources, *vecs)


def finish_small(
    nheads, small, par, par_h, par_s, gain_sum, gain_row, bc_out, dt_out, ci_out, cib_out, cs_out,
    csb_out, sb_out, rl_out, sg_out, gg_out, ng_out,
):
    width = par.shape[1]
    scols = par_s.shape[1]
    bc_out[...] = small[:, :scols]
    dt_out[...] = small[:, scols:].T[:nheads]
    ci_out[...] = par[0:4]
    cib_out[...] = par[4:5].reshape(width)
    gg_out[...] = par[5:6].reshape(width)
    cs_out[...] = par_s[0:4]
    csb_out[...] = par_s[4:5].reshape(scols)
    sb_out[...] = par_h[0:1, :nheads].reshape(nheads)
    rl_out[...] = par_h[1:2, :nheads].reshape(nheads)
    skip = jnp.zeros((8, 128), F32)
    for p in range(width // 128):
        skip = skip + split_dot(jnp.broadcast_to(par[6:7, p * 128 : (p + 1) * 128], (8, 128)), head_map(p))
    sg_out[...] = skip[0:1, :nheads].reshape(nheads)
    ng_out[...] = (gain_sum[0:1] / gain_row).reshape(gain_row.shape[1])


def finish_kernel(
    nheads, small, gate, inner, out, par, par_h, par_s, gain_sum, gain, tokens, cot, gnormed, projected,
    zx_out, bc_out, dt_out, out_out, ci_out, cib_out, cs_out, csb_out, sb_out, rl_out, sg_out, gg_out, ng_out, gin_out, block_out,
):
    gain_row = gain[...].reshape(1, gain.shape[0])
    zx_out[:, 0, :] = gate[...]
    zx_out[:, 1, :] = inner[...]
    out_out[...] = out[...]

    @pl.when(pl.program_id(0) == 0)
    def _():
        finish_small(nheads, small, par, par_h, par_s, gain_sum, gain_row, bc_out, dt_out, ci_out, cib_out, cs_out,
                     csb_out, sb_out, rl_out, sg_out, gg_out, ng_out)

    def rows(step, carry):
        at = pl.ds(pl.multiple_of(step * 32, 32), 32)
        wide = tokens[at].astype(F32)
        scale = lax.rsqrt(jnp.sum(wide * wide, axis=1, keepdims=True) / wide.shape[1] + EPS)
        pushed = gnormed[at].astype(F32) * gain_row
        mean = jnp.sum(pushed * wide, axis=1, keepdims=True) / wide.shape[1]
        grad = scale * pushed - wide * (scale * scale * scale * mean)
        gin_out[at] = (cot[at].astype(F32) + grad).astype(BF16)
        block_out[at] = (wide + projected[at].astype(F32)).astype(BF16)
        return carry

    lax.fori_loop(0, tokens.shape[0] // 32, rows, 0)


def run_finish(nheads, small, gate, inner, out, par, par_h, par_s, gain_sum, gain, tokens, cot, gnormed, projected):
    rows, width = gate.shape
    scols = par_s.shape[1]
    model = gain.shape[0]
    S = jax.ShapeDtypeStruct
    shapes = [
        (rows, 2, width), (rows, scols), (nheads, rows), (rows, width), (4, width), (width,), (4, scols), (scols,),
        (nheads,), (nheads,), (nheads,), (width,), (model,),
    ]
    steps = 4 if rows % 32 == 0 else 2
    block = rows // steps
    some = tokens.shape[0] // steps
    down = lambda n: (n, 0)
    whole = lambda shape: pl.BlockSpec(shape, lambda n: (0,) * len(shape))
    wide_spec = pl.BlockSpec((block, width), down)
    token_spec = pl.BlockSpec((some, model), down)
    return pl.pallas_call(
        functools.partial(finish_kernel, nheads),
        grid=(steps,),
        in_specs=[whole(small.shape), wide_spec, wide_spec, wide_spec, whole(par.shape), whole(par_h.shape),
                  whole(par_s.shape), whole(gain_sum.shape), whole(gain.shape)] + [token_spec] * 4,
        out_specs=[pl.BlockSpec((block, 2, width), lambda n: (n, 0, 0)), whole(shapes[1]), whole(shapes[2]), wide_spec]
        + [whole(shape) for shape in shapes[4:]] + [token_spec] * 2,
        out_shape=[S(shape, F32) for shape in shapes] + [S(tokens.shape, BF16)] * 2,
        name="finish",
    )(small, gate, inner, out, par, par_h, par_s, gain_sum, gain, tokens, cot, gnormed, projected)


def per_device(
    block_input, segment_ids, norm_gain, proj_zx, proj_bc, proj_dt, conv_inner, conv_inner_bias,
    conv_shared, conv_shared_bias, step_bias, rate_log, skip_gain, gated_gain, proj_out, cotangent,
):
    width = proj_zx.shape[2]
    scols = proj_bc.shape[1]
    nheads = proj_dt.shape[1]
    full_width = float(width * lax.axis_size("col"))
    (normed, gsmall, ggate, cot_all, gated_normed, ginner, part, par, par_s, par_h, gain_part, projected) = run_mixer(
        full_width, block_input, norm_gain, segment_ids, conv_inner, conv_inner_bias, gated_gain, conv_shared,
        conv_shared_bias, step_bias, rate_log, skip_gain, proj_zx, proj_bc, proj_dt.T, proj_out.T, cotangent,
    )
    gsm, gz, gout, gx, par, par_h, par_s, gain_sum, grad_normed = reduce_grads(
        (normed, gsmall, ggate, cot_all, gated_normed, ginner, part), (par, par_h, par_s, gain_part), scols
    )
    zx, gbc, gdt, gout, ci, cib, cs, csb, sb, rl, sg, gg, ng, grad_input, block_output = run_finish(
        nheads, gsm, gz, gx, gout, par, par_h, par_s, gain_sum, norm_gain, block_input, cotangent, grad_normed, projected
    )
    return (
        block_output, grad_input, ng, zx, gbc, gdt.T, ci, cib, cs, csb, sb, rl, sg, gg, gout.T,
    )


def solution(mesh):
    shards = ("dp", "row")
    tokens = P(("dp", "row", "col"), None)
    zx = P(shards, None, "col")
    in_specs = (
        tokens, P(("dp", "row", "col")), P(), zx, P(shards, None), P(shards, "col"), P(None, "col"), P("col"),
        P(), P(), P("col"), P("col"), P("col"), P("col"), P("col", shards), tokens,
    )
    out_specs = (
        tokens, tokens, P(), zx, P(shards, None), P(shards, "col"), P(None, "col"), P("col"),
        P(), P(), P("col"), P("col"), P("col"), P("col"), P("col", shards),
    )
    return jax.shard_map(per_device, mesh=mesh, in_specs=in_specs, out_specs=out_specs, check_vma=False)
```

```python
import functools
import jax, jax.numpy as jnp
from jax import lax
from jax.experimental import pallas as pl
from jax.experimental.pallas import tpu as pltpu
from jax.sharding import PartitionSpec as P

F32, BF16 = jnp.float32, jnp.bfloat16
HIGH = lax.Precision.HIGHEST
SPAN = 256
HALO = 16
EPS = 1e-5


def nn(a, b):
    return lax.dot_general(a, b, (((1,), (0,)), ((), ())), preferred_element_type=F32)


def nt(a, b):
    return lax.dot_general(a, b, (((1,), (1,)), ((), ())), preferred_element_type=F32)


def tn(a, b):
    return lax.dot_general(a, b, (((0,), (0,)), ((), ())), preferred_element_type=F32)


def iota(shape, axis):
    return lax.broadcasted_iota(jnp.int32, shape, axis)


def split_dot(a, b01):
    hi = a.astype(BF16)
    lo = (a - hi.astype(F32)).astype(BF16)
    return nn(hi, b01) + nn(lo, b01)


def sigmoid(v):
    return 0.5 * jnp.tanh(0.5 * v) + 0.5


def softplus(v):
    return jnp.maximum(v, 0.0) + jnp.log1p(jnp.exp(-jnp.abs(v)))


def columns(row):
    return jnp.broadcast_to(row, (128, row.shape[1])).T


def segments(seg_row, prev_row, tail_row):
    row = seg_row[0:1].astype(F32)
    seg = columns(row)[:, 0:1]
    length = row.shape[1]
    prev = columns(prev_row[0:1].astype(F32))[length - 8 :, 0:1]
    tail = tail_row[0:1, length - 1 :].astype(F32)
    return row, seg, prev, tail


def chunk_links(segc, halo):
    ext = jnp.concatenate([halo, segc], axis=0)
    length = segc.shape[0]
    return [(ext[8 - j : 8 - j + length] == segc).astype(F32) for j in range(1, 4)]


def conv_tile(cur, halo, links, taps, sl):
    v = jnp.concatenate([halo[HALO - 8 :, sl].astype(F32), cur[:, sl].astype(F32)], axis=0)
    length = cur.shape[0]
    pre = taps[4:5, sl] + taps[3:4, sl] * v[8:]
    for j in range(1, 4):
        pre = pre + taps[3 - j : 4 - j, sl] * (v[8 - j : 8 - j + length] * links[j - 1])
    return pre


def silu_and_slope(pre):
    s = sigmoid(pre)
    value = pre * s
    return value, s + value * (1.0 - s)


def pick(lo, cols, h):
    return jnp.where(lo, cols[:, h : h + 1], cols[:, h + 1 : h + 2])


def forward_body(
    inner, inner_halo, shared, shared_halo, step_raw, seg_row, seg_prev, seg_tail, taps, taps_s, heads,
    y_out, x_out, bc_out, dt_out, c_out, ct_out, dec_out, enter_out, slope_out, slope_s_out, state, total,
):
    length, width = inner.shape
    pairs = width // 128
    state_dim = state.shape[0]

    segr, seg, seg_halo, tail_seg = segments(seg_row, seg_prev, seg_tail)
    links = chunk_links(seg, seg_halo)
    closing = (seg == seg[length - 1 :]).astype(F32)
    entering = (seg == seg_halo[7:]).astype(F32)
    kept = (seg[length - 1 :] == seg_halo[7:]).astype(F32)
    dt = softplus(step_raw[...] + heads[0:1])
    log_decay = -jnp.exp(heads[1:2]) * dt
    rows, cols = iota((length, length), 0), iota((length, length), 1)
    lower = (rows >= cols).astype(F32)
    c = jnp.dot(lower, log_decay, precision=HIGH, preferred_element_type=F32)
    ct = c.T
    dt_out[...] = dt
    c_out[...] = c
    ct_out[...] = ct[: ct_out.shape[0]]
    whole = c + total[0:1]
    dec_out[...] = jnp.exp(whole) * (seg == tail_seg).astype(F32)
    total[0:1] = whole[length - 1 :]
    for half in range(2):
        sl = slice(half * state_dim, (half + 1) * state_dim)
        value, slope = silu_and_slope(conv_tile(shared, shared_halo, links, taps_s, sl))
        bc_out[:, sl] = value.astype(BF16)
        slope_s_out[:, sl] = slope.astype(BF16)
    b = bc_out[:, :state_dim]
    cc = bc_out[:, state_dim:]
    scores = jnp.where((rows >= cols) & (seg == segr), nt(cc, b), 0.0)
    lo = iota((length, 128), 1) < 64
    lo1 = lo[0:1]
    sides = [jnp.where(lo, 1.0, 0.0).astype(BF16), jnp.where(lo, 0.0, 1.0).astype(BF16)]
    arriving = jnp.exp(c) * entering
    leaving = jnp.exp(c[length - 1 :] - c) * closing
    held = jnp.exp(c[length - 1 :]) * kept
    enter_out[...] = state[...].astype(BF16)
    for p in range(pairs):
        sl = slice(p * 128, (p + 1) * 128)
        xp, slope = silu_and_slope(conv_tile(inner, inner_halo, links, taps, sl))
        xb = xp.astype(BF16)
        x_out[:, sl] = xb
        slope_out[:, sl] = slope.astype(BF16)
        xdt = xb.astype(F32) * pick(lo, dt, 2 * p)
        xdtb = xdt.astype(BF16)
        acc = nn(cc, state[:, sl].astype(BF16)) * pick(lo, arriving, 2 * p)
        for a in range(2):
            h = 2 * p + a
            weights = jnp.exp(jnp.minimum(c[:, h : h + 1] - ct[h : h + 1], 0.0)) * scores
            acc = acc + nn(weights.astype(BF16), xdtb * sides[a])
        y_out[:, sl] = acc
        moved = pick(lo, leaving, 2 * p) * xdt
        state[:, sl] = state[:, sl] * pick(lo1, held, 2 * p) + tn(b, moved.astype(BF16))


def row_sums(value):
    hi = value.astype(BF16)
    lo = (value - hi.astype(F32)).astype(BF16)
    ones = jnp.ones((8, value.shape[1]), BF16)
    return nt(ones, hi) + nt(ones, lo)


def first_rows(value):
    return jnp.where(iota(value.shape, 0) == 0, value, 0.0)


def head_map(p):
    lane, head = iota((128, 128), 0), iota((128, 128), 1)
    return (head == 2 * p + lane // 64).astype(BF16)


def gate_body(y, x, bc, dec, start, gate, taps, ssd_out, gained_out, sums_out):
    length, width = x.shape
    state_dim = start.shape[0]
    cc = bc[:, state_dim:]
    lo = iota((length, 128), 1) < 64
    squares = jnp.zeros((length, 128), F32)
    for p in range(width // 128):
        sl = slice(p * 128, (p + 1) * 128)
        corr = nn(cc, start[:, sl].astype(BF16)) * pick(lo, dec, 2 * p)
        ssd = y[:, sl] + corr + taps[6:7, sl] * x[:, sl].astype(F32)
        ssd_out[:, sl] = ssd
        g = gate[:, sl].astype(F32)
        gated = ssd * (g * sigmoid(g))
        gained_out[:, sl] = (gated * taps[5:6, sl]).astype(BF16)
        squares = squares + gated * gated
    sums_out[0:1] = row_sums(squares)[0:1]


def pull_body(cot, out_t, gained, back_out, sums_out):
    back = nn(cot[...], out_t[...])
    back_out[...] = back.astype(BF16)
    inner = jnp.zeros((cot.shape[0], 128), F32)
    for p in range(back.shape[1] // 128):
        sl = slice(p * 128, (p + 1) * 128)
        inner = inner + back[:, sl] * gained[:, sl].astype(F32)
    sums_out[1:2] = row_sums(inner)[0:1]


def back_body(
    full_width, ssd, x, bc, dec, gate, back, sums, taps,
    normed_out, dy_out, ggate_out, row_out, colsum_out, dstart_out,
):
    length, width = x.shape
    state_dim = dstart_out.shape[0]

    cc = bc[:, state_dim:]
    lo = iota((length, 128), 1) < 64
    rescale = columns(lax.rsqrt(sums[0:1] / full_width + EPS))
    pull = columns(sums[1:2]) * (rescale * rescale * rescale / full_width)
    rowterm = jnp.zeros((length, 128), F32)
    for p in range(width // 128):
        sl = slice(p * 128, (p + 1) * 128)
        s_ssd = ssd[:, sl]
        xp = x[:, sl].astype(F32)
        g = gate[:, sl].astype(F32)
        s = sigmoid(g)
        gated = s_ssd * (g * s)
        bk = back[:, sl].astype(F32)
        gain = taps[5:6, sl]
        normed_out[:, sl] = (gated * rescale * gain).astype(BF16)
        gg = rescale * (bk * gain) - gated * pull
        dy = gg * (g * s)
        dyb = dy.astype(BF16)
        dy_out[:, sl] = dyb
        ggate_out[:, sl] = (gg * s_ssd * s * (1.0 + g * (1.0 - s))).astype(BF16)
        colsum_out[5:6, sl] += jnp.sum(bk * gated * rescale, axis=0, keepdims=True)
        colsum_out[6:7, sl] += jnp.sum(dy * xp, axis=0, keepdims=True)
        dstart_out[:, sl] += tn(cc, (dy * pick(lo, dec, 2 * p)).astype(BF16))
        rowterm = rowterm + split_dot(dyb.astype(F32) * (s_ssd - taps[6:7, sl] * xp), head_map(p))
    row_out[...] = rowterm


def conv_back(dout, slope, cur, halo, links, taps, sl, carry, carry_links, par_out, first):
    length = dout.shape[0]
    dconv = dout * slope[:, sl].astype(F32)
    v = cur[:, sl].astype(F32)
    v_above = halo[HALO - 8 :, sl].astype(F32) * first
    nxt = carry[:, sl]
    grad = taps[3:4, sl] * dconv
    above = jnp.zeros((8, dout.shape[1]), F32)
    par_out[3:4, sl] += jnp.sum(dconv * v, axis=0, keepdims=True)
    par_out[4:5, sl] += jnp.sum(dconv, axis=0, keepdims=True)
    for j in range(1, 4):
        z = dconv * links[j - 1]
        w = taps[3 - j : 4 - j, sl]
        low = jnp.concatenate([z, nxt * carry_links[:, j - 1 : j]], axis=0)[j : j + length]
        high = jnp.concatenate([jnp.zeros_like(nxt), z[0:8]], axis=0)[j : j + 8]
        grad = grad + w * low
        above = above + w * high
        par_out[3 - j : 4 - j, sl] += jnp.sum(low * v, axis=0, keepdims=True) + jnp.sum(
            high * v_above, axis=0, keepdims=True
        )
    carry[:, sl] = dconv[0:8]
    return grad, above


def backward_body(
    k, chunks,
    inner, inner_halo, shared, shared_halo, step_raw, seg_row, seg_prev, seg_tail, taps, taps_s, heads,
    dy, x, bc, dt_in, c_in, ct_in, dec_halo, enter, slope, slope_s, start, row_in,
    ginner_out, gsmall_out, par_out, par_s_out, par_h_out, edge_out, last_out,
    dstate, carry, carry_s, carry_links, grads_bc,
):
    length, width = x.shape
    state_dim = dstate.shape[0]

    segr, seg, seg_halo, tail_seg = segments(seg_row, seg_prev, seg_tail)
    links = chunk_links(seg, seg_halo)
    closing = (seg == seg[length - 1 :]).astype(F32)
    entering = (seg == seg_halo[7:]).astype(F32)
    kept = (seg[length - 1 :] == seg_halo[7:]).astype(F32)
    next_links = carry_links[...]
    dt = dt_in[...]
    c = c_in[...]
    ct = ct_in[...]
    first = jnp.where(k == 0, 1.0, 0.0)
    reach = dec_halo[7:8] * (1.0 - first) + first
    b = bc[:, :state_dim]
    cc = bc[:, state_dim:]
    rows, cols = iota((length, length), 0), iota((length, length), 1)
    allowed = (rows <= cols) & (seg == segr)
    scores = jnp.where(allowed, nt(b, cc), 0.0)
    lo = iota((length, 128), 1) < 64
    lo1 = lo[0:1]
    sides = [jnp.where(lo, 1.0, 0.0).astype(BF16), jnp.where(lo, 0.0, 1.0).astype(BF16)]
    arriving = jnp.exp(c) * entering
    leaving_all = jnp.exp(c[length - 1 :] - c) * closing
    held_all = jnp.exp(c[length - 1 :]) * kept
    half = length // 2
    scores_top, scores_low = scores[:half], scores[half:, half:]
    top = jnp.zeros((half, length), F32)
    low = jnp.zeros((half, half), F32)
    db = jnp.zeros((length, state_dim), F32)
    dc_mat = jnp.zeros((length, state_dim), F32)
    direct = jnp.zeros((length, 128), F32)
    matched = jnp.zeros((length, 128), F32)
    closing_term = jnp.zeros((1, 128), F32)
    for p in range(width // 128):
        sl = slice(p * 128, (p + 1) * 128)
        dyb = dy[:, sl]
        dyf = dyb.astype(F32)
        xp = x[:, sl].astype(F32)
        dtb = pick(lo, dt, 2 * p)
        xdt = xp * dtb
        xdtb = xdt.astype(BF16)
        hm = head_map(p)
        entry = enter[:, sl].astype(F32) + start[:, sl] * pick(lo1, reach, 2 * p)
        entryb = entry.astype(BF16)
        ds = dstate[:, sl]
        dsb = ds.astype(BF16)
        leaving = pick(lo, leaving_all, 2 * p)
        bds = nn(b, dsb)
        dx_top = jnp.zeros((half, 128), F32)
        dx_low = jnp.zeros((half, 128), F32)
        for a in range(2):
            h = 2 * p + a
            mine = dyb * sides[a]
            decay = jnp.exp(jnp.minimum(ct[h : h + 1] - c[:half, h : h + 1], 0.0))
            top = top + decay * nt(xdtb[:half], mine)
            dx_top = dx_top + nn((decay * scores_top).astype(BF16), mine)
            decay = jnp.exp(jnp.minimum(ct[h : h + 1, half:] - c[half:, h : h + 1], 0.0))
            low = low + decay * nt(xdtb[half:], mine[half:])
            dx_low = dx_low + nn((decay * scores_low).astype(BF16), mine[half:])
        dxdt = jnp.concatenate([dx_top, dx_low], axis=0)
        spread = leaving * xdt
        moved = spread * bds
        matched = matched + split_dot(xdtb.astype(F32) * dxdt + moved, hm)
        dxdt = dxdt + leaving * bds
        held = pick(lo1, held_all, 2 * p)
        col = jnp.sum(moved, axis=0, keepdims=True) + held * jnp.sum(entry * ds, axis=0, keepdims=True)
        closing_term = closing_term + split_dot(jnp.broadcast_to(col, (8, 128)), hm)[0:1]
        direct = direct + nn((xp * dxdt).astype(BF16), hm)
        edy = (pick(lo, arriving, 2 * p) * dyf).astype(BF16)
        db = db + nt(spread.astype(BF16), dsb)
        dc_mat = dc_mat + nt(edy, entryb)
        dstate[:, sl] = ds * held + tn(cc, edy)
        dx = dtb * dxdt + taps[6:7, sl] * dyf
        grad, above = conv_back(dx, slope, inner, inner_halo, links, taps, sl, carry, next_links, par_out, first)
        ginner_out[:, sl] = grad.astype(BF16)
        edge_out[:, sl] = above

        @pl.when(k == chunks - 1)
        def _():
            last_out[:, sl] = grad[length - 8 :]

    low = jnp.concatenate([jnp.zeros((half, half), F32), low], axis=1)
    dsc = jnp.where(allowed, jnp.concatenate([top, low], axis=0), 0.0).astype(BF16)
    grads_bc[:, :state_dim] = db + nn(dsc, cc)
    grads_bc[:, state_dim:] = dc_mat + tn(dsc, b)
    for half in range(2):
        sl = slice(half * state_dim, (half + 1) * state_dim)
        grad, above = conv_back(
            grads_bc[:, sl], slope_s, shared, shared_halo, links, taps_s, sl, carry_s, next_links, par_s_out, first
        )
        gsmall_out[:, sl] = grad.astype(BF16)
        at = slice(width + half * state_dim, width + (half + 1) * state_dim)
        edge_out[:, at] = above

        @pl.when(k == chunks - 1)
        def _():
            last_out[:, at] = grad[length - 8 :]

    for j in range(3):
        carry_links[:, j : j + 1] = links[j][0:8]
    dcum = row_in[...] - matched
    upper = (rows <= cols).astype(F32)
    dlog = jnp.dot(upper, dcum, precision=HIGH, preferred_element_type=F32) + closing_term
    rate = -jnp.exp(heads[1:2])
    dstep = (direct + dlog * rate) * sigmoid(step_raw[...] + heads[0:1])
    gsmall_out[:, 2 * state_dim :] = dstep.astype(BF16)
    par_h_out[0:1] += jnp.sum(dstep, axis=0, keepdims=True)
    par_h_out[1:2] += jnp.sum(dlog * (rate * dt), axis=0, keepdims=True)


def spread_body(ggate, ginner, gsmall, w_in, w_small, normed, part_out, gain_out):
    width = ggate.shape[1]
    part = nt(ggate[...], w_in[:, :width]) + nt(ginner[...], w_in[:, width:]) + nt(gsmall[...], w_small[...])
    part_out[...] = part.astype(BF16)
    gain_out[...] = jnp.sum(part * normed[...].astype(F32), axis=0, keepdims=True)


PIECES = 2
MESH = pl.DeviceIdType.MESH
ANY = pl.BlockSpec(memory_space=pl.ANY)


def remote(src, dst, send, recv, **to):
    return pltpu.make_async_remote_copy(
        src_ref=src, dst_ref=dst, send_sem=send, recv_sem=recv, device_id=to, device_id_type=MESH
    )


def greet(barrier, when, **to):
    @pl.when(when)
    def _():
        pl.semaphore_signal(barrier, inc=1, device_id=to, device_id_type=MESH)


def line_of(ref):
    return ref[...].reshape(1, ref.shape[0])


def start(copies):
    for copy in copies:
        copy.start()


def guarded(when, action):
    @pl.when(when)
    def _():
        action()


class LineGather:
    def __init__(self, ncol, z, first, second, extra, sems):
        self.ncol, self.z, self.last = ncol, z, ncol - 1
        self.parts = (first, second)
        self.extra = extra
        self.sems = sems
        self.tokens = second[1].shape[0] // ncol
        self.part = self.tokens // PIECES

    def copies(self, kind, s, way, pieces, mine=False):
        source, dest = self.parts[kind]
        send, recv = self.sems[2 * kind : 2 * kind + 2]
        to = self.z + 1 if way == 0 else self.z - 1
        made = []
        for p in pieces:
            at = pl.ds(pl.multiple_of(s * self.tokens + p * self.part, self.part), self.part)
            src = source.at[pl.ds(p * self.part, self.part)] if mine and source is not None else dest.at[at]
            made.append(remote(src, dest.at[at], send.at[way, s, p], recv.at[s, p], col=to))
            if kind == 0 and p == PIECES - 1:
                place = self.extra.at[pl.ds(pl.multiple_of(s * 8, 8), 8)]
                made.append(remote(place, place, send.at[way, s, PIECES], recv.at[s, PIECES], col=to))
        return made

    def exit(self, way):
        return self.z < self.last if way == 0 else self.z > 0

    def depth(self, way):
        return self.z if way == 0 else self.last - self.z

    def begin(self):
        every = range(PIECES)
        for way in range(2):
            guarded(self.exit(way), lambda way=way: start(self.copies(0, self.z, way, every, True)))
        for way in range(2):
            guarded(self.depth(way) == 0, lambda way=way: start(self.copies(1, self.z, way, every, True)))

    ticks = property(lambda self: 2 * self.last * PIECES)

    def tick(self, tau):
        j, p = (tau - 1) // PIECES, (tau - 1) % PIECES
        for way in range(2):
            depth = self.depth(way)
            sign = -1 if way == 0 else 1

            def relay(kind, s, way=way, depth=depth):
                for copy in self.copies(kind, s, way, (p,)):
                    copy.wait_recv()
                guarded(self.exit(way), lambda: start(self.copies(kind, s, way, (p,))))
                if kind == 0 and p == PIECES - 1:
                    guarded(self.exit(way) & (j == depth - 1),
                            lambda: start(self.copies(1, self.z, way, range(PIECES), True)))

            guarded(j < depth, lambda s=self.z + sign * (j + 1), relay=relay: relay(0, s))
            guarded((j >= depth) & (j < 2 * depth),
                    lambda s=self.z + sign * (j - depth + 1), relay=relay: relay(1, s))

    def drain(self):
        for kind in range(2):
            for way in range(2):
                sign = -1 if way == 0 else 1
                for s in range(self.ncol):

                    def wait(kind=kind, way=way, s=s, sign=sign):
                        for copy in self.copies(kind, self.z + sign * s, way, range(PIECES)):
                            copy.wait_send()

                    guarded(self.exit(way) & (s <= self.depth(way)), wait)


def mixer_kernel(ncol, ndp, full_width, *refs):
    refs = list(refs)

    def take(number):
        taken = refs[:number]
        del refs[:number]
        return taken

    tokens_in, gain, seg_in, ci, cib, gg, cs, csb, sb, rl, sg = take(11)
    zx, bc_in, dt_in, w2, cot_in = take(5)
    normed_hbm, gsmall_hbm, ggate_hbm, cot_hbm, gnorm_hbm, ginner_hbm, part_hbm = take(7)
    par, par_s, par_h, gain_out, total_out = take(5)
    normed, seg, w_in, w_small, out_t, cot = take(6)
    taps, taps_s, heads = take(3)
    both, shared, step = take(3)
    ssd, x, bc, dt, c, ct, dec, enter, slope, slope_s, state, start_state, total = take(13)
    gained, gnorm, projected, back, dy, ggate, rowterm, dstart, dend = take(9)
    ginner, gsmall, part, edge, edge_in, last_rows = take(6)
    dstate, carry, carry_s, carry_links, grads_bc = take(5)
    sums, sums_all, own_scale, slots = take(4)
    line_box, line_send, line_recv = take(3)
    xs_send, xs_recv, cs_send, cs_recv, w_send, c_send, w_recv, t_send, t_recv = take(9)
    sum_send, sum_recv, row_send, row_recv, here = take(5)

    dp, row, z = lax.axis_index("dp"), lax.axis_index("row"), lax.axis_index("col")
    other = 1 - row
    last = ncol - 1
    tokens = tokens_in.shape[0]
    tail = HALO
    length = ncol * tokens
    width = taps.shape[1]
    scols = taps_s.shape[1]
    state_dim = scols // 2
    chunks = length // SPAN
    rows = bc_in.shape[0]
    me = dp * 2 + row
    sends_tail = (row == 0) & (z == last)

    barrier = pltpu.get_barrier_semaphore()
    for s in range(1, ncol):
        greet(barrier, row >= 0, col=lax.rem(z + s, ncol))
    greet(barrier, row >= 0, row=other)
    for m in range(1, ndp):
        greet(barrier, row >= 0, dp=dp ^ m)
    greet(barrier, row == 1, row=0, col=last)
    for s in range(ncol):
        greet(barrier, sends_tail, row=1, col=s)

    seg[pl.ds(pl.multiple_of(z * 8, 8), 8)] = jnp.broadcast_to(line_of(seg_in), (8, tokens))
    base = pl.multiple_of(z * tokens, 32)
    gain_row = line_of(gain)

    def normalize(n, carried):
        at = pl.multiple_of(n * 32, 32)
        wide = tokens_in[pl.ds(at, 32)].astype(F32)
        scale = lax.rsqrt(jnp.sum(wide * wide, axis=1, keepdims=True) / wide.shape[1] + EPS)
        normed[pl.ds(pl.multiple_of(base + at, 32), 32)] = (wide * scale * gain_row).astype(BF16)
        return carried

    lax.fori_loop(0, tokens // 32, normalize, 0)

    @pl.when(row == 0)
    def _():
        seg[pl.ds(ncol * 8, 8)] = jnp.full((8, tokens), -1, jnp.int32)
        normed[pl.ds(length, tail)] = jnp.zeros((tail, normed.shape[1]), BF16)
        start_state[...] = jnp.zeros_like(start_state)

    @pl.when(row == 1)
    def _():
        dend[...] = jnp.zeros_like(dend)
        edge_in[...] = jnp.zeros_like(edge_in)

    count = ncol - 1 + ndp + row + jnp.where(sends_tail, ncol, 0)
    pl.semaphore_wait(barrier, count)

    weights = ((None, w_in), (None, w_small), (w2, out_t))

    def weight_rows(j):
        return pl.ds(pl.multiple_of(j * rows, 16), rows)

    def weight_copies(j, mine, send, **to):
        copies = []
        for i, (src, dst) in enumerate(weights):
            place = dst.at[weight_rows(j)]
            from_input = mine and src is not None
            copies.append(remote(src if from_input else place, place, send.at[i], w_recv.at[j, i], **to))
        return copies

    def tail_copies(s):
        place = seg.at[pl.ds(pl.multiple_of(z * 8, 8), 8)]
        end = pl.multiple_of(z * tokens + tokens - tail, 16)
        return [
            remote(normed.at[pl.ds(end, tail)], normed.at[pl.ds(length, tail)],
                   t_send.at[s, 0], t_recv.at[0], row=1, col=s),
            remote(place, seg.at[pl.ds(ncol * 8, 8)], t_send.at[s, 1], t_recv.at[1], row=1, col=s),
        ]

    for s in range(ncol):
        guarded(sends_tail, lambda s=s: start(tail_copies(s)))
    gather = LineGather(ncol, z, (None, normed), (cot_in, cot), seg, (xs_send, xs_recv, cs_send, cs_recv))
    gather.begin()
    w_in[weight_rows(me), 0:width] = zx[:, 0, :]
    w_in[weight_rows(me), width : 2 * width] = zx[:, 1, :]
    w_small[weight_rows(me), 0:scols] = bc_in[...]
    dt_rows = jnp.concatenate([dt_in[...].astype(F32), jnp.zeros((128 - dt_in.shape[0], rows), F32)], axis=0)
    w_small[weight_rows(me), scols : scols + 128] = dt_rows.T.astype(BF16)
    local = [
        pltpu.make_async_copy(cot_in, cot.at[pl.ds(base, tokens)], here.at[0]),
        pltpu.make_async_copy(w2, out_t.at[weight_rows(me)], here.at[1]),
    ]
    start(local)
    taps[0:4] = ci[...]
    taps[4:5] = line_of(cib)
    taps[5:6] = line_of(gg)
    sg_row = line_of(sg)
    lo1 = iota((1, 128), 1) < 64
    for p in range(width // 128):
        taps[6:7, p * 128 : (p + 1) * 128] = pick(lo1, sg_row, 2 * p)
    taps_s[0:4] = cs[...]
    taps_s[4:5] = line_of(csb)
    heads[...] = jnp.zeros_like(heads)
    heads[0:1, : sb.shape[0]] = line_of(sb)
    heads[1:2, : rl.shape[0]] = line_of(rl)
    for ref in (state, total, dstart, carry, carry_s, carry_links, par, par_s, par_h, sums):
        ref[...] = jnp.zeros_like(ref)

    for m in range(1, ndp):
        start(weight_copies(me, True, w_send.at[m], dp=dp ^ m))
    start(weight_copies(me, True, c_send.at[0], row=other))

    def pass_weights(m):
        j = (dp ^ m) * 2 + row
        for copy in weight_copies(j, False, w_send.at[m], dp=dp ^ m):
            copy.wait_recv()
        start(weight_copies(j, False, c_send.at[m], row=other))

    half = gather.ticks // 2
    due = {tau: [] for tau in range(1, half + 1)}
    for m in range(1, ndp):
        due[min(half - 1, 2 + (3 * (m - 1)) // (ndp - 1) * (half - 3) // 2)].append(m)
    for tau in range(1, half):
        gather.tick(tau)
        for m in due[tau]:
            pass_weights(m)
    for m in range(ndp):
        for copy in weight_copies((dp ^ m) * 2 + other, False, c_send.at[m], row=other):
            copy.wait_recv()
    guarded(row == 1, lambda: [copy.wait_recv() for copy in tail_copies(0)])
    for copy in local:
        copy.wait()

    def nth(n):
        return pl.multiple_of(jnp.where(z * 2 < ncol, n, last - n) * tokens, tokens)

    def put(at, size, value, small):
        both[pl.ds(at, size)] = value.astype(BF16)
        shared[pl.ds(at, size)] = small[:, :scols].astype(BF16)
        step[pl.ds(at, size)] = small[:, scols:]

    def project_tokens(n, with_tail):
        at = nth(n)
        lhs = normed[pl.ds(at, tokens)]
        if with_tail:
            lhs = jnp.concatenate([lhs, normed[pl.ds(length, tail)]], axis=0)
        value, small = nn(lhs, w_in[...]), nn(lhs, w_small[...])
        put(at, tokens, value[:tokens], small[:tokens])
        if with_tail:
            put(length, tail, value[tokens:], small[tokens:])

    for n in range(ncol - 1):
        project_tokens(n, n == 0)
    gather.tick(half)
    project_tokens(ncol - 1, False)
    outs = [pltpu.make_async_copy(normed, normed_hbm, here.at[4])]
    outs[0].start()

    def at_rows(k):
        return pl.ds(pl.multiple_of(k * SPAN, SPAN), SPAN)

    def common(k):
        this = at_rows(k)
        above = pl.ds(pl.multiple_of(jnp.where(k == 0, length, k * SPAN - HALO), HALO), HALO)
        prev = pl.ds(pl.multiple_of(jnp.where(k == 0, chunks, k - 1) * 8, 8), 8)
        side = pl.ds(width, width)
        return (
            both.at[this, side], both.at[above, side], shared.at[this], shared.at[above], step.at[this],
            seg.at[pl.ds(pl.multiple_of(k * 8, 8), 8)], seg.at[prev], seg.at[pl.ds(chunks * 8, 8)], taps, taps_s, heads,
        )

    later = list(range(half + 1, gather.ticks + 1))

    def forward(k, carried):
        this = at_rows(k)
        forward_body(*common(k), ssd.at[this], x.at[this], bc.at[this], dt.at[this], c.at[this],
                     ct.at[:, this], dec.at[this], enter.at[k], slope.at[this], slope_s.at[this], state, total)
        guarded(k == chunks // 2, lambda: gather.tick(half + 1))
        return carried

    lax.fori_loop(0, chunks, forward, 0)
    later.pop(0)

    def row_copy(n, src, dst):
        return remote(src, dst, row_send.at[n], row_recv.at[n], row=other)

    guarded(row == 0, lambda: row_copy(0, state, start_state).start())
    gather.tick(later.pop(0))
    guarded(row == 1, lambda: row_copy(0, state, start_state).wait_recv())

    def gating(k, carried):
        this = at_rows(k)
        gate_body(ssd.at[this], x.at[this], bc.at[this], dec.at[this], start_state, both.at[this, pl.ds(0, width)],
                  taps, ssd.at[this], gained.at[this], sums.at[:, this])
        return carried

    lax.fori_loop(0, chunks, gating, 0)

    def sum_copy(s, source):
        return remote(sums, slots.at[source], sum_send.at[s], sum_recv.at[source], col=lax.rem(z + s, ncol))

    def sum_end():
        result = sums[...]
        for s in range(1, ncol):
            source = lax.rem(z + s, ncol)
            sum_copy(s, source).wait_recv()
            result = result + slots[source]
        sums_all[...] = result

    gather.tick(later.pop(0))

    def projecting(k, carried):
        this = at_rows(k)
        projected[this] = nt(gained[this], out_t[...]).astype(BF16)
        return carried

    lax.fori_loop(0, chunks, projecting, 0)
    line = LineReduce(ncol, z, projected, projected, line_box, line_send, line_recv, False)
    line.start()
    while len(later) > 2:
        gather.tick(later.pop(0))

    def pulling(n):
        this = pl.ds(nth(n), tokens)
        pull_body(cot.at[this], out_t, gained.at[this], back.at[this], sums.at[:, this])

    for n in range(ncol - 1):
        pulling(n)
        if n == 0:
            gather.tick(later.pop(0))
    gather.tick(later.pop(0))
    ticks = list(range(1, line.ticks + 1))
    pulling(ncol - 1)
    outs.append(pltpu.make_async_copy(cot, cot_hbm, here.at[5]))
    outs[-1].start()
    for s in range(1, ncol):
        sum_copy(s, z).start()
    line.start(2, line.ticks)
    line.tick(ticks.pop(0))
    sum_end()
    own_scale[...] = columns(lax.rsqrt(sums_all[0:1, pl.ds(pl.multiple_of(z * tokens, tokens), tokens)] / full_width + EPS))

    def pull_gate(k, carried):
        this = at_rows(k)
        back_body(full_width, ssd.at[this], x.at[this], bc.at[this], dec.at[this], both.at[this, pl.ds(0, width)],
                  back.at[this], sums_all.at[:, this], taps,
                  gnorm.at[this], dy.at[this], ggate.at[this], rowterm.at[this], par, dstart)
        return carried

    lax.fori_loop(0, chunks, pull_gate, 0)
    guarded(row == 1, lambda: row_copy(1, dstart, dend).start())
    outs.append(pltpu.make_async_copy(ggate, ggate_hbm, here.at[7]))
    outs.append(pltpu.make_async_copy(gnorm, gnorm_hbm, here.at[6]))
    start(outs[-2:])
    line.tick(ticks.pop(0))
    guarded(row == 0, lambda: row_copy(1, dstart, dend).wait_recv())
    dstate[...] = dend[...]

    spaced = {n: [tau] for n, tau in enumerate(ticks[:chunks])}
    ticks = ticks[chunks:]

    def backward(n, carried):
        k = chunks - 1 - n
        this = at_rows(k)
        before = pl.ds(pl.multiple_of(jnp.maximum(k * SPAN - 8, 0), 8), 8)
        backward_body(k, chunks, *common(k), dy.at[this], x.at[this], bc.at[this], dt.at[this], c.at[this],
                      ct.at[:, this], dec.at[before], enter.at[k], slope.at[this], slope_s.at[this], start_state, rowterm.at[this],
                      ginner.at[this], gsmall.at[this], par, par_s, par_h, edge, last_rows,
                      dstate, carry, carry_s, carry_links, grads_bc)
        for turn, taus in spaced.items():
            if turn < chunks - 1:
                for tau in taus:
                    guarded(n == turn, lambda tau=tau: line.tick(tau))
        return carried

    lax.fori_loop(0, chunks, backward, 0)
    guarded(row == 1, lambda: row_copy(2, edge, edge_in).start())
    for tau in spaced.get(chunks - 1, []):
        line.tick(tau)
    guarded(row == 0, lambda: row_copy(2, edge, edge_in).wait_recv())
    fixed = (last_rows[...] + edge_in[...]).astype(BF16)
    ginner[length - 8 :] = fixed[:, :width]
    gsmall[length - 8 :, : fixed.shape[1] - width] = fixed[:, width:]
    outs.append(pltpu.make_async_copy(ginner, ginner_hbm, here.at[8]))
    outs.append(pltpu.make_async_copy(gsmall, gsmall_hbm, here.at[9]))
    start(outs[-2:])

    tile = 256
    tiles = part.shape[1] // tile

    def part_copy(n):
        at = pl.ds(pl.multiple_of(n * tile, tile), tile)
        return pltpu.make_async_copy(part.at[:, at], part_hbm.at[:, at], here.at[10 + n])

    def spreading(n, carried):
        at = pl.ds(pl.multiple_of(n * tile, tile), tile)
        spread_body(ggate, ginner, gsmall, w_in.at[at], w_small.at[at], normed.at[pl.ds(0, length), at],
                    part.at[:, at], gain_out.at[:, at])
        guarded(n > 0, lambda: part_copy(jnp.maximum(n - 1, 0)).start())
        for tau in ticks[:-1]:
            guarded(n == tiles // 2, lambda tau=tau: line.tick(tau))
        return carried

    lax.fori_loop(0, tiles, spreading, 0)
    part_copy(tiles - 1).start()
    for tau in ticks[-1:]:
        line.tick(tau)

    def keep(at, value):
        here_rows = pl.ds(pl.multiple_of(at, 16), 16)
        total_out[here_rows] = (value * own_scale[here_rows, 0:1]).astype(BF16)

    line.total(keep)

    gather.drain()
    line.drain()
    for m in range(ndp):
        if m:
            for copy in weight_copies(me, True, w_send.at[m], dp=dp ^ m):
                copy.wait_send()
        for copy in weight_copies((dp ^ m) * 2 + row, m == 0, c_send.at[m], row=other):
            copy.wait_send()
    for s in range(ncol):
        guarded(sends_tail, lambda s=s: [copy.wait_send() for copy in tail_copies(s)])
    for s in range(1, ncol):
        sum_copy(s, z).wait_send()
    guarded(row == 0, lambda: row_copy(0, state, start_state).wait_send())
    guarded(row == 1, lambda: row_copy(1, dstart, dend).wait_send())
    guarded(row == 1, lambda: row_copy(2, edge, edge_in).wait_send())
    for copy in outs:
        copy.wait()
    for n in range(tiles):
        part_copy(n).wait()


def run_mixer(full_width, tokens_in, gain, seg, ci, cib, gg, cs, csb, sb, rl, sg, zx, bc, dt, w2, cot):
    ncol, ndp = lax.axis_size("col"), lax.axis_size("dp")
    tokens, model = tokens_in.shape
    width, scols = ci.shape[1], cs.shape[1]
    length = ncol * tokens
    chunks = length // SPAN
    state_dim = scols // 2
    small = scols + 128
    shards = 2 * ndp
    S = jax.ShapeDtypeStruct
    V = pltpu.VMEM
    dma = pltpu.SemaphoreType.DMA
    vmem = pl.BlockSpec(memory_space=V)
    return pl.pallas_call(
        functools.partial(mixer_kernel, ncol, ndp, full_width),
        in_specs=[vmem] * 14 + [ANY] * 2,
        out_specs=[ANY] * 7 + [vmem] * 5,
        out_shape=[
            S((length + HALO, model), BF16), S((length, small), BF16), S((length, width), BF16), S((length, model), BF16),
            S((length, width), BF16), S((length, width), BF16), S((length, model), BF16),
            S((8, width), F32), S((8, scols), F32), S((8, 128), F32), S((1, model), F32), S((tokens, model), BF16),
        ],
        scratch_shapes=[
            V((length + HALO, model), BF16), V(((ncol + 1) * 8, tokens), jnp.int32), V((model, 2 * width), BF16),
            V((model, small), BF16), V((model, width), BF16), V((length, model), BF16),
            V((8, width), F32), V((8, scols), F32), V((8, 128), F32),
            V((length + HALO, 2 * width), BF16), V((length + HALO, scols), BF16), V((length + HALO, 128), F32),
            V((length, width), F32), V((length, width), BF16), V((length, scols), BF16), V((length, 128), F32),
            V((length, 128), F32), V((16, length), F32), V((length, 128), F32), V((chunks, state_dim, width), BF16),
            V((length, width), BF16), V((length, scols), BF16),
            V((state_dim, width), F32), V((state_dim, width), F32), V((8, 128), F32),
            V((length, width), BF16), V((length, width), BF16), V((length, model), BF16), V((length, width), BF16),
            V((length, width), BF16), V((length, width), BF16), V((length, 128), F32), V((state_dim, width), F32),
            V((state_dim, width), F32),
            V((length, width), BF16), V((length, small), BF16), V((length, model), BF16),
            V((8, width + scols), F32), V((8, width + scols), F32), V((8, width + scols), F32),
            V((state_dim, width), F32), V((8, width), F32), V((8, scols), F32), V((8, 128), F32), V((SPAN, scols), F32),
            V((2, length), F32), V((2, length), F32), V((tokens, 128), F32), V((ncol, 2, length), F32),
            *line_scratch(ncol, tokens, model),
            dma((2, ncol, PIECES + 1)), dma((ncol, PIECES + 1)), dma((2, ncol, PIECES)), dma((ncol, PIECES)),
            dma((ndp, 3)), dma((ndp, 3)), dma((shards, 3)), dma((ncol, 2)), dma((2,)),
            dma((ncol,)), dma((ncol,)), dma((3,)), dma((3,)), dma((10 + model // 256,)),
        ],
        compiler_params=pltpu.CompilerParams(
            collective_id=1, has_side_effects=True, vmem_limit_bytes=63 * 1024 * 1024
        ),
        cost_estimate=pl.CostEstimate(flops=0, bytes_accessed=500_000_000, transcendentals=0),
        name="mixer",
    )(tokens_in, gain, seg, ci, cib, gg, cs, csb, sb, rl, sg, zx, bc, dt, w2, cot)
class LineReduce:
    def __init__(self, ncol, z, source, local, inbox, send, recv, paced):
        self.paced = paced
        self.ncol, self.z, self.last = ncol, z, ncol - 1
        self.source, self.local, self.inbox = source, local, inbox
        self.send, self.recv = send, recv
        self.tokens = local.shape[0] // ncol
        self.part = self.tokens // PIECES

    def rows(self, way, t, p):
        d = self.last - t if way == 0 else t
        return pl.multiple_of(d * self.tokens + p * self.part, self.part)

    def copy(self, way, t, p, first):
        src = self.source.at[pl.ds(self.rows(way, t, p), self.part)] if first else self.inbox.at[way, t, p]
        to = self.z + 1 if way == 0 else self.z - 1
        return remote(src, self.inbox.at[way, t, p], self.send.at[way, t, p], self.recv.at[way, t, p], col=to)

    def edge(self, way):
        return self.z == (0 if way == 0 else self.last)

    def depth(self, way):
        return self.z if way == 0 else self.last - self.z

    def start(self, first=0, stop=2):
        for way in range(2):

            @pl.when(self.edge(way))
            def _(way=way):
                for i in range(first, min(stop, self.ticks)):
                    self.copy(way, i // PIECES, i % PIECES, True).start()

    ticks = property(lambda self: self.last * PIECES)

    def tick(self, tau):
        for way in range(2):

            @pl.when(self.edge(way) & (self.paced and tau + 1 < self.ticks))
            def _(way=way):
                self.copy(way, (tau - 1) // PIECES, (tau - 1) % PIECES, True).wait_send()
                self.copy(way, (tau + 1) // PIECES, (tau + 1) % PIECES, True).start()

        for stage in range(2):
            for way in range(2):
                depth = self.depth(way)
                index = tau - (2 * depth - 1)
                t, p = index // PIECES, lax.rem(index, PIECES)

                @pl.when((depth > 0) & (index >= 0) & (index < (self.ncol - depth) * PIECES))
                def _(way=way, depth=depth, t=t, p=p, stage=stage):
                    onward = t < self.last - depth
                    if stage == 0:
                        self.copy(way, t, p, False).wait_recv()

                        @pl.when(onward)
                        def _():
                            base = self.rows(way, t, p)

                            def add(k, carry):
                                at = pl.multiple_of(k * 16, 16)
                                mine = self.local[pl.ds(pl.multiple_of(base + at, 16), 16)].astype(F32)
                                here = pl.ds(at, 16)
                                self.inbox[way, t, p, here] = (self.inbox[way, t, p, here].astype(F32) + mine).astype(BF16)
                                return carry

                            lax.fori_loop(0, self.part // 16, add, 0)
                    else:

                        @pl.when(onward)
                        def _():
                            self.copy(way, t, p, False).start()

    def total(self, store):
        z, last = self.z, self.last
        for p in range(PIECES):

            def add(k, carry, p=p):
                at = pl.multiple_of(k * 16, 16)
                here = pl.ds(at, 16)
                row = p * self.part + at
                value = self.local[pl.ds(pl.multiple_of(z * self.tokens + row, 16), 16)].astype(F32)
                low = self.inbox[0, jnp.minimum(last - z, last - 1), p, here].astype(F32)
                high = self.inbox[1, jnp.minimum(z, last - 1), p, here].astype(F32)
                value = value + jnp.where(z > 0, low, 0.0) + jnp.where(z < last, high, 0.0)
                store(row, value)
                return carry

            lax.fori_loop(0, self.part // 16, add, 0)

    def drain(self):
        for way in range(2):
            depth = self.depth(way)

            @pl.when(self.edge(way))
            def _(way=way):
                for i in range(self.ticks - 2 if self.paced else 0, self.ticks):
                    self.copy(way, i // PIECES, i % PIECES, True).wait_send()

            for t in range(self.last):

                @pl.when((depth > 0) & (t < self.last - depth))
                def _(way=way, t=t):
                    for p in range(PIECES):
                        self.copy(way, t, p, False).wait_send()


def line_scratch(ncol, tokens, width):
    shape = (2, ncol - 1, PIECES)
    dma = pltpu.SemaphoreType.DMA
    return [pltpu.VMEM(shape + (tokens // PIECES, width), BF16), dma(shape), dma(shape)]


def reduce_kernel(ncol, ndp, scols, *refs):
    count = 4
    refs = list(refs)

    def take(number):
        taken = refs[:number]
        del refs[:number]
        return taken

    sources = take(7)
    vecs = take(4)
    r, vec_outs, gsum_out = take(count), take(4), refs.pop(0)
    held = take(7)
    (line_box, line_send, line_recv) = take(3)
    g, near, sent, far = take(count), take(count), take(count), take(count)
    vec_slots, col_slots = take(4), take(2)
    col_sums = take(2)
    bc_slots, bc_sum, load, c_send, c_recv, p_send, p_recv, v_send, v_recv, u_send, u_recv, b_send, b_recv = refs
    dp, row, z = lax.axis_index("dp"), lax.axis_index("row"), lax.axis_index("col")
    other = 1 - row
    me = dp * 2 + row
    rows = [out.shape[0] for out in r]
    barrier = pltpu.get_barrier_semaphore()
    for q in range(1, 2 * ndp):
        greet(barrier, row >= 0, dp=dp ^ (q >> 1), row=row ^ (q & 1))
    for s in range(1, ncol):
        greet(barrier, row >= 0, col=lax.rem(z + s, ncol))
    loads = []
    for i, (src, dst) in enumerate(zip(sources, held)):
        src = src.at[pl.ds(0, dst.shape[0])]
        loads.append(pltpu.make_async_copy(src, dst, load.at[i]))
        loads[-1].start()
    normed, gsmall, ggate, cot, gnorm, ginner, part = held
    pl.semaphore_wait(barrier, 2 * ndp + ncol - 2)
    line = LineReduce(ncol, z, sources[6], part, line_box, line_send, line_recv, True)
    line.start()

    order = (0, 1, 2, 3)
    turns = [3, 1, 2, 0] if ndp == 4 else list(range(1, ndp)) + [0]

    def core_copy(i, d):
        return remote(g[i].at[pl.ds((d * 2 + other) * rows[i], rows[i])], near[i].at[d],
                      c_send.at[i, d], c_recv.at[i, d], row=other)

    def vec_copy(q, i, j):
        return remote(vecs[i], vec_slots[i].at[j], v_send.at[q, i], v_recv.at[j, i],
                      dp=dp ^ (q >> 1), row=row ^ (q & 1))

    for q in range(1, 2 * ndp):
        for i in range(4):
            vec_copy(q, i, me).start()

    waiting = []

    def later(copy):
        if waiting:
            waiting.pop().start()
        if copy is not None:
            waiting.append(copy)

    def accumulate(i, first, number, terms, store):
        def step(k, carry):
            at = first + pl.multiple_of(k * 16, 16)
            total = terms[0](at)
            for term in terms[1:]:
                total = total + term(at)
            store(at, total)
            return carry

        lax.fori_loop(0, number // 16, step, 0)

    def read(ref, index, shift=0):
        return lambda at: ref[index, pl.ds(at - shift, 16)].astype(F32)

    def mine(i, d):
        return lambda at: g[i][pl.ds(pl.multiple_of((d * 2 + row) * rows[i] + at, 16), 16)].astype(F32)

    def write(ref, index, shift):
        def store(at, total):
            ref[index, pl.ds(at - shift, 16)] = total.astype(BF16)

        return store

    def arrived(i, d):
        core_copy(i, d).wait_recv()

    def tick():
        if ticks:
            line.tick(ticks.pop(0))

    if ndp == 4:
        halves = ((0, 1, 2), (1, 2, 1))

        def leg(i, slot, m):
            return remote(sent[i].at[slot], far[i].at[slot], p_send.at[i, slot], p_recv.at[i, slot], dp=dp ^ m)

        def step_one(i):
            half = rows[i] // 2
            arrived(i, dp ^ 3)
            for h, m1, m2 in halves:
                accumulate(i, h * half, half, [mine(i, dp ^ 3), read(near[i], dp ^ 3)],
                           write(sent[i], 3 * h + 1, h * half))
                later(leg(i, 3 * h + 1, m1))
            for h, m1, m2 in halves:
                arrived(i, dp ^ m1)
                accumulate(i, h * half, half, [mine(i, dp ^ m1), read(near[i], dp ^ m1)],
                           write(sent[i], 3 * h, h * half))
                later(leg(i, 3 * h, m1))
            later(None)
            arrived(i, dp)

        def relay(i):
            half = rows[i] // 2
            for h, m1, m2 in halves:
                leg(i, 3 * h + 1, m1).wait_recv()
                accumulate(i, h * half, half,
                           [mine(i, dp ^ m2), read(near[i], dp ^ m2), read(far[i], 3 * h + 1, h * half)],
                           write(sent[i], 3 * h + 2, h * half))
                later(leg(i, 3 * h + 2, m2))
            later(None)

        def finish(i, store):
            half = rows[i] // 2
            for h, m1, m2 in halves:
                leg(i, 3 * h, m1).wait_recv()
                leg(i, 3 * h + 2, m2).wait_recv()
                accumulate(i, h * half, half,
                           [mine(i, dp), read(near[i], dp), read(far[i], 3 * h, h * half),
                            read(far[i], 3 * h + 2, h * half)], store)

        sends = [leg(i, 3 * h + k, m2 if k == 2 else m1) for i in order for h, m1, m2 in halves for k in range(3)]
    else:

        def peer(i, m):
            return remote(sent[i].at[m], far[i].at[m], p_send.at[i, m], p_recv.at[i, m], dp=dp ^ m)

        def step_one(i):
            for m in turns[:-1]:
                arrived(i, dp ^ m)
                accumulate(i, 0, rows[i], [mine(i, dp ^ m), read(near[i], dp ^ m)], write(sent[i], m, 0))
                later(peer(i, m))
            later(None)
            arrived(i, dp)

        def relay(i):
            pass

        def finish(i, store):
            for m in range(1, ndp):
                peer(i, m).wait_recv()
            accumulate(i, 0, rows[i],
                       [mine(i, dp), read(near[i], dp)] + [read(far[i], m) for m in range(1, ndp)], store)

        sends = [peer(i, m) for i in order for m in range(1, ndp)]

    def plain(i):
        def store(at, total):
            r[i][pl.ds(at, 16)] = total

        return store

    def shared_rows(at, total):
        r[0][pl.ds(at, 16)] = total
        bc_slots[z, pl.ds(at, 16)] = total[:, : bc_slots.shape[2]].astype(BF16)

    root = ncol // 2
    at_root = z == root

    def to_root(source):
        pairs = [(col_slots[i].at[source], u_send.at[0, i], u_recv.at[source, i]) for i in range(2)]
        pairs.append((bc_slots.at[source], b_send.at[0], b_recv.at[source]))
        return [remote(ref, ref, send, recv, col=root) for ref, send, recv in pairs]

    def from_root(target):
        pairs = [(col_sums[i], u_send.at[target, i], u_recv.at[root, i]) for i in range(2)]
        pairs.append((bc_sum, b_send.at[target], b_recv.at[root]))
        return [remote(ref, ref, send, recv, col=target) for ref, send, recv in pairs]

    others = [s for s in range(ncol) if s != root]

    def sum_at_root():
        @pl.when(at_root)
        def _():
            for s in others:
                for copy in to_root(s):
                    copy.wait_recv()
            for i in range(2):
                total = col_slots[i][0]
                for j in range(1, ncol):
                    total = total + col_slots[i][j]
                col_sums[i][...] = total
            total = bc_slots[0].astype(F32)
            for j in range(1, ncol):
                total = total + bc_slots[j].astype(F32)
            bc_sum[...] = total.astype(BF16)
            for s in others:
                for copy in from_root(s):
                    copy.start()

    model = normed.shape[1]
    block = model // 4
    products = ((normed, gsmall), (normed, ggate), (cot, gnorm), (normed, ginner))
    ready = {0: (0, 1), 1: (2,), 2: (3, 4), 3: (5,)}
    ticks = list(range(1, line.ticks + 1))
    for i in order:
        for at in ready[i]:
            loads[at].wait()
        left, right = products[i]
        for n, m in enumerate([3, 1, 2, 0] if ndp == 4 else range(4)):
            b = dp ^ m if ndp == 4 else m
            first = pl.multiple_of(b * block, 128)
            g[i][pl.ds(pl.multiple_of(b * block, 16), block)] = tn(left[:, pl.ds(first, block)], right[...]).astype(BF16)
            if ndp == 4:
                later(core_copy(i, b))
        if ndp != 4:
            for m in turns:
                later(core_copy(i, dp ^ m))
        if i == 1:
            loads[6].wait()
        if i > 0:
            step_one(i - 1)
        if i > 1:
            relay(i - 2)
        if i % 2:
            tick()
    later(None)
    step_one(3)
    relay(2)
    finish(0, shared_rows)
    for q in range(1, 2 * ndp):
        for i in range(4):
            vec_copy(q, i, me ^ q).wait_recv()
    for i in range(4):
        vec_slots[i][me] = vecs[i][...]
        total = vec_slots[i][0]
        for j in range(1, 2 * ndp):
            total = total + vec_slots[i][j]
        if i < 2:
            vec_outs[i][...] = total
        else:
            col_slots[i - 2][z] = total

    @pl.when(~at_root)
    def _():
        for copy in to_root(z):
            copy.start()

    tick()
    relay(3)
    while len(ticks) > 1:
        tick()
    sum_at_root()
    finish(1, plain(1))
    finish(2, plain(2))
    finish(3, plain(3))
    while ticks:
        tick()

    def keep(at, value):
        gsum_out[pl.ds(pl.multiple_of(at, 16), 16)] = value.astype(BF16)

    line.total(keep)
    @pl.when(~at_root)
    def _():
        for copy in from_root(z):
            copy.wait_recv()

    for i in range(2):
        vec_outs[2 + i][...] = col_sums[i][...]
    r[0][:, : bc_slots.shape[2]] = bc_sum[...].astype(F32)

    for q in range(1, 2 * ndp):
        for i in range(4):
            vec_copy(q, i, me).wait_send()
    for i in order:
        for m in turns:
            core_copy(i, dp ^ m).wait_send()
    for copy in sends:
        copy.wait_send()
    @pl.when(~at_root)
    def _():
        for copy in to_root(z):
            copy.wait_send()

    @pl.when(at_root)
    def _():
        for s in others:
            for copy in from_root(s):
                copy.wait_send()

    line.drain()


def reduce_grads(sources, vecs, scols):
    ncol, ndp = lax.axis_size("col"), lax.axis_size("dp")
    dma = pltpu.SemaphoreType.DMA
    vmem = pl.BlockSpec(memory_space=pltpu.VMEM)
    S = jax.ShapeDtypeStruct
    length = sources[1].shape[0]
    model = sources[0].shape[1]
    widths = [sources[1].shape[1], sources[2].shape[1], sources[4].shape[1], sources[5].shape[1]]
    count = len(widths)
    blocks = [(model // (2 * ndp), w) for w in widths]
    near = [pltpu.VMEM((ndp,) + b, BF16) for b in blocks]
    slots = 6 if ndp == 4 else ndp
    legs = [pltpu.VMEM((6, b[0] // 2, b[1]) if ndp == 4 else (ndp,) + b, BF16) for b in blocks]
    tokens = length // ncol
    return pl.pallas_call(
        functools.partial(reduce_kernel, ncol, ndp, scols),
        in_specs=[ANY] * 7 + [vmem] * 4,
        out_specs=[vmem] * (count + 5),
        out_shape=[S(b, F32) for b in blocks] + [S(v.shape, F32) for v in vecs] + [S((tokens, model), BF16)],
        scratch_shapes=[pltpu.VMEM((length, s.shape[1]), BF16) for s in sources]
        + line_scratch(ncol, tokens, model)
        + [pltpu.VMEM((model, w), BF16) for w in widths]
        + near + legs * 2
        + [pltpu.VMEM((2 * ndp,) + v.shape, F32) for v in vecs]
        + [pltpu.VMEM((ncol,) + v.shape, F32) for v in vecs[2:]]
        + [pltpu.VMEM(v.shape, F32) for v in vecs[2:]]
        + [pltpu.VMEM((ncol, blocks[0][0], scols), BF16), pltpu.VMEM((blocks[0][0], scols), BF16)]
        + [dma((7,))]
        + [dma((count, ndp))] * 2
        + [dma((count, slots))] * 2
        + [dma((2 * ndp, 4))] * 2
        + [dma((ncol, 2))] * 2
        + [dma((ncol,))] * 2,
        compiler_params=pltpu.CompilerParams(
            collective_id=2, has_side_effects=True, vmem_limit_bytes=60 * 1024 * 1024
        ),
        cost_estimate=pl.CostEstimate(flops=0, bytes_accessed=200_000_000, transcendentals=0),
        name="reduce_grads",
    )(*sources, *vecs)


def finish_small(
    nheads, small, par, par_h, par_s, gain_sum, gain_row, bc_out, dt_out, ci_out, cib_out, cs_out,
    csb_out, sb_out, rl_out, sg_out, gg_out, ng_out,
):
    width = par.shape[1]
    scols = par_s.shape[1]
    bc_out[...] = small[:, :scols]
    dt_out[...] = small[:, scols:].T[:nheads]
    ci_out[...] = par[0:4]
    cib_out[...] = par[4:5].reshape(width)
    gg_out[...] = par[5:6].reshape(width)
    cs_out[...] = par_s[0:4]
    csb_out[...] = par_s[4:5].reshape(scols)
    sb_out[...] = par_h[0:1, :nheads].reshape(nheads)
    rl_out[...] = par_h[1:2, :nheads].reshape(nheads)
    skip = jnp.zeros((8, 128), F32)
    for p in range(width // 128):
        skip = skip + split_dot(jnp.broadcast_to(par[6:7, p * 128 : (p + 1) * 128], (8, 128)), head_map(p))
    sg_out[...] = skip[0:1, :nheads].reshape(nheads)
    ng_out[...] = (gain_sum[0:1] / gain_row).reshape(gain_row.shape[1])


def finish_kernel(
    nheads, small, gate, inner, out, par, par_h, par_s, gain_sum, gain, tokens, cot, gnormed, projected,
    zx_out, bc_out, dt_out, out_out, ci_out, cib_out, cs_out, csb_out, sb_out, rl_out, sg_out, gg_out, ng_out, gin_out, block_out,
):
    gain_row = gain[...].reshape(1, gain.shape[0])
    zx_out[:, 0, :] = gate[...]
    zx_out[:, 1, :] = inner[...]
    out_out[...] = out[...]

    @pl.when(pl.program_id(0) == 0)
    def _():
        finish_small(nheads, small, par, par_h, par_s, gain_sum, gain_row, bc_out, dt_out, ci_out, cib_out, cs_out,
                     csb_out, sb_out, rl_out, sg_out, gg_out, ng_out)

    def rows(step, carry):
        at = pl.ds(pl.multiple_of(step * 32, 32), 32)
        wide = tokens[at].astype(F32)
        scale = lax.rsqrt(jnp.sum(wide * wide, axis=1, keepdims=True) / wide.shape[1] + EPS)
        pushed = gnormed[at].astype(F32) * gain_row
        mean = jnp.sum(pushed * wide, axis=1, keepdims=True) / wide.shape[1]
        grad = scale * pushed - wide * (scale * scale * scale * mean)
        gin_out[at] = (cot[at].astype(F32) + grad).astype(BF16)
        block_out[at] = (wide + projected[at].astype(F32)).astype(BF16)
        return carry

    lax.fori_loop(0, tokens.shape[0] // 32, rows, 0)


def run_finish(nheads, small, gate, inner, out, par, par_h, par_s, gain_sum, gain, tokens, cot, gnormed, projected):
    rows, width = gate.shape
    scols = par_s.shape[1]
    model = gain.shape[0]
    S = jax.ShapeDtypeStruct
    shapes = [
        (rows, 2, width), (rows, scols), (nheads, rows), (rows, width), (4, width), (width,), (4, scols), (scols,),
        (nheads,), (nheads,), (nheads,), (width,), (model,),
    ]
    steps = 4 if rows % 32 == 0 else 2
    block = rows // steps
    some = tokens.shape[0] // steps
    down = lambda n: (n, 0)
    whole = lambda shape: pl.BlockSpec(shape, lambda n: (0,) * len(shape))
    wide_spec = pl.BlockSpec((block, width), down)
    token_spec = pl.BlockSpec((some, model), down)
    return pl.pallas_call(
        functools.partial(finish_kernel, nheads),
        grid=(steps,),
        in_specs=[whole(small.shape), wide_spec, wide_spec, wide_spec, whole(par.shape), whole(par_h.shape),
                  whole(par_s.shape), whole(gain_sum.shape), whole(gain.shape)] + [token_spec] * 4,
        out_specs=[pl.BlockSpec((block, 2, width), lambda n: (n, 0, 0)), whole(shapes[1]), whole(shapes[2]), wide_spec]
        + [whole(shape) for shape in shapes[4:]] + [token_spec] * 2,
        out_shape=[S(shape, F32) for shape in shapes] + [S(tokens.shape, BF16)] * 2,
        name="finish",
    )(small, gate, inner, out, par, par_h, par_s, gain_sum, gain, tokens, cot, gnormed, projected)


def per_device(
    block_input, segment_ids, norm_gain, proj_zx, proj_bc, proj_dt, conv_inner, conv_inner_bias,
    conv_shared, conv_shared_bias, step_bias, rate_log, skip_gain, gated_gain, proj_out, cotangent,
):
    width = proj_zx.shape[2]
    scols = proj_bc.shape[1]
    nheads = proj_dt.shape[1]
    full_width = float(width * lax.axis_size("col"))
    (normed, gsmall, ggate, cot_all, gated_normed, ginner, part, par, par_s, par_h, gain_part, projected) = run_mixer(
        full_width, block_input, norm_gain, segment_ids, conv_inner, conv_inner_bias, gated_gain, conv_shared,
        conv_shared_bias, step_bias, rate_log, skip_gain, proj_zx, proj_bc, proj_dt.T, proj_out.T, cotangent,
    )
    gsm, gz, gout, gx, par, par_h, par_s, gain_sum, grad_normed = reduce_grads(
        (normed, gsmall, ggate, cot_all, gated_normed, ginner, part), (par, par_h, par_s, gain_part), scols
    )
    zx, gbc, gdt, gout, ci, cib, cs, csb, sb, rl, sg, gg, ng, grad_input, block_output = run_finish(
        nheads, gsm, gz, gx, gout, par, par_h, par_s, gain_sum, norm_gain, block_input, cotangent, grad_normed, projected
    )
    return (
        block_output, grad_input, ng, zx, gbc, gdt.T, ci, cib, cs, csb, sb, rl, sg, gg, gout.T,
    )


def solution(mesh):
    shards = ("dp", "row")
    tokens = P(("dp", "row", "col"), None)
    zx = P(shards, None, "col")
    in_specs = (
        tokens, P(("dp", "row", "col")), P(), zx, P(shards, None), P(shards, "col"), P(None, "col"), P("col"),
        P(), P(), P("col"), P("col"), P("col"), P("col"), P("col", shards), tokens,
    )
    out_specs = (
        tokens, tokens, P(), zx, P(shards, None), P(shards, "col"), P(None, "col"), P("col"),
        P(), P(), P("col"), P("col"), P("col"), P("col"), P("col", shards),
    )
    return jax.shard_map(per_device, mesh=mesh, in_specs=in_specs, out_specs=out_specs, check_vma=False)
```
